8 devices in a mesh: prob: 1 (over z), row: 2 (over y), col: 4 (over x, core).
Axes of the slice: x: 2, y: 2, z: 1, core: 2. Of those that a mesh axis runs over, the one named last changes fastest.
Arguments:
- kernel: bfloat16 [4096, 4096], P('row', 'col')
- cost_mat: bfloat16 [4096, 4096], P('row', 'col')
- src_mass: float32 [4096, 32], P('row', 'prob')
- tgt_mass: float32 [4096, 32], P('col', 'prob')
Outputs:
- output 1: float32 [4096, 32], P('row', 'prob')
- output 2: float32 [4096, 32], P('col', 'prob')
- output 3: float32 [32], P('prob')
All inputs are finite; a program needn't handle non-finite values.
Results may differ from the reference program's by a relative error of at most 0.001.
Values are sent between devices in bfloat16 or wider.
A program may use at most 1 GiB of HBM per device.

```python
import jax
import jax.numpy as jnp
from jax import lax

N_SRC = 4096
N_TGT = 4096
BATCH = 32
SWEEPS = 6
EPSILON = 0.1


def setup_inputs(seed: int = 0, part: int = 0) -> dict:
    base_key = jax.random.key(seed)
    key_src, key_tgt = jax.random.split(base_key, 2)
    src_pts = jax.random.uniform(key_src, (N_SRC, 3), jnp.float32)
    tgt_pts = jax.random.uniform(key_tgt, (N_TGT, 3), jnp.float32)
    cross_dot = jnp.dot(src_pts, tgt_pts.T)
    dist_sq = jnp.sum(src_pts * src_pts, axis=1)[:, None] + jnp.sum(tgt_pts * tgt_pts, axis=1)[None, :] - 2.0 * cross_dot
    cost_full = jnp.clip(dist_sq / 3.0, 0.0, 1.0)
    part_key = jax.random.fold_in(jax.random.key(seed + 1), part)
    key_a, key_b = jax.random.split(part_key, 2)
    src_mass = N_TGT * jax.random.uniform(key_a, (N_SRC, BATCH), jnp.float32, 0.25, 1.75)
    tgt_mass = N_SRC * jax.random.uniform(key_b, (N_TGT, BATCH), jnp.float32, 0.25, 1.75)
    return {"kernel": jnp.exp(-cost_full / EPSILON).astype(jnp.bfloat16), "cost_mat": cost_full.astype(jnp.bfloat16), "src_mass": src_mass, "tgt_mass": tgt_mass}


def reference(kernel, cost_mat, src_mass, tgt_mass):
    def sweep(carry, unused):
        tgt_scale = carry[1]
        row_sum = jnp.dot(kernel, tgt_scale.astype(jnp.bfloat16), preferred_element_type=jnp.float32)
        src_scale = src_mass / row_sum
        col_sum = lax.dot_general(kernel, src_scale.astype(jnp.bfloat16), (((0,), (0,)), ((), ())), preferred_element_type=jnp.float32)
        return (src_scale, tgt_mass / col_sum), None
    start = (jnp.zeros((N_SRC, BATCH), jnp.float32), jnp.ones((N_TGT, BATCH), jnp.float32))
    final, unused_hist = lax.scan(sweep, start, None, length=SWEEPS)
    src_scale, tgt_scale = final
    kern_cost = kernel * cost_mat
    weighted = jnp.dot(kern_cost, tgt_scale.astype(jnp.bfloat16), preferred_element_type=jnp.float32)
    transport = jnp.sum(src_scale * weighted, axis=0) / (N_SRC * N_TGT)
    return (src_scale, tgt_scale, transport)
```

```python
import jax
import jax.numpy as jnp
from jax import lax
from jax.experimental import pallas as pl
from jax.experimental.pallas import tpu as pltpu
from jax.sharding import PartitionSpec as P

SWEEPS = 6
F32 = jnp.float32
BF16 = jnp.bfloat16
MESH = pl.DeviceIdType.MESH


def sinkhorn_kernel(n_chunk, norm, k_hbm, c_hbm, a_hbm, b_hbm, u_hbm, v_hbm, cost_ref,
                    k_buf, kt_buf, c_buf, kct_buf, a_buf, b_buf, ub_buf, acc,
                    s_out, s_in, t_out, t_in, s0_buf, u_out, v_all, v_out, cost_part, cost_all,
                    k_sem, kp_send, kp_recv, c_sem, ab_sem, bp_sem, s0_send, s0_recv,
                    s_send, s_recv, t_send, t_recv, fin_sem, cs_send, cs_recv, out_sem):
    rows, half = k_hbm.shape
    cols = 2 * half
    rw = rows // n_chunk
    cw = cols // n_chunk
    per_half = n_chunk // 2
    nq = a_buf.shape[0]
    row = lax.axis_index("row")
    col = lax.axis_index("col")
    prob = lax.axis_index("prob")
    x = col // 2
    core = col % 2
    grp = (core + x + row) % 2
    me = row * 4 + col
    mine = pl.ds(pl.multiple_of(grp * nq, nq), nq)
    other = pl.ds(pl.multiple_of((1 - grp) * nq, nq), nq)

    def dev(r, c):
        return (prob, r, c)

    partner = dev(row, 2 * x + 1 - core)
    x_peer = dev(row, 2 * (1 - x) + 1 - core)
    y_peer = dev(1 - row, 2 * x + 1 - core)

    def remote(src, dst, send, recv, to):
        return pltpu.make_async_remote_copy(src_ref=src, dst_ref=dst, send_sem=send, recv_sem=recv,
                                            device_id=to, device_id_type=MESH)

    def krows(i):
        return pl.ds(i * rw, rw)

    k_load = [pltpu.make_async_copy(k_hbm.at[krows(i)], k_buf.at[core, krows(i)], k_sem.at[i]) for i in range(n_chunk)]
    c_load = [pltpu.make_async_copy(c_hbm.at[krows(i)], c_buf.at[krows(i)], c_sem.at[i]) for i in range(n_chunk)]
    a_load = pltpu.make_async_copy(a_hbm.at[mine], a_buf, ab_sem.at[0])
    b_load = pltpu.make_async_copy(b_hbm.at[mine], b_buf.at[core], ab_sem.at[1])
    for d in k_load:
        d.start()
    a_load.start()
    b_load.start()
    for d in c_load:
        d.start()

    barrier = pltpu.get_barrier_semaphore()
    for dr in range(2):
        for dc in range(4):
            if dr or dc:
                pl.semaphore_signal(barrier, inc=1, device_id=dev((row + dr) % 2, (col + dc) % 4), device_id_type=MESH)

    def transpose_rows(h, i):
        blk = 256
        def body(n, carry):
            jo = pl.multiple_of(n * blk, blk)
            for ii in range(rw // blk):
                kt_buf[pl.ds(pl.multiple_of(h * half + jo, blk), blk), pl.ds(i * rw + ii * blk, blk)] = (
                    k_buf[h, pl.ds(i * rw + ii * blk, blk), pl.ds(jo, blk)].T)
            return carry
        lax.fori_loop(0, half // blk, body, 0)

    ones = jnp.ones((nq, half), BF16)
    own_half = pl.ds(pl.multiple_of(core * half, half), half)
    for i in range(n_chunk):
        k_load[i].wait()
        transpose_rows(core, i)
        part = jnp.dot(ones, kt_buf[own_half, krows(i)], preferred_element_type=F32)
        for n in range(rw // 128):
            r = i * (rw // 128) + n
            s0_buf[col, r:r + 1, :] = part[0:1, n * 128:(n + 1) * 128]

    pl.semaphore_wait(barrier, 7)
    s0_copies = []
    for n in range(1, 4):
        d = remote(s0_buf.at[col], s0_buf.at[col], s0_send.at[n], s0_recv.at[n], dev(row, (col + n) % 4))
        d.start()
        s0_copies.append(d)
    k_push = [remote(k_buf.at[core, krows(i)], k_buf.at[core, krows(i)], kp_send.at[i], kp_recv.at[i], partner) for i in range(n_chunk)]
    for d in k_push:
        d.start()
    b_push = remote(b_hbm.at[other], b_buf.at[core], bp_sem.at[0], bp_sem.at[1], partner)
    b_push.start()

    for i in range(n_chunk):
        c_load[i].wait()
        blk = 256
        def body(n, carry):
            jo = pl.multiple_of(n * blk, blk)
            for ii in range(rw // blk):
                rs = pl.ds(i * rw + ii * blk, blk)
                kct_buf[pl.ds(jo, blk), rs] = (k_buf[core, rs, pl.ds(jo, blk)] * c_buf[rs, pl.ds(jo, blk)]).T
            return carry
        lax.fori_loop(0, half // blk, body, 0)

    a_load.wait()
    b_load.wait()
    for n in range(1, 4):
        frm = (col + 4 - n) % 4
        remote(s0_buf.at[frm], s0_buf.at[frm], s0_send.at[n], s0_recv.at[n], dev(row, frm)).wait_recv()
    s0 = (s0_buf[0] + s0_buf[1]) + (s0_buf[2] + s0_buf[3])
    for r in range(rows // 128):
        cs = slice(r * 128, (r + 1) * 128)
        ub_buf[:, cs] = (a_buf[:, cs] / s0[r:r + 1, :]).astype(BF16)

    def t_copy(par, o):
        return remote(t_out.at[o], t_in.at[par, o], t_send.at[o], t_recv.at[par, o], y_peer)

    def s_copy(par, o):
        return remote(s_out.at[o], s_in.at[par, o], s_send.at[o], s_recv.at[par, o], x_peer)

    def send_t_half(h):
        for n in range(per_half):
            o = h * per_half + n
            t_out[o] = jnp.dot(ub_buf[...], k_buf[h, :, n * cw:(n + 1) * cw], preferred_element_type=F32)
            t_copy(0, o).start()

    send_t_half(core)
    for i in range(n_chunk):
        remote(k_buf.at[1 - core, krows(i)], k_buf.at[1 - core, krows(i)], kp_send.at[i], kp_recv.at[i], partner).wait_recv()
    remote(b_hbm.at[other], b_buf.at[1 - core], bp_sem.at[0], bp_sem.at[1], partner).wait_recv()
    send_t_half(1 - core)
    for i in range(n_chunk):
        transpose_rows(1 - core, i)

    def sweep(t, carry):
        par_in = (t + 1) % 2
        par = t % 2
        for c in range(n_chunk):
            t_copy(par_in, c).wait()
            v = b_buf[c // per_half, :, (c % per_half) * cw:(c % per_half + 1) * cw] / (t_out[c] + t_in[par_in, c])
            vb = v.astype(BF16)
            w = slice(c * cw, (c + 1) * cw)
            if c < n_chunk - 1:
                prod = jnp.dot(vb, kt_buf[w, :], preferred_element_type=F32)
                acc[...] = prod if c == 0 else acc[...] + prod
            else:
                for o in range(n_chunk):
                    oc = slice(o * rw, (o + 1) * rw)
                    s_out[o] = acc[:, oc] + jnp.dot(vb, kt_buf[w, oc], preferred_element_type=F32)
                    s_copy(par, o).start()
        for c in range(n_chunk):
            s_copy(par, c).wait()
            w = slice(c * rw, (c + 1) * rw)
            u = a_buf[:, w] / (s_out[c] + s_in[par, c])
            u_out[mine, w] = u
            ub = u.astype(BF16)
            if c < n_chunk - 1:
                for h in range(2):
                    hc = slice(h * half, (h + 1) * half)
                    prod = jnp.dot(ub, k_buf[h, w, :], preferred_element_type=F32)
                    acc[:, hc] = prod if c == 0 else acc[:, hc] + prod
            else:
                for o in range(n_chunk):
                    oc = slice(o * cw, (o + 1) * cw)
                    hc = slice((o % per_half) * cw, (o % per_half + 1) * cw)
                    t_out[o] = acc[:, oc] + jnp.dot(ub, k_buf[o // per_half, w, hc], preferred_element_type=F32)
                    t_copy(par, o).start()
        return carry

    lax.fori_loop(1, SWEEPS, sweep, 0)

    u_push = remote(u_out.at[mine], u_out.at[mine], fin_sem.at[0], fin_sem.at[1], partner)
    u_push.start()
    last = (SWEEPS - 1) % 2
    for c in range(n_chunk):
        t_copy(last, c).wait()
        cs = slice((c % per_half) * cw, (c % per_half + 1) * cw)
        v_all[c // per_half, :, cs] = b_buf[c // per_half, :, cs] / (t_out[c] + t_in[last, c])
    v_push = remote(v_all.at[1 - core], v_out.at[mine], fin_sem.at[2], fin_sem.at[3], partner)
    v_push.start()
    v_own = v_all[core]
    v_out[mine] = v_own

    def cost_rows(v, who):
        w = jnp.dot(v.astype(BF16), kct_buf[...], preferred_element_type=F32) * u_out[who]
        tot = w[:, 0:128]
        for n in range(1, rows // 128):
            tot = tot + w[:, n * 128:(n + 1) * 128]
        cost_part[who] = tot

    cost_part[...] = jnp.zeros_like(cost_part)
    cost_rows(v_own, mine)
    remote(u_out.at[other], u_out.at[other], fin_sem.at[0], fin_sem.at[1], partner).wait_recv()
    u_push.wait_send()
    u_store = pltpu.make_async_copy(u_out, u_hbm, out_sem.at[0])
    u_store.start()
    remote(v_all.at[core], v_out.at[other], fin_sem.at[2], fin_sem.at[3], partner).wait_recv()
    v_push.wait_send()
    v_store = pltpu.make_async_copy(v_out, v_hbm, out_sem.at[1])
    v_store.start()
    cost_rows(v_out[other], other)
    cost_all[me] = jnp.sum(cost_part[...].T, axis=0, keepdims=True)
    cost_copies = []
    for dr in range(2):
        for dc in range(4):
            if dr or dc:
                n = dr * 4 + dc
                d = remote(cost_all.at[me], cost_all.at[me], cs_send.at[n], cs_recv.at[n], dev((row + dr) % 2, (col + dc) % 4))
                d.start()
                cost_copies.append((n, (row + dr) % 2, (col + 4 - dc) % 4, d))
    for d in s0_copies + k_push:
        d.wait_send()
    b_push.wait_send()
    for n, fr, fc, d in cost_copies:
        f = fr * 4 + fc
        remote(cost_all.at[f], cost_all.at[f], cs_send.at[n], cs_recv.at[n], dev(fr, fc)).wait_recv()
    total = cost_all[0]
    for n in range(1, 8):
        total = total + cost_all[n]
    cost_ref[...] = total[:, :cost_ref.shape[1]] * norm
    for n, fr, fc, d in cost_copies:
        d.wait_send()
    u_store.wait()
    v_store.wait()


def solution(mesh):
    n_chunk = 4

    def local_fn(kernel, cost_mat, src_mass, tgt_mass):
        rows, half = kernel.shape
        nprob = src_mass.shape[1]
        nq = nprob // 2
        cols = 2 * half
        rw, cw = rows // n_chunk, cols // n_chunk
        norm = 1.0 / float(rows * mesh.shape["row"] * half * mesh.shape["col"])
        any_spec = pl.BlockSpec(memory_space=pl.ANY)
        dma = pltpu.SemaphoreType.DMA
        u_t, v_t, cost = pl.pallas_call(
            lambda *refs: sinkhorn_kernel(n_chunk, norm, *refs),
            out_shape=(jax.ShapeDtypeStruct((nprob, rows), F32), jax.ShapeDtypeStruct((nprob, half), F32),
                       jax.ShapeDtypeStruct((1, nprob), F32)),
            in_specs=[any_spec] * 4,
            out_specs=(any_spec, any_spec, pl.BlockSpec(memory_space=pltpu.VMEM)),
            scratch_shapes=[
                pltpu.VMEM((2, rows, half), BF16),
                pltpu.VMEM((cols, rows), BF16),
                pltpu.VMEM((rows, half), BF16),
                pltpu.VMEM((half, rows), BF16),
                pltpu.VMEM((nq, rows), F32),
                pltpu.VMEM((2, nq, half), F32),
                pltpu.VMEM((nq, rows), BF16),
                pltpu.VMEM((nq, max(rows, cols)), F32),
                pltpu.VMEM((n_chunk, nq, rw), F32),
                pltpu.VMEM((2, n_chunk, nq, rw), F32),
                pltpu.VMEM((n_chunk, nq, cw), F32),
                pltpu.VMEM((2, n_chunk, nq, cw), F32),
                pltpu.VMEM((4, rows // 128, 128), F32),
                pltpu.VMEM((nprob, rows), F32),
                pltpu.VMEM((2, nq, half), F32),
                pltpu.VMEM((nprob, half), F32),
                pltpu.VMEM((128, 128), F32),
                pltpu.VMEM((8, 1, 128), F32),
                dma((n_chunk,)), dma((n_chunk,)), dma((n_chunk,)), dma((n_chunk,)), dma((2,)), dma((2,)), dma((4,)), dma((4,)),
                dma((n_chunk,)), dma((2, n_chunk)), dma((n_chunk,)), dma((2, n_chunk)), dma((4,)), dma((8,)), dma((8,)), dma((2,)),
            ],
            compiler_params=pltpu.CompilerParams(collective_id=0, has_side_effects=True, vmem_limit_bytes=60 * 1024 * 1024),
            name="sinkhorn",
        )(kernel, cost_mat, src_mass.T, tgt_mass.T)
        return u_t.T, v_t.T, cost.reshape(nprob)

    return jax.shard_map(local_fn, mesh=mesh, in_specs=(P("row", "col"), P("row", "col"), P("row", "prob"), P("col", "prob")), out_specs=(P("row", "prob"), P("col", "prob"), P("prob")), check_vma=False)
```

```python
import jax
import jax.numpy as jnp
from jax import lax
from jax.experimental import pallas as pl
from jax.experimental.pallas import tpu as pltpu
from jax.sharding import PartitionSpec as P

SWEEPS = 6
F32 = jnp.float32
BF16 = jnp.bfloat16
MESH = pl.DeviceIdType.MESH


def sinkhorn_kernel(n_chunk, norm, k_hbm, c_hbm, a_hbm, b_hbm, u_hbm, v_hbm, cost_ref,
                    k_buf, kt_buf, c_buf, kct_buf, a_buf, b_buf, ub_buf, acc,
                    s_out, s_in, t_out, t_in, s0_buf, u_out, v_all, v_out, cost_part, cost_all,
                    k_sem, kp_send, kp_recv, c_sem, ab_sem, bp_sem, s0_send, s0_recv,
                    s_send, s_recv, t_send, t_recv, fin_sem, cs_send, cs_recv, out_sem):
    rows, half = k_hbm.shape
    cols = 2 * half
    rw = rows // n_chunk
    cw = cols // n_chunk
    per_half = n_chunk // 2
    nq = a_buf.shape[0]
    row = lax.axis_index("row")
    col = lax.axis_index("col")
    prob = lax.axis_index("prob")
    x = col // 2
    core = col % 2
    grp = (core + x + row) % 2
    me = row * 4 + col
    mine = pl.ds(pl.multiple_of(grp * nq, nq), nq)
    other = pl.ds(pl.multiple_of((1 - grp) * nq, nq), nq)

    def dev(r, c):
        return (prob, r, c)

    partner = dev(row, 2 * x + 1 - core)
    x_peer = dev(row, 2 * (1 - x) + 1 - core)
    y_peer = dev(1 - row, 2 * x + 1 - core)

    def remote(src, dst, send, recv, to):
        return pltpu.make_async_remote_copy(src_ref=src, dst_ref=dst, send_sem=send, recv_sem=recv,
                                            device_id=to, device_id_type=MESH)

    def krows(i):
        return pl.ds(i * rw, rw)

    k_load = [pltpu.make_async_copy(k_hbm.at[krows(i)], k_buf.at[core, krows(i)], k_sem.at[i]) for i in range(n_chunk)]
    c_load = [pltpu.make_async_copy(c_hbm.at[krows(i)], c_buf.at[krows(i)], c_sem.at[i]) for i in range(n_chunk)]
    a_load = pltpu.make_async_copy(a_hbm.at[mine], a_buf, ab_sem.at[0])
    b_load = pltpu.make_async_copy(b_hbm.at[mine], b_buf.at[core], ab_sem.at[1])
    for d in k_load:
        d.start()
    a_load.start()
    b_load.start()
    for d in c_load:
        d.start()

    barrier = pltpu.get_barrier_semaphore()
    for dr in range(2):
        for dc in range(4):
            if dr or dc:
                pl.semaphore_signal(barrier, inc=1, device_id=dev((row + dr) % 2, (col + dc) % 4), device_id_type=MESH)

    def transpose_rows(h, i):
        blk = 256
        def body(n, carry):
            jo = pl.multiple_of(n * blk, blk)
            for ii in range(rw // blk):
                kt_buf[pl.ds(pl.multiple_of(h * half + jo, blk), blk), pl.ds(i * rw + ii * blk, blk)] = (
                    k_buf[h, pl.ds(i * rw + ii * blk, blk), pl.ds(jo, blk)].T)
            return carry
        lax.fori_loop(0, half // blk, body, 0)

    def build_kct():
        for i in range(n_chunk):
            c_load[i].wait()
            blk = 256
            def body(n, carry):
                jo = pl.multiple_of(n * blk, blk)
                for ii in range(rw // blk):
                    rs = pl.ds(i * rw + ii * blk, blk)
                    kct_buf[pl.ds(jo, blk), rs] = (k_buf[core, rs, pl.ds(jo, blk)] * c_buf[rs, pl.ds(jo, blk)]).T
                return carry
            lax.fori_loop(0, half // blk, body, 0)

    pl.semaphore_wait(barrier, 7)
    ones = jnp.ones((nq, half), BF16)
    k_push = [remote(k_buf.at[core, krows(i)], k_buf.at[core, krows(i)], kp_send.at[i], kp_recv.at[i], partner) for i in range(n_chunk)]
    for i in range(n_chunk):
        k_load[i].wait()
        k_push[i].start()
        part = lax.dot_general(ones, k_buf[core, krows(i)], (((1,), (1,)), ((), ())), preferred_element_type=F32)
        for n in range(rw // 128):
            r = i * (rw // 128) + n
            s0_buf[col, r:r + 1, :] = part[0:1, n * 128:(n + 1) * 128]
    s0_copies = []
    for n in range(1, 4):
        d = remote(s0_buf.at[col], s0_buf.at[col], s0_send.at[n], s0_recv.at[n], dev(row, (col + n) % 4))
        d.start()
        s0_copies.append(d)
    b_push = remote(b_hbm.at[other], b_buf.at[core], bp_sem.at[0], bp_sem.at[1], partner)
    b_push.start()
    for i in range(n_chunk):
        transpose_rows(core, i)

    a_load.wait()
    b_load.wait()
    for n in range(1, 4):
        frm = (col + 4 - n) % 4
        remote(s0_buf.at[frm], s0_buf.at[frm], s0_send.at[n], s0_recv.at[n], dev(row, frm)).wait_recv()
    s0 = (s0_buf[0] + s0_buf[1]) + (s0_buf[2] + s0_buf[3])
    for r in range(rows // 128):
        cs = slice(r * 128, (r + 1) * 128)
        ub_buf[:, cs] = (a_buf[:, cs] / s0[r:r + 1, :]).astype(BF16)

    def t_copy(par, o):
        return remote(t_out.at[o], t_in.at[par, o], t_send.at[o], t_recv.at[par, o], y_peer)

    def s_copy(par, o):
        return remote(s_out.at[o], s_in.at[par, o], s_send.at[o], s_recv.at[par, o], x_peer)

    def send_t_half(h):
        for n in range(per_half):
            o = h * per_half + n
            t_out[o] = jnp.dot(ub_buf[...], k_buf[h, :, n * cw:(n + 1) * cw], preferred_element_type=F32)
            t_copy(0, o).start()

    send_t_half(core)
    build_kct()
    for i in range(n_chunk):
        remote(k_buf.at[1 - core, krows(i)], k_buf.at[1 - core, krows(i)], kp_send.at[i], kp_recv.at[i], partner).wait_recv()
    remote(b_hbm.at[other], b_buf.at[1 - core], bp_sem.at[0], bp_sem.at[1], partner).wait_recv()

    def rest_of_kt():
        for i in range(n_chunk):
            transpose_rows(1 - core, i)

    @pl.when(grp == 1)
    def _():
        rest_of_kt()

    send_t_half(1 - core)

    @pl.when(grp == 0)
    def _():
        rest_of_kt()

    def sweep(t, carry):
        par_in = (t + 1) % 2
        par = t % 2
        for c in range(n_chunk):
            t_copy(par_in, c).wait()
            v = b_buf[c // per_half, :, (c % per_half) * cw:(c % per_half + 1) * cw] / (t_out[c] + t_in[par_in, c])
            vb = v.astype(BF16)
            w = slice(c * cw, (c + 1) * cw)
            if c < n_chunk - 1:
                prod = jnp.dot(vb, kt_buf[w, :], preferred_element_type=F32)
                acc[...] = prod if c == 0 else acc[...] + prod
            else:
                for o in range(n_chunk):
                    oc = slice(o * rw, (o + 1) * rw)
                    s_out[o] = acc[:, oc] + jnp.dot(vb, kt_buf[w, oc], preferred_element_type=F32)
                    s_copy(par, o).start()
        for c in range(n_chunk):
            s_copy(par, c).wait()
            w = slice(c * rw, (c + 1) * rw)
            u = a_buf[:, w] / (s_out[c] + s_in[par, c])
            u_out[mine, w] = u
            ub = u.astype(BF16)
            if c < n_chunk - 1:
                for h in range(2):
                    hc = slice(h * half, (h + 1) * half)
                    prod = jnp.dot(ub, k_buf[h, w, :], preferred_element_type=F32)
                    acc[:, hc] = prod if c == 0 else acc[:, hc] + prod
            else:
                for o in range(n_chunk):
                    oc = slice(o * cw, (o + 1) * cw)
                    hc = slice((o % per_half) * cw, (o % per_half + 1) * cw)
                    t_out[o] = acc[:, oc] + jnp.dot(ub, k_buf[o // per_half, w, hc], preferred_element_type=F32)
                    t_copy(par, o).start()
        return carry

    lax.fori_loop(1, SWEEPS, sweep, 0)

    u_push = remote(u_out.at[mine], u_out.at[mine], fin_sem.at[0], fin_sem.at[1], partner)
    u_push.start()
    last = (SWEEPS - 1) % 2
    for c in range(n_chunk):
        t_copy(last, c).wait()
        cs = slice((c % per_half) * cw, (c % per_half + 1) * cw)
        v_all[c // per_half, :, cs] = b_buf[c // per_half, :, cs] / (t_out[c] + t_in[last, c])
    v_push = remote(v_all.at[1 - core], v_out.at[mine], fin_sem.at[2], fin_sem.at[3], partner)
    v_push.start()
    v_own = v_all[core]
    v_out[mine] = v_own

    def cost_rows(v, who):
        w = jnp.dot(v.astype(BF16), kct_buf[...], preferred_element_type=F32) * u_out[who]
        tot = w[:, 0:128]
        for n in range(1, rows // 128):
            tot = tot + w[:, n * 128:(n + 1) * 128]
        cost_part[who] = tot

    cost_part[...] = jnp.zeros_like(cost_part)
    cost_rows(v_own, mine)
    remote(u_out.at[other], u_out.at[other], fin_sem.at[0], fin_sem.at[1], partner).wait_recv()
    u_push.wait_send()
    u_store = pltpu.make_async_copy(u_out, u_hbm, out_sem.at[0])
    u_store.start()
    remote(v_all.at[core], v_out.at[other], fin_sem.at[2], fin_sem.at[3], partner).wait_recv()
    v_push.wait_send()
    v_store = pltpu.make_async_copy(v_out, v_hbm, out_sem.at[1])
    v_store.start()
    cost_rows(v_out[other], other)
    cost_all[me] = jnp.sum(cost_part[...].T, axis=0, keepdims=True)
    cost_copies = []
    for dr in range(2):
        for dc in range(4):
            if dr or dc:
                n = dr * 4 + dc
                d = remote(cost_all.at[me], cost_all.at[me], cs_send.at[n], cs_recv.at[n], dev((row + dr) % 2, (col + dc) % 4))
                d.start()
                cost_copies.append((n, (row + dr) % 2, (col + 4 - dc) % 4, d))
    for d in s0_copies + k_push:
        d.wait_send()
    b_push.wait_send()
    for n, fr, fc, d in cost_copies:
        f = fr * 4 + fc
        remote(cost_all.at[f], cost_all.at[f], cs_send.at[n], cs_recv.at[n], dev(fr, fc)).wait_recv()
    total = cost_all[0]
    for n in range(1, 8):
        total = total + cost_all[n]
    cost_ref[...] = total[:, :cost_ref.shape[1]] * norm
    for n, fr, fc, d in cost_copies:
        d.wait_send()
    u_store.wait()
    v_store.wait()


def solution(mesh):
    n_chunk = 4

    def local_fn(kernel, cost_mat, src_mass, tgt_mass):
        rows, half = kernel.shape
        nprob = src_mass.shape[1]
        nq = nprob // 2
        cols = 2 * half
        rw, cw = rows // n_chunk, cols // n_chunk
        norm = 1.0 / float(rows * mesh.shape["row"] * half * mesh.shape["col"])
        any_spec = pl.BlockSpec(memory_space=pl.ANY)
        dma = pltpu.SemaphoreType.DMA
        u_t, v_t, cost = pl.pallas_call(
            lambda *refs: sinkhorn_kernel(n_chunk, norm, *refs),
            out_shape=(jax.ShapeDtypeStruct((nprob, rows), F32), jax.ShapeDtypeStruct((nprob, half), F32),
                       jax.ShapeDtypeStruct((1, nprob), F32)),
            in_specs=[any_spec] * 4,
            out_specs=(any_spec, any_spec, pl.BlockSpec(memory_space=pltpu.VMEM)),
            scratch_shapes=[
                pltpu.VMEM((2, rows, half), BF16),
                pltpu.VMEM((cols, rows), BF16),
                pltpu.VMEM((rows, half), BF16),
                pltpu.VMEM((half, rows), BF16),
                pltpu.VMEM((nq, rows), F32),
                pltpu.VMEM((2, nq, half), F32),
                pltpu.VMEM((nq, rows), BF16),
                pltpu.VMEM((nq, max(rows, cols)), F32),
                pltpu.VMEM((n_chunk, nq, rw), F32),
                pltpu.VMEM((2, n_chunk, nq, rw), F32),
                pltpu.VMEM((n_chunk, nq, cw), F32),
                pltpu.VMEM((2, n_chunk, nq, cw), F32),
                pltpu.VMEM((4, rows // 128, 128), F32),
                pltpu.VMEM((nprob, rows), F32),
                pltpu.VMEM((2, nq, half), F32),
                pltpu.VMEM((nprob, half), F32),
                pltpu.VMEM((128, 128), F32),
                pltpu.VMEM((8, 1, 128), F32),
                dma((n_chunk,)), dma((n_chunk,)), dma((n_chunk,)), dma((n_chunk,)), dma((2,)), dma((2,)), dma((4,)), dma((4,)),
                dma((n_chunk,)), dma((2, n_chunk)), dma((n_chunk,)), dma((2, n_chunk)), dma((4,)), dma((8,)), dma((8,)), dma((2,)),
            ],
            compiler_params=pltpu.CompilerParams(collective_id=0, has_side_effects=True, vmem_limit_bytes=60 * 1024 * 1024),
            name="sinkhorn",
        )(kernel, cost_mat, src_mass.T, tgt_mass.T)
        return u_t.T, v_t.T, cost.reshape(nprob)

    return jax.shard_map(local_fn, mesh=mesh, in_specs=(P("row", "col"), P("row", "col"), P("row", "prob"), P("col", "prob")), out_specs=(P("row", "prob"), P("col", "prob"), P("prob")), check_vma=False)
```

```python
import jax
import jax.numpy as jnp
from jax import lax
from jax.experimental import pallas as pl
from jax.experimental.pallas import tpu as pltpu
from jax.sharding import PartitionSpec as P

SWEEPS = 6
F32 = jnp.float32
BF16 = jnp.bfloat16
MESH = pl.DeviceIdType.MESH


def sinkhorn_kernel(n_chunk, norm, k_hbm, c_hbm, a_hbm, b_hbm, u_hbm, v_hbm, cost_ref,
                    k_buf, kt_buf, c_buf, kct_buf, a_buf, b_buf, ub_buf, acc,
                    vb_buf, s_out, s_in, t_out, t_in, t0_buf, s0_buf, u_out, v_all, v_out, cost_part, cost_all,
                    k_sem, kp_send, kp_recv, c_sem, ab_sem, bp_sem, s0_send, s0_recv,
                    s_send, s_recv, t_send, t_recv, fin_sem, cs_send, cs_recv, out_sem,
                    kc_send, kc_recv, t0_send_sem, t0p_send, t0p_recv):
    rows, half = k_hbm.shape
    cols = 2 * half
    rw = rows // n_chunk
    cw = cols // n_chunk
    per_half = n_chunk // 2
    nq = b_buf.shape[1]
    row = lax.axis_index("row")
    col = lax.axis_index("col")
    prob = lax.axis_index("prob")
    x = col // 2
    core = col % 2
    grp = (core + x + row) % 2
    me = row * 4 + col
    mine = pl.ds(pl.multiple_of(grp * nq, nq), nq)
    other = pl.ds(pl.multiple_of((1 - grp) * nq, nq), nq)

    def dev(r, c):
        return (prob, r, c)

    partner = dev(row, 2 * x + 1 - core)
    x_peer = dev(row, 2 * (1 - x) + 1 - core)
    y_peer = dev(1 - row, 2 * x + 1 - core)

    def remote(src, dst, send, recv, to):
        return pltpu.make_async_remote_copy(src_ref=src, dst_ref=dst, send_sem=send, recv_sem=recv,
                                            device_id=to, device_id_type=MESH)

    def krows(i):
        return pl.ds(i * rw, rw)

    k_load = [pltpu.make_async_copy(k_hbm.at[krows(i)], k_buf.at[core, krows(i)], k_sem.at[i]) for i in range(n_chunk)]
    c_load = [pltpu.make_async_copy(c_hbm.at[krows(i)], c_buf.at[krows(i)], c_sem.at[i]) for i in range(n_chunk)]
    a_load = pltpu.make_async_copy(a_hbm, a_buf, ab_sem.at[0])
    b_load = pltpu.make_async_copy(b_hbm.at[mine], b_buf.at[core], ab_sem.at[1])
    for d in k_load:
        d.start()
    a_load.start()
    b_load.start()

    barrier = pltpu.get_barrier_semaphore()
    for dr in range(2):
        for dc in range(4):
            if dr or dc:
                pl.semaphore_signal(barrier, inc=1, device_id=dev((row + dr) % 2, (col + dc) % 4), device_id_type=MESH)

    blk = 256

    def transpose_rows(h, i):
        def body(n, carry):
            jo = pl.multiple_of(n * blk, blk)
            for ii in range(rw // blk):
                kt_buf[pl.ds(pl.multiple_of(h * half + jo, blk), blk), pl.ds(i * rw + ii * blk, blk)] = (
                    k_buf[h, pl.ds(i * rw + ii * blk, blk), pl.ds(jo, blk)].T)
            return carry
        lax.fori_loop(0, half // blk, body, 0)

    def kct_copy(i):
        part = kct_buf.at[pl.ds(pl.multiple_of(core * half, half), half), pl.ds(pl.multiple_of(i * rw, rw), rw)]
        return remote(part, part, kc_send.at[i], kc_recv.at[i], partner)

    def build_kct(i):
        pltpu.make_async_copy(c_hbm.at[pl.ds(i * rw, rw)], c_buf.at[pl.ds(i * rw, rw)], c_sem.at[i]).wait()
        def body(n, carry):
            jo = pl.multiple_of(n * blk, blk)
            for ii in range(rw // blk):
                rs = pl.ds(pl.multiple_of(i * rw + ii * blk, blk), blk)
                kct_buf[pl.ds(pl.multiple_of(core * half + jo, blk), blk), rs] = (
                    k_buf[core, rs, pl.ds(jo, blk)] * c_buf[rs, pl.ds(jo, blk)]).T
            return carry
        lax.fori_loop(0, half // blk, body, 0)
        kct_copy(i).start()

    k_push = [remote(k_buf.at[core, krows(i)], k_buf.at[core, krows(i)], kp_send.at[i], kp_recv.at[i], partner) for i in range(n_chunk)]
    b_push = remote(b_hbm.at[other], b_buf.at[core], bp_sem.at[0], bp_sem.at[1], partner)
    pl.semaphore_wait(barrier, 7)
    b_push.start()
    ones = jnp.ones((nq, half), BF16)
    for i in range(n_chunk):
        k_load[i].wait()
        if i == 0:
            k_push[0].start()
        part = lax.dot_general(ones, k_buf[core, krows(i)], (((1,), (1,)), ((), ())), preferred_element_type=F32)
        for n in range(rw // 128):
            r = i * (rw // 128) + n
            s0_buf[col, r:r + 1, :] = part[0:1, n * 128:(n + 1) * 128]
    s0_copies = []
    for n in range(1, 4):
        d = remote(s0_buf.at[col], s0_buf.at[col], s0_send.at[n], s0_recv.at[n], dev(row, (col + n) % 4))
        d.start()
        s0_copies.append(d)
    for i in range(1, n_chunk - 1):
        k_push[i].start()
    for d in c_load:
        d.start()
    for i in range(n_chunk):
        transpose_rows(core, i)
    a_load.wait()
    b_load.wait()
    for n in range(1, 4):
        frm = (col + 4 - n) % 4
        remote(s0_buf.at[frm], s0_buf.at[frm], s0_send.at[n], s0_recv.at[n], dev(row, frm)).wait_recv()
    s0 = (s0_buf[0] + s0_buf[1]) + (s0_buf[2] + s0_buf[3])
    for r in range(rows // 128):
        cs = slice(r * 128, (r + 1) * 128)
        ub_buf[:, cs] = (a_buf[:, cs] / s0[r:r + 1, :]).astype(BF16)

    def t_copy(par, o):
        return remote(t_out.at[o], t_in.at[par, o], t_send.at[o], t_recv.at[par, o], y_peer)

    def s_copy(par, o):
        return remote(s_out.at[o], s_in.at[par, o], s_send.at[o], s_recv.at[par, o], x_peer)

    t0_copies = []

    def t0_send(g, n):
        d = remote(t0_buf.at[g, n], t_in.at[0, core * per_half + n], t0_send_sem.at[g, n], t_recv.at[0, core * per_half + n],
                   dev(1 - row, 2 * x + (g + x + 1 - row) % 2))
        d.start()
        t0_copies.append(d)

    for n in range(per_half):
        part = jnp.dot(ub_buf[...], k_buf[core, :, n * cw:(n + 1) * cw], preferred_element_type=F32)
        for g in range(2):
            t0_buf[g, n] = part[g * nq:(g + 1) * nq]
        t0_send(0, n)
    for n in range(per_half):
        t0_send(1, n)
    for n in range(per_half):
        o = core * per_half + n
        d = remote(t0_buf.at[1 - grp, n], t_out.at[o], t0p_send.at[n], t0p_recv.at[n], partner)
        d.start()
        t0_copies.append(d)
        t_out[o] = t0_buf[grp, n]
    k_push[n_chunk - 1].start()

    def v_of(par, o):
        return b_buf[o // per_half, :, (o % per_half) * cw:(o % per_half + 1) * cw] / (t_out[o] + t_in[par, o])

    def first_v(h, n):
        o = h * per_half + n
        remote(t0_buf.at[0, n], t_in.at[0, o], t0_send_sem.at[0, n], t_recv.at[0, o], y_peer).wait_recv()
        return (b_buf[h, :, n * cw:(n + 1) * cw] / (t_out[o] + t_in[0, o])).astype(BF16)

    remote(b_hbm.at[other], b_buf.at[1 - core], bp_sem.at[0], bp_sem.at[1], partner).wait_recv()
    for n in range(per_half):
        prod = jnp.dot(first_v(core, n), kt_buf[pl.ds(pl.multiple_of(core * half + n * cw, cw), cw), :], preferred_element_type=F32)
        acc[...] = prod if n == 0 else acc[...] + prod
    for n in range(per_half):
        o = (1 - core) * per_half + n
        remote(t0_buf.at[0, n], t_out.at[o], t0p_send.at[n], t0p_recv.at[n], partner).wait_recv()
        vb_buf[:, n * cw:(n + 1) * cw] = first_v(1 - core, n)
    for o in range(n_chunk):
        remote(k_buf.at[1 - core, krows(o)], k_buf.at[1 - core, krows(o)], kp_send.at[o], kp_recv.at[o], partner).wait_recv()
        prod = lax.dot_general(vb_buf[...], k_buf[1 - core, krows(o)], (((1,), (1,)), ((), ())), preferred_element_type=F32)
        s_out[o] = acc[:, o * rw:(o + 1) * rw] + prod
        s_copy(1, o).start()
    for d in t0_copies:
        d.wait_send()
    for i in range(n_chunk):
        transpose_rows(1 - core, i)

    def u_and_t(par):
        for c in range(n_chunk):
            s_copy(par, c).wait()
            w = slice(c * rw, (c + 1) * rw)
            u = a_buf[mine, w] / (s_out[c] + s_in[par, c])
            u_out[mine, w] = u
            ub = u.astype(BF16)
            if c < n_chunk - 1:
                for h in range(2):
                    hc = slice(h * half, (h + 1) * half)
                    prod = jnp.dot(ub, k_buf[h, w, :], preferred_element_type=F32)
                    acc[:, hc] = prod if c == 0 else acc[:, hc] + prod
            else:
                for o in range(n_chunk):
                    oc = slice(o * cw, (o + 1) * cw)
                    hc = slice((o % per_half) * cw, (o % per_half + 1) * cw)
                    t_out[o] = acc[:, oc] + jnp.dot(ub, k_buf[o // per_half, w, hc], preferred_element_type=F32)
                    t_copy(par, o).start()

    def v_and_s(par_in, par):
        for c in range(n_chunk):
            t_copy(par_in, c).wait()
            vb = v_of(par_in, c).astype(BF16)
            w = slice(c * cw, (c + 1) * cw)
            if c < n_chunk - 1:
                prod = jnp.dot(vb, kt_buf[w, :], preferred_element_type=F32)
                acc[...] = prod if c == 0 else acc[...] + prod
            else:
                for o in range(n_chunk):
                    oc = slice(o * rw, (o + 1) * rw)
                    s_out[o] = acc[:, oc] + jnp.dot(vb, kt_buf[w, oc], preferred_element_type=F32)
                    s_copy(par, o).start()

    def sweep(t, carry):
        u_and_t(t % 2)
        build_kct(t - 1)
        v_and_s(t % 2, (t + 1) % 2)
        return carry

    lax.fori_loop(1, SWEEPS - 1, sweep, 0)
    last = (SWEEPS - 1) % 2
    u_and_t(last)

    u_push = remote(u_out.at[mine], u_out.at[mine], fin_sem.at[0], fin_sem.at[1], partner)
    u_push.start()
    cost_part[...] = jnp.zeros_like(cost_part)
    for d in s0_copies + k_push:
        d.wait_send()
    b_push.wait_send()
    for i in range(n_chunk):
        other_part = kct_buf.at[pl.ds(pl.multiple_of((1 - core) * half, half), half), krows(i)]
        remote(other_part, other_part, kc_send.at[i], kc_recv.at[i], partner).wait_recv()
        kct_copy(i).wait_send()
    for c in range(n_chunk):
        t_copy(last, c).wait()
        v = v_of(last, c)
        v_all[c // per_half, :, (c % per_half) * cw:(c % per_half + 1) * cw] = v
        prod = jnp.dot(v.astype(BF16), kct_buf[c * cw:(c + 1) * cw, :], preferred_element_type=F32)
        if c < n_chunk - 1:
            acc[...] = prod if c == 0 else acc[...] + prod
        else:
            w = (acc[...] + prod) * u_out[mine]
    v_push = remote(v_all.at[1 - core], v_out.at[mine], fin_sem.at[2], fin_sem.at[3], partner)
    v_push.start()
    tot = w[:, 0:128]
    for n in range(1, rows // 128):
        tot = tot + w[:, n * 128:(n + 1) * 128]
    cost_part[mine] = tot
    cost_all[me] = jnp.sum(cost_part[...].T, axis=0, keepdims=True)
    cost_copies = []
    for dr in range(2):
        for dc in range(4):
            if dr or dc:
                n = dr * 4 + dc
                d = remote(cost_all.at[me], cost_all.at[me], cs_send.at[n], cs_recv.at[n], dev((row + dr) % 2, (col + dc) % 4))
                d.start()
                cost_copies.append((n, (row + dr) % 2, (col + 4 - dc) % 4, d))
    v_out[mine] = v_all[core]
    remote(u_out.at[other], u_out.at[other], fin_sem.at[0], fin_sem.at[1], partner).wait_recv()
    u_push.wait_send()
    u_store = pltpu.make_async_copy(u_out, u_hbm, out_sem.at[0])
    u_store.start()
    remote(v_all.at[core], v_out.at[other], fin_sem.at[2], fin_sem.at[3], partner).wait_recv()
    v_push.wait_send()
    v_store = pltpu.make_async_copy(v_out, v_hbm, out_sem.at[1])
    v_store.start()
    for n, fr, fc, d in cost_copies:
        f = fr * 4 + fc
        remote(cost_all.at[f], cost_all.at[f], cs_send.at[n], cs_recv.at[n], dev(fr, fc)).wait_recv()
    total = cost_all[0]
    for n in range(1, 8):
        total = total + cost_all[n]
    cost_ref[...] = total[:, :cost_ref.shape[1]] * norm
    for n, fr, fc, d in cost_copies:
        d.wait_send()
    u_store.wait()
    v_store.wait()


def solution(mesh):
    n_chunk = 4

    def local_fn(kernel, cost_mat, src_mass, tgt_mass):
        rows, half = kernel.shape
        nprob = src_mass.shape[1]
        nq = nprob // 2
        cols = 2 * half
        rw, cw = rows // n_chunk, cols // n_chunk
        norm = 1.0 / float(rows * mesh.shape["row"] * half * mesh.shape["col"])
        any_spec = pl.BlockSpec(memory_space=pl.ANY)
        dma = pltpu.SemaphoreType.DMA
        u_t, v_t, cost = pl.pallas_call(
            lambda *refs: sinkhorn_kernel(n_chunk, norm, *refs),
            out_shape=(jax.ShapeDtypeStruct((nprob, rows), F32), jax.ShapeDtypeStruct((nprob, half), F32),
                       jax.ShapeDtypeStruct((1, nprob), F32)),
            in_specs=[any_spec] * 4,
            out_specs=(any_spec, any_spec, pl.BlockSpec(memory_space=pltpu.VMEM)),
            scratch_shapes=[
                pltpu.VMEM((2, rows, half), BF16),
                pltpu.VMEM((cols, rows), BF16),
                pltpu.VMEM((rows, half), BF16),
                pltpu.VMEM((cols, rows), BF16),
                pltpu.VMEM((nprob, rows), F32),
                pltpu.VMEM((2, nq, half), F32),
                pltpu.VMEM((nprob, rows), BF16),
                pltpu.VMEM((nq, max(rows, cols)), F32),
                pltpu.VMEM((nq, half), BF16),
                pltpu.VMEM((n_chunk, nq, rw), F32),
                pltpu.VMEM((2, n_chunk, nq, rw), F32),
                pltpu.VMEM((n_chunk, nq, cw), F32),
                pltpu.VMEM((2, n_chunk, nq, cw), F32),
                pltpu.VMEM((2, n_chunk // 2, nq, cw), F32),
                pltpu.VMEM((4, rows // 128, 128), F32),
                pltpu.VMEM((nprob, rows), F32),
                pltpu.VMEM((2, nq, half), F32),
                pltpu.VMEM((nprob, half), F32),
                pltpu.VMEM((128, 128), F32),
                pltpu.VMEM((8, 1, 128), F32),
                dma((n_chunk,)), dma((n_chunk,)), dma((n_chunk,)), dma((n_chunk,)), dma((2,)), dma((2,)), dma((4,)), dma((4,)),
                dma((n_chunk,)), dma((2, n_chunk)), dma((n_chunk,)), dma((2, n_chunk)), dma((4,)), dma((8,)), dma((8,)), dma((2,)),
                dma((n_chunk,)), dma((n_chunk,)), dma((2, n_chunk // 2)), dma((n_chunk // 2,)), dma((n_chunk // 2,)),
            ],
            compiler_params=pltpu.CompilerParams(collective_id=0, has_side_effects=True, vmem_limit_bytes=60 * 1024 * 1024),
            name="sinkhorn",
        )(kernel, cost_mat, src_mass.T, tgt_mass.T)
        return u_t.T, v_t.T, cost.reshape(nprob)

    return jax.shard_map(local_fn, mesh=mesh, in_specs=(P("row", "col"), P("row", "col"), P("row", "prob"), P("col", "prob")), out_specs=(P("row", "prob"), P("col", "prob"), P("prob")), check_vma=False)
```

```python
import jax
import jax.numpy as jnp
from jax import lax
from jax.experimental import pallas as pl
from jax.experimental.pallas import tpu as pltpu
from jax.sharding import PartitionSpec as P

SWEEPS = 6
F32 = jnp.float32
BF16 = jnp.bfloat16
MESH = pl.DeviceIdType.MESH


def sinkhorn_kernel(n_chunk, norm, k_hbm, c_hbm, a_hbm, b_hbm, u_hbm, v_hbm, cost_ref,
                    k_buf, kt_buf, c_buf, kct_buf, a_buf, b_buf, ub_buf, acc,
                    s_out, s_in, t_out, t_in, t0_buf, s0_buf, u_out, v_all, v_out, cost_part, cost_all,
                    k_sem, kp_send, kp_recv, c_sem, ab_sem, bp_sem, s0_send, s0_recv,
                    s_send, s_recv, t_send, t_recv, fin_sem, cs_send, cs_recv, out_sem,
                    kc_send, kc_recv, t0_send_sem, t0p_send, t0p_recv):
    rows, half = k_hbm.shape
    cols = 2 * half
    rw = rows // n_chunk
    cw = cols // n_chunk
    per_half = n_chunk // 2
    nq = b_buf.shape[1]
    row = lax.axis_index("row")
    col = lax.axis_index("col")
    prob = lax.axis_index("prob")
    x = col // 2
    core = col % 2
    grp = (core + x + row) % 2
    me = row * 4 + col
    mine = pl.ds(pl.multiple_of(grp * nq, nq), nq)
    other = pl.ds(pl.multiple_of((1 - grp) * nq, nq), nq)

    def dev(r, c):
        return (prob, r, c)

    partner = dev(row, 2 * x + 1 - core)
    x_peer = dev(row, 2 * (1 - x) + 1 - core)
    y_peer = dev(1 - row, 2 * x + 1 - core)

    def remote(src, dst, send, recv, to):
        return pltpu.make_async_remote_copy(src_ref=src, dst_ref=dst, send_sem=send, recv_sem=recv,
                                            device_id=to, device_id_type=MESH)

    def krows(i):
        return pl.ds(i * rw, rw)

    k_load = [pltpu.make_async_copy(k_hbm.at[krows(i)], k_buf.at[core, krows(i)], k_sem.at[i]) for i in range(n_chunk)]
    c_load = [pltpu.make_async_copy(c_hbm.at[krows(i)], c_buf.at[krows(i)], c_sem.at[i]) for i in range(n_chunk)]
    a_load = pltpu.make_async_copy(a_hbm, a_buf, ab_sem.at[0])
    b_load = pltpu.make_async_copy(b_hbm.at[mine], b_buf.at[core], ab_sem.at[1])
    for d in k_load:
        d.start()
    a_load.start()
    b_load.start()

    barrier = pltpu.get_barrier_semaphore()
    for dr in range(2):
        for dc in range(4):
            if dr or dc:
                pl.semaphore_signal(barrier, inc=1, device_id=dev((row + dr) % 2, (col + dc) % 4), device_id_type=MESH)

    blk = 256

    def transpose_rows(h, i):
        def body(n, carry):
            jo = pl.multiple_of(n * blk, blk)
            for ii in range(rw // blk):
                kt_buf[pl.ds(pl.multiple_of(h * half + jo, blk), blk), pl.ds(i * rw + ii * blk, blk)] = (
                    k_buf[h, pl.ds(i * rw + ii * blk, blk), pl.ds(jo, blk)].T)
            return carry
        lax.fori_loop(0, half // blk, body, 0)

    def kct_copy(i):
        part = kct_buf.at[pl.ds(pl.multiple_of(core * half, half), half), pl.ds(pl.multiple_of(i * rw, rw), rw)]
        return remote(part, part, kc_send.at[i], kc_recv.at[i], partner)

    def build_kct(i):
        pltpu.make_async_copy(c_hbm.at[pl.ds(i * rw, rw)], c_buf.at[pl.ds(i * rw, rw)], c_sem.at[i]).wait()
        def body(n, carry):
            jo = pl.multiple_of(n * blk, blk)
            for ii in range(rw // blk):
                rs = pl.ds(pl.multiple_of(i * rw + ii * blk, blk), blk)
                kct_buf[pl.ds(pl.multiple_of(core * half + jo, blk), blk), rs] = (
                    k_buf[core, rs, pl.ds(jo, blk)] * c_buf[rs, pl.ds(jo, blk)]).T
            return carry
        lax.fori_loop(0, half // blk, body, 0)
        kct_copy(i).start()

    k_push = [remote(k_buf.at[core, krows(i)], k_buf.at[core, krows(i)], kp_send.at[i], kp_recv.at[i], partner) for i in range(n_chunk)]
    b_push = remote(b_hbm.at[other], b_buf.at[core], bp_sem.at[0], bp_sem.at[1], partner)
    pl.semaphore_wait(barrier, 7)
    b_push.start()
    ones = jnp.ones((nq, half), BF16)
    for i in range(n_chunk):
        k_load[i].wait()
        if i == 0:
            k_push[0].start()
        part = lax.dot_general(ones, k_buf[core, krows(i)], (((1,), (1,)), ((), ())), preferred_element_type=F32)
        for n in range(rw // 128):
            r = i * (rw // 128) + n
            s0_buf[col, r:r + 1, :] = part[0:1, n * 128:(n + 1) * 128]
    s0_copies = []
    for n in range(1, 4):
        d = remote(s0_buf.at[col], s0_buf.at[col], s0_send.at[n], s0_recv.at[n], dev(row, (col + n) % 4))
        d.start()
        s0_copies.append(d)
    for i in range(1, n_chunk - 1):
        k_push[i].start()
    for d in c_load:
        d.start()
    for i in range(n_chunk):
        transpose_rows(core, i)
    a_load.wait()
    b_load.wait()
    for n in range(1, 4):
        frm = (col + 4 - n) % 4
        remote(s0_buf.at[frm], s0_buf.at[frm], s0_send.at[n], s0_recv.at[n], dev(row, frm)).wait_recv()
    s0 = (s0_buf[0] + s0_buf[1]) + (s0_buf[2] + s0_buf[3])
    for r in range(rows // 128):
        cs = slice(r * 128, (r + 1) * 128)
        ub_buf[:, cs] = (a_buf[:, cs] / s0[r:r + 1, :]).astype(BF16)

    def t_copy(par, o):
        return remote(t_out.at[o], t_in.at[par, o], t_send.at[o], t_recv.at[par, o], y_peer)

    def s_copy(par, o):
        return remote(s_out.at[o], s_in.at[par, o], s_send.at[o], s_recv.at[par, o], x_peer)

    t0_copies = []

    def t0_send(g, n):
        d = remote(t0_buf.at[g, n], t_in.at[0, core * per_half + n], t0_send_sem.at[g, n], t_recv.at[0, core * per_half + n],
                   dev(1 - row, 2 * x + (g + x + 1 - row) % 2))
        d.start()
        t0_copies.append(d)

    for n in range(per_half):
        part = jnp.dot(ub_buf[...], k_buf[core, :, n * cw:(n + 1) * cw], preferred_element_type=F32)
        for g in range(2):
            t0_buf[g, n] = part[g * nq:(g + 1) * nq]
        t0_send(0, n)
    for n in range(per_half):
        t0_send(1, n)
    for n in range(per_half):
        o = core * per_half + n
        d = remote(t0_buf.at[1 - grp, n], t_out.at[o], t0p_send.at[n], t0p_recv.at[n], partner)
        d.start()
        t0_copies.append(d)
        t_out[o] = t0_buf[grp, n]
    k_push[n_chunk - 1].start()

    def v_of(par, o):
        return b_buf[o // per_half, :, (o % per_half) * cw:(o % per_half + 1) * cw] / (t_out[o] + t_in[par, o])

    def first_v(h, n):
        o = h * per_half + n
        remote(t0_buf.at[0, n], t_in.at[0, o], t0_send_sem.at[0, n], t_recv.at[0, o], y_peer).wait_recv()
        return (b_buf[h, :, n * cw:(n + 1) * cw] / (t_out[o] + t_in[0, o])).astype(BF16)

    remote(b_hbm.at[other], b_buf.at[1 - core], bp_sem.at[0], bp_sem.at[1], partner).wait_recv()
    for i in range(n_chunk):
        remote(k_buf.at[1 - core, krows(i)], k_buf.at[1 - core, krows(i)], kp_send.at[i], kp_recv.at[i], partner).wait_recv()
        transpose_rows(1 - core, i)

    @pl.when(grp == 1)
    def _():
        for i in range(n_chunk):
            build_kct(i)

    for m in range(n_chunk):
        h = core if m < per_half else 1 - core
        n = m % per_half
        if m >= per_half:
            remote(t0_buf.at[0, n], t_out.at[h * per_half + n], t0p_send.at[n], t0p_recv.at[n], partner).wait_recv()
        vb = first_v(h, n)
        js = pl.ds(pl.multiple_of(h * half + n * cw, cw), cw)
        if m < n_chunk - 1:
            prod = jnp.dot(vb, kt_buf[js, :], preferred_element_type=F32)
            acc[...] = prod if m == 0 else acc[...] + prod
        else:
            for o in range(n_chunk):
                s_out[o] = acc[:, o * rw:(o + 1) * rw] + jnp.dot(vb, kt_buf[js, o * rw:(o + 1) * rw], preferred_element_type=F32)
                s_copy(1, o).start()
    for d in t0_copies:
        d.wait_send()

    def u_and_t(par):
        for c in range(n_chunk):
            s_copy(par, c).wait()
            w = slice(c * rw, (c + 1) * rw)
            u = a_buf[mine, w] / (s_out[c] + s_in[par, c])
            u_out[mine, w] = u
            ub = u.astype(BF16)
            if c < n_chunk - 1:
                for h in range(2):
                    hc = slice(h * half, (h + 1) * half)
                    prod = jnp.dot(ub, k_buf[h, w, :], preferred_element_type=F32)
                    acc[:, hc] = prod if c == 0 else acc[:, hc] + prod
            else:
                for o in range(n_chunk):
                    oc = slice(o * cw, (o + 1) * cw)
                    hc = slice((o % per_half) * cw, (o % per_half + 1) * cw)
                    t_out[o] = acc[:, oc] + jnp.dot(ub, k_buf[o // per_half, w, hc], preferred_element_type=F32)
                    t_copy(par, o).start()

    def v_and_s(par_in, par):
        for c in range(n_chunk):
            t_copy(par_in, c).wait()
            vb = v_of(par_in, c).astype(BF16)
            w = slice(c * cw, (c + 1) * cw)
            if c < n_chunk - 1:
                prod = jnp.dot(vb, kt_buf[w, :], preferred_element_type=F32)
                acc[...] = prod if c == 0 else acc[...] + prod
            else:
                for o in range(n_chunk):
                    oc = slice(o * rw, (o + 1) * rw)
                    s_out[o] = acc[:, oc] + jnp.dot(vb, kt_buf[w, oc], preferred_element_type=F32)
                    s_copy(par, o).start()

    def sweep(t, carry):
        u_and_t(t % 2)

        @pl.when(grp == 0)
        def _():
            build_kct(t - 1)

        v_and_s(t % 2, (t + 1) % 2)
        return carry

    lax.fori_loop(1, SWEEPS - 1, sweep, 0)
    last = (SWEEPS - 1) % 2
    u_and_t(last)

    u_push = remote(u_out.at[mine], u_out.at[mine], fin_sem.at[0], fin_sem.at[1], partner)
    u_push.start()
    cost_part[...] = jnp.zeros_like(cost_part)
    for d in s0_copies + k_push:
        d.wait_send()
    b_push.wait_send()
    for i in range(n_chunk):
        other_part = kct_buf.at[pl.ds(pl.multiple_of((1 - core) * half, half), half), krows(i)]
        remote(other_part, other_part, kc_send.at[i], kc_recv.at[i], partner).wait_recv()
        kct_copy(i).wait_send()
    for c in range(n_chunk):
        t_copy(last, c).wait()
        v = v_of(last, c)
        v_all[c // per_half, :, (c % per_half) * cw:(c % per_half + 1) * cw] = v
        prod = jnp.dot(v.astype(BF16), kct_buf[c * cw:(c + 1) * cw, :], preferred_element_type=F32)
        if c < n_chunk - 1:
            acc[...] = prod if c == 0 else acc[...] + prod
        else:
            w = (acc[...] + prod) * u_out[mine]
    v_push = remote(v_all.at[1 - core], v_out.at[mine], fin_sem.at[2], fin_sem.at[3], partner)
    v_push.start()
    tot = w[:, 0:128]
    for n in range(1, rows // 128):
        tot = tot + w[:, n * 128:(n + 1) * 128]
    cost_part[mine] = tot
    cost_all[me] = jnp.sum(cost_part[...].T, axis=0, keepdims=True)
    cost_copies = []
    for dr in range(2):
        for dc in range(4):
            if dr or dc:
                n = dr * 4 + dc
                d = remote(cost_all.at[me], cost_all.at[me], cs_send.at[n], cs_recv.at[n], dev((row + dr) % 2, (col + dc) % 4))
                d.start()
                cost_copies.append((n, (row + dr) % 2, (col + 4 - dc) % 4, d))
    v_out[mine] = v_all[core]
    remote(u_out.at[other], u_out.at[other], fin_sem.at[0], fin_sem.at[1], partner).wait_recv()
    u_push.wait_send()
    u_store = pltpu.make_async_copy(u_out, u_hbm, out_sem.at[0])
    u_store.start()
    remote(v_all.at[core], v_out.at[other], fin_sem.at[2], fin_sem.at[3], partner).wait_recv()
    v_push.wait_send()
    v_store = pltpu.make_async_copy(v_out, v_hbm, out_sem.at[1])
    v_store.start()
    for n, fr, fc, d in cost_copies:
        f = fr * 4 + fc
        remote(cost_all.at[f], cost_all.at[f], cs_send.at[n], cs_recv.at[n], dev(fr, fc)).wait_recv()
    total = cost_all[0]
    for n in range(1, 8):
        total = total + cost_all[n]
    cost_ref[...] = total[:, :cost_ref.shape[1]] * norm
    for n, fr, fc, d in cost_copies:
        d.wait_send()
    u_store.wait()
    v_store.wait()


def solution(mesh):
    n_chunk = 4

    def local_fn(kernel, cost_mat, src_mass, tgt_mass):
        rows, half = kernel.shape
        nprob = src_mass.shape[1]
        nq = nprob // 2
        cols = 2 * half
        rw, cw = rows // n_chunk, cols // n_chunk
        norm = 1.0 / float(rows * mesh.shape["row"] * half * mesh.shape["col"])
        any_spec = pl.BlockSpec(memory_space=pl.ANY)
        dma = pltpu.SemaphoreType.DMA
        u_t, v_t, cost = pl.pallas_call(
            lambda *refs: sinkhorn_kernel(n_chunk, norm, *refs),
            out_shape=(jax.ShapeDtypeStruct((nprob, rows), F32), jax.ShapeDtypeStruct((nprob, half), F32),
                       jax.ShapeDtypeStruct((1, nprob), F32)),
            in_specs=[any_spec] * 4,
            out_specs=(any_spec, any_spec, pl.BlockSpec(memory_space=pltpu.VMEM)),
            scratch_shapes=[
                pltpu.VMEM((2, rows, half), BF16),
                pltpu.VMEM((cols, rows), BF16),
                pltpu.VMEM((rows, half), BF16),
                pltpu.VMEM((cols, rows), BF16),
                pltpu.VMEM((nprob, rows), F32),
                pltpu.VMEM((2, nq, half), F32),
                pltpu.VMEM((nprob, rows), BF16),
                pltpu.VMEM((nq, max(rows, cols)), F32),
                pltpu.VMEM((n_chunk, nq, rw), F32),
                pltpu.VMEM((2, n_chunk, nq, rw), F32),
                pltpu.VMEM((n_chunk, nq, cw), F32),
                pltpu.VMEM((2, n_chunk, nq, cw), F32),
                pltpu.VMEM((2, n_chunk // 2, nq, cw), F32),
                pltpu.VMEM((4, rows // 128, 128), F32),
                pltpu.VMEM((nprob, rows), F32),
                pltpu.VMEM((2, nq, half), F32),
                pltpu.VMEM((nprob, half), F32),
                pltpu.VMEM((128, 128), F32),
                pltpu.VMEM((8, 1, 128), F32),
                dma((n_chunk,)), dma((n_chunk,)), dma((n_chunk,)), dma((n_chunk,)), dma((2,)), dma((2,)), dma((4,)), dma((4,)),
                dma((n_chunk,)), dma((2, n_chunk)), dma((n_chunk,)), dma((2, n_chunk)), dma((4,)), dma((8,)), dma((8,)), dma((2,)),
                dma((n_chunk,)), dma((n_chunk,)), dma((2, n_chunk // 2)), dma((n_chunk // 2,)), dma((n_chunk // 2,)),
            ],
            compiler_params=pltpu.CompilerParams(collective_id=0, has_side_effects=True, vmem_limit_bytes=60 * 1024 * 1024),
            name="sinkhorn",
        )(kernel, cost_mat, src_mass.T, tgt_mass.T)
        return u_t.T, v_t.T, cost.reshape(nprob)

    return jax.shard_map(local_fn, mesh=mesh, in_specs=(P("row", "col"), P("row", "col"), P("row", "prob"), P("col", "prob")), out_specs=(P("row", "prob"), P("col", "prob"), P("prob")), check_vma=False)
```

```python
import jax
import jax.numpy as jnp
from jax import lax
from jax.experimental import pallas as pl
from jax.experimental.pallas import tpu as pltpu
from jax.sharding import PartitionSpec as P

SWEEPS = 6
F32 = jnp.float32
BF16 = jnp.bfloat16
MESH = pl.DeviceIdType.MESH


def sinkhorn_kernel(n_chunk, k_hbm, c_hbm, a_hbm, b_hbm, u_out, v_out, cost_all,
                    k_buf, kt_buf, c_buf, kct_buf, a_buf, b_buf, ub_buf, acc,
                    s_out, s_in, t_out, t_in, t0_buf, s0_buf, v_all, cost_part,
                    k_sem, kp_send, kp_recv, c_sem, ab_sem, bp_sem, s0_send, s0_recv,
                    s_send, s_recv, t_send, t_recv, fin_sem, cs_send, cs_recv,
                    kc_send, kc_recv, t0_send_sem, t0p_send, t0p_recv):
    rows, half = k_hbm.shape
    cols = 2 * half
    rw = rows // n_chunk
    cw = cols // n_chunk
    per_half = n_chunk // 2
    nq = b_buf.shape[1]
    row = lax.axis_index("row")
    col = lax.axis_index("col")
    prob = lax.axis_index("prob")
    x = col // 2
    core = col % 2
    grp = (core + x + row) % 2
    me = row * 4 + col
    mine = pl.ds(pl.multiple_of(grp * nq, nq), nq)
    other = pl.ds(pl.multiple_of((1 - grp) * nq, nq), nq)

    def dev(r, c):
        return (prob, r, c)

    partner = dev(row, 2 * x + 1 - core)
    x_peer = dev(row, 2 * (1 - x) + 1 - core)
    y_peer = dev(1 - row, 2 * x + 1 - core)

    def remote(src, dst, send, recv, to):
        return pltpu.make_async_remote_copy(src_ref=src, dst_ref=dst, send_sem=send, recv_sem=recv,
                                            device_id=to, device_id_type=MESH)

    def krows(i):
        return pl.ds(i * rw, rw)

    k_load = [pltpu.make_async_copy(k_hbm.at[krows(i)], k_buf.at[core, krows(i)], k_sem.at[i]) for i in range(n_chunk)]
    c_load = [pltpu.make_async_copy(c_hbm.at[krows(i)], c_buf.at[krows(i)], c_sem.at[i]) for i in range(n_chunk)]
    a_load = pltpu.make_async_copy(a_hbm, a_buf, ab_sem.at[0])
    b_load = pltpu.make_async_copy(b_hbm.at[mine], b_buf.at[core], ab_sem.at[1])
    for d in k_load:
        d.start()
    a_load.start()
    b_load.start()

    barrier = pltpu.get_barrier_semaphore()
    for dr in range(2):
        for dc in range(4):
            if dr or dc:
                pl.semaphore_signal(barrier, inc=1, device_id=dev((row + dr) % 2, (col + dc) % 4), device_id_type=MESH)

    blk = 256

    def transpose_rows(h, i):
        def body(n, carry):
            jo = pl.multiple_of(n * blk, blk)
            for ii in range(rw // blk):
                kt_buf[pl.ds(pl.multiple_of(h * half + jo, blk), blk), pl.ds(i * rw + ii * blk, blk)] = (
                    k_buf[h, pl.ds(i * rw + ii * blk, blk), pl.ds(jo, blk)].T)
            return carry
        lax.fori_loop(0, half // blk, body, 0)

    def kct_copy(i):
        part = kct_buf.at[pl.ds(pl.multiple_of(core * half, half), half), pl.ds(pl.multiple_of(i * rw, rw), rw)]
        return remote(part, part, kc_send.at[i], kc_recv.at[i], partner)

    def build_kct(i):
        pltpu.make_async_copy(c_hbm.at[pl.ds(i * rw, rw)], c_buf.at[pl.ds(i * rw, rw)], c_sem.at[i]).wait()
        def body(n, carry):
            jo = pl.multiple_of(n * blk, blk)
            for ii in range(rw // blk):
                rs = pl.ds(pl.multiple_of(i * rw + ii * blk, blk), blk)
                kct_buf[pl.ds(pl.multiple_of(core * half + jo, blk), blk), rs] = (
                    k_buf[core, rs, pl.ds(jo, blk)] * c_buf[rs, pl.ds(jo, blk)]).T
            return carry
        lax.fori_loop(0, half // blk, body, 0)
        kct_copy(i).start()

    k_push = [remote(k_buf.at[core, krows(i)], k_buf.at[core, krows(i)], kp_send.at[i], kp_recv.at[i], partner) for i in range(n_chunk)]
    b_push = remote(b_hbm.at[other], b_buf.at[core], bp_sem.at[0], bp_sem.at[1], partner)
    pl.semaphore_wait(barrier, 7)
    b_push.start()
    ones = jnp.ones((nq, half), BF16)
    for i in range(n_chunk):
        k_load[i].wait()
        if i == 0:
            k_push[0].start()
        part = lax.dot_general(ones, k_buf[core, krows(i)], (((1,), (1,)), ((), ())), preferred_element_type=F32)
        for n in range(rw // 128):
            r = i * (rw // 128) + n
            s0_buf[col, r:r + 1, :] = part[0:1, n * 128:(n + 1) * 128]
    s0_copies = []
    for n in range(1, 4):
        d = remote(s0_buf.at[col], s0_buf.at[col], s0_send.at[n], s0_recv.at[n], dev(row, (col + n) % 4))
        d.start()
        s0_copies.append(d)
    for i in range(1, n_chunk - 1):
        k_push[i].start()
    for d in c_load:
        d.start()
    for i in range(n_chunk):
        transpose_rows(core, i)
    a_load.wait()
    b_load.wait()
    for n in range(1, 4):
        frm = (col + 4 - n) % 4
        remote(s0_buf.at[frm], s0_buf.at[frm], s0_send.at[n], s0_recv.at[n], dev(row, frm)).wait_recv()
    s0 = (s0_buf[0] + s0_buf[1]) + (s0_buf[2] + s0_buf[3])
    for r in range(rows // 128):
        cs = slice(r * 128, (r + 1) * 128)
        ub_buf[:, cs] = (a_buf[:, cs] / s0[r:r + 1, :]).astype(BF16)

    def t_copy(par, o):
        return remote(t_out.at[o], t_in.at[par, o], t_send.at[o], t_recv.at[par, o], y_peer)

    def s_copy(par, o):
        return remote(s_out.at[o], s_in.at[par, o], s_send.at[o], s_recv.at[par, o], x_peer)

    t0_copies = []

    def t0_send(g, n):
        d = remote(t0_buf.at[g, n], t_in.at[0, core * per_half + n], t0_send_sem.at[g, n], t_recv.at[0, core * per_half + n],
                   dev(1 - row, 2 * x + (g + x + 1 - row) % 2))
        d.start()
        t0_copies.append(d)

    for n in range(per_half):
        part = jnp.dot(ub_buf[...], k_buf[core, :, n * cw:(n + 1) * cw], preferred_element_type=F32)
        for g in range(2):
            t0_buf[g, n] = part[g * nq:(g + 1) * nq]
        t0_send(0, n)
    for n in range(per_half):
        t0_send(1, n)
    for n in range(per_half):
        o = core * per_half + n
        d = remote(t0_buf.at[1 - grp, n], t_out.at[o], t0p_send.at[n], t0p_recv.at[n], partner)
        d.start()
        t0_copies.append(d)
        t_out[o] = t0_buf[grp, n]
    k_push[n_chunk - 1].start()

    def v_of(par, o):
        return b_buf[o // per_half, :, (o % per_half) * cw:(o % per_half + 1) * cw] / (t_out[o] + t_in[par, o])

    def first_v(h, n):
        o = h * per_half + n
        remote(t0_buf.at[0, n], t_in.at[0, o], t0_send_sem.at[0, n], t_recv.at[0, o], y_peer).wait_recv()
        return (b_buf[h, :, n * cw:(n + 1) * cw] / (t_out[o] + t_in[0, o])).astype(BF16)

    remote(b_hbm.at[other], b_buf.at[1 - core], bp_sem.at[0], bp_sem.at[1], partner).wait_recv()
    for i in range(n_chunk):
        remote(k_buf.at[1 - core, krows(i)], k_buf.at[1 - core, krows(i)], kp_send.at[i], kp_recv.at[i], partner).wait_recv()
        transpose_rows(1 - core, i)

    @pl.when(grp == 1)
    def _():
        for i in range(n_chunk):
            build_kct(i)

    for m in range(n_chunk):
        h = core if m < per_half else 1 - core
        n = m % per_half
        if m >= per_half:
            remote(t0_buf.at[0, n], t_out.at[h * per_half + n], t0p_send.at[n], t0p_recv.at[n], partner).wait_recv()
        vb = first_v(h, n)
        js = pl.ds(pl.multiple_of(h * half + n * cw, cw), cw)
        if m < n_chunk - 1:
            prod = jnp.dot(vb, kt_buf[js, :], preferred_element_type=F32)
            acc[...] = prod if m == 0 else acc[...] + prod
        else:
            for o in range(n_chunk):
                s_out[o] = acc[:, o * rw:(o + 1) * rw] + jnp.dot(vb, kt_buf[js, o * rw:(o + 1) * rw], preferred_element_type=F32)
                s_copy(1, o).start()
    for d in t0_copies:
        d.wait_send()

    def u_and_t(par):
        for c in range(n_chunk):
            s_copy(par, c).wait()
            w = slice(c * rw, (c + 1) * rw)
            u = a_buf[mine, w] / (s_out[c] + s_in[par, c])
            u_out[mine, w] = u
            ub = u.astype(BF16)
            if c < n_chunk - 1:
                for h in range(2):
                    hc = slice(h * half, (h + 1) * half)
                    prod = jnp.dot(ub, k_buf[h, w, :], preferred_element_type=F32)
                    acc[:, hc] = prod if c == 0 else acc[:, hc] + prod
            else:
                for o in range(n_chunk):
                    oc = slice(o * cw, (o + 1) * cw)
                    hc = slice((o % per_half) * cw, (o % per_half + 1) * cw)
                    t_out[o] = acc[:, oc] + jnp.dot(ub, k_buf[o // per_half, w, hc], preferred_element_type=F32)
                    t_copy(par, o).start()

    def v_and_s(par_in, par):
        for c in range(n_chunk):
            t_copy(par_in, c).wait()
            vb = v_of(par_in, c).astype(BF16)
            w = slice(c * cw, (c + 1) * cw)
            if c < n_chunk - 1:
                prod = jnp.dot(vb, kt_buf[w, :], preferred_element_type=F32)
                acc[...] = prod if c == 0 else acc[...] + prod
            else:
                for o in range(n_chunk):
                    oc = slice(o * rw, (o + 1) * rw)
                    s_out[o] = acc[:, oc] + jnp.dot(vb, kt_buf[w, oc], preferred_element_type=F32)
                    s_copy(par, o).start()

    def sweep(t, carry):
        u_and_t(t % 2)

        @pl.when(grp == 0)
        def _():
            build_kct(t - 1)

        v_and_s(t % 2, (t + 1) % 2)
        return carry

    lax.fori_loop(1, SWEEPS - 1, sweep, 0)
    last = (SWEEPS - 1) % 2
    u_and_t(last)

    u_push = remote(u_out.at[mine], u_out.at[mine], fin_sem.at[0], fin_sem.at[1], partner)
    u_push.start()
    cost_part[...] = jnp.zeros_like(cost_part)
    for d in s0_copies + k_push:
        d.wait_send()
    b_push.wait_send()
    for i in range(n_chunk):
        other_part = kct_buf.at[pl.ds(pl.multiple_of((1 - core) * half, half), half), krows(i)]
        remote(other_part, other_part, kc_send.at[i], kc_recv.at[i], partner).wait_recv()
        kct_copy(i).wait_send()
    for c in range(n_chunk):
        t_copy(last, c).wait()
        v = v_of(last, c)
        v_all[c // per_half, :, (c % per_half) * cw:(c % per_half + 1) * cw] = v
        prod = jnp.dot(v.astype(BF16), kct_buf[c * cw:(c + 1) * cw, :], preferred_element_type=F32)
        if c < n_chunk - 1:
            acc[...] = prod if c == 0 else acc[...] + prod
        else:
            w = (acc[...] + prod) * u_out[mine]
    v_push = remote(v_all.at[1 - core], v_out.at[mine], fin_sem.at[2], fin_sem.at[3], partner)
    v_push.start()
    tot = w[:, 0:128]
    for n in range(1, rows // 128):
        tot = tot + w[:, n * 128:(n + 1) * 128]
    cost_part[mine] = tot
    cost_all[me] = jnp.sum(cost_part[...].T, axis=0, keepdims=True)
    cost_copies = []
    for dr in range(2):
        for dc in range(4):
            if dr or dc:
                n = dr * 4 + dc
                d = remote(cost_all.at[me], cost_all.at[me], cs_send.at[n], cs_recv.at[n], dev((row + dr) % 2, (col + dc) % 4))
                d.start()
                cost_copies.append((n, (row + dr) % 2, (col + 4 - dc) % 4, d))
    v_out[mine] = v_all[core]
    remote(u_out.at[other], u_out.at[other], fin_sem.at[0], fin_sem.at[1], partner).wait_recv()
    u_push.wait_send()
    remote(v_all.at[core], v_out.at[other], fin_sem.at[2], fin_sem.at[3], partner).wait_recv()
    v_push.wait_send()
    for n, fr, fc, d in cost_copies:
        f = fr * 4 + fc
        remote(cost_all.at[f], cost_all.at[f], cs_send.at[n], cs_recv.at[n], dev(fr, fc)).wait_recv()
    for n, fr, fc, d in cost_copies:
        d.wait_send()


def output_kernel(norm, u_ref, v_ref, c_ref, u_hbm, v_hbm, cost_ref, sem):
    stores = [pltpu.make_async_copy(u_ref, u_hbm, sem.at[0]), pltpu.make_async_copy(v_ref, v_hbm, sem.at[1])]
    for d in stores:
        d.start()
    total = c_ref[0]
    for n in range(1, 8):
        total = total + c_ref[n]
    cost_ref[...] = total[:, :cost_ref.shape[1]] * norm
    for d in stores:
        d.wait()


def solution(mesh):
    n_chunk = 4

    def local_fn(kernel, cost_mat, src_mass, tgt_mass):
        rows, half = kernel.shape
        nprob = src_mass.shape[1]
        nq = nprob // 2
        cols = 2 * half
        rw, cw = rows // n_chunk, cols // n_chunk
        norm = 1.0 / float(rows * mesh.shape["row"] * half * mesh.shape["col"])
        vmem_spec = pl.BlockSpec(memory_space=pltpu.VMEM)
        any_spec = pl.BlockSpec(memory_space=pl.ANY)
        dma = pltpu.SemaphoreType.DMA
        u_vm, v_vm, c_vm = pl.pallas_call(
            lambda *refs: sinkhorn_kernel(n_chunk, *refs),
            out_shape=(pltpu.VMEM((nprob, rows), F32), pltpu.VMEM((nprob, half), F32), pltpu.VMEM((8, 1, 128), F32)),
            in_specs=[any_spec] * 4,
            out_specs=(vmem_spec, vmem_spec, vmem_spec),
            scratch_shapes=[
                pltpu.VMEM((2, rows, half), BF16),
                pltpu.VMEM((cols, rows), BF16),
                pltpu.VMEM((rows, half), BF16),
                pltpu.VMEM((cols, rows), BF16),
                pltpu.VMEM((nprob, rows), F32),
                pltpu.VMEM((2, nq, half), F32),
                pltpu.VMEM((nprob, rows), BF16),
                pltpu.VMEM((nq, max(rows, cols)), F32),
                pltpu.VMEM((n_chunk, nq, rw), F32),
                pltpu.VMEM((2, n_chunk, nq, rw), F32),
                pltpu.VMEM((n_chunk, nq, cw), F32),
                pltpu.VMEM((2, n_chunk, nq, cw), F32),
                pltpu.VMEM((2, n_chunk // 2, nq, cw), F32),
                pltpu.VMEM((4, rows // 128, 128), F32),
                pltpu.VMEM((2, nq, half), F32),
                pltpu.VMEM((128, 128), F32),
                dma((n_chunk,)), dma((n_chunk,)), dma((n_chunk,)), dma((n_chunk,)), dma((2,)), dma((2,)), dma((4,)), dma((4,)),
                dma((n_chunk,)), dma((2, n_chunk)), dma((n_chunk,)), dma((2, n_chunk)), dma((4,)), dma((8,)), dma((8,)),
                dma((n_chunk,)), dma((n_chunk,)), dma((2, n_chunk // 2)), dma((n_chunk // 2,)), dma((n_chunk // 2,)),
            ],
            compiler_params=pltpu.CompilerParams(collective_id=0, has_side_effects=True, vmem_limit_bytes=60 * 1024 * 1024),
            name="sinkhorn",
        )(kernel, cost_mat, src_mass.T, tgt_mass.T)
        u_t, v_t, cost = pl.pallas_call(
            lambda *refs: output_kernel(norm, *refs),
            out_shape=(jax.ShapeDtypeStruct((nprob, rows), F32), jax.ShapeDtypeStruct((nprob, half), F32),
                       jax.ShapeDtypeStruct((1, nprob), F32)),
            in_specs=[vmem_spec] * 3,
            out_specs=(any_spec, any_spec, vmem_spec),
            scratch_shapes=[dma((2,))],
            name="outputs",
        )(*(pltpu.with_memory_space_constraint(r, pltpu.VMEM) for r in (u_vm, v_vm, c_vm)))
        return u_t.T, v_t.T, cost.reshape(nprob)

    return jax.shard_map(local_fn, mesh=mesh, in_specs=(P("row", "col"), P("row", "col"), P("row", "prob"), P("col", "prob")), out_specs=(P("row", "prob"), P("col", "prob"), P("prob")), check_vma=False)
```

```python
import jax
import jax.numpy as jnp
from jax import lax
from jax.experimental import pallas as pl
from jax.experimental.pallas import tpu as pltpu
from jax.sharding import PartitionSpec as P

SWEEPS = 6
F32 = jnp.float32
BF16 = jnp.bfloat16
MESH = pl.DeviceIdType.MESH


def sinkhorn_kernel(n_chunk, k_hbm, c_hbm, a_hbm, b_hbm, u_out, v_out, cost_all,
                    k_buf, kt_buf, c_buf, kct_buf, a_buf, b_buf, ub_buf, acc,
                    s_out, s_in, t_out, t_in, t0_buf, s0_buf, v_all, cost_part,
                    load_sem, send_sem, kp_recv, s_recv, t_recv, one_recv):
    rows, half = k_hbm.shape
    cols = 2 * half
    rw = rows // n_chunk
    cw = cols // n_chunk
    per_half = n_chunk // 2
    nq = b_buf.shape[1]
    row = lax.axis_index("row")
    col = lax.axis_index("col")
    prob = lax.axis_index("prob")
    x = col // 2
    core = col % 2
    grp = (core + x + row) % 2
    me = row * 4 + col
    mine = pl.ds(pl.multiple_of(grp * nq, nq), nq)
    other = pl.ds(pl.multiple_of((1 - grp) * nq, nq), nq)

    def dev(r, c):
        return (prob, r, c)

    partner = dev(row, 2 * x + 1 - core)
    x_peer = dev(row, 2 * (1 - x) + 1 - core)
    y_peer = dev(1 - row, 2 * x + 1 - core)

    def remote(src, dst, send, recv, to):
        return pltpu.make_async_remote_copy(src_ref=src, dst_ref=dst, send_sem=send, recv_sem=recv,
                                            device_id=to, device_id_type=MESH)

    KP, BP, S0, SS, TT, T0, TP, KC, US, VS, CS = range(11)

    def all_sent(ref, kind):
        remote(ref, ref, send_sem.at[kind], one_recv.at[0], partner).wait_send()

    def all_here(ref, recv):
        remote(ref, ref, send_sem.at[0], recv, partner).wait_recv()

    def krows(i):
        return pl.ds(i * rw, rw)

    k_load = [pltpu.make_async_copy(k_hbm.at[krows(i)], k_buf.at[core, krows(i)], load_sem.at[i]) for i in range(n_chunk)]
    c_load = [pltpu.make_async_copy(c_hbm.at[krows(i)], c_buf.at[krows(i)], load_sem.at[i]) for i in range(n_chunk)]
    a_load = pltpu.make_async_copy(a_hbm, a_buf, load_sem.at[n_chunk])
    b_load = pltpu.make_async_copy(b_hbm.at[mine], b_buf.at[core], load_sem.at[n_chunk + 1])
    for d in k_load:
        d.start()
    a_load.start()
    b_load.start()

    barrier = pltpu.get_barrier_semaphore()
    for dr in range(2):
        for dc in range(4):
            if dr or dc:
                pl.semaphore_signal(barrier, inc=1, device_id=dev((row + dr) % 2, (col + dc) % 4), device_id_type=MESH)

    blk = 256

    def transpose_rows(h, i):
        def body(n, carry):
            jo = pl.multiple_of(n * blk, blk)
            for ii in range(rw // blk):
                kt_buf[pl.ds(pl.multiple_of(h * half + jo, blk), blk), pl.ds(i * rw + ii * blk, blk)] = (
                    k_buf[h, pl.ds(i * rw + ii * blk, blk), pl.ds(jo, blk)].T)
            return carry
        lax.fori_loop(0, half // blk, body, 0)

    def kct_copy(i):
        part = kct_buf.at[pl.ds(pl.multiple_of(core * half, half), half), pl.ds(pl.multiple_of(i * rw, rw), rw)]
        return remote(part, part, send_sem.at[KC], one_recv.at[5], partner)

    def build_kct(i):
        pltpu.make_async_copy(c_hbm.at[pl.ds(i * rw, rw)], c_buf.at[pl.ds(i * rw, rw)], load_sem.at[i]).wait()
        def body(n, carry):
            jo = pl.multiple_of(n * blk, blk)
            for ii in range(rw // blk):
                rs = pl.ds(pl.multiple_of(i * rw + ii * blk, blk), blk)
                kct_buf[pl.ds(pl.multiple_of(core * half + jo, blk), blk), rs] = (
                    k_buf[core, rs, pl.ds(jo, blk)] * c_buf[rs, pl.ds(jo, blk)]).T
            return carry
        lax.fori_loop(0, half // blk, body, 0)
        kct_copy(i).start()

    k_push = [remote(k_buf.at[core, krows(i)], k_buf.at[core, krows(i)], send_sem.at[KP], kp_recv.at[i], partner) for i in range(n_chunk)]
    b_push = remote(b_hbm.at[other], b_buf.at[core], send_sem.at[BP], one_recv.at[0], partner)
    pl.semaphore_wait(barrier, 7)
    b_push.start()
    ones = jnp.ones((nq, half), BF16)
    for i in range(n_chunk):
        k_load[i].wait()
        if i == 0:
            k_push[0].start()
        if i % 2:
            part = lax.dot_general(ones, k_buf[core, pl.ds((i - 1) * rw, 2 * rw)], (((1,), (1,)), ((), ())), preferred_element_type=F32)
            for n in range(2 * rw // 128):
                r = (i - 1) * (rw // 128) + n
                s0_buf[col, r:r + 1, :] = part[0:1, n * 128:(n + 1) * 128]
    for n in range(1, 4):
        remote(s0_buf.at[col], s0_buf.at[col], send_sem.at[S0], one_recv.at[1], dev(row, (col + n) % 4)).start()
    for i in range(1, n_chunk):
        k_push[i].start()
    for d in c_load:
        d.start()
    for i in range(n_chunk):
        transpose_rows(core, i)
    a_load.wait()
    b_load.wait()
    all_here(s0_buf.at[0:3], one_recv.at[1])
    s0 = (s0_buf[0] + s0_buf[1]) + (s0_buf[2] + s0_buf[3])
    for r in range(rows // 128):
        cs = slice(r * 128, (r + 1) * 128)
        ub_buf[:, cs] = (a_buf[:, cs] / s0[r:r + 1, :]).astype(BF16)

    def t_copy(par, o):
        return remote(t_out.at[o], t_in.at[par, o], send_sem.at[TT], t_recv.at[par, o], y_peer)

    def s_copy(par, o):
        return remote(s_out.at[o], s_in.at[par, o], send_sem.at[SS], s_recv.at[par, o], x_peer)

    def t0_send(g, n):
        remote(t0_buf.at[g, n], t_in.at[0, core * per_half + n], send_sem.at[T0], t_recv.at[0, core * per_half + n],
               dev(1 - row, 2 * x + (g + x + 1 - row) % 2)).start()

    for n in range(per_half):
        part = jnp.dot(ub_buf[...], k_buf[core, :, n * cw:(n + 1) * cw], preferred_element_type=F32)
        for g in range(2):
            t0_buf[g, n] = part[g * nq:(g + 1) * nq]
        t0_send(0, n)
    for n in range(per_half):
        t0_send(1, n)
    for n in range(per_half):
        o = core * per_half + n
        remote(t0_buf.at[1 - grp, n], t_out.at[o], send_sem.at[TP], one_recv.at[2], partner).start()
        t_out[o] = t0_buf[grp, n]

    def v_of(par, o):
        return b_buf[o // per_half, :, (o % per_half) * cw:(o % per_half + 1) * cw] / (t_out[o] + t_in[par, o])

    all_here(b_buf.at[0], one_recv.at[0])
    for i in range(n_chunk):
        all_here(k_buf.at[1 - core, krows(i)], kp_recv.at[i])
        transpose_rows(1 - core, i)

    @pl.when(grp == 1)
    def _():
        for i in range(n_chunk):
            build_kct(i)

    all_here(t0_buf.at[0], one_recv.at[2])
    order = list(range(per_half, n_chunk)) + list(range(per_half))
    for c in order:
        all_here(t_in.at[0, c], t_recv.at[0, c])
        vb = v_of(0, c).astype(BF16)
        js = slice(c * cw, (c + 1) * cw)
        if c != order[-1]:
            prod = jnp.dot(vb, kt_buf[js, :], preferred_element_type=F32)
            acc[...] = prod if c == order[0] else acc[...] + prod
        else:
            for o in range(n_chunk):
                s_out[o] = acc[:, o * rw:(o + 1) * rw] + jnp.dot(vb, kt_buf[js, o * rw:(o + 1) * rw], preferred_element_type=F32)
                s_copy(1, o).start()
    all_sent(t0_buf, T0)
    all_sent(t0_buf.at[0], TP)
    all_sent(s0_buf.at[0:3], S0)
    all_sent(k_buf.at[0], KP)
    all_sent(b_buf.at[0], BP)

    @pl.when(grp == 0)
    def _():
        for i in range(n_chunk - 1):
            build_kct(i)

    def u_and_t(par):
        for c in range(n_chunk):
            all_here(s_in.at[par, c], s_recv.at[par, c])
            w = slice(c * rw, (c + 1) * rw)
            u = a_buf[mine, w] / (s_out[c] + s_in[par, c])
            u_out[mine, w] = u
            ub = u.astype(BF16)
            if c < n_chunk - 1:
                for h in range(2):
                    hc = slice(h * half, (h + 1) * half)
                    prod = jnp.dot(ub, k_buf[h, w, :], preferred_element_type=F32)
                    acc[:, hc] = prod if c == 0 else acc[:, hc] + prod
            else:
                all_sent(s_out, SS)
                for o in range(n_chunk):
                    oc = slice(o * cw, (o + 1) * cw)
                    hc = slice((o % per_half) * cw, (o % per_half + 1) * cw)
                    t_out[o] = acc[:, oc] + jnp.dot(ub, k_buf[o // per_half, w, hc], preferred_element_type=F32)
                    t_copy(par, o).start()

    def v_and_s(par_in, par):
        for c in range(n_chunk):
            all_here(t_in.at[par_in, c], t_recv.at[par_in, c])
            vb = v_of(par_in, c).astype(BF16)
            w = slice(c * cw, (c + 1) * cw)
            if c < n_chunk - 1:
                prod = jnp.dot(vb, kt_buf[w, :], preferred_element_type=F32)
                acc[...] = prod if c == 0 else acc[...] + prod
            else:
                all_sent(t_out, TT)
                for o in range(n_chunk):
                    oc = slice(o * rw, (o + 1) * rw)
                    s_out[o] = acc[:, oc] + jnp.dot(vb, kt_buf[w, oc], preferred_element_type=F32)
                    s_copy(par, o).start()

    def sweep(t, carry):
        u_and_t(t % 2)

        @pl.when((grp == 0) & (t == 1))
        def _():
            build_kct(n_chunk - 1)

        v_and_s(t % 2, (t + 1) % 2)
        return carry

    lax.fori_loop(1, SWEEPS - 1, sweep, 0)
    last = (SWEEPS - 1) % 2
    u_and_t(last)

    u_push = remote(u_out.at[mine], u_out.at[mine], send_sem.at[US], one_recv.at[3], partner)
    u_push.start()
    cost_part[...] = jnp.zeros_like(cost_part)
    all_here(kct_buf.at[0:half], one_recv.at[5])
    all_sent(kct_buf.at[0:half], KC)
    for c in range(n_chunk):
        all_here(t_in.at[last, c], t_recv.at[last, c])
        v = v_of(last, c)
        v_all[c // per_half, :, (c % per_half) * cw:(c % per_half + 1) * cw] = v
        prod = jnp.dot(v.astype(BF16), kct_buf[c * cw:(c + 1) * cw, :], preferred_element_type=F32)
        if c < n_chunk - 1:
            acc[...] = prod if c == 0 else acc[...] + prod
        else:
            w = (acc[...] + prod) * u_out[mine]
    v_push = remote(v_all.at[1 - core], v_out.at[mine], send_sem.at[VS], one_recv.at[4], partner)
    v_push.start()
    tot = w[:, 0:128]
    for n in range(1, rows // 128):
        tot = tot + w[:, n * 128:(n + 1) * 128]
    cost_part[mine] = tot
    cost_all[me] = jnp.sum(cost_part[...].T, axis=0, keepdims=True)
    for dr in range(2):
        for dc in range(4):
            if dr or dc:
                remote(cost_all.at[me], cost_all.at[me], send_sem.at[CS], one_recv.at[6], dev((row + dr) % 2, (col + dc) % 4)).start()
    v_out[mine] = v_all[core]
    all_sent(t_out, TT)
    all_here(u_out.at[other], one_recv.at[3])
    u_push.wait_send()
    all_here(v_out.at[other], one_recv.at[4])
    v_push.wait_send()
    all_here(cost_all.at[0:7], one_recv.at[6])
    all_sent(cost_all.at[0:7], CS)


def output_kernel(norm, u_ref, v_ref, c_ref, u_hbm, v_hbm, cost_ref, sem):
    stores = [pltpu.make_async_copy(u_ref, u_hbm, sem.at[0]), pltpu.make_async_copy(v_ref, v_hbm, sem.at[1])]
    for d in stores:
        d.start()
    total = c_ref[0]
    for n in range(1, 8):
        total = total + c_ref[n]
    cost_ref[...] = total[:, :cost_ref.shape[1]] * norm
    for d in stores:
        d.wait()


def solution(mesh):
    n_chunk = 4

    def local_fn(kernel, cost_mat, src_mass, tgt_mass):
        rows, half = kernel.shape
        nprob = src_mass.shape[1]
        nq = nprob // 2
        cols = 2 * half
        rw, cw = rows // n_chunk, cols // n_chunk
        norm = 1.0 / float(rows * mesh.shape["row"] * half * mesh.shape["col"])
        vmem_spec = pl.BlockSpec(memory_space=pltpu.VMEM)
        any_spec = pl.BlockSpec(memory_space=pl.ANY)
        dma = pltpu.SemaphoreType.DMA
        u_vm, v_vm, c_vm = pl.pallas_call(
            lambda *refs: sinkhorn_kernel(n_chunk, *refs),
            out_shape=(pltpu.VMEM((nprob, rows), F32), pltpu.VMEM((nprob, half), F32), pltpu.VMEM((8, 1, 128), F32)),
            in_specs=[any_spec] * 4,
            out_specs=(vmem_spec, vmem_spec, vmem_spec),
            scratch_shapes=[
                pltpu.VMEM((2, rows, half), BF16),
                pltpu.VMEM((cols, rows), BF16),
                pltpu.VMEM((rows, half), BF16),
                pltpu.VMEM((cols, rows), BF16),
                pltpu.VMEM((nprob, rows), F32),
                pltpu.VMEM((2, nq, half), F32),
                pltpu.VMEM((nprob, rows), BF16),
                pltpu.VMEM((nq, max(rows, cols)), F32),
                pltpu.VMEM((n_chunk, nq, rw), F32),
                pltpu.VMEM((2, n_chunk, nq, rw), F32),
                pltpu.VMEM((n_chunk, nq, cw), F32),
                pltpu.VMEM((2, n_chunk, nq, cw), F32),
                pltpu.VMEM((2, n_chunk // 2, nq, cw), F32),
                pltpu.VMEM((4, rows // 128, 128), F32),
                pltpu.VMEM((2, nq, half), F32),
                pltpu.VMEM((128, 128), F32),
                dma((n_chunk + 2,)), dma((11,)), dma((n_chunk,)), dma((2, n_chunk)), dma((2, n_chunk)), dma((7,)),
            ],
            compiler_params=pltpu.CompilerParams(collective_id=0, has_side_effects=True, vmem_limit_bytes=60 * 1024 * 1024),
            name="sinkhorn",
        )(kernel, cost_mat, src_mass.T, tgt_mass.T)
        u_t, v_t, cost = pl.pallas_call(
            lambda *refs: output_kernel(norm, *refs),
            out_shape=(jax.ShapeDtypeStruct((nprob, rows), F32), jax.ShapeDtypeStruct((nprob, half), F32),
                       jax.ShapeDtypeStruct((1, nprob), F32)),
            in_specs=[vmem_spec] * 3,
            out_specs=(any_spec, any_spec, vmem_spec),
            scratch_shapes=[dma((2,))],
            name="outputs",
        )(*(pltpu.with_memory_space_constraint(r, pltpu.VMEM) for r in (u_vm, v_vm, c_vm)))
        return u_t.T, v_t.T, cost.reshape(nprob)

    return jax.shard_map(local_fn, mesh=mesh, in_specs=(P("row", "col"), P("row", "col"), P("row", "prob"), P("col", "prob")), out_specs=(P("row", "prob"), P("col", "prob"), P("prob")), check_vma=False)
```

```python
import jax
import jax.numpy as jnp
from jax import lax
from jax.experimental import pallas as pl
from jax.experimental.pallas import tpu as pltpu
from jax.sharding import PartitionSpec as P

SWEEPS = 6
F32 = jnp.float32
BF16 = jnp.bfloat16
MESH = pl.DeviceIdType.MESH


def sinkhorn_kernel(n_chunk, k_hbm, c_hbm, a_hbm, b_hbm, u_out, v_out, cost_all,
                    k_buf, kt_buf, c_buf, kct_buf, a_buf, b_buf, ub_buf, acc,
                    s_out, s_in, t_out, t_in, t0_buf, s0_buf, v_all, cost_part,
                    load_sem, send_sem, kp_recv, s_recv, t_recv, one_recv):
    rows, half = k_hbm.shape
    cols = 2 * half
    rw = rows // n_chunk
    cw = cols // n_chunk
    per_half = n_chunk // 2
    nq = b_buf.shape[1]
    row = lax.axis_index("row")
    col = lax.axis_index("col")
    prob = lax.axis_index("prob")
    x = col // 2
    core = col % 2
    grp = (core + x + row) % 2
    me = row * 4 + col
    mine = pl.ds(pl.multiple_of(grp * nq, nq), nq)
    other = pl.ds(pl.multiple_of((1 - grp) * nq, nq), nq)

    def dev(r, c):
        return (prob, r, c)

    partner = dev(row, 2 * x + 1 - core)
    x_peer = dev(row, 2 * (1 - x) + 1 - core)
    y_peer = dev(1 - row, 2 * x + 1 - core)

    def remote(src, dst, send, recv, to):
        return pltpu.make_async_remote_copy(src_ref=src, dst_ref=dst, send_sem=send, recv_sem=recv,
                                            device_id=to, device_id_type=MESH)

    KP, BP, S0, SS, TT, T0, TP, KC, US, VS, CS = range(11)

    def all_sent(ref, kind):
        remote(ref, ref, send_sem.at[kind], one_recv.at[0], partner).wait_send()

    def all_here(ref, recv):
        remote(ref, ref, send_sem.at[0], recv, partner).wait_recv()

    def krows(i):
        return pl.ds(i * rw, rw)

    k_load = [pltpu.make_async_copy(k_hbm.at[krows(i)], k_buf.at[core, krows(i)], load_sem.at[i]) for i in range(n_chunk)]
    c_load = [pltpu.make_async_copy(c_hbm.at[krows(i)], c_buf.at[krows(i)], load_sem.at[i]) for i in range(n_chunk)]
    a_load = pltpu.make_async_copy(a_hbm, a_buf, load_sem.at[n_chunk])
    b_load = pltpu.make_async_copy(b_hbm.at[mine], b_buf.at[core], load_sem.at[n_chunk + 1])
    for d in k_load:
        d.start()
    a_load.start()
    b_load.start()

    barrier = pltpu.get_barrier_semaphore()
    for dr in range(2):
        for dc in range(4):
            if dr or dc:
                pl.semaphore_signal(barrier, inc=1, device_id=dev((row + dr) % 2, (col + dc) % 4), device_id_type=MESH)

    blk = 256

    def transpose_rows(h, i):
        def body(n, carry):
            jo = pl.multiple_of(n * blk, blk)
            for ii in range(rw // blk):
                kt_buf[pl.ds(pl.multiple_of(h * half + jo, blk), blk), pl.ds(i * rw + ii * blk, blk)] = (
                    k_buf[h, pl.ds(i * rw + ii * blk, blk), pl.ds(jo, blk)].T)
            return carry
        lax.fori_loop(0, half // blk, body, 0)

    def kct_copy(i):
        part = kct_buf.at[pl.ds(pl.multiple_of(core * half, half), half), pl.ds(pl.multiple_of(i * rw, rw), rw)]
        return remote(part, part, send_sem.at[KC], one_recv.at[5], partner)

    def build_kct(i):
        pltpu.make_async_copy(c_hbm.at[pl.ds(i * rw, rw)], c_buf.at[pl.ds(i * rw, rw)], load_sem.at[i]).wait()
        def body(n, carry):
            jo = pl.multiple_of(n * blk, blk)
            for ii in range(rw // blk):
                rs = pl.ds(pl.multiple_of(i * rw + ii * blk, blk), blk)
                kct_buf[pl.ds(pl.multiple_of(core * half + jo, blk), blk), rs] = (
                    k_buf[core, rs, pl.ds(jo, blk)] * c_buf[rs, pl.ds(jo, blk)]).T
            return carry
        lax.fori_loop(0, half // blk, body, 0)
        kct_copy(i).start()

    k_push = [remote(k_buf.at[core, krows(i)], k_buf.at[core, krows(i)], send_sem.at[KP], kp_recv.at[i], partner) for i in range(n_chunk)]
    b_push = remote(b_hbm.at[other], b_buf.at[core], send_sem.at[BP], one_recv.at[0], partner)
    ones = jnp.ones((nq, half), BF16)
    for i in range(n_chunk):
        k_load[i].wait()
        if i % 2:
            part = lax.dot_general(ones, k_buf[core, pl.ds((i - 1) * rw, 2 * rw)], (((1,), (1,)), ((), ())), preferred_element_type=F32)
            for n in range(2 * rw // 128):
                r = (i - 1) * (rw // 128) + n
                s0_buf[col, r:r + 1, :] = part[0:1, n * 128:(n + 1) * 128]
    pl.semaphore_wait(barrier, 7)
    for n in range(1, 4):
        remote(s0_buf.at[col], s0_buf.at[col], send_sem.at[S0], one_recv.at[1], dev(row, (col + n) % 4)).start()
    b_push.start()
    for d in k_push:
        d.start()
    for d in c_load:
        d.start()
    for i in range(n_chunk):
        transpose_rows(core, i)
    a_load.wait()
    b_load.wait()
    all_here(s0_buf.at[0:3], one_recv.at[1])
    s0 = (s0_buf[0] + s0_buf[1]) + (s0_buf[2] + s0_buf[3])
    for r in range(rows // 128):
        cs = slice(r * 128, (r + 1) * 128)
        ub_buf[:, cs] = (a_buf[:, cs] / s0[r:r + 1, :]).astype(BF16)

    def t_copy(par, o):
        return remote(t_out.at[o], t_in.at[par, o], send_sem.at[TT], t_recv.at[par, o], y_peer)

    def s_copy(par, o):
        return remote(s_out.at[o], s_in.at[par, o], send_sem.at[SS], s_recv.at[par, o], x_peer)

    def t0_send(g, n):
        remote(t0_buf.at[g, n], t_in.at[0, core * per_half + n], send_sem.at[T0], t_recv.at[0, core * per_half + n],
               dev(1 - row, 2 * x + (g + x + 1 - row) % 2)).start()

    for n in range(per_half):
        part = jnp.dot(ub_buf[...], k_buf[core, :, n * cw:(n + 1) * cw], preferred_element_type=F32)
        for g in range(2):
            t0_buf[g, n] = part[g * nq:(g + 1) * nq]
        t0_send(0, n)
    for n in range(per_half):
        t0_send(1, n)
    for n in range(per_half):
        o = core * per_half + n
        remote(t0_buf.at[1 - grp, n], t_out.at[o], send_sem.at[TP], one_recv.at[2], partner).start()
        t_out[o] = t0_buf[grp, n]

    def v_of(par, o):
        return b_buf[o // per_half, :, (o % per_half) * cw:(o % per_half + 1) * cw] / (t_out[o] + t_in[par, o])

    all_here(b_buf.at[0], one_recv.at[0])
    for i in range(n_chunk):
        all_here(k_buf.at[1 - core, krows(i)], kp_recv.at[i])
        transpose_rows(1 - core, i)

    @pl.when(grp == 1)
    def _():
        for i in range(per_half):
            build_kct(i)

    all_here(t0_buf.at[0], one_recv.at[2])
    order = list(range(per_half, n_chunk)) + list(range(per_half))
    for c in order:
        all_here(t_in.at[0, c], t_recv.at[0, c])
        vb = v_of(0, c).astype(BF16)
        js = slice(c * cw, (c + 1) * cw)
        if c != order[-1]:
            prod = jnp.dot(vb, kt_buf[js, :], preferred_element_type=F32)
            acc[...] = prod if c == order[0] else acc[...] + prod
        else:
            for o in range(n_chunk):
                s_out[o] = acc[:, o * rw:(o + 1) * rw] + jnp.dot(vb, kt_buf[js, o * rw:(o + 1) * rw], preferred_element_type=F32)
                s_copy(1, o).start()
    all_sent(t0_buf, T0)
    all_sent(t0_buf.at[0], TP)
    all_sent(s0_buf.at[0:3], S0)
    all_sent(k_buf.at[0], KP)
    all_sent(b_buf.at[0], BP)

    for i in range(per_half):
        build_kct(i + grp * per_half)

    def u_and_t(par):
        for c in range(n_chunk):
            all_here(s_in.at[par, c], s_recv.at[par, c])
            w = slice(c * rw, (c + 1) * rw)
            u = a_buf[mine, w] / (s_out[c] + s_in[par, c])
            u_out[mine, w] = u
            ub = u.astype(BF16)
            if c < n_chunk - 1:
                for h in range(2):
                    hc = slice(h * half, (h + 1) * half)
                    prod = jnp.dot(ub, k_buf[h, w, :], preferred_element_type=F32)
                    acc[:, hc] = prod if c == 0 else acc[:, hc] + prod
            else:
                all_sent(s_out, SS)
                for o in range(n_chunk):
                    oc = slice(o * cw, (o + 1) * cw)
                    hc = slice((o % per_half) * cw, (o % per_half + 1) * cw)
                    t_out[o] = acc[:, oc] + jnp.dot(ub, k_buf[o // per_half, w, hc], preferred_element_type=F32)
                    t_copy(par, o).start()

    def v_and_s(par_in, par):
        for c in range(n_chunk):
            all_here(t_in.at[par_in, c], t_recv.at[par_in, c])
            vb = v_of(par_in, c).astype(BF16)
            w = slice(c * cw, (c + 1) * cw)
            if c < n_chunk - 1:
                prod = jnp.dot(vb, kt_buf[w, :], preferred_element_type=F32)
                acc[...] = prod if c == 0 else acc[...] + prod
            else:
                all_sent(t_out, TT)
                for o in range(n_chunk):
                    oc = slice(o * rw, (o + 1) * rw)
                    s_out[o] = acc[:, oc] + jnp.dot(vb, kt_buf[w, oc], preferred_element_type=F32)
                    s_copy(par, o).start()

    def sweep(t, carry):
        u_and_t(t % 2)

        @pl.when((grp == 0) & (t == 1))
        def _():
            for i in range(per_half, n_chunk):
                build_kct(i)

        v_and_s(t % 2, (t + 1) % 2)
        return carry

    lax.fori_loop(1, SWEEPS - 1, sweep, 0)
    last = (SWEEPS - 1) % 2
    u_and_t(last)

    u_push = remote(u_out.at[mine], u_out.at[mine], send_sem.at[US], one_recv.at[3], partner)
    u_push.start()
    cost_part[...] = jnp.zeros_like(cost_part)
    all_here(kct_buf.at[0:half], one_recv.at[5])
    all_sent(kct_buf.at[0:half], KC)
    for c in range(n_chunk):
        all_here(t_in.at[last, c], t_recv.at[last, c])
        v = v_of(last, c)
        v_all[c // per_half, :, (c % per_half) * cw:(c % per_half + 1) * cw] = v
        prod = jnp.dot(v.astype(BF16), kct_buf[c * cw:(c + 1) * cw, :], preferred_element_type=F32)
        if c < n_chunk - 1:
            acc[...] = prod if c == 0 else acc[...] + prod
        else:
            w = (acc[...] + prod) * u_out[mine]
    v_push = remote(v_all.at[1 - core], v_out.at[mine], send_sem.at[VS], one_recv.at[4], partner)
    v_push.start()
    tot = w[:, 0:128]
    for n in range(1, rows // 128):
        tot = tot + w[:, n * 128:(n + 1) * 128]
    cost_part[mine] = tot
    cost_all[me] = jnp.sum(cost_part[...].T, axis=0, keepdims=True)
    for dr in range(2):
        for dc in range(4):
            if dr or dc:
                remote(cost_all.at[me], cost_all.at[me], send_sem.at[CS], one_recv.at[6], dev((row + dr) % 2, (col + dc) % 4)).start()
    v_out[mine] = v_all[core]
    all_sent(t_out, TT)
    all_here(u_out.at[other], one_recv.at[3])
    u_push.wait_send()
    all_here(v_out.at[other], one_recv.at[4])
    v_push.wait_send()
    all_here(cost_all.at[0:7], one_recv.at[6])
    all_sent(cost_all.at[0:7], CS)


def output_kernel(norm, u_ref, v_ref, c_ref, u_hbm, v_hbm, cost_ref, sem):
    stores = [pltpu.make_async_copy(u_ref, u_hbm, sem.at[0]), pltpu.make_async_copy(v_ref, v_hbm, sem.at[1])]
    for d in stores:
        d.start()
    total = c_ref[0]
    for n in range(1, 8):
        total = total + c_ref[n]
    cost_ref[...] = total[:, :cost_ref.shape[1]] * norm
    for d in stores:
        d.wait()


def solution(mesh):
    n_chunk = 4

    def local_fn(kernel, cost_mat, src_mass, tgt_mass):
        rows, half = kernel.shape
        nprob = src_mass.shape[1]
        nq = nprob // 2
        cols = 2 * half
        rw, cw = rows // n_chunk, cols // n_chunk
        norm = 1.0 / float(rows * mesh.shape["row"] * half * mesh.shape["col"])
        vmem_spec = pl.BlockSpec(memory_space=pltpu.VMEM)
        any_spec = pl.BlockSpec(memory_space=pl.ANY)
        dma = pltpu.SemaphoreType.DMA
        u_vm, v_vm, c_vm = pl.pallas_call(
            lambda *refs: sinkhorn_kernel(n_chunk, *refs),
            out_shape=(pltpu.VMEM((nprob, rows), F32), pltpu.VMEM((nprob, half), F32), pltpu.VMEM((8, 1, 128), F32)),
            in_specs=[any_spec] * 4,
            out_specs=(vmem_spec, vmem_spec, vmem_spec),
            scratch_shapes=[
                pltpu.VMEM((2, rows, half), BF16),
                pltpu.VMEM((cols, rows), BF16),
                pltpu.VMEM((rows, half), BF16),
                pltpu.VMEM((cols, rows), BF16),
                pltpu.VMEM((nprob, rows), F32),
                pltpu.VMEM((2, nq, half), F32),
                pltpu.VMEM((nprob, rows), BF16),
                pltpu.VMEM((nq, max(rows, cols)), F32),
                pltpu.VMEM((n_chunk, nq, rw), F32),
                pltpu.VMEM((2, n_chunk, nq, rw), F32),
                pltpu.VMEM((n_chunk, nq, cw), F32),
                pltpu.VMEM((2, n_chunk, nq, cw), F32),
                pltpu.VMEM((2, n_chunk // 2, nq, cw), F32),
                pltpu.VMEM((4, rows // 128, 128), F32),
                pltpu.VMEM((2, nq, half), F32),
                pltpu.VMEM((128, 128), F32),
                dma((n_chunk + 2,)), dma((11,)), dma((n_chunk,)), dma((2, n_chunk)), dma((2, n_chunk)), dma((7,)),
            ],
            compiler_params=pltpu.CompilerParams(collective_id=0, has_side_effects=True, vmem_limit_bytes=60 * 1024 * 1024),
            name="sinkhorn",
        )(kernel, cost_mat, src_mass.T, tgt_mass.T)
        u_t, v_t, cost = pl.pallas_call(
            lambda *refs: output_kernel(norm, *refs),
            out_shape=(jax.ShapeDtypeStruct((nprob, rows), F32), jax.ShapeDtypeStruct((nprob, half), F32),
                       jax.ShapeDtypeStruct((1, nprob), F32)),
            in_specs=[vmem_spec] * 3,
            out_specs=(any_spec, any_spec, vmem_spec),
            scratch_shapes=[dma((2,))],
            name="outputs",
        )(*(pltpu.with_memory_space_constraint(r, pltpu.VMEM) for r in (u_vm, v_vm, c_vm)))
        return u_t.T, v_t.T, cost.reshape(nprob)

    return jax.shard_map(local_fn, mesh=mesh, in_specs=(P("row", "col"), P("row", "col"), P("row", "prob"), P("col", "prob")), out_specs=(P("row", "prob"), P("col", "prob"), P("prob")), check_vma=False)
```

```python
import jax
import jax.numpy as jnp
from jax import lax
from jax.experimental import pallas as pl
from jax.experimental.pallas import tpu as pltpu
from jax.sharding import PartitionSpec as P

SWEEPS = 6
F32 = jnp.float32
BF16 = jnp.bfloat16
MESH = pl.DeviceIdType.MESH


def sinkhorn_kernel(n_chunk, k_hbm, c_hbm, a_hbm, b_hbm, u_out, v_out, cost_all,
                    k_buf, kt_buf, c_buf, kct_buf, a_buf, b_buf, ub_buf, acc,
                    s_out, s_in, t_out, t_in, t0_buf, s0_buf, v_all, cost_part,
                    load_sem, send_sem, kp_recv, s_recv, t_recv, one_recv):
    rows, half = k_hbm.shape
    cols = 2 * half
    rw = rows // n_chunk
    cw = cols // n_chunk
    per_half = n_chunk // 2
    nq = b_buf.shape[1]
    row = lax.axis_index("row")
    col = lax.axis_index("col")
    prob = lax.axis_index("prob")
    x = col // 2
    core = col % 2
    grp = (core + x + row) % 2
    me = row * 4 + col
    mine = pl.ds(pl.multiple_of(grp * nq, nq), nq)
    other = pl.ds(pl.multiple_of((1 - grp) * nq, nq), nq)

    def dev(r, c):
        return (prob, r, c)

    partner = dev(row, 2 * x + 1 - core)
    x_peer = dev(row, 2 * (1 - x) + 1 - core)
    y_peer = dev(1 - row, 2 * x + 1 - core)

    def remote(src, dst, send, recv, to):
        return pltpu.make_async_remote_copy(src_ref=src, dst_ref=dst, send_sem=send, recv_sem=recv,
                                            device_id=to, device_id_type=MESH)

    KP, BP, S0, SS, TT, T0, TP, KC, US, VS, CS = range(11)

    def all_sent(ref, kind):
        remote(ref, ref, send_sem.at[kind], one_recv.at[0], partner).wait_send()

    def all_here(ref, recv):
        remote(ref, ref, send_sem.at[0], recv, partner).wait_recv()

    def krows(i):
        return pl.ds(i * rw, rw)

    k_load = [pltpu.make_async_copy(k_hbm.at[krows(i)], k_buf.at[core, krows(i)], load_sem.at[i]) for i in range(n_chunk)]
    c_load = [pltpu.make_async_copy(c_hbm.at[krows(i)], c_buf.at[krows(i)], load_sem.at[i]) for i in range(n_chunk)]
    a_load = pltpu.make_async_copy(a_hbm, a_buf, load_sem.at[n_chunk])
    b_load = pltpu.make_async_copy(b_hbm.at[mine], b_buf.at[core], load_sem.at[n_chunk + 1])
    for d in k_load:
        d.start()
    a_load.start()
    b_load.start()

    barrier = pltpu.get_barrier_semaphore()
    for dr in range(2):
        for dc in range(4):
            if dr or dc:
                pl.semaphore_signal(barrier, inc=1, device_id=dev((row + dr) % 2, (col + dc) % 4), device_id_type=MESH)

    blk = 256

    def transpose_rows(h, i):
        def body(n, carry):
            jo = pl.multiple_of(n * blk, blk)
            for ii in range(rw // blk):
                kt_buf[pl.ds(pl.multiple_of(h * half + jo, blk), blk), pl.ds(i * rw + ii * blk, blk)] = (
                    k_buf[h, pl.ds(i * rw + ii * blk, blk), pl.ds(jo, blk)].T)
            return carry
        lax.fori_loop(0, half // blk, body, 0)

    def kct_copy(i):
        part = kct_buf.at[pl.ds(pl.multiple_of(core * half, half), half), pl.ds(pl.multiple_of(i * rw, rw), rw)]
        return remote(part, part, send_sem.at[KC], one_recv.at[5], partner)

    def build_kct(i):
        pltpu.make_async_copy(c_hbm.at[pl.ds(i * rw, rw)], c_buf.at[pl.ds(i * rw, rw)], load_sem.at[i]).wait()
        def body(n, carry):
            jo = pl.multiple_of(n * blk, blk)
            for ii in range(rw // blk):
                rs = pl.ds(pl.multiple_of(i * rw + ii * blk, blk), blk)
                kct_buf[pl.ds(pl.multiple_of(core * half + jo, blk), blk), rs] = (
                    k_buf[core, rs, pl.ds(jo, blk)] * c_buf[rs, pl.ds(jo, blk)]).T
            return carry
        lax.fori_loop(0, half // blk, body, 0)
        kct_copy(i).start()

    k_push = [remote(k_buf.at[core, krows(i)], k_buf.at[core, krows(i)], send_sem.at[KP], kp_recv.at[i], partner) for i in range(n_chunk)]
    b_push = remote(b_hbm.at[other], b_buf.at[core], send_sem.at[BP], one_recv.at[0], partner)
    pl.semaphore_wait(barrier, 7)
    b_push.start()
    ones = jnp.ones((nq, half), BF16)
    for i in range(n_chunk):
        k_load[i].wait()
        if i == 0:
            k_push[0].start()
        if i % 2:
            part = lax.dot_general(ones, k_buf[core, pl.ds((i - 1) * rw, 2 * rw)], (((1,), (1,)), ((), ())), preferred_element_type=F32)
            for n in range(2 * rw // 128):
                r = (i - 1) * (rw // 128) + n
                s0_buf[col, r:r + 1, :] = part[0:1, n * 128:(n + 1) * 128]
    for n in range(1, 4):
        remote(s0_buf.at[col], s0_buf.at[col], send_sem.at[S0], one_recv.at[1], dev(row, (col + n) % 4)).start()
    for i in range(1, n_chunk):
        k_push[i].start()
    for d in c_load:
        d.start()
    for i in range(n_chunk):
        transpose_rows(core, i)
    a_load.wait()
    b_load.wait()
    all_here(s0_buf.at[0:3], one_recv.at[1])
    s0 = (s0_buf[0] + s0_buf[1]) + (s0_buf[2] + s0_buf[3])
    for r in range(rows // 128):
        cs = slice(r * 128, (r + 1) * 128)
        ub_buf[:, cs] = (a_buf[:, cs] / s0[r:r + 1, :]).astype(BF16)

    def t_copy(par, o):
        return remote(t_out.at[o], t_in.at[par, o], send_sem.at[TT], t_recv.at[par, o], y_peer)

    def s_copy(par, o):
        return remote(s_out.at[o], s_in.at[par, o], send_sem.at[SS], s_recv.at[par, o], x_peer)

    def t0_send(g, n):
        remote(t0_buf.at[g, n], t_in.at[0, core * per_half + n], send_sem.at[T0], t_recv.at[0, core * per_half + n],
               dev(1 - row, 2 * x + (g + x + 1 - row) % 2)).start()

    for n in range(per_half):
        part = jnp.dot(ub_buf[...], k_buf[core, :, n * cw:(n + 1) * cw], preferred_element_type=F32)
        for g in range(2):
            t0_buf[g, n] = part[g * nq:(g + 1) * nq]
        t0_send(0, n)
    for n in range(per_half):
        t0_send(1, n)
    for n in range(per_half):
        o = core * per_half + n
        remote(t0_buf.at[1 - grp, n], t_out.at[o], send_sem.at[TP], one_recv.at[2], partner).start()
        t_out[o] = t0_buf[grp, n]

    def v_of(par, o):
        return b_buf[o // per_half, :, (o % per_half) * cw:(o % per_half + 1) * cw] / (t_out[o] + t_in[par, o])

    all_here(b_buf.at[0], one_recv.at[0])
    for i in range(n_chunk):
        all_here(k_buf.at[1 - core, krows(i)], kp_recv.at[i])
        transpose_rows(1 - core, i)

    @pl.when(grp == 1)
    def _():
        for i in range(n_chunk - 1):
            build_kct(i)

    all_here(t0_buf.at[0], one_recv.at[2])
    order = list(range(per_half, n_chunk)) + list(range(per_half))
    for c in order:
        all_here(t_in.at[0, c], t_recv.at[0, c])
        vb = v_of(0, c).astype(BF16)
        js = slice(c * cw, (c + 1) * cw)
        if c != order[-1]:
            prod = jnp.dot(vb, kt_buf[js, :], preferred_element_type=F32)
            acc[...] = prod if c == order[0] else acc[...] + prod
        else:
            for o in range(n_chunk):
                s_out[o] = acc[:, o * rw:(o + 1) * rw] + jnp.dot(vb, kt_buf[js, o * rw:(o + 1) * rw], preferred_element_type=F32)
                s_copy(1, o).start()
    all_sent(t0_buf, T0)
    all_sent(t0_buf.at[0], TP)
    all_sent(s0_buf.at[0:3], S0)
    all_sent(k_buf.at[0], KP)
    all_sent(b_buf.at[0], BP)

    @pl.when(grp == 0)
    def _():
        for i in range(per_half):
            build_kct(i)

    @pl.when(grp == 1)
    def _():
        build_kct(n_chunk - 1)

    def u_and_t(par):
        for c in range(n_chunk):
            all_here(s_in.at[par, c], s_recv.at[par, c])
            w = slice(c * rw, (c + 1) * rw)
            u = a_buf[mine, w] / (s_out[c] + s_in[par, c])
            u_out[mine, w] = u
            ub = u.astype(BF16)
            if c < n_chunk - 1:
                for h in range(2):
                    hc = slice(h * half, (h + 1) * half)
                    prod = jnp.dot(ub, k_buf[h, w, :], preferred_element_type=F32)
                    acc[:, hc] = prod if c == 0 else acc[:, hc] + prod
            else:
                all_sent(s_out, SS)
                for o in range(n_chunk):
                    oc = slice(o * cw, (o + 1) * cw)
                    hc = slice((o % per_half) * cw, (o % per_half + 1) * cw)
                    t_out[o] = acc[:, oc] + jnp.dot(ub, k_buf[o // per_half, w, hc], preferred_element_type=F32)
                    t_copy(par, o).start()

    def v_and_s(par_in, par):
        for c in range(n_chunk):
            all_here(t_in.at[par_in, c], t_recv.at[par_in, c])
            vb = v_of(par_in, c).astype(BF16)
            w = slice(c * cw, (c + 1) * cw)
            if c < n_chunk - 1:
                prod = jnp.dot(vb, kt_buf[w, :], preferred_element_type=F32)
                acc[...] = prod if c == 0 else acc[...] + prod
            else:
                all_sent(t_out, TT)
                for o in range(n_chunk):
                    oc = slice(o * rw, (o + 1) * rw)
                    s_out[o] = acc[:, oc] + jnp.dot(vb, kt_buf[w, oc], preferred_element_type=F32)
                    s_copy(par, o).start()

    def sweep(t, carry):
        u_and_t(t % 2)

        @pl.when((grp == 0) & (t == 1))
        def _():
            for i in range(per_half, n_chunk):
                build_kct(i)

        v_and_s(t % 2, (t + 1) % 2)
        return carry

    lax.fori_loop(1, SWEEPS - 1, sweep, 0)
    last = (SWEEPS - 1) % 2
    u_and_t(last)

    u_push = remote(u_out.at[mine], u_out.at[mine], send_sem.at[US], one_recv.at[3], partner)
    u_push.start()
    cost_part[...] = jnp.zeros_like(cost_part)
    all_here(kct_buf.at[0:half], one_recv.at[5])
    all_sent(kct_buf.at[0:half], KC)
    for c in range(n_chunk):
        all_here(t_in.at[last, c], t_recv.at[last, c])
        v = v_of(last, c)
        v_all[c // per_half, :, (c % per_half) * cw:(c % per_half + 1) * cw] = v
        prod = jnp.dot(v.astype(BF16), kct_buf[c * cw:(c + 1) * cw, :], preferred_element_type=F32)
        if c < n_chunk - 1:
            acc[...] = prod if c == 0 else acc[...] + prod
        else:
            w = (acc[...] + prod) * u_out[mine]
    v_push = remote(v_all.at[1 - core], v_out.at[mine], send_sem.at[VS], one_recv.at[4], partner)
    v_push.start()
    tot = w[:, 0:128]
    for n in range(1, rows // 128):
        tot = tot + w[:, n * 128:(n + 1) * 128]
    cost_part[mine] = tot
    cost_all[me] = jnp.sum(cost_part[...].T, axis=0, keepdims=True)
    for dr in range(2):
        for dc in range(4):
            if dr or dc:
                remote(cost_all.at[me], cost_all.at[me], send_sem.at[CS], one_recv.at[6], dev((row + dr) % 2, (col + dc) % 4)).start()
    v_out[mine] = v_all[core]
    all_sent(t_out, TT)
    all_here(u_out.at[other], one_recv.at[3])
    u_push.wait_send()
    all_here(v_out.at[other], one_recv.at[4])
    v_push.wait_send()
    all_here(cost_all.at[0:7], one_recv.at[6])
    all_sent(cost_all.at[0:7], CS)


def output_kernel(norm, u_ref, v_ref, c_ref, u_hbm, v_hbm, cost_ref, sem):
    stores = [pltpu.make_async_copy(u_ref, u_hbm, sem.at[0]), pltpu.make_async_copy(v_ref, v_hbm, sem.at[1])]
    for d in stores:
        d.start()
    total = c_ref[0]
    for n in range(1, 8):
        total = total + c_ref[n]
    cost_ref[...] = total[:, :cost_ref.shape[1]] * norm
    for d in stores:
        d.wait()


def solution(mesh):
    n_chunk = 4

    def local_fn(kernel, cost_mat, src_mass, tgt_mass):
        rows, half = kernel.shape
        nprob = src_mass.shape[1]
        nq = nprob // 2
        cols = 2 * half
        rw, cw = rows // n_chunk, cols // n_chunk
        norm = 1.0 / float(rows * mesh.shape["row"] * half * mesh.shape["col"])
        vmem_spec = pl.BlockSpec(memory_space=pltpu.VMEM)
        any_spec = pl.BlockSpec(memory_space=pl.ANY)
        dma = pltpu.SemaphoreType.DMA
        u_vm, v_vm, c_vm = pl.pallas_call(
            lambda *refs: sinkhorn_kernel(n_chunk, *refs),
            out_shape=(pltpu.VMEM((nprob, rows), F32), pltpu.VMEM((nprob, half), F32), pltpu.VMEM((8, 1, 128), F32)),
            in_specs=[any_spec] * 4,
            out_specs=(vmem_spec, vmem_spec, vmem_spec),
            scratch_shapes=[
                pltpu.VMEM((2, rows, half), BF16),
                pltpu.VMEM((cols, rows), BF16),
                pltpu.VMEM((rows, half), BF16),
                pltpu.VMEM((cols, rows), BF16),
                pltpu.VMEM((nprob, rows), F32),
                pltpu.VMEM((2, nq, half), F32),
                pltpu.VMEM((nprob, rows), BF16),
                pltpu.VMEM((nq, max(rows, cols)), F32),
                pltpu.VMEM((n_chunk, nq, rw), F32),
                pltpu.VMEM((2, n_chunk, nq, rw), F32),
                pltpu.VMEM((n_chunk, nq, cw), F32),
                pltpu.VMEM((2, n_chunk, nq, cw), F32),
                pltpu.VMEM((2, n_chunk // 2, nq, cw), F32),
                pltpu.VMEM((4, rows // 128, 128), F32),
                pltpu.VMEM((2, nq, half), F32),
                pltpu.VMEM((128, 128), F32),
                dma((n_chunk + 2,)), dma((11,)), dma((n_chunk,)), dma((2, n_chunk)), dma((2, n_chunk)), dma((7,)),
            ],
            compiler_params=pltpu.CompilerParams(collective_id=0, has_side_effects=True, vmem_limit_bytes=60 * 1024 * 1024),
            name="sinkhorn",
        )(kernel, cost_mat, src_mass.T, tgt_mass.T)
        u_t, v_t, cost = pl.pallas_call(
            lambda *refs: output_kernel(norm, *refs),
            out_shape=(jax.ShapeDtypeStruct((nprob, rows), F32), jax.ShapeDtypeStruct((nprob, half), F32),
                       jax.ShapeDtypeStruct((1, nprob), F32)),
            in_specs=[vmem_spec] * 3,
            out_specs=(any_spec, any_spec, vmem_spec),
            scratch_shapes=[dma((2,))],
            name="outputs",
        )(*(pltpu.with_memory_space_constraint(r, pltpu.VMEM) for r in (u_vm, v_vm, c_vm)))
        return u_t.T, v_t.T, cost.reshape(nprob)

    return jax.shard_map(local_fn, mesh=mesh, in_specs=(P("row", "col"), P("row", "col"), P("row", "prob"), P("col", "prob")), out_specs=(P("row", "prob"), P("col", "prob"), P("prob")), check_vma=False)
```

```python
import jax
import jax.numpy as jnp
from jax import lax
from jax.experimental import pallas as pl
from jax.experimental.pallas import tpu as pltpu
from jax.sharding import PartitionSpec as P

SWEEPS = 6
F32 = jnp.float32
BF16 = jnp.bfloat16
MESH = pl.DeviceIdType.MESH


def sinkhorn_kernel(n_chunk, k_hbm, c_hbm, a_hbm, b_hbm, u_out, v_out, cost_all,
                    k_buf, kt_buf, c_buf, kct_buf, a_buf, b_buf, ub_buf, acc,
                    s_out, s_in, t_out, t_in, t0_buf, s0_buf, v_all, cost_part,
                    load_sem, send_sem, kp_recv, s_recv, t_recv, one_recv):
    rows, half = k_hbm.shape
    cols = 2 * half
    rw = rows // n_chunk
    cw = cols // n_chunk
    per_half = n_chunk // 2
    nq = b_buf.shape[1]
    row = lax.axis_index("row")
    col = lax.axis_index("col")
    prob = lax.axis_index("prob")
    x = col // 2
    core = col % 2
    grp = (core + x + row) % 2
    me = row * 4 + col
    mine = pl.ds(pl.multiple_of(grp * nq, nq), nq)
    other = pl.ds(pl.multiple_of((1 - grp) * nq, nq), nq)

    def dev(r, c):
        return (prob, r, c)

    partner = dev(row, 2 * x + 1 - core)
    x_peer = dev(row, 2 * (1 - x) + 1 - core)
    y_peer = dev(1 - row, 2 * x + 1 - core)

    def remote(src, dst, send, recv, to):
        return pltpu.make_async_remote_copy(src_ref=src, dst_ref=dst, send_sem=send, recv_sem=recv,
                                            device_id=to, device_id_type=MESH)

    KP, BP, S0, SS, TT, T0, TP, KC, US, VS, CS = range(11)

    def all_sent(ref, kind):
        remote(ref, ref, send_sem.at[kind], one_recv.at[0], partner).wait_send()

    def all_here(ref, recv):
        remote(ref, ref, send_sem.at[0], recv, partner).wait_recv()

    def krows(i):
        return pl.ds(i * rw, rw)

    k_load = [pltpu.make_async_copy(k_hbm.at[krows(i)], k_buf.at[core, krows(i)], load_sem.at[i]) for i in range(n_chunk)]
    c_load = [pltpu.make_async_copy(c_hbm.at[krows(i)], c_buf.at[krows(i)], load_sem.at[i]) for i in range(n_chunk)]
    a_load = pltpu.make_async_copy(a_hbm, a_buf, load_sem.at[n_chunk])
    b_load = pltpu.make_async_copy(b_hbm.at[mine], b_buf.at[core], load_sem.at[n_chunk + 1])
    for d in k_load:
        d.start()
    a_load.start()
    b_load.start()

    barrier = pltpu.get_barrier_semaphore()
    for dr in range(2):
        for dc in range(4):
            if dr or dc:
                pl.semaphore_signal(barrier, inc=1, device_id=dev((row + dr) % 2, (col + dc) % 4), device_id_type=MESH)

    blk = 256

    def transpose_rows(h, i):
        def body(n, carry):
            jo = pl.multiple_of(n * blk, blk)
            for ii in range(rw // blk):
                kt_buf[pl.ds(pl.multiple_of(h * half + jo, blk), blk), pl.ds(i * rw + ii * blk, blk)] = (
                    k_buf[h, pl.ds(i * rw + ii * blk, blk), pl.ds(jo, blk)].T)
            return carry
        lax.fori_loop(0, half // blk, body, 0)

    def kct_copy(i):
        part = kct_buf.at[pl.ds(pl.multiple_of(core * half, half), half), pl.ds(pl.multiple_of(i * rw, rw), rw)]
        return remote(part, part, send_sem.at[KC], one_recv.at[5], partner)

    def build_kct(i):
        pltpu.make_async_copy(c_hbm.at[pl.ds(i * rw, rw)], c_buf.at[pl.ds(i * rw, rw)], load_sem.at[i]).wait()
        def body(n, carry):
            jo = pl.multiple_of(n * blk, blk)
            for ii in range(rw // blk):
                rs = pl.ds(pl.multiple_of(i * rw + ii * blk, blk), blk)
                kct_buf[pl.ds(pl.multiple_of(core * half + jo, blk), blk), rs] = (
                    k_buf[core, rs, pl.ds(jo, blk)] * c_buf[rs, pl.ds(jo, blk)]).T
            return carry
        lax.fori_loop(0, half // blk, body, 0)
        kct_copy(i).start()

    k_push = [remote(k_buf.at[core, krows(i)], k_buf.at[core, krows(i)], send_sem.at[KP], kp_recv.at[i], partner) for i in range(n_chunk)]
    b_push = remote(b_hbm.at[other], b_buf.at[core], send_sem.at[BP], one_recv.at[0], partner)
    pl.semaphore_wait(barrier, 7)
    b_push.start()
    ones = jnp.ones((nq, half), BF16)
    for i in range(n_chunk):
        k_load[i].wait()
        if i == 0:
            k_push[0].start()
        if i % 2:
            part = lax.dot_general(ones, k_buf[core, pl.ds((i - 1) * rw, 2 * rw)], (((1,), (1,)), ((), ())), preferred_element_type=F32)
            for n in range(2 * rw // 128):
                r = (i - 1) * (rw // 128) + n
                s0_buf[col, r:r + 1, :] = part[0:1, n * 128:(n + 1) * 128]
    for n in range(1, 4):
        remote(s0_buf.at[col], s0_buf.at[col], send_sem.at[S0], one_recv.at[1], dev(row, (col + n) % 4)).start()
    for i in range(1, n_chunk):
        k_push[i].start()
    for d in c_load:
        d.start()
    for i in range(n_chunk):
        transpose_rows(core, i)
    a_load.wait()
    b_load.wait()
    all_here(s0_buf.at[0:3], one_recv.at[1])
    s0 = (s0_buf[0] + s0_buf[1]) + (s0_buf[2] + s0_buf[3])
    for r in range(rows // 128):
        cs = slice(r * 128, (r + 1) * 128)
        ub_buf[:, cs] = (a_buf[:, cs] / s0[r:r + 1, :]).astype(BF16)

    def t_copy(par, o):
        return remote(t_out.at[o], t_in.at[par, o], send_sem.at[TT], t_recv.at[par, o], y_peer)

    def s_copy(par, o):
        return remote(s_out.at[o], s_in.at[par, o], send_sem.at[SS], s_recv.at[par, o], x_peer)

    def t0_send(g, n):
        remote(t0_buf.at[g, n], t_in.at[0, core * per_half + n], send_sem.at[T0], t_recv.at[0, core * per_half + n],
               dev(1 - row, 2 * x + (g + x + 1 - row) % 2)).start()

    for n in range(per_half):
        part = jnp.dot(ub_buf[...], k_buf[core, :, n * cw:(n + 1) * cw], preferred_element_type=F32)
        for g in range(2):
            t0_buf[g, n] = part[g * nq:(g + 1) * nq]
        t0_send(0, n)
    for n in range(per_half):
        t0_send(1, n)
    for n in range(per_half):
        o = core * per_half + n
        remote(t0_buf.at[1 - grp, n], t_out.at[o], send_sem.at[TP], one_recv.at[2], partner).start()
        t_out[o] = t0_buf[grp, n]

    def v_of(par, o):
        return b_buf[o // per_half, :, (o % per_half) * cw:(o % per_half + 1) * cw] / (t_out[o] + t_in[par, o])

    all_here(b_buf.at[0], one_recv.at[0])
    for i in range(n_chunk):
        all_here(k_buf.at[1 - core, krows(i)], kp_recv.at[i])
        transpose_rows(1 - core, i)

    @pl.when(grp == 1)
    def _():
        for i in range(n_chunk - 1):
            build_kct(i)

    @pl.when((grp == 1) & (core == 0))
    def _():
        build_kct(n_chunk - 1)

    all_here(t0_buf.at[0], one_recv.at[2])
    order = list(range(per_half, n_chunk)) + list(range(per_half))
    for c in order:
        all_here(t_in.at[0, c], t_recv.at[0, c])
        vb = v_of(0, c).astype(BF16)
        js = slice(c * cw, (c + 1) * cw)
        if c != order[-1]:
            prod = jnp.dot(vb, kt_buf[js, :], preferred_element_type=F32)
            acc[...] = prod if c == order[0] else acc[...] + prod
        else:
            for o in range(n_chunk):
                s_out[o] = acc[:, o * rw:(o + 1) * rw] + jnp.dot(vb, kt_buf[js, o * rw:(o + 1) * rw], preferred_element_type=F32)
                s_copy(1, o).start()
    all_sent(t0_buf, T0)
    all_sent(t0_buf.at[0], TP)
    all_sent(s0_buf.at[0:3], S0)
    all_sent(k_buf.at[0], KP)
    all_sent(b_buf.at[0], BP)

    @pl.when(grp == 0)
    def _():
        for i in range(per_half):
            build_kct(i)

    @pl.when((grp == 1) & (core == 1))
    def _():
        build_kct(n_chunk - 1)

    def u_and_t(par):
        for c in range(n_chunk):
            all_here(s_in.at[par, c], s_recv.at[par, c])
            w = slice(c * rw, (c + 1) * rw)
            u = a_buf[mine, w] / (s_out[c] + s_in[par, c])
            u_out[mine, w] = u
            ub = u.astype(BF16)
            if c < n_chunk - 1:
                for h in range(2):
                    hc = slice(h * half, (h + 1) * half)
                    prod = jnp.dot(ub, k_buf[h, w, :], preferred_element_type=F32)
                    acc[:, hc] = prod if c == 0 else acc[:, hc] + prod
            else:
                all_sent(s_out, SS)
                for o in range(n_chunk):
                    oc = slice(o * cw, (o + 1) * cw)
                    hc = slice((o % per_half) * cw, (o % per_half + 1) * cw)
                    t_out[o] = acc[:, oc] + jnp.dot(ub, k_buf[o // per_half, w, hc], preferred_element_type=F32)
                    t_copy(par, o).start()

    def v_and_s(par_in, par):
        for c in range(n_chunk):
            all_here(t_in.at[par_in, c], t_recv.at[par_in, c])
            vb = v_of(par_in, c).astype(BF16)
            w = slice(c * cw, (c + 1) * cw)
            if c < n_chunk - 1:
                prod = jnp.dot(vb, kt_buf[w, :], preferred_element_type=F32)
                acc[...] = prod if c == 0 else acc[...] + prod
            else:
                all_sent(t_out, TT)
                for o in range(n_chunk):
                    oc = slice(o * rw, (o + 1) * rw)
                    s_out[o] = acc[:, oc] + jnp.dot(vb, kt_buf[w, oc], preferred_element_type=F32)
                    s_copy(par, o).start()

    def sweep(t, carry):
        u_and_t(t % 2)

        @pl.when((grp == 0) & (t == 1))
        def _():
            for i in range(per_half, n_chunk):
                build_kct(i)

        v_and_s(t % 2, (t + 1) % 2)
        return carry

    lax.fori_loop(1, SWEEPS - 1, sweep, 0)
    last = (SWEEPS - 1) % 2
    u_and_t(last)

    u_push = remote(u_out.at[mine], u_out.at[mine], send_sem.at[US], one_recv.at[3], partner)
    u_push.start()
    cost_part[...] = jnp.zeros_like(cost_part)
    all_here(kct_buf.at[0:half], one_recv.at[5])
    all_sent(kct_buf.at[0:half], KC)
    for c in range(n_chunk):
        all_here(t_in.at[last, c], t_recv.at[last, c])
        v = v_of(last, c)
        v_all[c // per_half, :, (c % per_half) * cw:(c % per_half + 1) * cw] = v
        prod = jnp.dot(v.astype(BF16), kct_buf[c * cw:(c + 1) * cw, :], preferred_element_type=F32)
        if c < n_chunk - 1:
            acc[...] = prod if c == 0 else acc[...] + prod
        else:
            w = (acc[...] + prod) * u_out[mine]
    v_push = remote(v_all.at[1 - core], v_out.at[mine], send_sem.at[VS], one_recv.at[4], partner)
    v_push.start()
    tot = w[:, 0:128]
    for n in range(1, rows // 128):
        tot = tot + w[:, n * 128:(n + 1) * 128]
    cost_part[mine] = tot
    cost_all[me] = jnp.sum(cost_part[...].T, axis=0, keepdims=True)
    for dr in range(2):
        for dc in range(4):
            if dr or dc:
                remote(cost_all.at[me], cost_all.at[me], send_sem.at[CS], one_recv.at[6], dev((row + dr) % 2, (col + dc) % 4)).start()
    v_out[mine] = v_all[core]
    all_sent(t_out, TT)
    all_here(u_out.at[other], one_recv.at[3])
    u_push.wait_send()
    all_here(v_out.at[other], one_recv.at[4])
    v_push.wait_send()
    all_here(cost_all.at[0:7], one_recv.at[6])
    all_sent(cost_all.at[0:7], CS)


def output_kernel(norm, u_ref, v_ref, c_ref, u_hbm, v_hbm, cost_ref, sem):
    stores = [pltpu.make_async_copy(u_ref, u_hbm, sem.at[0]), pltpu.make_async_copy(v_ref, v_hbm, sem.at[1])]
    for d in stores:
        d.start()
    total = c_ref[0]
    for n in range(1, 8):
        total = total + c_ref[n]
    cost_ref[...] = total[:, :cost_ref.shape[1]] * norm
    for d in stores:
        d.wait()


def solution(mesh):
    n_chunk = 4

    def local_fn(kernel, cost_mat, src_mass, tgt_mass):
        rows, half = kernel.shape
        nprob = src_mass.shape[1]
        nq = nprob // 2
        cols = 2 * half
        rw, cw = rows // n_chunk, cols // n_chunk
        norm = 1.0 / float(rows * mesh.shape["row"] * half * mesh.shape["col"])
        vmem_spec = pl.BlockSpec(memory_space=pltpu.VMEM)
        any_spec = pl.BlockSpec(memory_space=pl.ANY)
        dma = pltpu.SemaphoreType.DMA
        u_vm, v_vm, c_vm = pl.pallas_call(
            lambda *refs: sinkhorn_kernel(n_chunk, *refs),
            out_shape=(pltpu.VMEM((nprob, rows), F32), pltpu.VMEM((nprob, half), F32), pltpu.VMEM((8, 1, 128), F32)),
            in_specs=[any_spec] * 4,
            out_specs=(vmem_spec, vmem_spec, vmem_spec),
            scratch_shapes=[
                pltpu.VMEM((2, rows, half), BF16),
                pltpu.VMEM((cols, rows), BF16),
                pltpu.VMEM((rows, half), BF16),
                pltpu.VMEM((cols, rows), BF16),
                pltpu.VMEM((nprob, rows), F32),
                pltpu.VMEM((2, nq, half), F32),
                pltpu.VMEM((nprob, rows), BF16),
                pltpu.VMEM((nq, max(rows, cols)), F32),
                pltpu.VMEM((n_chunk, nq, rw), F32),
                pltpu.VMEM((2, n_chunk, nq, rw), F32),
                pltpu.VMEM((n_chunk, nq, cw), F32),
                pltpu.VMEM((2, n_chunk, nq, cw), F32),
                pltpu.VMEM((2, n_chunk // 2, nq, cw), F32),
                pltpu.VMEM((4, rows // 128, 128), F32),
                pltpu.VMEM((2, nq, half), F32),
                pltpu.VMEM((128, 128), F32),
                dma((n_chunk + 2,)), dma((11,)), dma((n_chunk,)), dma((2, n_chunk)), dma((2, n_chunk)), dma((7,)),
            ],
            compiler_params=pltpu.CompilerParams(collective_id=0, has_side_effects=True, vmem_limit_bytes=60 * 1024 * 1024),
            name="sinkhorn",
        )(kernel, cost_mat, src_mass.T, tgt_mass.T)
        u_t, v_t, cost = pl.pallas_call(
            lambda *refs: output_kernel(norm, *refs),
            out_shape=(jax.ShapeDtypeStruct((nprob, rows), F32), jax.ShapeDtypeStruct((nprob, half), F32),
                       jax.ShapeDtypeStruct((1, nprob), F32)),
            in_specs=[vmem_spec] * 3,
            out_specs=(any_spec, any_spec, vmem_spec),
            scratch_shapes=[dma((2,))],
            name="outputs",
        )(*(pltpu.with_memory_space_constraint(r, pltpu.VMEM) for r in (u_vm, v_vm, c_vm)))
        return u_t.T, v_t.T, cost.reshape(nprob)

    return jax.shard_map(local_fn, mesh=mesh, in_specs=(P("row", "col"), P("row", "col"), P("row", "prob"), P("col", "prob")), out_specs=(P("row", "prob"), P("col", "prob"), P("prob")), check_vma=False)
```

```python
import jax
import jax.numpy as jnp
from jax import lax
from jax.experimental import pallas as pl
from jax.experimental.pallas import tpu as pltpu
from jax.sharding import PartitionSpec as P

SWEEPS = 6
F32 = jnp.float32
BF16 = jnp.bfloat16
MESH = pl.DeviceIdType.MESH


def sinkhorn_kernel(n_chunk, k_hbm, c_hbm, a_hbm, b_hbm, u_out, v_out, cost_all,
                    k_buf, kt_buf, c_buf, kct_buf, a_buf, b_buf, ub_buf, acc,
                    s_out, s_in, t_out, t_in, t0_buf, s0_buf, v_all, cost_part,
                    load_sem, send_sem, kp_recv, s_recv, t_recv, one_recv):
    rows, half = k_hbm.shape
    cols = 2 * half
    rw = rows // n_chunk
    cw = cols // n_chunk
    per_half = n_chunk // 2
    nq = b_buf.shape[1]
    row = lax.axis_index("row")
    col = lax.axis_index("col")
    prob = lax.axis_index("prob")
    x = col // 2
    core = col % 2
    grp = (core + x + row) % 2
    me = row * 4 + col
    mine = pl.ds(pl.multiple_of(grp * nq, nq), nq)
    other = pl.ds(pl.multiple_of((1 - grp) * nq, nq), nq)

    def dev(r, c):
        return (prob, r, c)

    partner = dev(row, 2 * x + 1 - core)
    x_peer = dev(row, 2 * (1 - x) + 1 - core)
    y_peer = dev(1 - row, 2 * x + 1 - core)

    def remote(src, dst, send, recv, to):
        return pltpu.make_async_remote_copy(src_ref=src, dst_ref=dst, send_sem=send, recv_sem=recv,
                                            device_id=to, device_id_type=MESH)

    KP, BP, S0, SS, TT, T0, TP, KC, US, VS, CS = range(11)

    def all_sent(ref, kind):
        remote(ref, ref, send_sem.at[kind], one_recv.at[0], partner).wait_send()

    def all_here(ref, recv):
        remote(ref, ref, send_sem.at[0], recv, partner).wait_recv()

    def krows(i):
        return pl.ds(i * rw, rw)

    k_load = [pltpu.make_async_copy(k_hbm.at[krows(i)], k_buf.at[core, krows(i)], load_sem.at[i]) for i in range(n_chunk)]
    c_load = [pltpu.make_async_copy(c_hbm.at[krows(i)], c_buf.at[krows(i)], load_sem.at[i]) for i in range(n_chunk)]
    a_load = pltpu.make_async_copy(a_hbm, a_buf, load_sem.at[n_chunk])
    b_load = pltpu.make_async_copy(b_hbm.at[mine], b_buf.at[core], load_sem.at[n_chunk + 1])
    for d in k_load[:per_half]:
        d.start()

    barrier = pltpu.get_barrier_semaphore()
    for dr in range(2):
        for dc in range(4):
            if dr or dc:
                pl.semaphore_signal(barrier, inc=1, device_id=dev((row + dr) % 2, (col + dc) % 4), device_id_type=MESH)

    blk = 256

    def transpose_rows(h, i):
        def body(n, carry):
            jo = pl.multiple_of(n * blk, blk)
            for ii in range(rw // blk):
                kt_buf[pl.ds(pl.multiple_of(h * half + jo, blk), blk), pl.ds(i * rw + ii * blk, blk)] = (
                    k_buf[h, pl.ds(i * rw + ii * blk, blk), pl.ds(jo, blk)].T)
            return carry
        lax.fori_loop(0, half // blk, body, 0)

    def kct_copy(i):
        part = kct_buf.at[pl.ds(pl.multiple_of(core * half, half), half), pl.ds(pl.multiple_of(i * rw, rw), rw)]
        return remote(part, part, send_sem.at[KC], one_recv.at[5], partner)

    def build_kct(i):
        pltpu.make_async_copy(c_hbm.at[pl.ds(i * rw, rw)], c_buf.at[pl.ds(i * rw, rw)], load_sem.at[i]).wait()
        def body(n, carry):
            jo = pl.multiple_of(n * blk, blk)
            for ii in range(rw // blk):
                rs = pl.ds(pl.multiple_of(i * rw + ii * blk, blk), blk)
                kct_buf[pl.ds(pl.multiple_of(core * half + jo, blk), blk), rs] = (
                    k_buf[core, rs, pl.ds(jo, blk)] * c_buf[rs, pl.ds(jo, blk)]).T
            return carry
        lax.fori_loop(0, half // blk, body, 0)
        kct_copy(i).start()

    k_push = [remote(k_buf.at[core, krows(i)], k_buf.at[core, krows(i)], send_sem.at[KP], kp_recv.at[i], partner) for i in range(n_chunk)]
    b_push = remote(b_hbm.at[other], b_buf.at[core], send_sem.at[BP], one_recv.at[0], partner)
    ones = jnp.ones((nq, half), BF16)

    def first_s(i):
        part = lax.dot_general(ones, k_buf[core, pl.ds(i * rw, per_half * rw)], (((1,), (1,)), ((), ())), preferred_element_type=F32)
        for n in range(per_half * rw // 128):
            r = i * (rw // 128) + n
            s0_buf[col, r:r + 1, :] = part[0:1, n * 128:(n + 1) * 128]

    for d in k_load[:per_half]:
        d.wait()
    for d in k_load[per_half:]:
        d.start()
    a_load.start()
    b_load.start()
    first_s(0)
    pl.semaphore_wait(barrier, 7)
    b_push.start()
    for d in k_push[:per_half]:
        d.start()
    for d in k_load[per_half:]:
        d.wait()
    first_s(per_half)
    for n in range(1, 4):
        remote(s0_buf.at[col], s0_buf.at[col], send_sem.at[S0], one_recv.at[1], dev(row, (col + n) % 4)).start()
    for d in k_push[per_half:]:
        d.start()
    for d in c_load:
        d.start()
    for i in range(n_chunk):
        transpose_rows(core, i)
    a_load.wait()
    b_load.wait()
    all_here(s0_buf.at[0:3], one_recv.at[1])
    s0 = (s0_buf[0] + s0_buf[1]) + (s0_buf[2] + s0_buf[3])
    for r in range(rows // 128):
        cs = slice(r * 128, (r + 1) * 128)
        ub_buf[:, cs] = (a_buf[:, cs] / s0[r:r + 1, :]).astype(BF16)

    def t_copy(par, o):
        return remote(t_out.at[o], t_in.at[par, o], send_sem.at[TT], t_recv.at[par, o], y_peer)

    def s_copy(par, o):
        return remote(s_out.at[o], s_in.at[par, o], send_sem.at[SS], s_recv.at[par, o], x_peer)

    def t0_send(g, n):
        remote(t0_buf.at[g, n], t_in.at[0, core * per_half + n], send_sem.at[T0], t_recv.at[0, core * per_half + n],
               dev(1 - row, 2 * x + (g + x + 1 - row) % 2)).start()

    for n in range(per_half):
        part = jnp.dot(ub_buf[...], k_buf[core, :, n * cw:(n + 1) * cw], preferred_element_type=F32)
        for g in range(2):
            t0_buf[g, n] = part[g * nq:(g + 1) * nq]
        t0_send(0, n)
    for n in range(per_half):
        t0_send(1, n)
    for n in range(per_half):
        o = core * per_half + n
        remote(t0_buf.at[1 - grp, n], t_out.at[o], send_sem.at[TP], one_recv.at[2], partner).start()
        t_out[o] = t0_buf[grp, n]

    def v_of(par, o):
        return b_buf[o // per_half, :, (o % per_half) * cw:(o % per_half + 1) * cw] / (t_out[o] + t_in[par, o])

    all_here(b_buf.at[0], one_recv.at[0])
    for i in range(n_chunk):
        all_here(k_buf.at[1 - core, krows(i)], kp_recv.at[i])
        transpose_rows(1 - core, i)

    @pl.when(grp == 1)
    def _():
        for i in range(n_chunk - 1):
            build_kct(i)

    @pl.when((grp == 1) & (core == 0))
    def _():
        build_kct(n_chunk - 1)

    all_here(t0_buf.at[0], one_recv.at[2])
    order = list(range(per_half, n_chunk)) + list(range(per_half))
    for c in order:
        all_here(t_in.at[0, c], t_recv.at[0, c])
        vb = v_of(0, c).astype(BF16)
        js = slice(c * cw, (c + 1) * cw)
        if c != order[-1]:
            prod = jnp.dot(vb, kt_buf[js, :], preferred_element_type=F32)
            acc[...] = prod if c == order[0] else acc[...] + prod
        else:
            for o in range(n_chunk):
                s_out[o] = acc[:, o * rw:(o + 1) * rw] + jnp.dot(vb, kt_buf[js, o * rw:(o + 1) * rw], preferred_element_type=F32)
                s_copy(1, o).start()
    all_sent(t0_buf, T0)
    all_sent(t0_buf.at[0], TP)
    all_sent(s0_buf.at[0:3], S0)
    all_sent(k_buf.at[0], KP)
    all_sent(b_buf.at[0], BP)

    @pl.when(grp == 0)
    def _():
        for i in range(per_half):
            build_kct(i)

    @pl.when((grp == 1) & (core == 1))
    def _():
        build_kct(n_chunk - 1)

    def u_and_t(par):
        for c in range(n_chunk):
            all_here(s_in.at[par, c], s_recv.at[par, c])
            w = slice(c * rw, (c + 1) * rw)
            u = a_buf[mine, w] / (s_out[c] + s_in[par, c])
            u_out[mine, w] = u
            ub = u.astype(BF16)
            if c < n_chunk - 1:
                for h in range(2):
                    hc = slice(h * half, (h + 1) * half)
                    prod = jnp.dot(ub, k_buf[h, w, :], preferred_element_type=F32)
                    acc[:, hc] = prod if c == 0 else acc[:, hc] + prod
            else:
                all_sent(s_out, SS)
                for o in range(n_chunk):
                    oc = slice(o * cw, (o + 1) * cw)
                    hc = slice((o % per_half) * cw, (o % per_half + 1) * cw)
                    t_out[o] = acc[:, oc] + jnp.dot(ub, k_buf[o // per_half, w, hc], preferred_element_type=F32)
                    t_copy(par, o).start()

    def v_and_s(par_in, par):
        for c in range(n_chunk):
            all_here(t_in.at[par_in, c], t_recv.at[par_in, c])
            vb = v_of(par_in, c).astype(BF16)
            w = slice(c * cw, (c + 1) * cw)
            if c < n_chunk - 1:
                prod = jnp.dot(vb, kt_buf[w, :], preferred_element_type=F32)
                acc[...] = prod if c == 0 else acc[...] + prod
            else:
                all_sent(t_out, TT)
                for o in range(n_chunk):
                    oc = slice(o * rw, (o + 1) * rw)
                    s_out[o] = acc[:, oc] + jnp.dot(vb, kt_buf[w, oc], preferred_element_type=F32)
                    s_copy(par, o).start()

    def sweep(t, carry):
        u_and_t(t % 2)

        @pl.when((grp == 0) & (t == 1))
        def _():
            for i in range(per_half, n_chunk):
                build_kct(i)

        v_and_s(t % 2, (t + 1) % 2)
        return carry

    lax.fori_loop(1, SWEEPS - 1, sweep, 0)
    last = (SWEEPS - 1) % 2
    u_and_t(last)

    u_push = remote(u_out.at[mine], u_out.at[mine], send_sem.at[US], one_recv.at[3], partner)
    u_push.start()
    cost_part[...] = jnp.zeros_like(cost_part)
    all_here(kct_buf.at[0:half], one_recv.at[5])
    all_sent(kct_buf.at[0:half], KC)
    for c in range(n_chunk):
        all_here(t_in.at[last, c], t_recv.at[last, c])
        v = v_of(last, c)
        v_all[c // per_half, :, (c % per_half) * cw:(c % per_half + 1) * cw] = v
        prod = jnp.dot(v.astype(BF16), kct_buf[c * cw:(c + 1) * cw, :], preferred_element_type=F32)
        if c < n_chunk - 1:
            acc[...] = prod if c == 0 else acc[...] + prod
        else:
            w = (acc[...] + prod) * u_out[mine]
    v_push = remote(v_all.at[1 - core], v_out.at[mine], send_sem.at[VS], one_recv.at[4], partner)
    v_push.start()
    tot = w[:, 0:128]
    for n in range(1, rows // 128):
        tot = tot + w[:, n * 128:(n + 1) * 128]
    cost_part[mine] = tot
    cost_all[me] = jnp.sum(cost_part[...].T, axis=0, keepdims=True)
    for dr in range(2):
        for dc in range(4):
            if dr or dc:
                remote(cost_all.at[me], cost_all.at[me], send_sem.at[CS], one_recv.at[6], dev((row + dr) % 2, (col + dc) % 4)).start()
    v_out[mine] = v_all[core]
    all_sent(t_out, TT)
    all_here(u_out.at[other], one_recv.at[3])
    u_push.wait_send()
    all_here(v_out.at[other], one_recv.at[4])
    v_push.wait_send()
    all_here(cost_all.at[0:7], one_recv.at[6])
    all_sent(cost_all.at[0:7], CS)


def output_kernel(norm, u_ref, v_ref, c_ref, u_hbm, v_hbm, cost_ref, sem):
    stores = [pltpu.make_async_copy(u_ref, u_hbm, sem.at[0]), pltpu.make_async_copy(v_ref, v_hbm, sem.at[1])]
    for d in stores:
        d.start()
    total = c_ref[0]
    for n in range(1, 8):
        total = total + c_ref[n]
    cost_ref[...] = total[:, :cost_ref.shape[1]] * norm
    for d in stores:
        d.wait()


def solution(mesh):
    n_chunk = 4

    def local_fn(kernel, cost_mat, src_mass, tgt_mass):
        rows, half = kernel.shape
        nprob = src_mass.shape[1]
        nq = nprob // 2
        cols = 2 * half
        rw, cw = rows // n_chunk, cols // n_chunk
        norm = 1.0 / float(rows * mesh.shape["row"] * half * mesh.shape["col"])
        vmem_spec = pl.BlockSpec(memory_space=pltpu.VMEM)
        any_spec = pl.BlockSpec(memory_space=pl.ANY)
        dma = pltpu.SemaphoreType.DMA
        u_vm, v_vm, c_vm = pl.pallas_call(
            lambda *refs: sinkhorn_kernel(n_chunk, *refs),
            out_shape=(pltpu.VMEM((nprob, rows), F32), pltpu.VMEM((nprob, half), F32), pltpu.VMEM((8, 1, 128), F32)),
            in_specs=[any_spec] * 4,
            out_specs=(vmem_spec, vmem_spec, vmem_spec),
            scratch_shapes=[
                pltpu.VMEM((2, rows, half), BF16),
                pltpu.VMEM((cols, rows), BF16),
                pltpu.VMEM((rows, half), BF16),
                pltpu.VMEM((cols, rows), BF16),
                pltpu.VMEM((nprob, rows), F32),
                pltpu.VMEM((2, nq, half), F32),
                pltpu.VMEM((nprob, rows), BF16),
                pltpu.VMEM((nq, max(rows, cols)), F32),
                pltpu.VMEM((n_chunk, nq, rw), F32),
                pltpu.VMEM((2, n_chunk, nq, rw), F32),
                pltpu.VMEM((n_chunk, nq, cw), F32),
                pltpu.VMEM((2, n_chunk, nq, cw), F32),
                pltpu.VMEM((2, n_chunk // 2, nq, cw), F32),
                pltpu.VMEM((4, rows // 128, 128), F32),
                pltpu.VMEM((2, nq, half), F32),
                pltpu.VMEM((128, 128), F32),
                dma((n_chunk + 2,)), dma((11,)), dma((n_chunk,)), dma((2, n_chunk)), dma((2, n_chunk)), dma((7,)),
            ],
            compiler_params=pltpu.CompilerParams(collective_id=0, has_side_effects=True, vmem_limit_bytes=60 * 1024 * 1024),
            name="sinkhorn",
        )(kernel, cost_mat, src_mass.T, tgt_mass.T)
        u_t, v_t, cost = pl.pallas_call(
            lambda *refs: output_kernel(norm, *refs),
            out_shape=(jax.ShapeDtypeStruct((nprob, rows), F32), jax.ShapeDtypeStruct((nprob, half), F32),
                       jax.ShapeDtypeStruct((1, nprob), F32)),
            in_specs=[vmem_spec] * 3,
            out_specs=(any_spec, any_spec, vmem_spec),
            scratch_shapes=[dma((2,))],
            name="outputs",
        )(*(pltpu.with_memory_space_constraint(r, pltpu.VMEM) for r in (u_vm, v_vm, c_vm)))
        return u_t.T, v_t.T, cost.reshape(nprob)

    return jax.shard_map(local_fn, mesh=mesh, in_specs=(P("row", "col"), P("row", "col"), P("row", "prob"), P("col", "prob")), out_specs=(P("row", "prob"), P("col", "prob"), P("prob")), check_vma=False)
```

```python
import jax
import jax.numpy as jnp
from jax import lax
from jax.experimental import pallas as pl
from jax.experimental.pallas import tpu as pltpu
from jax.sharding import PartitionSpec as P

SWEEPS = 6
AHEAD = (7, 5)
F32 = jnp.float32
BF16 = jnp.bfloat16
MESH = pl.DeviceIdType.MESH


def sinkhorn_kernel(n_chunk, k_hbm, c_hbm, a_hbm, b_hbm, u_out, v_out, cost_all,
                    k_buf, kt_buf, c_buf, kct_buf, a_buf, b_buf, ub_buf, acc,
                    s_out, s_in, t_out, t_in, t0_buf, s0_buf, v_all, cost_part,
                    load_sem, send_sem, kp_recv, s_recv, t_recv, one_recv):
    rows, half = k_hbm.shape
    cols = 2 * half
    rw = rows // n_chunk
    cw = cols // n_chunk
    per_half = n_chunk // 2
    nq = b_buf.shape[1]
    row = lax.axis_index("row")
    col = lax.axis_index("col")
    prob = lax.axis_index("prob")
    x = col // 2
    core = col % 2
    grp = (core + x + row) % 2
    me = row * 4 + col
    mine = pl.ds(pl.multiple_of(grp * nq, nq), nq)
    other = pl.ds(pl.multiple_of((1 - grp) * nq, nq), nq)

    def dev(r, c):
        return (prob, r, c)

    partner = dev(row, 2 * x + 1 - core)
    x_peer = dev(row, 2 * (1 - x) + 1 - core)
    y_peer = dev(1 - row, 2 * x + 1 - core)

    def remote(src, dst, send, recv, to):
        return pltpu.make_async_remote_copy(src_ref=src, dst_ref=dst, send_sem=send, recv_sem=recv,
                                            device_id=to, device_id_type=MESH)

    KP, BP, S0, SS, TT, T0, TP, KC, US, VS, CS = range(11)

    def all_sent(ref, kind):
        remote(ref, ref, send_sem.at[kind], one_recv.at[0], partner).wait_send()

    def all_here(ref, recv):
        remote(ref, ref, send_sem.at[0], recv, partner).wait_recv()

    def krows(i):
        return pl.ds(i * rw, rw)

    k_load = [pltpu.make_async_copy(k_hbm.at[krows(i)], k_buf.at[core, krows(i)], load_sem.at[i]) for i in range(n_chunk)]
    c_load = [pltpu.make_async_copy(c_hbm.at[krows(i)], c_buf.at[krows(i)], load_sem.at[i]) for i in range(n_chunk)]
    a_load = pltpu.make_async_copy(a_hbm, a_buf, load_sem.at[n_chunk])
    b_load = pltpu.make_async_copy(b_hbm.at[mine], b_buf.at[core], load_sem.at[n_chunk + 1])
    for d in k_load:
        d.start()
    a_load.start()
    b_load.start()

    barrier = pltpu.get_barrier_semaphore()
    for dr in range(2):
        for dc in range(4):
            if dr or dc:
                pl.semaphore_signal(barrier, inc=1, device_id=dev((row + dr) % 2, (col + dc) % 4), device_id_type=MESH)

    blk = 256

    def transpose_rows(h, i):
        def body(n, carry):
            jo = pl.multiple_of(n * blk, blk)
            for ii in range(rw // blk):
                kt_buf[pl.ds(pl.multiple_of(h * half + jo, blk), blk), pl.ds(i * rw + ii * blk, blk)] = (
                    k_buf[h, pl.ds(i * rw + ii * blk, blk), pl.ds(jo, blk)].T)
            return carry
        lax.fori_loop(0, half // blk, body, 0)

    kct_pieces = 2 * n_chunk
    kw = rows // kct_pieces

    def build_kct(lo, hi):
        def piece(i, carry):
            rs = pl.ds(pl.multiple_of(i * kw, kw), kw)
            for n in range(half // blk):
                kct_buf[pl.ds(pl.multiple_of(core * half + n * blk, blk), blk), rs] = (
                    k_buf[core, rs, n * blk:(n + 1) * blk] * c_buf[rs, n * blk:(n + 1) * blk]).T
            part = kct_buf.at[pl.ds(pl.multiple_of(core * half, half), half), rs]
            remote(part, part, send_sem.at[KC], one_recv.at[5], partner).start()
            return carry
        lax.fori_loop(lo, hi, piece, 0)

    ahead = grp * (AHEAD[0] + core * (AHEAD[1] - AHEAD[0]))
    middle = grp * kct_pieces + (1 - grp) * (kct_pieces // 2)

    k_push = [remote(k_buf.at[core, krows(i)], k_buf.at[core, krows(i)], send_sem.at[KP], kp_recv.at[i], partner) for i in range(n_chunk)]
    b_push = remote(b_hbm.at[other], b_buf.at[core], send_sem.at[BP], one_recv.at[0], partner)
    pl.semaphore_wait(barrier, 7)
    b_push.start()
    ones = jnp.ones((nq, half), BF16)
    for i in range(n_chunk):
        k_load[i].wait()
        if i == 0:
            k_push[0].start()
        if i % 2:
            part = lax.dot_general(ones, k_buf[core, pl.ds((i - 1) * rw, 2 * rw)], (((1,), (1,)), ((), ())), preferred_element_type=F32)
            for n in range(2 * rw // 128):
                r = (i - 1) * (rw // 128) + n
                s0_buf[col, r:r + 1, :] = part[0:1, n * 128:(n + 1) * 128]
    for n in range(1, 4):
        remote(s0_buf.at[col], s0_buf.at[col], send_sem.at[S0], one_recv.at[1], dev(row, (col + n) % 4)).start()
    for i in range(1, n_chunk):
        k_push[i].start()
    for d in c_load:
        d.start()
    for i in range(n_chunk):
        transpose_rows(core, i)
    a_load.wait()
    b_load.wait()
    all_here(s0_buf.at[0:3], one_recv.at[1])
    s0 = (s0_buf[0] + s0_buf[1]) + (s0_buf[2] + s0_buf[3])
    for r in range(rows // 128):
        cs = slice(r * 128, (r + 1) * 128)
        ub_buf[:, cs] = (a_buf[:, cs] / s0[r:r + 1, :]).astype(BF16)

    def t_copy(par, o):
        return remote(t_out.at[o], t_in.at[par, o], send_sem.at[TT], t_recv.at[par, o], y_peer)

    def s_copy(par, o):
        return remote(s_out.at[o], s_in.at[par, o], send_sem.at[SS], s_recv.at[par, o], x_peer)

    def t0_send(g, n):
        remote(t0_buf.at[g, n], t_in.at[0, core * per_half + n], send_sem.at[T0], t_recv.at[0, core * per_half + n],
               dev(1 - row, 2 * x + (g + x + 1 - row) % 2)).start()

    for n in range(per_half):
        part = jnp.dot(ub_buf[...], k_buf[core, :, n * cw:(n + 1) * cw], preferred_element_type=F32)
        for g in range(2):
            t0_buf[g, n] = part[g * nq:(g + 1) * nq]
        t0_send(0, n)
    for n in range(per_half):
        o = core * per_half + n
        remote(t0_buf.at[1 - grp, n], t_out.at[o], send_sem.at[TP], one_recv.at[2], partner).start()
        t_out[o] = t0_buf[grp, n]

    def v_of(par, o):
        return b_buf[o // per_half, :, (o % per_half) * cw:(o % per_half + 1) * cw] / (t_out[o] + t_in[par, o])

    all_here(b_buf.at[0], one_recv.at[0])
    for i in range(n_chunk):
        all_here(k_buf.at[1 - core, krows(i)], kp_recv.at[i])
        transpose_rows(1 - core, i)
        if i == 0:
            for n in range(per_half):
                t0_send(1, n)

    for d in c_load:
        d.wait()
    build_kct(0, ahead)

    all_here(t0_buf.at[0], one_recv.at[2])
    order = list(range(per_half, n_chunk)) + list(range(per_half))
    for c in order:
        all_here(t_in.at[0, c], t_recv.at[0, c])
        vb = v_of(0, c).astype(BF16)
        js = slice(c * cw, (c + 1) * cw)
        if c != order[-1]:
            prod = jnp.dot(vb, kt_buf[js, :], preferred_element_type=F32)
            acc[...] = prod if c == order[0] else acc[...] + prod
        else:
            for o in range(n_chunk):
                s_out[o] = acc[:, o * rw:(o + 1) * rw] + jnp.dot(vb, kt_buf[js, o * rw:(o + 1) * rw], preferred_element_type=F32)
                s_copy(1, o).start()
    all_sent(t0_buf, T0)
    all_sent(t0_buf.at[0], TP)
    all_sent(s0_buf.at[0:3], S0)
    all_sent(k_buf.at[0], KP)
    all_sent(b_buf.at[0], BP)

    build_kct(ahead, middle)

    def u_and_t(par):
        for c in range(n_chunk):
            all_here(s_in.at[par, c], s_recv.at[par, c])
            w = slice(c * rw, (c + 1) * rw)
            u = a_buf[mine, w] / (s_out[c] + s_in[par, c])
            u_out[mine, w] = u
            ub = u.astype(BF16)
            if c < n_chunk - 1:
                for h in range(2):
                    hc = slice(h * half, (h + 1) * half)
                    prod = jnp.dot(ub, k_buf[h, w, :], preferred_element_type=F32)
                    acc[:, hc] = prod if c == 0 else acc[:, hc] + prod
            else:
                for o in range(n_chunk):
                    oc = slice(o * cw, (o + 1) * cw)
                    hc = slice((o % per_half) * cw, (o % per_half + 1) * cw)
                    t_out[o] = acc[:, oc] + jnp.dot(ub, k_buf[o // per_half, w, hc], preferred_element_type=F32)
                    t_copy(par, o).start()
                all_sent(s_out, SS)

    def v_and_s(par_in, par):
        for c in range(n_chunk):
            all_here(t_in.at[par_in, c], t_recv.at[par_in, c])
            vb = v_of(par_in, c).astype(BF16)
            w = slice(c * cw, (c + 1) * cw)
            if c < n_chunk - 1:
                prod = jnp.dot(vb, kt_buf[w, :], preferred_element_type=F32)
                acc[...] = prod if c == 0 else acc[...] + prod
            else:
                for o in range(n_chunk):
                    oc = slice(o * rw, (o + 1) * rw)
                    s_out[o] = acc[:, oc] + jnp.dot(vb, kt_buf[w, oc], preferred_element_type=F32)
                    s_copy(par, o).start()
                all_sent(t_out, TT)

    def sweep(t, carry):
        u_and_t(t % 2)

        @pl.when(t == 1)
        def _():
            build_kct(middle, kct_pieces)

        v_and_s(t % 2, (t + 1) % 2)
        return carry

    lax.fori_loop(1, SWEEPS - 1, sweep, 0)
    last = (SWEEPS - 1) % 2
    u_and_t(last)

    u_push = remote(u_out.at[mine], u_out.at[mine], send_sem.at[US], one_recv.at[3], partner)
    u_push.start()
    cost_part[...] = jnp.zeros_like(cost_part)
    all_here(kct_buf.at[0:half], one_recv.at[5])
    all_sent(kct_buf.at[0:half], KC)
    for c in range(n_chunk):
        all_here(t_in.at[last, c], t_recv.at[last, c])
        v = v_of(last, c)
        v_all[c // per_half, :, (c % per_half) * cw:(c % per_half + 1) * cw] = v
        prod = jnp.dot(v.astype(BF16), kct_buf[c * cw:(c + 1) * cw, :], preferred_element_type=F32)
        if c < n_chunk - 1:
            acc[...] = prod if c == 0 else acc[...] + prod
        else:
            w = (acc[...] + prod) * u_out[mine]
    v_push = remote(v_all.at[1 - core], v_out.at[mine], send_sem.at[VS], one_recv.at[4], partner)
    v_push.start()
    tot = w[:, 0:128]
    for n in range(1, rows // 128):
        tot = tot + w[:, n * 128:(n + 1) * 128]
    cost_part[mine] = tot
    cost_all[me] = jnp.sum(cost_part[...].T, axis=0, keepdims=True)
    for dr in range(2):
        for dc in range(4):
            if dr or dc:
                remote(cost_all.at[me], cost_all.at[me], send_sem.at[CS], one_recv.at[6], dev((row + dr) % 2, (col + dc) % 4)).start()
    v_out[mine] = v_all[core]
    all_sent(t_out, TT)
    all_here(u_out.at[other], one_recv.at[3])
    u_push.wait_send()
    all_here(v_out.at[other], one_recv.at[4])
    v_push.wait_send()
    all_here(cost_all.at[0:7], one_recv.at[6])
    all_sent(cost_all.at[0:7], CS)


def output_kernel(norm, u_ref, v_ref, c_ref, u_hbm, v_hbm, cost_ref, sem):
    stores = [pltpu.make_async_copy(u_ref, u_hbm, sem.at[0]), pltpu.make_async_copy(v_ref, v_hbm, sem.at[1])]
    for d in stores:
        d.start()
    total = c_ref[0]
    for n in range(1, 8):
        total = total + c_ref[n]
    cost_ref[...] = total[:, :cost_ref.shape[1]] * norm
    for d in stores:
        d.wait()


def solution(mesh):
    n_chunk = 4

    def local_fn(kernel, cost_mat, src_mass, tgt_mass):
        rows, half = kernel.shape
        nprob = src_mass.shape[1]
        nq = nprob // 2
        cols = 2 * half
        rw, cw = rows // n_chunk, cols // n_chunk
        norm = 1.0 / float(rows * mesh.shape["row"] * half * mesh.shape["col"])
        vmem_spec = pl.BlockSpec(memory_space=pltpu.VMEM)
        any_spec = pl.BlockSpec(memory_space=pl.ANY)
        dma = pltpu.SemaphoreType.DMA
        u_vm, v_vm, c_vm = pl.pallas_call(
            lambda *refs: sinkhorn_kernel(n_chunk, *refs),
            out_shape=(pltpu.VMEM((nprob, rows), F32), pltpu.VMEM((nprob, half), F32), pltpu.VMEM((8, 1, 128), F32)),
            in_specs=[any_spec] * 4,
            out_specs=(vmem_spec, vmem_spec, vmem_spec),
            scratch_shapes=[
                pltpu.VMEM((2, rows, half), BF16),
                pltpu.VMEM((cols, rows), BF16),
                pltpu.VMEM((rows, half), BF16),
                pltpu.VMEM((cols, rows), BF16),
                pltpu.VMEM((nprob, rows), F32),
                pltpu.VMEM((2, nq, half), F32),
                pltpu.VMEM((nprob, rows), BF16),
                pltpu.VMEM((nq, max(rows, cols)), F32),
                pltpu.VMEM((n_chunk, nq, rw), F32),
                pltpu.VMEM((2, n_chunk, nq, rw), F32),
                pltpu.VMEM((n_chunk, nq, cw), F32),
                pltpu.VMEM((2, n_chunk, nq, cw), F32),
                pltpu.VMEM((2, n_chunk // 2, nq, cw), F32),
                pltpu.VMEM((4, rows // 128, 128), F32),
                pltpu.VMEM((2, nq, half), F32),
                pltpu.VMEM((128, 128), F32),
                dma((n_chunk + 2,)), dma((11,)), dma((n_chunk,)), dma((2, n_chunk)), dma((2, n_chunk)), dma((7,)),
            ],
            compiler_params=pltpu.CompilerParams(collective_id=0, has_side_effects=True, vmem_limit_bytes=60 * 1024 * 1024),
            name="sinkhorn",
        )(kernel, cost_mat, src_mass.T, tgt_mass.T)
        u_t, v_t, cost = pl.pallas_call(
            lambda *refs: output_kernel(norm, *refs),
            out_shape=(jax.ShapeDtypeStruct((nprob, rows), F32), jax.ShapeDtypeStruct((nprob, half), F32),
                       jax.ShapeDtypeStruct((1, nprob), F32)),
            in_specs=[vmem_spec] * 3,
            out_specs=(any_spec, any_spec, vmem_spec),
            scratch_shapes=[dma((2,))],
            name="outputs",
        )(*(pltpu.with_memory_space_constraint(r, pltpu.VMEM) for r in (u_vm, v_vm, c_vm)))
        return u_t.T, v_t.T, cost.reshape(nprob)

    return jax.shard_map(local_fn, mesh=mesh, in_specs=(P("row", "col"), P("row", "col"), P("row", "prob"), P("col", "prob")), out_specs=(P("row", "prob"), P("col", "prob"), P("prob")), check_vma=False)
```

```python
import jax
import jax.numpy as jnp
from jax import lax
from jax.experimental import pallas as pl
from jax.experimental.pallas import tpu as pltpu
from jax.sharding import PartitionSpec as P

SWEEPS = 6
AHEAD = (8, 6)
WAIT_NS = 700
F32 = jnp.float32
BF16 = jnp.bfloat16
MESH = pl.DeviceIdType.MESH


def sinkhorn_kernel(n_chunk, k_hbm, c_hbm, a_hbm, b_hbm, u_out, v_out, cost_all,
                    k_buf, kt_buf, c_buf, kct_buf, a_buf, b_buf, ub_buf, acc,
                    s_out, s_in, t_out, t_in, t0_buf, s0_buf, v_all, cost_part,
                    load_sem, send_sem, kp_recv, s_recv, t_recv, one_recv):
    rows, half = k_hbm.shape
    cols = 2 * half
    rw = rows // n_chunk
    cw = cols // n_chunk
    per_half = n_chunk // 2
    nq = b_buf.shape[1]
    row = lax.axis_index("row")
    col = lax.axis_index("col")
    prob = lax.axis_index("prob")
    x = col // 2
    core = col % 2
    grp = (core + x + row) % 2
    me = row * 4 + col
    mine = pl.ds(pl.multiple_of(grp * nq, nq), nq)
    other = pl.ds(pl.multiple_of((1 - grp) * nq, nq), nq)

    def dev(r, c):
        return (prob, r, c)

    partner = dev(row, 2 * x + 1 - core)
    x_peer = dev(row, 2 * (1 - x) + 1 - core)
    y_peer = dev(1 - row, 2 * x + 1 - core)

    def remote(src, dst, send, recv, to):
        return pltpu.make_async_remote_copy(src_ref=src, dst_ref=dst, send_sem=send, recv_sem=recv,
                                            device_id=to, device_id_type=MESH)

    KP, BP, S0, SS, TT, T0, TP, KC, US, VS, CS = range(11)

    def all_sent(ref, kind):
        remote(ref, ref, send_sem.at[kind], one_recv.at[0], partner).wait_send()

    def all_here(ref, recv):
        remote(ref, ref, send_sem.at[0], recv, partner).wait_recv()

    def krows(i):
        return pl.ds(i * rw, rw)

    k_load = [pltpu.make_async_copy(k_hbm.at[krows(i)], k_buf.at[core, krows(i)], load_sem.at[i]) for i in range(n_chunk)]
    c_load = [pltpu.make_async_copy(c_hbm.at[krows(i)], c_buf.at[krows(i)], load_sem.at[i]) for i in range(n_chunk)]
    a_load = pltpu.make_async_copy(a_hbm, a_buf, load_sem.at[n_chunk])
    b_load = pltpu.make_async_copy(b_hbm.at[mine], b_buf.at[core], load_sem.at[n_chunk + 1])
    for d in k_load:
        d.start()
    a_load.start()
    b_load.start()

    barrier = pltpu.get_barrier_semaphore()
    for dr in range(2):
        for dc in range(4):
            if dr or dc:
                pl.semaphore_signal(barrier, inc=1, device_id=dev((row + dr) % 2, (col + dc) % 4), device_id_type=MESH)

    blk = 256

    def transpose_rows(h, i):
        def body(n, carry):
            jo = pl.multiple_of(n * blk, blk)
            for ii in range(rw // blk):
                kt_buf[pl.ds(pl.multiple_of(h * half + jo, blk), blk), pl.ds(i * rw + ii * blk, blk)] = (
                    k_buf[h, pl.ds(i * rw + ii * blk, blk), pl.ds(jo, blk)].T)
            return carry
        lax.fori_loop(0, half // blk, body, 0)

    kct_pieces = 2 * n_chunk
    kw = rows // kct_pieces

    def build_kct(lo, hi):
        def piece(i, carry):
            rs = pl.ds(pl.multiple_of(i * kw, kw), kw)
            for n in range(half // blk):
                kct_buf[pl.ds(pl.multiple_of(core * half + n * blk, blk), blk), rs] = (
                    k_buf[core, rs, n * blk:(n + 1) * blk] * c_buf[rs, n * blk:(n + 1) * blk]).T
            part = kct_buf.at[pl.ds(pl.multiple_of(core * half, half), half), rs]
            remote(part, part, send_sem.at[KC], one_recv.at[5], partner).start()
            return carry
        lax.fori_loop(lo, hi, piece, 0)

    ahead = grp * (AHEAD[0] + core * (AHEAD[1] - AHEAD[0]))
    middle = grp * kct_pieces + (1 - grp) * (kct_pieces // 2)

    k_push = [remote(k_buf.at[core, krows(i)], k_buf.at[core, krows(i)], send_sem.at[KP], kp_recv.at[i], partner) for i in range(n_chunk)]
    b_push = remote(b_hbm.at[other], b_buf.at[core], send_sem.at[BP], one_recv.at[0], partner)
    pl.semaphore_wait(barrier, 7)
    b_push.start()
    ones = jnp.ones((nq, half), BF16)
    for i in range(n_chunk):
        k_load[i].wait()
        if i == 0:
            k_push[0].start()
        if i % 2:
            part = lax.dot_general(ones, k_buf[core, pl.ds((i - 1) * rw, 2 * rw)], (((1,), (1,)), ((), ())), preferred_element_type=F32)
            for n in range(2 * rw // 128):
                r = (i - 1) * (rw // 128) + n
                s0_buf[col, r:r + 1, :] = part[0:1, n * 128:(n + 1) * 128]
    for n in range(1, 4):
        remote(s0_buf.at[col], s0_buf.at[col], send_sem.at[S0], one_recv.at[1], dev(row, (col + n) % 4)).start()
    for i in range(1, n_chunk):
        k_push[i].start()
    for d in c_load:
        d.start()
    for i in range(n_chunk):
        transpose_rows(core, i)
    a_load.wait()
    b_load.wait()
    all_here(s0_buf.at[0:3], one_recv.at[1])
    s0 = (s0_buf[0] + s0_buf[1]) + (s0_buf[2] + s0_buf[3])
    for r in range(rows // 128):
        cs = slice(r * 128, (r + 1) * 128)
        ub_buf[:, cs] = (a_buf[:, cs] / s0[r:r + 1, :]).astype(BF16)

    def t_copy(par, o):
        return remote(t_out.at[o], t_in.at[par, o], send_sem.at[TT], t_recv.at[par, o], y_peer)

    def s_copy(par, o):
        return remote(s_out.at[o], s_in.at[par, o], send_sem.at[SS], s_recv.at[par, o], x_peer)

    def t0_send(g, n):
        remote(t0_buf.at[g, n], t_in.at[0, core * per_half + n], send_sem.at[T0], t_recv.at[0, core * per_half + n],
               dev(1 - row, 2 * x + (g + x + 1 - row) % 2)).start()

    for n in range(per_half):
        part = jnp.dot(ub_buf[...], k_buf[core, :, n * cw:(n + 1) * cw], preferred_element_type=F32)
        for g in range(2):
            t0_buf[g, n] = part[g * nq:(g + 1) * nq]
        t0_send(0, n)
    for n in range(per_half):
        o = core * per_half + n
        remote(t0_buf.at[1 - grp, n], t_out.at[o], send_sem.at[TP], one_recv.at[2], partner).start()
        t_out[o] = t0_buf[grp, n]

    def v_of(par, o):
        return b_buf[o // per_half, :, (o % per_half) * cw:(o % per_half + 1) * cw] / (t_out[o] + t_in[par, o])

    all_here(b_buf.at[0], one_recv.at[0])
    for i in range(n_chunk):
        all_here(k_buf.at[1 - core, krows(i)], kp_recv.at[i])
        transpose_rows(1 - core, i)
        if i == 0:
            for n in range(per_half):
                t0_send(1, n)

    for d in c_load:
        d.wait()
    build_kct(0, ahead)

    @pl.when(grp == 1)
    def _():
        pl.delay(WAIT_NS)

    all_here(t0_buf.at[0], one_recv.at[2])
    order = list(range(per_half, n_chunk)) + list(range(per_half))
    for c in order:
        all_here(t_in.at[0, c], t_recv.at[0, c])
        vb = v_of(0, c).astype(BF16)
        js = slice(c * cw, (c + 1) * cw)
        if c != order[-1]:
            prod = jnp.dot(vb, kt_buf[js, :], preferred_element_type=F32)
            acc[...] = prod if c == order[0] else acc[...] + prod
        else:
            for o in range(n_chunk):
                s_out[o] = acc[:, o * rw:(o + 1) * rw] + jnp.dot(vb, kt_buf[js, o * rw:(o + 1) * rw], preferred_element_type=F32)
                s_copy(1, o).start()
    all_sent(t0_buf, T0)
    all_sent(t0_buf.at[0], TP)
    all_sent(s0_buf.at[0:3], S0)
    all_sent(k_buf.at[0], KP)
    all_sent(b_buf.at[0], BP)

    build_kct(ahead, middle)

    def u_and_t(par):
        for c in range(n_chunk):
            all_here(s_in.at[par, c], s_recv.at[par, c])
            w = slice(c * rw, (c + 1) * rw)
            u = a_buf[mine, w] / (s_out[c] + s_in[par, c])
            u_out[mine, w] = u
            ub = u.astype(BF16)
            if c < n_chunk - 1:
                for h in range(2):
                    hc = slice(h * half, (h + 1) * half)
                    prod = jnp.dot(ub, k_buf[h, w, :], preferred_element_type=F32)
                    acc[:, hc] = prod if c == 0 else acc[:, hc] + prod
            else:
                for o in range(n_chunk):
                    oc = slice(o * cw, (o + 1) * cw)
                    hc = slice((o % per_half) * cw, (o % per_half + 1) * cw)
                    t_out[o] = acc[:, oc] + jnp.dot(ub, k_buf[o // per_half, w, hc], preferred_element_type=F32)
                    t_copy(par, o).start()
                all_sent(s_out, SS)

    def v_and_s(par_in, par):
        for c in range(n_chunk):
            all_here(t_in.at[par_in, c], t_recv.at[par_in, c])
            vb = v_of(par_in, c).astype(BF16)
            w = slice(c * cw, (c + 1) * cw)
            if c < n_chunk - 1:
                prod = jnp.dot(vb, kt_buf[w, :], preferred_element_type=F32)
                acc[...] = prod if c == 0 else acc[...] + prod
            else:
                for o in range(n_chunk):
                    oc = slice(o * rw, (o + 1) * rw)
                    s_out[o] = acc[:, oc] + jnp.dot(vb, kt_buf[w, oc], preferred_element_type=F32)
                    s_copy(par, o).start()
                all_sent(t_out, TT)

    def sweep(t, carry):
        u_and_t(t % 2)

        @pl.when(t == 1)
        def _():
            build_kct(middle, kct_pieces)

        v_and_s(t % 2, (t + 1) % 2)
        return carry

    lax.fori_loop(1, SWEEPS - 1, sweep, 0)
    last = (SWEEPS - 1) % 2
    u_and_t(last)

    u_push = remote(u_out.at[mine], u_out.at[mine], send_sem.at[US], one_recv.at[3], partner)
    u_push.start()
    cost_part[...] = jnp.zeros_like(cost_part)
    all_here(kct_buf.at[0:half], one_recv.at[5])
    all_sent(kct_buf.at[0:half], KC)
    for c in range(n_chunk):
        all_here(t_in.at[last, c], t_recv.at[last, c])
        v = v_of(last, c)
        v_all[c // per_half, :, (c % per_half) * cw:(c % per_half + 1) * cw] = v
        prod = jnp.dot(v.astype(BF16), kct_buf[c * cw:(c + 1) * cw, :], preferred_element_type=F32)
        if c < n_chunk - 1:
            acc[...] = prod if c == 0 else acc[...] + prod
        else:
            w = (acc[...] + prod) * u_out[mine]
    v_push = remote(v_all.at[1 - core], v_out.at[mine], send_sem.at[VS], one_recv.at[4], partner)
    v_push.start()
    tot = w[:, 0:128]
    for n in range(1, rows // 128):
        tot = tot + w[:, n * 128:(n + 1) * 128]
    cost_part[mine] = tot
    cost_all[me] = jnp.sum(cost_part[...].T, axis=0, keepdims=True)
    for dr in range(2):
        for dc in range(4):
            if dr or dc:
                remote(cost_all.at[me], cost_all.at[me], send_sem.at[CS], one_recv.at[6], dev((row + dr) % 2, (col + dc) % 4)).start()
    v_out[mine] = v_all[core]
    all_sent(t_out, TT)
    all_here(u_out.at[other], one_recv.at[3])
    u_push.wait_send()
    all_here(v_out.at[other], one_recv.at[4])
    v_push.wait_send()
    all_here(cost_all.at[0:7], one_recv.at[6])
    all_sent(cost_all.at[0:7], CS)


def output_kernel(norm, u_ref, v_ref, c_ref, u_hbm, v_hbm, cost_ref, sem):
    stores = [pltpu.make_async_copy(u_ref, u_hbm, sem.at[0]), pltpu.make_async_copy(v_ref, v_hbm, sem.at[1])]
    for d in stores:
        d.start()
    total = c_ref[0]
    for n in range(1, 8):
        total = total + c_ref[n]
    cost_ref[...] = total[:, :cost_ref.shape[1]] * norm
    for d in stores:
        d.wait()


def solution(mesh):
    n_chunk = 4

    def local_fn(kernel, cost_mat, src_mass, tgt_mass):
        rows, half = kernel.shape
        nprob = src_mass.shape[1]
        nq = nprob // 2
        cols = 2 * half
        rw, cw = rows // n_chunk, cols // n_chunk
        norm = 1.0 / float(rows * mesh.shape["row"] * half * mesh.shape["col"])
        vmem_spec = pl.BlockSpec(memory_space=pltpu.VMEM)
        any_spec = pl.BlockSpec(memory_space=pl.ANY)
        dma = pltpu.SemaphoreType.DMA
        u_vm, v_vm, c_vm = pl.pallas_call(
            lambda *refs: sinkhorn_kernel(n_chunk, *refs),
            out_shape=(pltpu.VMEM((nprob, rows), F32), pltpu.VMEM((nprob, half), F32), pltpu.VMEM((8, 1, 128), F32)),
            in_specs=[any_spec] * 4,
            out_specs=(vmem_spec, vmem_spec, vmem_spec),
            scratch_shapes=[
                pltpu.VMEM((2, rows, half), BF16),
                pltpu.VMEM((cols, rows), BF16),
                pltpu.VMEM((rows, half), BF16),
                pltpu.VMEM((cols, rows), BF16),
                pltpu.VMEM((nprob, rows), F32),
                pltpu.VMEM((2, nq, half), F32),
                pltpu.VMEM((nprob, rows), BF16),
                pltpu.VMEM((nq, max(rows, cols)), F32),
                pltpu.VMEM((n_chunk, nq, rw), F32),
                pltpu.VMEM((2, n_chunk, nq, rw), F32),
                pltpu.VMEM((n_chunk, nq, cw), F32),
                pltpu.VMEM((2, n_chunk, nq, cw), F32),
                pltpu.VMEM((2, n_chunk // 2, nq, cw), F32),
                pltpu.VMEM((4, rows // 128, 128), F32),
                pltpu.VMEM((2, nq, half), F32),
                pltpu.VMEM((128, 128), F32),
                dma((n_chunk + 2,)), dma((11,)), dma((n_chunk,)), dma((2, n_chunk)), dma((2, n_chunk)), dma((7,)),
            ],
            compiler_params=pltpu.CompilerParams(collective_id=0, has_side_effects=True, vmem_limit_bytes=60 * 1024 * 1024),
            name="sinkhorn",
        )(kernel, cost_mat, src_mass.T, tgt_mass.T)
        u_t, v_t, cost = pl.pallas_call(
            lambda *refs: output_kernel(norm, *refs),
            out_shape=(jax.ShapeDtypeStruct((nprob, rows), F32), jax.ShapeDtypeStruct((nprob, half), F32),
                       jax.ShapeDtypeStruct((1, nprob), F32)),
            in_specs=[vmem_spec] * 3,
            out_specs=(any_spec, any_spec, vmem_spec),
            scratch_shapes=[dma((2,))],
            name="outputs",
        )(*(pltpu.with_memory_space_constraint(r, pltpu.VMEM) for r in (u_vm, v_vm, c_vm)))
        return u_t.T, v_t.T, cost.reshape(nprob)

    return jax.shard_map(local_fn, mesh=mesh, in_specs=(P("row", "col"), P("row", "col"), P("row", "prob"), P("col", "prob")), out_specs=(P("row", "prob"), P("col", "prob"), P("prob")), check_vma=False)
```

```python
import jax
import jax.numpy as jnp
from jax import lax
from jax.experimental import pallas as pl
from jax.experimental.pallas import tpu as pltpu
from jax.sharding import PartitionSpec as P

SWEEPS = 6
AHEAD = (8, 6)
WAIT_NS = 1000
F32 = jnp.float32
BF16 = jnp.bfloat16
MESH = pl.DeviceIdType.MESH


def sinkhorn_kernel(n_chunk, k_hbm, c_hbm, a_hbm, b_hbm, u_out, v_out, cost_all,
                    k_buf, kt_buf, c_buf, kct_buf, a_buf, b_buf, ub_buf, acc,
                    s_out, s_in, t_out, t_in, t0_buf, s0_buf, v_all, cost_part,
                    load_sem, send_sem, kp_recv, s_recv, t_recv, one_recv):
    rows, half = k_hbm.shape
    cols = 2 * half
    rw = rows // n_chunk
    cw = cols // n_chunk
    per_half = n_chunk // 2
    nq = b_buf.shape[1]
    row = lax.axis_index("row")
    col = lax.axis_index("col")
    prob = lax.axis_index("prob")
    x = col // 2
    core = col % 2
    grp = (core + x + row) % 2
    me = row * 4 + col
    mine = pl.ds(pl.multiple_of(grp * nq, nq), nq)
    other = pl.ds(pl.multiple_of((1 - grp) * nq, nq), nq)

    def dev(r, c):
        return (prob, r, c)

    partner = dev(row, 2 * x + 1 - core)
    x_peer = dev(row, 2 * (1 - x) + 1 - core)
    y_peer = dev(1 - row, 2 * x + 1 - core)

    def remote(src, dst, send, recv, to):
        return pltpu.make_async_remote_copy(src_ref=src, dst_ref=dst, send_sem=send, recv_sem=recv,
                                            device_id=to, device_id_type=MESH)

    KP, BP, S0, SS, TT, T0, TP, KC, US, VS, CS = range(11)

    def all_sent(ref, kind):
        remote(ref, ref, send_sem.at[kind], one_recv.at[0], partner).wait_send()

    def all_here(ref, recv):
        remote(ref, ref, send_sem.at[0], recv, partner).wait_recv()

    def krows(i):
        return pl.ds(i * rw, rw)

    k_load = [pltpu.make_async_copy(k_hbm.at[krows(i)], k_buf.at[core, krows(i)], load_sem.at[i]) for i in range(n_chunk)]
    c_load = [pltpu.make_async_copy(c_hbm.at[krows(i)], c_buf.at[krows(i)], load_sem.at[i]) for i in range(n_chunk)]
    a_load = pltpu.make_async_copy(a_hbm, a_buf, load_sem.at[n_chunk])
    b_load = pltpu.make_async_copy(b_hbm.at[mine], b_buf.at[core], load_sem.at[n_chunk + 1])
    for d in k_load:
        d.start()
    a_load.start()
    b_load.start()

    barrier = pltpu.get_barrier_semaphore()
    for dr in range(2):
        for dc in range(4):
            if dr or dc:
                pl.semaphore_signal(barrier, inc=1, device_id=dev((row + dr) % 2, (col + dc) % 4), device_id_type=MESH)

    blk = 256

    def transpose_rows(h, i):
        def body(n, carry):
            jo = pl.multiple_of(n * blk, blk)
            for ii in range(rw // blk):
                kt_buf[pl.ds(pl.multiple_of(h * half + jo, blk), blk), pl.ds(i * rw + ii * blk, blk)] = (
                    k_buf[h, pl.ds(i * rw + ii * blk, blk), pl.ds(jo, blk)].T)
            return carry
        lax.fori_loop(0, half // blk, body, 0)

    kct_pieces = 2 * n_chunk
    kw = rows // kct_pieces

    def build_kct(lo, hi):
        def piece(i, carry):
            rs = pl.ds(pl.multiple_of(i * kw, kw), kw)
            for n in range(half // blk):
                kct_buf[pl.ds(pl.multiple_of(core * half + n * blk, blk), blk), rs] = (
                    k_buf[core, rs, n * blk:(n + 1) * blk] * c_buf[rs, n * blk:(n + 1) * blk]).T
            part = kct_buf.at[pl.ds(pl.multiple_of(core * half, half), half), rs]
            remote(part, part, send_sem.at[KC], one_recv.at[5], partner).start()
            return carry
        lax.fori_loop(lo, hi, piece, 0)

    ahead = grp * (AHEAD[0] + core * (AHEAD[1] - AHEAD[0]))
    middle = grp * kct_pieces + (1 - grp) * (kct_pieces // 2)

    k_push = [remote(k_buf.at[core, krows(i)], k_buf.at[core, krows(i)], send_sem.at[KP], kp_recv.at[i], partner) for i in range(n_chunk)]
    b_push = remote(b_hbm.at[other], b_buf.at[core], send_sem.at[BP], one_recv.at[0], partner)
    pl.semaphore_wait(barrier, 7)
    b_push.start()
    ones = jnp.ones((nq, half), BF16)
    for i in range(n_chunk):
        k_load[i].wait()
        if i == 0:
            k_push[0].start()
        if i % 2:
            part = lax.dot_general(ones, k_buf[core, pl.ds((i - 1) * rw, 2 * rw)], (((1,), (1,)), ((), ())), preferred_element_type=F32)
            for n in range(2 * rw // 128):
                r = (i - 1) * (rw // 128) + n
                s0_buf[col, r:r + 1, :] = part[0:1, n * 128:(n + 1) * 128]
    for n in range(1, 4):
        remote(s0_buf.at[col], s0_buf.at[col], send_sem.at[S0], one_recv.at[1], dev(row, (col + n) % 4)).start()
    for i in range(1, n_chunk):
        k_push[i].start()
    for d in c_load:
        d.start()
    for i in range(n_chunk):
        transpose_rows(core, i)
    a_load.wait()
    b_load.wait()
    all_here(s0_buf.at[0:3], one_recv.at[1])
    s0 = (s0_buf[0] + s0_buf[1]) + (s0_buf[2] + s0_buf[3])
    for r in range(rows // 128):
        cs = slice(r * 128, (r + 1) * 128)
        ub_buf[:, cs] = (a_buf[:, cs] / s0[r:r + 1, :]).astype(BF16)

    def t_copy(par, o):
        return remote(t_out.at[o], t_in.at[par, o], send_sem.at[TT], t_recv.at[par, o], y_peer)

    def s_copy(par, o):
        return remote(s_out.at[o], s_in.at[par, o], send_sem.at[SS], s_recv.at[par, o], x_peer)

    def t0_send(g, n):
        remote(t0_buf.at[g, n], t_in.at[0, core * per_half + n], send_sem.at[T0], t_recv.at[0, core * per_half + n],
               dev(1 - row, 2 * x + (g + x + 1 - row) % 2)).start()

    for n in range(per_half):
        part = jnp.dot(ub_buf[...], k_buf[core, :, n * cw:(n + 1) * cw], preferred_element_type=F32)
        for g in range(2):
            t0_buf[g, n] = part[g * nq:(g + 1) * nq]
        t0_send(0, n)
    for n in range(per_half):
        o = core * per_half + n
        remote(t0_buf.at[1 - grp, n], t_out.at[o], send_sem.at[TP], one_recv.at[2], partner).start()
        t_out[o] = t0_buf[grp, n]

    def v_of(par, o):
        return b_buf[o // per_half, :, (o % per_half) * cw:(o % per_half + 1) * cw] / (t_out[o] + t_in[par, o])

    all_here(b_buf.at[0], one_recv.at[0])
    for i in range(n_chunk):
        all_here(k_buf.at[1 - core, krows(i)], kp_recv.at[i])
        transpose_rows(1 - core, i)
        if i == 0:
            for n in range(per_half):
                t0_send(1, n)

    for d in c_load:
        d.wait()
    build_kct(0, ahead)

    @pl.when(grp == 1)
    def _():
        pl.delay(WAIT_NS)

    all_here(t0_buf.at[0], one_recv.at[2])
    order = list(range(per_half, n_chunk)) + list(range(per_half))
    for c in order:
        all_here(t_in.at[0, c], t_recv.at[0, c])
        vb = v_of(0, c).astype(BF16)
        js = slice(c * cw, (c + 1) * cw)
        if c != order[-1]:
            prod = jnp.dot(vb, kt_buf[js, :], preferred_element_type=F32)
            acc[...] = prod if c == order[0] else acc[...] + prod
        else:
            for o in range(n_chunk):
                s_out[o] = acc[:, o * rw:(o + 1) * rw] + jnp.dot(vb, kt_buf[js, o * rw:(o + 1) * rw], preferred_element_type=F32)
                s_copy(1, o).start()
    all_sent(t0_buf, T0)
    all_sent(t0_buf.at[0], TP)
    all_sent(s0_buf.at[0:3], S0)
    all_sent(k_buf.at[0], KP)
    all_sent(b_buf.at[0], BP)

    build_kct(ahead, middle)

    def u_and_t(par):
        for c in range(n_chunk):
            all_here(s_in.at[par, c], s_recv.at[par, c])
            w = slice(c * rw, (c + 1) * rw)
            u = a_buf[mine, w] / (s_out[c] + s_in[par, c])
            u_out[mine, w] = u
            ub = u.astype(BF16)
            if c < n_chunk - 1:
                for h in range(2):
                    hc = slice(h * half, (h + 1) * half)
                    prod = jnp.dot(ub, k_buf[h, w, :], preferred_element_type=F32)
                    acc[:, hc] = prod if c == 0 else acc[:, hc] + prod
            else:
                for o in range(n_chunk):
                    oc = slice(o * cw, (o + 1) * cw)
                    hc = slice((o % per_half) * cw, (o % per_half + 1) * cw)
                    t_out[o] = acc[:, oc] + jnp.dot(ub, k_buf[o // per_half, w, hc], preferred_element_type=F32)
                    t_copy(par, o).start()
                all_sent(s_out, SS)

    def v_and_s(par_in, par):
        for c in range(n_chunk):
            all_here(t_in.at[par_in, c], t_recv.at[par_in, c])
            vb = v_of(par_in, c).astype(BF16)
            w = slice(c * cw, (c + 1) * cw)
            if c < n_chunk - 1:
                prod = jnp.dot(vb, kt_buf[w, :], preferred_element_type=F32)
                acc[...] = prod if c == 0 else acc[...] + prod
            else:
                for o in range(n_chunk):
                    oc = slice(o * rw, (o + 1) * rw)
                    s_out[o] = acc[:, oc] + jnp.dot(vb, kt_buf[w, oc], preferred_element_type=F32)
                    s_copy(par, o).start()
                all_sent(t_out, TT)

    def sweep(t, carry):
        u_and_t(t % 2)

        @pl.when(t == 1)
        def _():
            build_kct(middle, kct_pieces)

        v_and_s(t % 2, (t + 1) % 2)
        return carry

    lax.fori_loop(1, SWEEPS - 1, sweep, 0)
    last = (SWEEPS - 1) % 2
    u_and_t(last)

    u_push = remote(u_out.at[mine], u_out.at[mine], send_sem.at[US], one_recv.at[3], partner)
    u_push.start()
    cost_part[...] = jnp.zeros_like(cost_part)
    all_here(kct_buf.at[0:half], one_recv.at[5])
    all_sent(kct_buf.at[0:half], KC)
    for c in range(n_chunk):
        all_here(t_in.at[last, c], t_recv.at[last, c])
        v = v_of(last, c)
        v_all[c // per_half, :, (c % per_half) * cw:(c % per_half + 1) * cw] = v
        prod = jnp.dot(v.astype(BF16), kct_buf[c * cw:(c + 1) * cw, :], preferred_element_type=F32)
        if c < n_chunk - 1:
            acc[...] = prod if c == 0 else acc[...] + prod
        else:
            w = (acc[...] + prod) * u_out[mine]
    v_push = remote(v_all.at[1 - core], v_out.at[mine], send_sem.at[VS], one_recv.at[4], partner)
    v_push.start()
    tot = w[:, 0:128]
    for n in range(1, rows // 128):
        tot = tot + w[:, n * 128:(n + 1) * 128]
    cost_part[mine] = tot
    cost_all[me] = jnp.sum(cost_part[...].T, axis=0, keepdims=True)
    for dr in range(2):
        for dc in range(4):
            if dr or dc:
                remote(cost_all.at[me], cost_all.at[me], send_sem.at[CS], one_recv.at[6], dev((row + dr) % 2, (col + dc) % 4)).start()
    v_out[mine] = v_all[core]
    all_sent(t_out, TT)
    all_here(u_out.at[other], one_recv.at[3])
    u_push.wait_send()
    all_here(v_out.at[other], one_recv.at[4])
    v_push.wait_send()
    all_here(cost_all.at[0:7], one_recv.at[6])
    all_sent(cost_all.at[0:7], CS)


def output_kernel(norm, u_ref, v_ref, c_ref, u_hbm, v_hbm, cost_ref, sem):
    stores = [pltpu.make_async_copy(u_ref, u_hbm, sem.at[0]), pltpu.make_async_copy(v_ref, v_hbm, sem.at[1])]
    for d in stores:
        d.start()
    total = c_ref[0]
    for n in range(1, 8):
        total = total + c_ref[n]
    cost_ref[...] = total[:, :cost_ref.shape[1]] * norm
    for d in stores:
        d.wait()


def solution(mesh):
    n_chunk = 4

    def local_fn(kernel, cost_mat, src_mass, tgt_mass):
        rows, half = kernel.shape
        nprob = src_mass.shape[1]
        nq = nprob // 2
        cols = 2 * half
        rw, cw = rows // n_chunk, cols // n_chunk
        norm = 1.0 / float(rows * mesh.shape["row"] * half * mesh.shape["col"])
        vmem_spec = pl.BlockSpec(memory_space=pltpu.VMEM)
        any_spec = pl.BlockSpec(memory_space=pl.ANY)
        dma = pltpu.SemaphoreType.DMA
        u_vm, v_vm, c_vm = pl.pallas_call(
            lambda *refs: sinkhorn_kernel(n_chunk, *refs),
            out_shape=(pltpu.VMEM((nprob, rows), F32), pltpu.VMEM((nprob, half), F32), pltpu.VMEM((8, 1, 128), F32)),
            in_specs=[any_spec] * 4,
            out_specs=(vmem_spec, vmem_spec, vmem_spec),
            scratch_shapes=[
                pltpu.VMEM((2, rows, half), BF16),
                pltpu.VMEM((cols, rows), BF16),
                pltpu.VMEM((rows, half), BF16),
                pltpu.VMEM((cols, rows), BF16),
                pltpu.VMEM((nprob, rows), F32),
                pltpu.VMEM((2, nq, half), F32),
                pltpu.VMEM((nprob, rows), BF16),
                pltpu.VMEM((nq, max(rows, cols)), F32),
                pltpu.VMEM((n_chunk, nq, rw), F32),
                pltpu.VMEM((2, n_chunk, nq, rw), F32),
                pltpu.VMEM((n_chunk, nq, cw), F32),
                pltpu.VMEM((2, n_chunk, nq, cw), F32),
                pltpu.VMEM((2, n_chunk // 2, nq, cw), F32),
                pltpu.VMEM((4, rows // 128, 128), F32),
                pltpu.VMEM((2, nq, half), F32),
                pltpu.VMEM((128, 128), F32),
                dma((n_chunk + 2,)), dma((11,)), dma((n_chunk,)), dma((2, n_chunk)), dma((2, n_chunk)), dma((7,)),
            ],
            compiler_params=pltpu.CompilerParams(collective_id=0, has_side_effects=True, vmem_limit_bytes=60 * 1024 * 1024),
            name="sinkhorn",
        )(kernel, cost_mat, src_mass.T, tgt_mass.T)
        u_t, v_t, cost = pl.pallas_call(
            lambda *refs: output_kernel(norm, *refs),
            out_shape=(jax.ShapeDtypeStruct((nprob, rows), F32), jax.ShapeDtypeStruct((nprob, half), F32),
                       jax.ShapeDtypeStruct((1, nprob), F32)),
            in_specs=[vmem_spec] * 3,
            out_specs=(any_spec, any_spec, vmem_spec),
            scratch_shapes=[dma((2,))],
            name="outputs",
        )(*(pltpu.with_memory_space_constraint(r, pltpu.VMEM) for r in (u_vm, v_vm, c_vm)))
        return u_t.T, v_t.T, cost.reshape(nprob)

    return jax.shard_map(local_fn, mesh=mesh, in_specs=(P("row", "col"), P("row", "col"), P("row", "prob"), P("col", "prob")), out_specs=(P("row", "prob"), P("col", "prob"), P("prob")), check_vma=False)
```

```python
import jax
import jax.numpy as jnp
from jax import lax
from jax.experimental import pallas as pl
from jax.experimental.pallas import tpu as pltpu
from jax.sharding import PartitionSpec as P

SWEEPS = 6
AHEAD = (8, 6)
WAIT_NS = 850
F32 = jnp.float32
BF16 = jnp.bfloat16
MESH = pl.DeviceIdType.MESH


def sinkhorn_kernel(n_chunk, k_hbm, c_hbm, a_hbm, b_hbm, u_out, v_out, cost_all,
                    k_buf, kt_buf, c_buf, kct_buf, a_buf, b_buf, ub_buf, acc,
                    s_out, s_in, t_out, t_in, t0_buf, s0_buf, v_all, cost_part,
                    load_sem, send_sem, kp_recv, s_recv, t_recv, one_recv):
    rows, half = k_hbm.shape
    cols = 2 * half
    rw = rows // n_chunk
    cw = cols // n_chunk
    per_half = n_chunk // 2
    nq = b_buf.shape[1]
    row = lax.axis_index("row")
    col = lax.axis_index("col")
    prob = lax.axis_index("prob")
    x = col // 2
    core = col % 2
    grp = (core + x + row) % 2
    me = row * 4 + col
    mine = pl.ds(pl.multiple_of(grp * nq, nq), nq)
    other = pl.ds(pl.multiple_of((1 - grp) * nq, nq), nq)

    def dev(r, c):
        return (prob, r, c)

    partner = dev(row, 2 * x + 1 - core)
    x_peer = dev(row, 2 * (1 - x) + 1 - core)
    y_peer = dev(1 - row, 2 * x + 1 - core)

    def remote(src, dst, send, recv, to):
        return pltpu.make_async_remote_copy(src_ref=src, dst_ref=dst, send_sem=send, recv_sem=recv,
                                            device_id=to, device_id_type=MESH)

    KP, BP, S0, SS, TT, T0, TP, KC, US, VS, CS = range(11)

    def all_sent(ref, kind):
        remote(ref, ref, send_sem.at[kind], one_recv.at[0], partner).wait_send()

    def all_here(ref, recv):
        remote(ref, ref, send_sem.at[0], recv, partner).wait_recv()

    def krows(i):
        return pl.ds(i * rw, rw)

    k_load = [pltpu.make_async_copy(k_hbm.at[krows(i)], k_buf.at[core, krows(i)], load_sem.at[i]) for i in range(n_chunk)]
    c_load = [pltpu.make_async_copy(c_hbm.at[krows(i)], c_buf.at[krows(i)], load_sem.at[i]) for i in range(n_chunk)]
    a_load = pltpu.make_async_copy(a_hbm, a_buf, load_sem.at[n_chunk])
    b_load = pltpu.make_async_copy(b_hbm.at[mine], b_buf.at[core], load_sem.at[n_chunk + 1])
    for d in k_load:
        d.start()
    a_load.start()
    b_load.start()

    barrier = pltpu.get_barrier_semaphore()
    for dr in range(2):
        for dc in range(4):
            if dr or dc:
                pl.semaphore_signal(barrier, inc=1, device_id=dev((row + dr) % 2, (col + dc) % 4), device_id_type=MESH)

    blk = 256

    def transpose_rows(h, i):
        def body(n, carry):
            jo = pl.multiple_of(n * blk, blk)
            for ii in range(rw // blk):
                kt_buf[pl.ds(pl.multiple_of(h * half + jo, blk), blk), pl.ds(i * rw + ii * blk, blk)] = (
                    k_buf[h, pl.ds(i * rw + ii * blk, blk), pl.ds(jo, blk)].T)
            return carry
        lax.fori_loop(0, half // blk, body, 0)

    kct_pieces = 2 * n_chunk
    kw = rows // kct_pieces

    def build_kct(lo, hi):
        def piece(i, carry):
            rs = pl.ds(pl.multiple_of(i * kw, kw), kw)
            for n in range(half // blk):
                kct_buf[pl.ds(pl.multiple_of(core * half + n * blk, blk), blk), rs] = (
                    k_buf[core, rs, n * blk:(n + 1) * blk] * c_buf[rs, n * blk:(n + 1) * blk]).T
            part = kct_buf.at[pl.ds(pl.multiple_of(core * half, half), half), rs]
            remote(part, part, send_sem.at[KC], one_recv.at[5], partner).start()
            return carry
        lax.fori_loop(lo, hi, piece, 0)

    ahead = grp * (AHEAD[0] + core * (AHEAD[1] - AHEAD[0]))
    middle = grp * kct_pieces + (1 - grp) * (kct_pieces // 2)

    k_push = [remote(k_buf.at[core, krows(i)], k_buf.at[core, krows(i)], send_sem.at[KP], kp_recv.at[i], partner) for i in range(n_chunk)]
    b_push = remote(b_hbm.at[other], b_buf.at[core], send_sem.at[BP], one_recv.at[0], partner)
    pl.semaphore_wait(barrier, 7)
    b_push.start()
    ones = jnp.ones((nq, half), BF16)
    for i in range(n_chunk):
        k_load[i].wait()
        if i == 0:
            k_push[0].start()
        if i % 2:
            part = lax.dot_general(ones, k_buf[core, pl.ds((i - 1) * rw, 2 * rw)], (((1,), (1,)), ((), ())), preferred_element_type=F32)
            for n in range(2 * rw // 128):
                r = (i - 1) * (rw // 128) + n
                s0_buf[col, r:r + 1, :] = part[0:1, n * 128:(n + 1) * 128]
    for n in range(1, 4):
        remote(s0_buf.at[col], s0_buf.at[col], send_sem.at[S0], one_recv.at[1], dev(row, (col + n) % 4)).start()
    for i in range(1, n_chunk):
        k_push[i].start()
    for d in c_load:
        d.start()
    for i in range(n_chunk):
        transpose_rows(core, i)
    a_load.wait()
    b_load.wait()
    all_here(s0_buf.at[0:3], one_recv.at[1])
    s0 = (s0_buf[0] + s0_buf[1]) + (s0_buf[2] + s0_buf[3])
    for r in range(rows // 128):
        cs = slice(r * 128, (r + 1) * 128)
        ub_buf[:, cs] = (a_buf[:, cs] / s0[r:r + 1, :]).astype(BF16)

    def t_copy(par, o):
        return remote(t_out.at[o], t_in.at[par, o], send_sem.at[TT], t_recv.at[par, o], y_peer)

    def s_copy(par, o):
        return remote(s_out.at[o], s_in.at[par, o], send_sem.at[SS], s_recv.at[par, o], x_peer)

    def t0_send(g, n):
        remote(t0_buf.at[g, n], t_in.at[0, core * per_half + n], send_sem.at[T0], t_recv.at[0, core * per_half + n],
               dev(1 - row, 2 * x + (g + x + 1 - row) % 2)).start()

    for n in range(per_half):
        part = jnp.dot(ub_buf[...], k_buf[core, :, n * cw:(n + 1) * cw], preferred_element_type=F32)
        for g in range(2):
            t0_buf[g, n] = part[g * nq:(g + 1) * nq]
        t0_send(0, n)
    for n in range(per_half):
        o = core * per_half + n
        remote(t0_buf.at[1 - grp, n], t_out.at[o], send_sem.at[TP], one_recv.at[2], partner).start()
        t_out[o] = t0_buf[grp, n]

    def v_of(par, o):
        return b_buf[o // per_half, :, (o % per_half) * cw:(o % per_half + 1) * cw] / (t_out[o] + t_in[par, o])

    all_here(b_buf.at[0], one_recv.at[0])
    for i in range(n_chunk):
        all_here(k_buf.at[1 - core, krows(i)], kp_recv.at[i])
        transpose_rows(1 - core, i)
        if i == 0:
            for n in range(per_half):
                t0_send(1, n)

    for d in c_load:
        d.wait()
    build_kct(0, ahead)

    @pl.when(grp == 1)
    def _():
        pl.delay(WAIT_NS)

    all_here(t0_buf.at[0], one_recv.at[2])
    order = list(range(per_half, n_chunk)) + list(range(per_half))
    for c in order:
        all_here(t_in.at[0, c], t_recv.at[0, c])
        vb = v_of(0, c).astype(BF16)
        js = slice(c * cw, (c + 1) * cw)
        if c != order[-1]:
            prod = jnp.dot(vb, kt_buf[js, :], preferred_element_type=F32)
            acc[...] = prod if c == order[0] else acc[...] + prod
        else:
            for o in range(n_chunk):
                s_out[o] = acc[:, o * rw:(o + 1) * rw] + jnp.dot(vb, kt_buf[js, o * rw:(o + 1) * rw], preferred_element_type=F32)
                s_copy(1, o).start()
    all_sent(t0_buf, T0)
    all_sent(t0_buf.at[0], TP)
    all_sent(s0_buf.at[0:3], S0)
    all_sent(k_buf.at[0], KP)
    all_sent(b_buf.at[0], BP)

    build_kct(ahead, middle)

    def u_and_t(par):
        for c in range(n_chunk):
            all_here(s_in.at[par, c], s_recv.at[par, c])
            w = slice(c * rw, (c + 1) * rw)
            u = a_buf[mine, w] / (s_out[c] + s_in[par, c])
            u_out[mine, w] = u
            ub = u.astype(BF16)
            if c < n_chunk - 1:
                for h in range(2):
                    hc = slice(h * half, (h + 1) * half)
                    prod = jnp.dot(ub, k_buf[h, w, :], preferred_element_type=F32)
                    acc[:, hc] = prod if c == 0 else acc[:, hc] + prod
            else:
                for o in range(n_chunk):
                    oc = slice(o * cw, (o + 1) * cw)
                    hc = slice((o % per_half) * cw, (o % per_half + 1) * cw)
                    t_out[o] = acc[:, oc] + jnp.dot(ub, k_buf[o // per_half, w, hc], preferred_element_type=F32)
                    t_copy(par, o).start()
                all_sent(s_out, SS)

    def v_and_s(par_in, par):
        for c in range(n_chunk):
            all_here(t_in.at[par_in, c], t_recv.at[par_in, c])
            vb = v_of(par_in, c).astype(BF16)
            w = slice(c * cw, (c + 1) * cw)
            if c < n_chunk - 1:
                prod = jnp.dot(vb, kt_buf[w, :], preferred_element_type=F32)
                acc[...] = prod if c == 0 else acc[...] + prod
            else:
                for o in range(n_chunk):
                    oc = slice(o * rw, (o + 1) * rw)
                    s_out[o] = acc[:, oc] + jnp.dot(vb, kt_buf[w, oc], preferred_element_type=F32)
                    s_copy(par, o).start()
                all_sent(t_out, TT)

    def sweep(t, carry):
        u_and_t(t % 2)

        @pl.when(t == 1)
        def _():
            build_kct(middle, kct_pieces)

        v_and_s(t % 2, (t + 1) % 2)
        return carry

    lax.fori_loop(1, SWEEPS - 1, sweep, 0)
    last = (SWEEPS - 1) % 2
    u_and_t(last)

    u_push = remote(u_out.at[mine], u_out.at[mine], send_sem.at[US], one_recv.at[3], partner)
    u_push.start()
    cost_part[...] = jnp.zeros_like(cost_part)
    all_here(kct_buf.at[0:half], one_recv.at[5])
    all_sent(kct_buf.at[0:half], KC)
    for c in range(n_chunk):
        all_here(t_in.at[last, c], t_recv.at[last, c])
        v = v_of(last, c)
        v_all[c // per_half, :, (c % per_half) * cw:(c % per_half + 1) * cw] = v
        prod = jnp.dot(v.astype(BF16), kct_buf[c * cw:(c + 1) * cw, :], preferred_element_type=F32)
        if c < n_chunk - 1:
            acc[...] = prod if c == 0 else acc[...] + prod
        else:
            w = (acc[...] + prod) * u_out[mine]
    v_push = remote(v_all.at[1 - core], v_out.at[mine], send_sem.at[VS], one_recv.at[4], partner)
    v_push.start()
    tot = w[:, 0:128]
    for n in range(1, rows // 128):
        tot = tot + w[:, n * 128:(n + 1) * 128]
    cost_part[mine] = tot
    cost_all[me] = jnp.sum(cost_part[...].T, axis=0, keepdims=True)
    for dr in range(2):
        for dc in range(4):
            if dr or dc:
                remote(cost_all.at[me], cost_all.at[me], send_sem.at[CS], one_recv.at[6], dev((row + dr) % 2, (col + dc) % 4)).start()
    v_out[mine] = v_all[core]
    all_sent(t_out, TT)
    all_here(u_out.at[other], one_recv.at[3])
    u_push.wait_send()
    all_here(v_out.at[other], one_recv.at[4])
    v_push.wait_send()
    all_here(cost_all.at[0:7], one_recv.at[6])
    all_sent(cost_all.at[0:7], CS)


def output_kernel(norm, u_ref, v_ref, c_ref, u_hbm, v_hbm, cost_ref, sem):
    stores = [pltpu.make_async_copy(u_ref, u_hbm, sem.at[0]), pltpu.make_async_copy(v_ref, v_hbm, sem.at[1])]
    for d in stores:
        d.start()
    total = c_ref[0]
    for n in range(1, 8):
        total = total + c_ref[n]
    cost_ref[...] = total[:, :cost_ref.shape[1]] * norm
    for d in stores:
        d.wait()


def solution(mesh):
    n_chunk = 4

    def local_fn(kernel, cost_mat, src_mass, tgt_mass):
        rows, half = kernel.shape
        nprob = src_mass.shape[1]
        nq = nprob // 2
        cols = 2 * half
        rw, cw = rows // n_chunk, cols // n_chunk
        norm = 1.0 / float(rows * mesh.shape["row"] * half * mesh.shape["col"])
        vmem_spec = pl.BlockSpec(memory_space=pltpu.VMEM)
        any_spec = pl.BlockSpec(memory_space=pl.ANY)
        dma = pltpu.SemaphoreType.DMA
        u_vm, v_vm, c_vm = pl.pallas_call(
            lambda *refs: sinkhorn_kernel(n_chunk, *refs),
            out_shape=(pltpu.VMEM((nprob, rows), F32), pltpu.VMEM((nprob, half), F32), pltpu.VMEM((8, 1, 128), F32)),
            in_specs=[any_spec] * 4,
            out_specs=(vmem_spec, vmem_spec, vmem_spec),
            scratch_shapes=[
                pltpu.VMEM((2, rows, half), BF16),
                pltpu.VMEM((cols, rows), BF16),
                pltpu.VMEM((rows, half), BF16),
                pltpu.VMEM((cols, rows), BF16),
                pltpu.VMEM((nprob, rows), F32),
                pltpu.VMEM((2, nq, half), F32),
                pltpu.VMEM((nprob, rows), BF16),
                pltpu.VMEM((nq, max(rows, cols)), F32),
                pltpu.VMEM((n_chunk, nq, rw), F32),
                pltpu.VMEM((2, n_chunk, nq, rw), F32),
                pltpu.VMEM((n_chunk, nq, cw), F32),
                pltpu.VMEM((2, n_chunk, nq, cw), F32),
                pltpu.VMEM((2, n_chunk // 2, nq, cw), F32),
                pltpu.VMEM((4, rows // 128, 128), F32),
                pltpu.VMEM((2, nq, half), F32),
                pltpu.VMEM((128, 128), F32),
                dma((n_chunk + 2,)), dma((11,)), dma((n_chunk,)), dma((2, n_chunk)), dma((2, n_chunk)), dma((7,)),
            ],
            compiler_params=pltpu.CompilerParams(collective_id=0, has_side_effects=True, vmem_limit_bytes=60 * 1024 * 1024),
            name="sinkhorn",
        )(kernel, cost_mat, src_mass.T, tgt_mass.T)
        u_t, v_t, cost = pl.pallas_call(
            lambda *refs: output_kernel(norm, *refs),
            out_shape=(jax.ShapeDtypeStruct((nprob, rows), F32), jax.ShapeDtypeStruct((nprob, half), F32),
                       jax.ShapeDtypeStruct((1, nprob), F32)),
            in_specs=[vmem_spec] * 3,
            out_specs=(any_spec, any_spec, vmem_spec),
            scratch_shapes=[dma((2,))],
            name="outputs",
        )(*(pltpu.with_memory_space_constraint(r, pltpu.VMEM) for r in (u_vm, v_vm, c_vm)))
        return u_t.T, v_t.T, cost.reshape(nprob)

    return jax.shard_map(local_fn, mesh=mesh, in_specs=(P("row", "col"), P("row", "col"), P("row", "prob"), P("col", "prob")), out_specs=(P("row", "prob"), P("col", "prob"), P("prob")), check_vma=False)
```

```python
import jax
import jax.numpy as jnp
from jax import lax
from jax.experimental import pallas as pl
from jax.experimental.pallas import tpu as pltpu
from jax.sharding import PartitionSpec as P

SWEEPS = 6
AHEAD = (8, 6)
WAIT_NS = 550
F32 = jnp.float32
BF16 = jnp.bfloat16
MESH = pl.DeviceIdType.MESH


def sinkhorn_kernel(n_chunk, k_hbm, c_hbm, a_hbm, b_hbm, u_out, v_out, cost_all,
                    k_buf, kt_buf, c_buf, kct_buf, a_buf, b_buf, ub_buf, acc,
                    s_out, s_in, t_out, t_in, t0_buf, s0_buf, v_all, cost_part,
                    load_sem, send_sem, kp_recv, s_recv, t_recv, one_recv):
    rows, half = k_hbm.shape
    cols = 2 * half
    rw = rows // n_chunk
    cw = cols // n_chunk
    per_half = n_chunk // 2
    nq = b_buf.shape[1]
    row = lax.axis_index("row")
    col = lax.axis_index("col")
    prob = lax.axis_index("prob")
    x = col // 2
    core = col % 2
    grp = (core + x + row) % 2
    me = row * 4 + col
    mine = pl.ds(pl.multiple_of(grp * nq, nq), nq)
    other = pl.ds(pl.multiple_of((1 - grp) * nq, nq), nq)

    def dev(r, c):
        return (prob, r, c)

    partner = dev(row, 2 * x + 1 - core)
    x_peer = dev(row, 2 * (1 - x) + 1 - core)
    y_peer = dev(1 - row, 2 * x + 1 - core)

    def remote(src, dst, send, recv, to):
        return pltpu.make_async_remote_copy(src_ref=src, dst_ref=dst, send_sem=send, recv_sem=recv,
                                            device_id=to, device_id_type=MESH)

    KP, BP, S0, SS, TT, T0, TP, KC, US, VS, CS = range(11)

    def all_sent(ref, kind):
        remote(ref, ref, send_sem.at[kind], one_recv.at[0], partner).wait_send()

    def all_here(ref, recv):
        remote(ref, ref, send_sem.at[0], recv, partner).wait_recv()

    def krows(i):
        return pl.ds(i * rw, rw)

    k_load = [pltpu.make_async_copy(k_hbm.at[krows(i)], k_buf.at[core, krows(i)], load_sem.at[i]) for i in range(n_chunk)]
    c_load = [pltpu.make_async_copy(c_hbm.at[krows(i)], c_buf.at[krows(i)], load_sem.at[i]) for i in range(n_chunk)]
    a_load = pltpu.make_async_copy(a_hbm, a_buf, load_sem.at[n_chunk])
    b_load = pltpu.make_async_copy(b_hbm.at[mine], b_buf.at[core], load_sem.at[n_chunk + 1])
    for d in k_load:
        d.start()
    a_load.start()
    b_load.start()

    barrier = pltpu.get_barrier_semaphore()
    for dr in range(2):
        for dc in range(4):
            if dr or dc:
                pl.semaphore_signal(barrier, inc=1, device_id=dev((row + dr) % 2, (col + dc) % 4), device_id_type=MESH)

    blk = 256

    def transpose_rows(h, i):
        def body(n, carry):
            jo = pl.multiple_of(n * blk, blk)
            for ii in range(rw // blk):
                kt_buf[pl.ds(pl.multiple_of(h * half + jo, blk), blk), pl.ds(i * rw + ii * blk, blk)] = (
                    k_buf[h, pl.ds(i * rw + ii * blk, blk), pl.ds(jo, blk)].T)
            return carry
        lax.fori_loop(0, half // blk, body, 0)

    kct_pieces = 2 * n_chunk
    kw = rows // kct_pieces

    def build_kct(lo, hi):
        def piece(i, carry):
            rs = pl.ds(pl.multiple_of(i * kw, kw), kw)
            for n in range(half // blk):
                kct_buf[pl.ds(pl.multiple_of(core * half + n * blk, blk), blk), rs] = (
                    k_buf[core, rs, n * blk:(n + 1) * blk] * c_buf[rs, n * blk:(n + 1) * blk]).T
            part = kct_buf.at[pl.ds(pl.multiple_of(core * half, half), half), rs]
            remote(part, part, send_sem.at[KC], one_recv.at[5], partner).start()
            return carry
        lax.fori_loop(lo, hi, piece, 0)

    ahead = grp * (AHEAD[0] + core * (AHEAD[1] - AHEAD[0]))
    middle = grp * kct_pieces + (1 - grp) * (kct_pieces // 2)

    k_push = [remote(k_buf.at[core, krows(i)], k_buf.at[core, krows(i)], send_sem.at[KP], kp_recv.at[i], partner) for i in range(n_chunk)]
    b_push = remote(b_hbm.at[other], b_buf.at[core], send_sem.at[BP], one_recv.at[0], partner)
    pl.semaphore_wait(barrier, 7)
    b_push.start()
    ones = jnp.ones((nq, half), BF16)
    for i in range(n_chunk):
        k_load[i].wait()
        if i == 0:
            k_push[0].start()
        if i % 2:
            part = lax.dot_general(ones, k_buf[core, pl.ds((i - 1) * rw, 2 * rw)], (((1,), (1,)), ((), ())), preferred_element_type=F32)
            for n in range(2 * rw // 128):
                r = (i - 1) * (rw // 128) + n
                s0_buf[col, r:r + 1, :] = part[0:1, n * 128:(n + 1) * 128]
    for n in range(1, 4):
        remote(s0_buf.at[col], s0_buf.at[col], send_sem.at[S0], one_recv.at[1], dev(row, (col + n) % 4)).start()
    for i in range(1, n_chunk):
        k_push[i].start()
    for d in c_load:
        d.start()
    for i in range(n_chunk):
        transpose_rows(core, i)
    a_load.wait()
    b_load.wait()
    all_here(s0_buf.at[0:3], one_recv.at[1])
    s0 = (s0_buf[0] + s0_buf[1]) + (s0_buf[2] + s0_buf[3])
    for r in range(rows // 128):
        cs = slice(r * 128, (r + 1) * 128)
        ub_buf[:, cs] = (a_buf[:, cs] / s0[r:r + 1, :]).astype(BF16)

    def t_copy(par, o):
        return remote(t_out.at[o], t_in.at[par, o], send_sem.at[TT], t_recv.at[par, o], y_peer)

    def s_copy(par, o):
        return remote(s_out.at[o], s_in.at[par, o], send_sem.at[SS], s_recv.at[par, o], x_peer)

    def t0_send(g, n):
        remote(t0_buf.at[g, n], t_in.at[0, core * per_half + n], send_sem.at[T0], t_recv.at[0, core * per_half + n],
               dev(1 - row, 2 * x + (g + x + 1 - row) % 2)).start()

    for n in range(per_half):
        part = jnp.dot(ub_buf[...], k_buf[core, :, n * cw:(n + 1) * cw], preferred_element_type=F32)
        for g in range(2):
            t0_buf[g, n] = part[g * nq:(g + 1) * nq]
        t0_send(0, n)
    for n in range(per_half):
        o = core * per_half + n
        remote(t0_buf.at[1 - grp, n], t_out.at[o], send_sem.at[TP], one_recv.at[2], partner).start()
        t_out[o] = t0_buf[grp, n]

    def v_of(par, o):
        return b_buf[o // per_half, :, (o % per_half) * cw:(o % per_half + 1) * cw] / (t_out[o] + t_in[par, o])

    all_here(b_buf.at[0], one_recv.at[0])
    for i in range(n_chunk):
        all_here(k_buf.at[1 - core, krows(i)], kp_recv.at[i])
        transpose_rows(1 - core, i)
        if i == 0:
            for n in range(per_half):
                t0_send(1, n)

    for d in c_load:
        d.wait()
    build_kct(0, ahead)

    @pl.when(grp == 1)
    def _():
        pl.delay(WAIT_NS)

    all_here(t0_buf.at[0], one_recv.at[2])
    order = list(range(per_half, n_chunk)) + list(range(per_half))
    for c in order:
        all_here(t_in.at[0, c], t_recv.at[0, c])
        vb = v_of(0, c).astype(BF16)
        js = slice(c * cw, (c + 1) * cw)
        if c != order[-1]:
            prod = jnp.dot(vb, kt_buf[js, :], preferred_element_type=F32)
            acc[...] = prod if c == order[0] else acc[...] + prod
        else:
            for o in range(n_chunk):
                s_out[o] = acc[:, o * rw:(o + 1) * rw] + jnp.dot(vb, kt_buf[js, o * rw:(o + 1) * rw], preferred_element_type=F32)
                s_copy(1, o).start()
    all_sent(t0_buf, T0)
    all_sent(t0_buf.at[0], TP)
    all_sent(s0_buf.at[0:3], S0)
    all_sent(k_buf.at[0], KP)
    all_sent(b_buf.at[0], BP)

    build_kct(ahead, middle)

    def u_and_t(par):
        for c in range(n_chunk):
            all_here(s_in.at[par, c], s_recv.at[par, c])
            w = slice(c * rw, (c + 1) * rw)
            u = a_buf[mine, w] / (s_out[c] + s_in[par, c])
            u_out[mine, w] = u
            ub = u.astype(BF16)
            if c < n_chunk - 1:
                for h in range(2):
                    hc = slice(h * half, (h + 1) * half)
                    prod = jnp.dot(ub, k_buf[h, w, :], preferred_element_type=F32)
                    acc[:, hc] = prod if c == 0 else acc[:, hc] + prod
            else:
                for o in range(n_chunk):
                    oc = slice(o * cw, (o + 1) * cw)
                    hc = slice((o % per_half) * cw, (o % per_half + 1) * cw)
                    t_out[o] = acc[:, oc] + jnp.dot(ub, k_buf[o // per_half, w, hc], preferred_element_type=F32)
                    t_copy(par, o).start()
                all_sent(s_out, SS)

    def v_and_s(par_in, par):
        for c in range(n_chunk):
            all_here(t_in.at[par_in, c], t_recv.at[par_in, c])
            vb = v_of(par_in, c).astype(BF16)
            w = slice(c * cw, (c + 1) * cw)
            if c < n_chunk - 1:
                prod = jnp.dot(vb, kt_buf[w, :], preferred_element_type=F32)
                acc[...] = prod if c == 0 else acc[...] + prod
            else:
                for o in range(n_chunk):
                    oc = slice(o * rw, (o + 1) * rw)
                    s_out[o] = acc[:, oc] + jnp.dot(vb, kt_buf[w, oc], preferred_element_type=F32)
                    s_copy(par, o).start()
                all_sent(t_out, TT)

    def sweep(t, carry):
        u_and_t(t % 2)

        @pl.when(t == 1)
        def _():
            build_kct(middle, kct_pieces)

        v_and_s(t % 2, (t + 1) % 2)
        return carry

    lax.fori_loop(1, SWEEPS - 1, sweep, 0)
    last = (SWEEPS - 1) % 2
    u_and_t(last)

    u_push = remote(u_out.at[mine], u_out.at[mine], send_sem.at[US], one_recv.at[3], partner)
    u_push.start()
    cost_part[...] = jnp.zeros_like(cost_part)
    all_here(kct_buf.at[0:half], one_recv.at[5])
    all_sent(kct_buf.at[0:half], KC)
    for c in range(n_chunk):
        all_here(t_in.at[last, c], t_recv.at[last, c])
        v = v_of(last, c)
        v_all[c // per_half, :, (c % per_half) * cw:(c % per_half + 1) * cw] = v
        prod = jnp.dot(v.astype(BF16), kct_buf[c * cw:(c + 1) * cw, :], preferred_element_type=F32)
        if c < n_chunk - 1:
            acc[...] = prod if c == 0 else acc[...] + prod
        else:
            w = (acc[...] + prod) * u_out[mine]
    v_push = remote(v_all.at[1 - core], v_out.at[mine], send_sem.at[VS], one_recv.at[4], partner)
    v_push.start()
    tot = w[:, 0:128]
    for n in range(1, rows // 128):
        tot = tot + w[:, n * 128:(n + 1) * 128]
    cost_part[mine] = tot
    cost_all[me] = jnp.sum(cost_part[...].T, axis=0, keepdims=True)
    for dr in range(2):
        for dc in range(4):
            if dr or dc:
                remote(cost_all.at[me], cost_all.at[me], send_sem.at[CS], one_recv.at[6], dev((row + dr) % 2, (col + dc) % 4)).start()
    v_out[mine] = v_all[core]
    all_sent(t_out, TT)
    all_here(u_out.at[other], one_recv.at[3])
    u_push.wait_send()
    all_here(v_out.at[other], one_recv.at[4])
    v_push.wait_send()
    all_here(cost_all.at[0:7], one_recv.at[6])
    all_sent(cost_all.at[0:7], CS)


def output_kernel(norm, u_ref, v_ref, c_ref, u_hbm, v_hbm, cost_ref, sem):
    stores = [pltpu.make_async_copy(u_ref, u_hbm, sem.at[0]), pltpu.make_async_copy(v_ref, v_hbm, sem.at[1])]
    for d in stores:
        d.start()
    total = c_ref[0]
    for n in range(1, 8):
        total = total + c_ref[n]
    cost_ref[...] = total[:, :cost_ref.shape[1]] * norm
    for d in stores:
        d.wait()


def solution(mesh):
    n_chunk = 4

    def local_fn(kernel, cost_mat, src_mass, tgt_mass):
        rows, half = kernel.shape
        nprob = src_mass.shape[1]
        nq = nprob // 2
        cols = 2 * half
        rw, cw = rows // n_chunk, cols // n_chunk
        norm = 1.0 / float(rows * mesh.shape["row"] * half * mesh.shape["col"])
        vmem_spec = pl.BlockSpec(memory_space=pltpu.VMEM)
        any_spec = pl.BlockSpec(memory_space=pl.ANY)
        dma = pltpu.SemaphoreType.DMA
        u_vm, v_vm, c_vm = pl.pallas_call(
            lambda *refs: sinkhorn_kernel(n_chunk, *refs),
            out_shape=(pltpu.VMEM((nprob, rows), F32), pltpu.VMEM((nprob, half), F32), pltpu.VMEM((8, 1, 128), F32)),
            in_specs=[any_spec] * 4,
            out_specs=(vmem_spec, vmem_spec, vmem_spec),
            scratch_shapes=[
                pltpu.VMEM((2, rows, half), BF16),
                pltpu.VMEM((cols, rows), BF16),
                pltpu.VMEM((rows, half), BF16),
                pltpu.VMEM((cols, rows), BF16),
                pltpu.VMEM((nprob, rows), F32),
                pltpu.VMEM((2, nq, half), F32),
                pltpu.VMEM((nprob, rows), BF16),
                pltpu.VMEM((nq, max(rows, cols)), F32),
                pltpu.VMEM((n_chunk, nq, rw), F32),
                pltpu.VMEM((2, n_chunk, nq, rw), F32),
                pltpu.VMEM((n_chunk, nq, cw), F32),
                pltpu.VMEM((2, n_chunk, nq, cw), F32),
                pltpu.VMEM((2, n_chunk // 2, nq, cw), F32),
                pltpu.VMEM((4, rows // 128, 128), F32),
                pltpu.VMEM((2, nq, half), F32),
                pltpu.VMEM((128, 128), F32),
                dma((n_chunk + 2,)), dma((11,)), dma((n_chunk,)), dma((2, n_chunk)), dma((2, n_chunk)), dma((7,)),
            ],
            compiler_params=pltpu.CompilerParams(collective_id=0, has_side_effects=True, vmem_limit_bytes=60 * 1024 * 1024),
            name="sinkhorn",
        )(kernel, cost_mat, src_mass.T, tgt_mass.T)
        u_t, v_t, cost = pl.pallas_call(
            lambda *refs: output_kernel(norm, *refs),
            out_shape=(jax.ShapeDtypeStruct((nprob, rows), F32), jax.ShapeDtypeStruct((nprob, half), F32),
                       jax.ShapeDtypeStruct((1, nprob), F32)),
            in_specs=[vmem_spec] * 3,
            out_specs=(any_spec, any_spec, vmem_spec),
            scratch_shapes=[dma((2,))],
            name="outputs",
        )(*(pltpu.with_memory_space_constraint(r, pltpu.VMEM) for r in (u_vm, v_vm, c_vm)))
        return u_t.T, v_t.T, cost.reshape(nprob)

    return jax.shard_map(local_fn, mesh=mesh, in_specs=(P("row", "col"), P("row", "col"), P("row", "prob"), P("col", "prob")), out_specs=(P("row", "prob"), P("col", "prob"), P("prob")), check_vma=False)
```

```python
import jax
import jax.numpy as jnp
from jax import lax
from jax.experimental import pallas as pl
from jax.experimental.pallas import tpu as pltpu
from jax.sharding import PartitionSpec as P

SWEEPS = 6
AHEAD = (8, 7)
WAIT_NS = ((0, 350), (650, 600))
F32 = jnp.float32
BF16 = jnp.bfloat16
MESH = pl.DeviceIdType.MESH


def sinkhorn_kernel(n_chunk, k_hbm, c_hbm, a_hbm, b_hbm, u_out, v_out, cost_all,
                    k_buf, kt_buf, c_buf, kct_buf, a_buf, b_buf, ub_buf, acc,
                    s_out, s_in, t_out, t_in, t0_buf, s0_buf, v_all, cost_part,
                    load_sem, send_sem, kp_recv, s_recv, t_recv, one_recv):
    rows, half = k_hbm.shape
    cols = 2 * half
    rw = rows // n_chunk
    cw = cols // n_chunk
    per_half = n_chunk // 2
    nq = b_buf.shape[1]
    row = lax.axis_index("row")
    col = lax.axis_index("col")
    prob = lax.axis_index("prob")
    x = col // 2
    core = col % 2
    grp = (core + x + row) % 2
    me = row * 4 + col
    mine = pl.ds(pl.multiple_of(grp * nq, nq), nq)
    other = pl.ds(pl.multiple_of((1 - grp) * nq, nq), nq)

    def dev(r, c):
        return (prob, r, c)

    partner = dev(row, 2 * x + 1 - core)
    x_peer = dev(row, 2 * (1 - x) + 1 - core)
    y_peer = dev(1 - row, 2 * x + 1 - core)

    def remote(src, dst, send, recv, to):
        return pltpu.make_async_remote_copy(src_ref=src, dst_ref=dst, send_sem=send, recv_sem=recv,
                                            device_id=to, device_id_type=MESH)

    KP, BP, S0, SS, TT, T0, TP, KC, US, VS, CS = range(11)

    def all_sent(ref, kind):
        remote(ref, ref, send_sem.at[kind], one_recv.at[0], partner).wait_send()

    def all_here(ref, recv):
        remote(ref, ref, send_sem.at[0], recv, partner).wait_recv()

    def krows(i):
        return pl.ds(i * rw, rw)

    k_load = [pltpu.make_async_copy(k_hbm.at[krows(i)], k_buf.at[core, krows(i)], load_sem.at[i]) for i in range(n_chunk)]
    c_load = [pltpu.make_async_copy(c_hbm.at[krows(i)], c_buf.at[krows(i)], load_sem.at[i]) for i in range(n_chunk)]
    a_load = pltpu.make_async_copy(a_hbm, a_buf, load_sem.at[n_chunk])
    b_load = pltpu.make_async_copy(b_hbm.at[mine], b_buf.at[core], load_sem.at[n_chunk + 1])
    for d in k_load:
        d.start()
    a_load.start()
    b_load.start()

    barrier = pltpu.get_barrier_semaphore()
    for dr in range(2):
        for dc in range(4):
            if dr or dc:
                pl.semaphore_signal(barrier, inc=1, device_id=dev((row + dr) % 2, (col + dc) % 4), device_id_type=MESH)

    blk = 256

    def transpose_rows(h, i):
        def body(n, carry):
            jo = pl.multiple_of(n * blk, blk)
            for ii in range(rw // blk):
                kt_buf[pl.ds(pl.multiple_of(h * half + jo, blk), blk), pl.ds(i * rw + ii * blk, blk)] = (
                    k_buf[h, pl.ds(i * rw + ii * blk, blk), pl.ds(jo, blk)].T)
            return carry
        lax.fori_loop(0, half // blk, body, 0)

    kct_pieces = 2 * n_chunk
    kw = rows // kct_pieces

    def build_kct(lo, hi):
        def piece(i, carry):
            rs = pl.ds(pl.multiple_of(i * kw, kw), kw)
            for n in range(half // blk):
                kct_buf[pl.ds(pl.multiple_of(core * half + n * blk, blk), blk), rs] = (
                    k_buf[core, rs, n * blk:(n + 1) * blk] * c_buf[rs, n * blk:(n + 1) * blk]).T
            part = kct_buf.at[pl.ds(pl.multiple_of(core * half, half), half), rs]
            remote(part, part, send_sem.at[KC], one_recv.at[5], partner).start()
            return carry
        lax.fori_loop(lo, hi, piece, 0)

    ahead = grp * (AHEAD[0] + core * (AHEAD[1] - AHEAD[0]))
    middle = grp * kct_pieces + (1 - grp) * (kct_pieces // 2)

    k_push = [remote(k_buf.at[core, krows(i)], k_buf.at[core, krows(i)], send_sem.at[KP], kp_recv.at[i], partner) for i in range(n_chunk)]
    b_push = remote(b_hbm.at[other], b_buf.at[core], send_sem.at[BP], one_recv.at[0], partner)
    pl.semaphore_wait(barrier, 7)
    b_push.start()
    ones = jnp.ones((nq, half), BF16)
    for i in range(n_chunk):
        k_load[i].wait()
        if i == 0:
            k_push[0].start()
        if i % 2:
            part = lax.dot_general(ones, k_buf[core, pl.ds((i - 1) * rw, 2 * rw)], (((1,), (1,)), ((), ())), preferred_element_type=F32)
            for n in range(2 * rw // 128):
                r = (i - 1) * (rw // 128) + n
                s0_buf[col, r:r + 1, :] = part[0:1, n * 128:(n + 1) * 128]
    for n in range(1, 4):
        remote(s0_buf.at[col], s0_buf.at[col], send_sem.at[S0], one_recv.at[1], dev(row, (col + n) % 4)).start()
    for i in range(1, n_chunk):
        k_push[i].start()
    for d in c_load:
        d.start()
    for i in range(n_chunk):
        transpose_rows(core, i)
    a_load.wait()
    b_load.wait()
    all_here(s0_buf.at[0:3], one_recv.at[1])
    s0 = (s0_buf[0] + s0_buf[1]) + (s0_buf[2] + s0_buf[3])
    for r in range(rows // 128):
        cs = slice(r * 128, (r + 1) * 128)
        ub_buf[:, cs] = (a_buf[:, cs] / s0[r:r + 1, :]).astype(BF16)

    def t_copy(par, o):
        return remote(t_out.at[o], t_in.at[par, o], send_sem.at[TT], t_recv.at[par, o], y_peer)

    def s_copy(par, o):
        return remote(s_out.at[o], s_in.at[par, o], send_sem.at[SS], s_recv.at[par, o], x_peer)

    def t0_send(g, n):
        remote(t0_buf.at[g, n], t_in.at[0, core * per_half + n], send_sem.at[T0], t_recv.at[0, core * per_half + n],
               dev(1 - row, 2 * x + (g + x + 1 - row) % 2)).start()

    for n in range(per_half):
        part = jnp.dot(ub_buf[...], k_buf[core, :, n * cw:(n + 1) * cw], preferred_element_type=F32)
        for g in range(2):
            t0_buf[g, n] = part[g * nq:(g + 1) * nq]
        t0_send(0, n)
    for n in range(per_half):
        o = core * per_half + n
        remote(t0_buf.at[1 - grp, n], t_out.at[o], send_sem.at[TP], one_recv.at[2], partner).start()
        t_out[o] = t0_buf[grp, n]

    def v_of(par, o):
        return b_buf[o // per_half, :, (o % per_half) * cw:(o % per_half + 1) * cw] / (t_out[o] + t_in[par, o])

    all_here(b_buf.at[0], one_recv.at[0])
    for i in range(n_chunk):
        all_here(k_buf.at[1 - core, krows(i)], kp_recv.at[i])
        transpose_rows(1 - core, i)
        if i == 0:
            for n in range(per_half):
                t0_send(1, n)

    for d in c_load:
        d.wait()
    build_kct(0, ahead)

    for g in range(2):
        for c in range(2):
            if WAIT_NS[g][c]:
                @pl.when((grp == g) & (core == c))
                def _(g=g, c=c):
                    pl.delay(WAIT_NS[g][c])

    all_here(t0_buf.at[0], one_recv.at[2])
    order = list(range(per_half, n_chunk)) + list(range(per_half))
    for c in order:
        all_here(t_in.at[0, c], t_recv.at[0, c])
        vb = v_of(0, c).astype(BF16)
        js = slice(c * cw, (c + 1) * cw)
        if c != order[-1]:
            prod = jnp.dot(vb, kt_buf[js, :], preferred_element_type=F32)
            acc[...] = prod if c == order[0] else acc[...] + prod
        else:
            for o in range(n_chunk):
                s_out[o] = acc[:, o * rw:(o + 1) * rw] + jnp.dot(vb, kt_buf[js, o * rw:(o + 1) * rw], preferred_element_type=F32)
                s_copy(1, o).start()
    all_sent(t0_buf, T0)
    all_sent(t0_buf.at[0], TP)
    all_sent(s0_buf.at[0:3], S0)
    all_sent(k_buf.at[0], KP)
    all_sent(b_buf.at[0], BP)

    build_kct(ahead, middle)

    def u_and_t(par):
        for c in range(n_chunk):
            all_here(s_in.at[par, c], s_recv.at[par, c])
            w = slice(c * rw, (c + 1) * rw)
            u = a_buf[mine, w] / (s_out[c] + s_in[par, c])
            u_out[mine, w] = u
            ub = u.astype(BF16)
            if c < n_chunk - 1:
                for h in range(2):
                    hc = slice(h * half, (h + 1) * half)
                    prod = jnp.dot(ub, k_buf[h, w, :], preferred_element_type=F32)
                    acc[:, hc] = prod if c == 0 else acc[:, hc] + prod
            else:
                for o in range(n_chunk):
                    oc = slice(o * cw, (o + 1) * cw)
                    hc = slice((o % per_half) * cw, (o % per_half + 1) * cw)
                    t_out[o] = acc[:, oc] + jnp.dot(ub, k_buf[o // per_half, w, hc], preferred_element_type=F32)
                    t_copy(par, o).start()
                all_sent(s_out, SS)

    def v_and_s(par_in, par):
        for c in range(n_chunk):
            all_here(t_in.at[par_in, c], t_recv.at[par_in, c])
            vb = v_of(par_in, c).astype(BF16)
            w = slice(c * cw, (c + 1) * cw)
            if c < n_chunk - 1:
                prod = jnp.dot(vb, kt_buf[w, :], preferred_element_type=F32)
                acc[...] = prod if c == 0 else acc[...] + prod
            else:
                for o in range(n_chunk):
                    oc = slice(o * rw, (o + 1) * rw)
                    s_out[o] = acc[:, oc] + jnp.dot(vb, kt_buf[w, oc], preferred_element_type=F32)
                    s_copy(par, o).start()
                all_sent(t_out, TT)

    def sweep(t, carry):
        u_and_t(t % 2)

        @pl.when(t == 1)
        def _():
            build_kct(middle, kct_pieces)

        v_and_s(t % 2, (t + 1) % 2)
        return carry

    lax.fori_loop(1, SWEEPS - 1, sweep, 0)
    last = (SWEEPS - 1) % 2
    u_and_t(last)

    u_push = remote(u_out.at[mine], u_out.at[mine], send_sem.at[US], one_recv.at[3], partner)
    u_push.start()
    cost_part[...] = jnp.zeros_like(cost_part)
    all_here(kct_buf.at[0:half], one_recv.at[5])
    all_sent(kct_buf.at[0:half], KC)
    for c in range(n_chunk):
        all_here(t_in.at[last, c], t_recv.at[last, c])
        v = v_of(last, c)
        v_all[c // per_half, :, (c % per_half) * cw:(c % per_half + 1) * cw] = v
        prod = jnp.dot(v.astype(BF16), kct_buf[c * cw:(c + 1) * cw, :], preferred_element_type=F32)
        if c < n_chunk - 1:
            acc[...] = prod if c == 0 else acc[...] + prod
        else:
            w = (acc[...] + prod) * u_out[mine]
    v_push = remote(v_all.at[1 - core], v_out.at[mine], send_sem.at[VS], one_recv.at[4], partner)
    v_push.start()
    tot = w[:, 0:128]
    for n in range(1, rows // 128):
        tot = tot + w[:, n * 128:(n + 1) * 128]
    cost_part[mine] = tot
    cost_all[me] = jnp.sum(cost_part[...].T, axis=0, keepdims=True)
    for dr in range(2):
        for dc in range(4):
            if dr or dc:
                remote(cost_all.at[me], cost_all.at[me], send_sem.at[CS], one_recv.at[6], dev((row + dr) % 2, (col + dc) % 4)).start()
    v_out[mine] = v_all[core]
    all_sent(t_out, TT)
    all_here(u_out.at[other], one_recv.at[3])
    u_push.wait_send()
    all_here(v_out.at[other], one_recv.at[4])
    v_push.wait_send()
    all_here(cost_all.at[0:7], one_recv.at[6])
    all_sent(cost_all.at[0:7], CS)


def output_kernel(norm, u_ref, v_ref, c_ref, u_hbm, v_hbm, cost_ref, sem):
    stores = [pltpu.make_async_copy(u_ref, u_hbm, sem.at[0]), pltpu.make_async_copy(v_ref, v_hbm, sem.at[1])]
    for d in stores:
        d.start()
    total = c_ref[0]
    for n in range(1, 8):
        total = total + c_ref[n]
    cost_ref[...] = total[:, :cost_ref.shape[1]] * norm
    for d in stores:
        d.wait()


def solution(mesh):
    n_chunk = 4

    def local_fn(kernel, cost_mat, src_mass, tgt_mass):
        rows, half = kernel.shape
        nprob = src_mass.shape[1]
        nq = nprob // 2
        cols = 2 * half
        rw, cw = rows // n_chunk, cols // n_chunk
        norm = 1.0 / float(rows * mesh.shape["row"] * half * mesh.shape["col"])
        vmem_spec = pl.BlockSpec(memory_space=pltpu.VMEM)
        any_spec = pl.BlockSpec(memory_space=pl.ANY)
        dma = pltpu.SemaphoreType.DMA
        u_vm, v_vm, c_vm = pl.pallas_call(
            lambda *refs: sinkhorn_kernel(n_chunk, *refs),
            out_shape=(pltpu.VMEM((nprob, rows), F32), pltpu.VMEM((nprob, half), F32), pltpu.VMEM((8, 1, 128), F32)),
            in_specs=[any_spec] * 4,
            out_specs=(vmem_spec, vmem_spec, vmem_spec),
            scratch_shapes=[
                pltpu.VMEM((2, rows, half), BF16),
                pltpu.VMEM((cols, rows), BF16),
                pltpu.VMEM((rows, half), BF16),
                pltpu.VMEM((cols, rows), BF16),
                pltpu.VMEM((nprob, rows), F32),
                pltpu.VMEM((2, nq, half), F32),
                pltpu.VMEM((nprob, rows), BF16),
                pltpu.VMEM((nq, max(rows, cols)), F32),
                pltpu.VMEM((n_chunk, nq, rw), F32),
                pltpu.VMEM((2, n_chunk, nq, rw), F32),
                pltpu.VMEM((n_chunk, nq, cw), F32),
                pltpu.VMEM((2, n_chunk, nq, cw), F32),
                pltpu.VMEM((2, n_chunk // 2, nq, cw), F32),
                pltpu.VMEM((4, rows // 128, 128), F32),
                pltpu.VMEM((2, nq, half), F32),
                pltpu.VMEM((128, 128), F32),
                dma((n_chunk + 2,)), dma((11,)), dma((n_chunk,)), dma((2, n_chunk)), dma((2, n_chunk)), dma((7,)),
            ],
            compiler_params=pltpu.CompilerParams(collective_id=0, has_side_effects=True, vmem_limit_bytes=60 * 1024 * 1024),
            name="sinkhorn",
        )(kernel, cost_mat, src_mass.T, tgt_mass.T)
        u_t, v_t, cost = pl.pallas_call(
            lambda *refs: output_kernel(norm, *refs),
            out_shape=(jax.ShapeDtypeStruct((nprob, rows), F32), jax.ShapeDtypeStruct((nprob, half), F32),
                       jax.ShapeDtypeStruct((1, nprob), F32)),
            in_specs=[vmem_spec] * 3,
            out_specs=(any_spec, any_spec, vmem_spec),
            scratch_shapes=[dma((2,))],
            name="outputs",
        )(*(pltpu.with_memory_space_constraint(r, pltpu.VMEM) for r in (u_vm, v_vm, c_vm)))
        return u_t.T, v_t.T, cost.reshape(nprob)

    return jax.shard_map(local_fn, mesh=mesh, in_specs=(P("row", "col"), P("row", "col"), P("row", "prob"), P("col", "prob")), out_specs=(P("row", "prob"), P("col", "prob"), P("prob")), check_vma=False)
```

```python
import jax
import jax.numpy as jnp
from jax import lax
from jax.experimental import pallas as pl
from jax.experimental.pallas import tpu as pltpu
from jax.sharding import PartitionSpec as P

SWEEPS = 6
AHEAD = (8, 7)
WAIT_NS = ((0, 700), (650, 600))
F32 = jnp.float32
BF16 = jnp.bfloat16
MESH = pl.DeviceIdType.MESH


def sinkhorn_kernel(n_chunk, k_hbm, c_hbm, a_hbm, b_hbm, u_out, v_out, cost_all,
                    k_buf, kt_buf, c_buf, kct_buf, a_buf, b_buf, ub_buf, acc,
                    s_out, s_in, t_out, t_in, t0_buf, s0_buf, v_all, cost_part,
                    load_sem, send_sem, kp_recv, s_recv, t_recv, one_recv):
    rows, half = k_hbm.shape
    cols = 2 * half
    rw = rows // n_chunk
    cw = cols // n_chunk
    per_half = n_chunk // 2
    nq = b_buf.shape[1]
    row = lax.axis_index("row")
    col = lax.axis_index("col")
    prob = lax.axis_index("prob")
    x = col // 2
    core = col % 2
    grp = (core + x + row) % 2
    me = row * 4 + col
    mine = pl.ds(pl.multiple_of(grp * nq, nq), nq)
    other = pl.ds(pl.multiple_of((1 - grp) * nq, nq), nq)

    def dev(r, c):
        return (prob, r, c)

    partner = dev(row, 2 * x + 1 - core)
    x_peer = dev(row, 2 * (1 - x) + 1 - core)
    y_peer = dev(1 - row, 2 * x + 1 - core)

    def remote(src, dst, send, recv, to):
        return pltpu.make_async_remote_copy(src_ref=src, dst_ref=dst, send_sem=send, recv_sem=recv,
                                            device_id=to, device_id_type=MESH)

    KP, BP, S0, SS, TT, T0, TP, KC, US, VS, CS = range(11)

    def all_sent(ref, kind):
        remote(ref, ref, send_sem.at[kind], one_recv.at[0], partner).wait_send()

    def all_here(ref, recv):
        remote(ref, ref, send_sem.at[0], recv, partner).wait_recv()

    def krows(i):
        return pl.ds(i * rw, rw)

    k_load = [pltpu.make_async_copy(k_hbm.at[krows(i)], k_buf.at[core, krows(i)], load_sem.at[i]) for i in range(n_chunk)]
    c_load = [pltpu.make_async_copy(c_hbm.at[krows(i)], c_buf.at[krows(i)], load_sem.at[i]) for i in range(n_chunk)]
    a_load = pltpu.make_async_copy(a_hbm, a_buf, load_sem.at[n_chunk])
    b_load = pltpu.make_async_copy(b_hbm.at[mine], b_buf.at[core], load_sem.at[n_chunk + 1])
    for d in k_load:
        d.start()
    a_load.start()
    b_load.start()

    barrier = pltpu.get_barrier_semaphore()
    for dr in range(2):
        for dc in range(4):
            if dr or dc:
                pl.semaphore_signal(barrier, inc=1, device_id=dev((row + dr) % 2, (col + dc) % 4), device_id_type=MESH)

    blk = 256

    def transpose_rows(h, i):
        def body(n, carry):
            jo = pl.multiple_of(n * blk, blk)
            for ii in range(rw // blk):
                kt_buf[pl.ds(pl.multiple_of(h * half + jo, blk), blk), pl.ds(i * rw + ii * blk, blk)] = (
                    k_buf[h, pl.ds(i * rw + ii * blk, blk), pl.ds(jo, blk)].T)
            return carry
        lax.fori_loop(0, half // blk, body, 0)

    kct_pieces = 2 * n_chunk
    kw = rows // kct_pieces

    def build_kct(lo, hi):
        def piece(i, carry):
            rs = pl.ds(pl.multiple_of(i * kw, kw), kw)
            for n in range(half // blk):
                kct_buf[pl.ds(pl.multiple_of(core * half + n * blk, blk), blk), rs] = (
                    k_buf[core, rs, n * blk:(n + 1) * blk] * c_buf[rs, n * blk:(n + 1) * blk]).T
            part = kct_buf.at[pl.ds(pl.multiple_of(core * half, half), half), rs]
            remote(part, part, send_sem.at[KC], one_recv.at[5], partner).start()
            return carry
        lax.fori_loop(lo, hi, piece, 0)

    ahead = grp * (AHEAD[0] + core * (AHEAD[1] - AHEAD[0]))
    middle = grp * kct_pieces + (1 - grp) * (kct_pieces // 2)

    k_push = [remote(k_buf.at[core, krows(i)], k_buf.at[core, krows(i)], send_sem.at[KP], kp_recv.at[i], partner) for i in range(n_chunk)]
    b_push = remote(b_hbm.at[other], b_buf.at[core], send_sem.at[BP], one_recv.at[0], partner)
    pl.semaphore_wait(barrier, 7)
    b_push.start()
    ones = jnp.ones((nq, half), BF16)
    for i in range(n_chunk):
        k_load[i].wait()
        if i == 0:
            k_push[0].start()
        if i % 2:
            part = lax.dot_general(ones, k_buf[core, pl.ds((i - 1) * rw, 2 * rw)], (((1,), (1,)), ((), ())), preferred_element_type=F32)
            for n in range(2 * rw // 128):
                r = (i - 1) * (rw // 128) + n
                s0_buf[col, r:r + 1, :] = part[0:1, n * 128:(n + 1) * 128]
    for n in range(1, 4):
        remote(s0_buf.at[col], s0_buf.at[col], send_sem.at[S0], one_recv.at[1], dev(row, (col + n) % 4)).start()
    for i in range(1, n_chunk):
        k_push[i].start()
    for d in c_load:
        d.start()
    for i in range(n_chunk):
        transpose_rows(core, i)
    a_load.wait()
    b_load.wait()
    all_here(s0_buf.at[0:3], one_recv.at[1])
    s0 = (s0_buf[0] + s0_buf[1]) + (s0_buf[2] + s0_buf[3])
    for r in range(rows // 128):
        cs = slice(r * 128, (r + 1) * 128)
        ub_buf[:, cs] = (a_buf[:, cs] / s0[r:r + 1, :]).astype(BF16)

    def t_copy(par, o):
        return remote(t_out.at[o], t_in.at[par, o], send_sem.at[TT], t_recv.at[par, o], y_peer)

    def s_copy(par, o):
        return remote(s_out.at[o], s_in.at[par, o], send_sem.at[SS], s_recv.at[par, o], x_peer)

    def t0_send(g, n):
        remote(t0_buf.at[g, n], t_in.at[0, core * per_half + n], send_sem.at[T0], t_recv.at[0, core * per_half + n],
               dev(1 - row, 2 * x + (g + x + 1 - row) % 2)).start()

    for n in range(per_half):
        part = jnp.dot(ub_buf[...], k_buf[core, :, n * cw:(n + 1) * cw], preferred_element_type=F32)
        for g in range(2):
            t0_buf[g, n] = part[g * nq:(g + 1) * nq]
        t0_send(0, n)
    for n in range(per_half):
        o = core * per_half + n
        remote(t0_buf.at[1 - grp, n], t_out.at[o], send_sem.at[TP], one_recv.at[2], partner).start()
        t_out[o] = t0_buf[grp, n]

    def v_of(par, o):
        return b_buf[o // per_half, :, (o % per_half) * cw:(o % per_half + 1) * cw] / (t_out[o] + t_in[par, o])

    all_here(b_buf.at[0], one_recv.at[0])
    for i in range(n_chunk):
        all_here(k_buf.at[1 - core, krows(i)], kp_recv.at[i])
        transpose_rows(1 - core, i)
        if i == 0:
            for n in range(per_half):
                t0_send(1, n)

    for d in c_load:
        d.wait()
    build_kct(0, ahead)

    for g in range(2):
        for c in range(2):
            if WAIT_NS[g][c]:
                @pl.when((grp == g) & (core == c))
                def _(g=g, c=c):
                    pl.delay(WAIT_NS[g][c])

    all_here(t0_buf.at[0], one_recv.at[2])
    order = list(range(per_half, n_chunk)) + list(range(per_half))
    for c in order:
        all_here(t_in.at[0, c], t_recv.at[0, c])
        vb = v_of(0, c).astype(BF16)
        js = slice(c * cw, (c + 1) * cw)
        if c != order[-1]:
            prod = jnp.dot(vb, kt_buf[js, :], preferred_element_type=F32)
            acc[...] = prod if c == order[0] else acc[...] + prod
        else:
            for o in range(n_chunk):
                s_out[o] = acc[:, o * rw:(o + 1) * rw] + jnp.dot(vb, kt_buf[js, o * rw:(o + 1) * rw], preferred_element_type=F32)
                s_copy(1, o).start()
    all_sent(t0_buf, T0)
    all_sent(t0_buf.at[0], TP)
    all_sent(s0_buf.at[0:3], S0)
    all_sent(k_buf.at[0], KP)
    all_sent(b_buf.at[0], BP)

    build_kct(ahead, middle)

    def u_and_t(par):
        for c in range(n_chunk):
            all_here(s_in.at[par, c], s_recv.at[par, c])
            w = slice(c * rw, (c + 1) * rw)
            u = a_buf[mine, w] / (s_out[c] + s_in[par, c])
            u_out[mine, w] = u
            ub = u.astype(BF16)
            if c < n_chunk - 1:
                for h in range(2):
                    hc = slice(h * half, (h + 1) * half)
                    prod = jnp.dot(ub, k_buf[h, w, :], preferred_element_type=F32)
                    acc[:, hc] = prod if c == 0 else acc[:, hc] + prod
            else:
                for o in range(n_chunk):
                    oc = slice(o * cw, (o + 1) * cw)
                    hc = slice((o % per_half) * cw, (o % per_half + 1) * cw)
                    t_out[o] = acc[:, oc] + jnp.dot(ub, k_buf[o // per_half, w, hc], preferred_element_type=F32)
                    t_copy(par, o).start()
                all_sent(s_out, SS)

    def v_and_s(par_in, par):
        for c in range(n_chunk):
            all_here(t_in.at[par_in, c], t_recv.at[par_in, c])
            vb = v_of(par_in, c).astype(BF16)
            w = slice(c * cw, (c + 1) * cw)
            if c < n_chunk - 1:
                prod = jnp.dot(vb, kt_buf[w, :], preferred_element_type=F32)
                acc[...] = prod if c == 0 else acc[...] + prod
            else:
                for o in range(n_chunk):
                    oc = slice(o * rw, (o + 1) * rw)
                    s_out[o] = acc[:, oc] + jnp.dot(vb, kt_buf[w, oc], preferred_element_type=F32)
                    s_copy(par, o).start()
                all_sent(t_out, TT)

    def sweep(t, carry):
        u_and_t(t % 2)

        @pl.when(t == 1)
        def _():
            build_kct(middle, kct_pieces)

        v_and_s(t % 2, (t + 1) % 2)
        return carry

    lax.fori_loop(1, SWEEPS - 1, sweep, 0)
    last = (SWEEPS - 1) % 2
    u_and_t(last)

    u_push = remote(u_out.at[mine], u_out.at[mine], send_sem.at[US], one_recv.at[3], partner)
    u_push.start()
    cost_part[...] = jnp.zeros_like(cost_part)
    all_here(kct_buf.at[0:half], one_recv.at[5])
    all_sent(kct_buf.at[0:half], KC)
    for c in range(n_chunk):
        all_here(t_in.at[last, c], t_recv.at[last, c])
        v = v_of(last, c)
        v_all[c // per_half, :, (c % per_half) * cw:(c % per_half + 1) * cw] = v
        prod = jnp.dot(v.astype(BF16), kct_buf[c * cw:(c + 1) * cw, :], preferred_element_type=F32)
        if c < n_chunk - 1:
            acc[...] = prod if c == 0 else acc[...] + prod
        else:
            w = (acc[...] + prod) * u_out[mine]
    v_push = remote(v_all.at[1 - core], v_out.at[mine], send_sem.at[VS], one_recv.at[4], partner)
    v_push.start()
    tot = w[:, 0:128]
    for n in range(1, rows // 128):
        tot = tot + w[:, n * 128:(n + 1) * 128]
    cost_part[mine] = tot
    cost_all[me] = jnp.sum(cost_part[...].T, axis=0, keepdims=True)
    for dr in range(2):
        for dc in range(4):
            if dr or dc:
                remote(cost_all.at[me], cost_all.at[me], send_sem.at[CS], one_recv.at[6], dev((row + dr) % 2, (col + dc) % 4)).start()
    v_out[mine] = v_all[core]
    all_sent(t_out, TT)
    all_here(u_out.at[other], one_recv.at[3])
    u_push.wait_send()
    all_here(v_out.at[other], one_recv.at[4])
    v_push.wait_send()
    all_here(cost_all.at[0:7], one_recv.at[6])
    all_sent(cost_all.at[0:7], CS)


def output_kernel(norm, u_ref, v_ref, c_ref, u_hbm, v_hbm, cost_ref, sem):
    stores = [pltpu.make_async_copy(u_ref, u_hbm, sem.at[0]), pltpu.make_async_copy(v_ref, v_hbm, sem.at[1])]
    for d in stores:
        d.start()
    total = c_ref[0]
    for n in range(1, 8):
        total = total + c_ref[n]
    cost_ref[...] = total[:, :cost_ref.shape[1]] * norm
    for d in stores:
        d.wait()


def solution(mesh):
    n_chunk = 4

    def local_fn(kernel, cost_mat, src_mass, tgt_mass):
        rows, half = kernel.shape
        nprob = src_mass.shape[1]
        nq = nprob // 2
        cols = 2 * half
        rw, cw = rows // n_chunk, cols // n_chunk
        norm = 1.0 / float(rows * mesh.shape["row"] * half * mesh.shape["col"])
        vmem_spec = pl.BlockSpec(memory_space=pltpu.VMEM)
        any_spec = pl.BlockSpec(memory_space=pl.ANY)
        dma = pltpu.SemaphoreType.DMA
        u_vm, v_vm, c_vm = pl.pallas_call(
            lambda *refs: sinkhorn_kernel(n_chunk, *refs),
            out_shape=(pltpu.VMEM((nprob, rows), F32), pltpu.VMEM((nprob, half), F32), pltpu.VMEM((8, 1, 128), F32)),
            in_specs=[any_spec] * 4,
            out_specs=(vmem_spec, vmem_spec, vmem_spec),
            scratch_shapes=[
                pltpu.VMEM((2, rows, half), BF16),
                pltpu.VMEM((cols, rows), BF16),
                pltpu.VMEM((rows, half), BF16),
                pltpu.VMEM((cols, rows), BF16),
                pltpu.VMEM((nprob, rows), F32),
                pltpu.VMEM((2, nq, half), F32),
                pltpu.VMEM((nprob, rows), BF16),
                pltpu.VMEM((nq, max(rows, cols)), F32),
                pltpu.VMEM((n_chunk, nq, rw), F32),
                pltpu.VMEM((2, n_chunk, nq, rw), F32),
                pltpu.VMEM((n_chunk, nq, cw), F32),
                pltpu.VMEM((2, n_chunk, nq, cw), F32),
                pltpu.VMEM((2, n_chunk // 2, nq, cw), F32),
                pltpu.VMEM((4, rows // 128, 128), F32),
                pltpu.VMEM((2, nq, half), F32),
                pltpu.VMEM((128, 128), F32),
                dma((n_chunk + 2,)), dma((11,)), dma((n_chunk,)), dma((2, n_chunk)), dma((2, n_chunk)), dma((7,)),
            ],
            compiler_params=pltpu.CompilerParams(collective_id=0, has_side_effects=True, vmem_limit_bytes=60 * 1024 * 1024),
            name="sinkhorn",
        )(kernel, cost_mat, src_mass.T, tgt_mass.T)
        u_t, v_t, cost = pl.pallas_call(
            lambda *refs: output_kernel(norm, *refs),
            out_shape=(jax.ShapeDtypeStruct((nprob, rows), F32), jax.ShapeDtypeStruct((nprob, half), F32),
                       jax.ShapeDtypeStruct((1, nprob), F32)),
            in_specs=[vmem_spec] * 3,
            out_specs=(any_spec, any_spec, vmem_spec),
            scratch_shapes=[dma((2,))],
            name="outputs",
        )(*(pltpu.with_memory_space_constraint(r, pltpu.VMEM) for r in (u_vm, v_vm, c_vm)))
        return u_t.T, v_t.T, cost.reshape(nprob)

    return jax.shard_map(local_fn, mesh=mesh, in_specs=(P("row", "col"), P("row", "col"), P("row", "prob"), P("col", "prob")), out_specs=(P("row", "prob"), P("col", "prob"), P("prob")), check_vma=False)
```

```python
import jax
import jax.numpy as jnp
from jax import lax
from jax.experimental import pallas as pl
from jax.experimental.pallas import tpu as pltpu
from jax.sharding import PartitionSpec as P

SWEEPS = 6
AHEAD = (8, 7)
WAIT_NS = ((0, 350), (550, 400))
F32 = jnp.float32
BF16 = jnp.bfloat16
MESH = pl.DeviceIdType.MESH


def sinkhorn_kernel(n_chunk, k_hbm, c_hbm, a_hbm, b_hbm, u_out, v_out, cost_all,
                    k_buf, kt_buf, c_buf, kct_buf, a_buf, b_buf, ub_buf, acc,
                    s_out, s_in, t_out, t_in, t0_buf, s0_buf, v_all, cost_part,
                    load_sem, send_sem, kp_recv, s_recv, t_recv, one_recv):
    rows, half = k_hbm.shape
    cols = 2 * half
    rw = rows // n_chunk
    cw = cols // n_chunk
    per_half = n_chunk // 2
    nq = b_buf.shape[1]
    row = lax.axis_index("row")
    col = lax.axis_index("col")
    prob = lax.axis_index("prob")
    x = col // 2
    core = col % 2
    grp = (core + x + row) % 2
    me = row * 4 + col
    mine = pl.ds(pl.multiple_of(grp * nq, nq), nq)
    other = pl.ds(pl.multiple_of((1 - grp) * nq, nq), nq)

    def dev(r, c):
        return (prob, r, c)

    partner = dev(row, 2 * x + 1 - core)
    x_peer = dev(row, 2 * (1 - x) + 1 - core)
    y_peer = dev(1 - row, 2 * x + 1 - core)

    def remote(src, dst, send, recv, to):
        return pltpu.make_async_remote_copy(src_ref=src, dst_ref=dst, send_sem=send, recv_sem=recv,
                                            device_id=to, device_id_type=MESH)

    KP, BP, S0, SS, TT, T0, TP, KC, US, VS, CS = range(11)

    def all_sent(ref, kind):
        remote(ref, ref, send_sem.at[kind], one_recv.at[0], partner).wait_send()

    def all_here(ref, recv):
        remote(ref, ref, send_sem.at[0], recv, partner).wait_recv()

    def krows(i):
        return pl.ds(i * rw, rw)

    k_load = [pltpu.make_async_copy(k_hbm.at[krows(i)], k_buf.at[core, krows(i)], load_sem.at[i]) for i in range(n_chunk)]
    c_load = [pltpu.make_async_copy(c_hbm.at[krows(i)], c_buf.at[krows(i)], load_sem.at[i]) for i in range(n_chunk)]
    a_load = pltpu.make_async_copy(a_hbm, a_buf, load_sem.at[n_chunk])
    b_load = pltpu.make_async_copy(b_hbm.at[mine], b_buf.at[core], load_sem.at[n_chunk + 1])
    for d in k_load:
        d.start()
    a_load.start()
    b_load.start()

    barrier = pltpu.get_barrier_semaphore()
    for dr in range(2):
        for dc in range(4):
            if dr or dc:
                pl.semaphore_signal(barrier, inc=1, device_id=dev((row + dr) % 2, (col + dc) % 4), device_id_type=MESH)

    blk = 256

    def transpose_rows(h, i):
        def body(n, carry):
            jo = pl.multiple_of(n * blk, blk)
            for ii in range(rw // blk):
                kt_buf[pl.ds(pl.multiple_of(h * half + jo, blk), blk), pl.ds(i * rw + ii * blk, blk)] = (
                    k_buf[h, pl.ds(i * rw + ii * blk, blk), pl.ds(jo, blk)].T)
            return carry
        lax.fori_loop(0, half // blk, body, 0)

    kct_pieces = 2 * n_chunk
    kw = rows // kct_pieces

    def build_kct(lo, hi):
        def piece(i, carry):
            rs = pl.ds(pl.multiple_of(i * kw, kw), kw)
            for n in range(half // blk):
                kct_buf[pl.ds(pl.multiple_of(core * half + n * blk, blk), blk), rs] = (
                    k_buf[core, rs, n * blk:(n + 1) * blk] * c_buf[rs, n * blk:(n + 1) * blk]).T
            part = kct_buf.at[pl.ds(pl.multiple_of(core * half, half), half), rs]
            remote(part, part, send_sem.at[KC], one_recv.at[5], partner).start()
            return carry
        lax.fori_loop(lo, hi, piece, 0)

    ahead = grp * (AHEAD[0] + core * (AHEAD[1] - AHEAD[0]))
    middle = grp * kct_pieces + (1 - grp) * (kct_pieces // 2)

    k_push = [remote(k_buf.at[core, krows(i)], k_buf.at[core, krows(i)], send_sem.at[KP], kp_recv.at[i], partner) for i in range(n_chunk)]
    b_push = remote(b_hbm.at[other], b_buf.at[core], send_sem.at[BP], one_recv.at[0], partner)
    pl.semaphore_wait(barrier, 7)
    b_push.start()
    ones = jnp.ones((nq, half), BF16)
    for i in range(n_chunk):
        k_load[i].wait()
        if i == 0:
            k_push[0].start()
        if i % 2:
            part = lax.dot_general(ones, k_buf[core, pl.ds((i - 1) * rw, 2 * rw)], (((1,), (1,)), ((), ())), preferred_element_type=F32)
            for n in range(2 * rw // 128):
                r = (i - 1) * (rw // 128) + n
                s0_buf[col, r:r + 1, :] = part[0:1, n * 128:(n + 1) * 128]
    for n in range(1, 4):
        remote(s0_buf.at[col], s0_buf.at[col], send_sem.at[S0], one_recv.at[1], dev(row, (col + n) % 4)).start()
    for i in range(1, n_chunk):
        k_push[i].start()
    for d in c_load:
        d.start()
    for i in range(n_chunk):
        transpose_rows(core, i)
    a_load.wait()
    b_load.wait()
    all_here(s0_buf.at[0:3], one_recv.at[1])
    s0 = (s0_buf[0] + s0_buf[1]) + (s0_buf[2] + s0_buf[3])
    for r in range(rows // 128):
        cs = slice(r * 128, (r + 1) * 128)
        ub_buf[:, cs] = (a_buf[:, cs] / s0[r:r + 1, :]).astype(BF16)

    def t_copy(par, o):
        return remote(t_out.at[o], t_in.at[par, o], send_sem.at[TT], t_recv.at[par, o], y_peer)

    def s_copy(par, o):
        return remote(s_out.at[o], s_in.at[par, o], send_sem.at[SS], s_recv.at[par, o], x_peer)

    def t0_send(g, n):
        remote(t0_buf.at[g, n], t_in.at[0, core * per_half + n], send_sem.at[T0], t_recv.at[0, core * per_half + n],
               dev(1 - row, 2 * x + (g + x + 1 - row) % 2)).start()

    for n in range(per_half):
        part = jnp.dot(ub_buf[...], k_buf[core, :, n * cw:(n + 1) * cw], preferred_element_type=F32)
        for g in range(2):
            t0_buf[g, n] = part[g * nq:(g + 1) * nq]
        t0_send(0, n)
    for n in range(per_half):
        o = core * per_half + n
        remote(t0_buf.at[1 - grp, n], t_out.at[o], send_sem.at[TP], one_recv.at[2], partner).start()
        t_out[o] = t0_buf[grp, n]

    def v_of(par, o):
        return b_buf[o // per_half, :, (o % per_half) * cw:(o % per_half + 1) * cw] / (t_out[o] + t_in[par, o])

    all_here(b_buf.at[0], one_recv.at[0])
    for i in range(n_chunk):
        all_here(k_buf.at[1 - core, krows(i)], kp_recv.at[i])
        transpose_rows(1 - core, i)
        if i == 0:
            for n in range(per_half):
                t0_send(1, n)

    for d in c_load:
        d.wait()
    build_kct(0, ahead)

    for g in range(2):
        for c in range(2):
            if WAIT_NS[g][c]:
                @pl.when((grp == g) & (core == c))
                def _(g=g, c=c):
                    pl.delay(WAIT_NS[g][c])

    all_here(t0_buf.at[0], one_recv.at[2])
    order = list(range(per_half, n_chunk)) + list(range(per_half))
    for c in order:
        all_here(t_in.at[0, c], t_recv.at[0, c])
        vb = v_of(0, c).astype(BF16)
        js = slice(c * cw, (c + 1) * cw)
        if c != order[-1]:
            prod = jnp.dot(vb, kt_buf[js, :], preferred_element_type=F32)
            acc[...] = prod if c == order[0] else acc[...] + prod
        else:
            for o in range(n_chunk):
                s_out[o] = acc[:, o * rw:(o + 1) * rw] + jnp.dot(vb, kt_buf[js, o * rw:(o + 1) * rw], preferred_element_type=F32)
                s_copy(1, o).start()
    all_sent(t0_buf, T0)
    all_sent(t0_buf.at[0], TP)
    all_sent(s0_buf.at[0:3], S0)
    all_sent(k_buf.at[0], KP)
    all_sent(b_buf.at[0], BP)

    build_kct(ahead, middle)

    def u_and_t(par):
        for c in range(n_chunk):
            all_here(s_in.at[par, c], s_recv.at[par, c])
            w = slice(c * rw, (c + 1) * rw)
            u = a_buf[mine, w] / (s_out[c] + s_in[par, c])
            u_out[mine, w] = u
            ub = u.astype(BF16)
            if c < n_chunk - 1:
                for h in range(2):
                    hc = slice(h * half, (h + 1) * half)
                    prod = jnp.dot(ub, k_buf[h, w, :], preferred_element_type=F32)
                    acc[:, hc] = prod if c == 0 else acc[:, hc] + prod
            else:
                for o in range(n_chunk):
                    oc = slice(o * cw, (o + 1) * cw)
                    hc = slice((o % per_half) * cw, (o % per_half + 1) * cw)
                    t_out[o] = acc[:, oc] + jnp.dot(ub, k_buf[o // per_half, w, hc], preferred_element_type=F32)
                    t_copy(par, o).start()
                all_sent(s_out, SS)

    def v_and_s(par_in, par):
        for c in range(n_chunk):
            all_here(t_in.at[par_in, c], t_recv.at[par_in, c])
            vb = v_of(par_in, c).astype(BF16)
            w = slice(c * cw, (c + 1) * cw)
            if c < n_chunk - 1:
                prod = jnp.dot(vb, kt_buf[w, :], preferred_element_type=F32)
                acc[...] = prod if c == 0 else acc[...] + prod
            else:
                for o in range(n_chunk):
                    oc = slice(o * rw, (o + 1) * rw)
                    s_out[o] = acc[:, oc] + jnp.dot(vb, kt_buf[w, oc], preferred_element_type=F32)
                    s_copy(par, o).start()
                all_sent(t_out, TT)

    def sweep(t, carry):
        u_and_t(t % 2)

        @pl.when(t == 1)
        def _():
            build_kct(middle, kct_pieces)

        v_and_s(t % 2, (t + 1) % 2)
        return carry

    lax.fori_loop(1, SWEEPS - 1, sweep, 0)
    last = (SWEEPS - 1) % 2
    u_and_t(last)

    u_push = remote(u_out.at[mine], u_out.at[mine], send_sem.at[US], one_recv.at[3], partner)
    u_push.start()
    cost_part[...] = jnp.zeros_like(cost_part)
    all_here(kct_buf.at[0:half], one_recv.at[5])
    all_sent(kct_buf.at[0:half], KC)
    for c in range(n_chunk):
        all_here(t_in.at[last, c], t_recv.at[last, c])
        v = v_of(last, c)
        v_all[c // per_half, :, (c % per_half) * cw:(c % per_half + 1) * cw] = v
        prod = jnp.dot(v.astype(BF16), kct_buf[c * cw:(c + 1) * cw, :], preferred_element_type=F32)
        if c < n_chunk - 1:
            acc[...] = prod if c == 0 else acc[...] + prod
        else:
            w = (acc[...] + prod) * u_out[mine]
    v_push = remote(v_all.at[1 - core], v_out.at[mine], send_sem.at[VS], one_recv.at[4], partner)
    v_push.start()
    tot = w[:, 0:128]
    for n in range(1, rows // 128):
        tot = tot + w[:, n * 128:(n + 1) * 128]
    cost_part[mine] = tot
    cost_all[me] = jnp.sum(cost_part[...].T, axis=0, keepdims=True)
    for dr in range(2):
        for dc in range(4):
            if dr or dc:
                remote(cost_all.at[me], cost_all.at[me], send_sem.at[CS], one_recv.at[6], dev((row + dr) % 2, (col + dc) % 4)).start()
    v_out[mine] = v_all[core]
    all_sent(t_out, TT)
    all_here(u_out.at[other], one_recv.at[3])
    u_push.wait_send()
    all_here(v_out.at[other], one_recv.at[4])
    v_push.wait_send()
    all_here(cost_all.at[0:7], one_recv.at[6])
    all_sent(cost_all.at[0:7], CS)


def output_kernel(norm, u_ref, v_ref, c_ref, u_hbm, v_hbm, cost_ref, sem):
    stores = [pltpu.make_async_copy(u_ref, u_hbm, sem.at[0]), pltpu.make_async_copy(v_ref, v_hbm, sem.at[1])]
    for d in stores:
        d.start()
    total = c_ref[0]
    for n in range(1, 8):
        total = total + c_ref[n]
    cost_ref[...] = total[:, :cost_ref.shape[1]] * norm
    for d in stores:
        d.wait()


def solution(mesh):
    n_chunk = 4

    def local_fn(kernel, cost_mat, src_mass, tgt_mass):
        rows, half = kernel.shape
        nprob = src_mass.shape[1]
        nq = nprob // 2
        cols = 2 * half
        rw, cw = rows // n_chunk, cols // n_chunk
        norm = 1.0 / float(rows * mesh.shape["row"] * half * mesh.shape["col"])
        vmem_spec = pl.BlockSpec(memory_space=pltpu.VMEM)
        any_spec = pl.BlockSpec(memory_space=pl.ANY)
        dma = pltpu.SemaphoreType.DMA
        u_vm, v_vm, c_vm = pl.pallas_call(
            lambda *refs: sinkhorn_kernel(n_chunk, *refs),
            out_shape=(pltpu.VMEM((nprob, rows), F32), pltpu.VMEM((nprob, half), F32), pltpu.VMEM((8, 1, 128), F32)),
            in_specs=[any_spec] * 4,
            out_specs=(vmem_spec, vmem_spec, vmem_spec),
            scratch_shapes=[
                pltpu.VMEM((2, rows, half), BF16),
                pltpu.VMEM((cols, rows), BF16),
                pltpu.VMEM((rows, half), BF16),
                pltpu.VMEM((cols, rows), BF16),
                pltpu.VMEM((nprob, rows), F32),
                pltpu.VMEM((2, nq, half), F32),
                pltpu.VMEM((nprob, rows), BF16),
                pltpu.VMEM((nq, max(rows, cols)), F32),
                pltpu.VMEM((n_chunk, nq, rw), F32),
                pltpu.VMEM((2, n_chunk, nq, rw), F32),
                pltpu.VMEM((n_chunk, nq, cw), F32),
                pltpu.VMEM((2, n_chunk, nq, cw), F32),
                pltpu.VMEM((2, n_chunk // 2, nq, cw), F32),
                pltpu.VMEM((4, rows // 128, 128), F32),
                pltpu.VMEM((2, nq, half), F32),
                pltpu.VMEM((128, 128), F32),
                dma((n_chunk + 2,)), dma((11,)), dma((n_chunk,)), dma((2, n_chunk)), dma((2, n_chunk)), dma((7,)),
            ],
            compiler_params=pltpu.CompilerParams(collective_id=0, has_side_effects=True, vmem_limit_bytes=60 * 1024 * 1024),
            name="sinkhorn",
        )(kernel, cost_mat, src_mass.T, tgt_mass.T)
        u_t, v_t, cost = pl.pallas_call(
            lambda *refs: output_kernel(norm, *refs),
            out_shape=(jax.ShapeDtypeStruct((nprob, rows), F32), jax.ShapeDtypeStruct((nprob, half), F32),
                       jax.ShapeDtypeStruct((1, nprob), F32)),
            in_specs=[vmem_spec] * 3,
            out_specs=(any_spec, any_spec, vmem_spec),
            scratch_shapes=[dma((2,))],
            name="outputs",
        )(*(pltpu.with_memory_space_constraint(r, pltpu.VMEM) for r in (u_vm, v_vm, c_vm)))
        return u_t.T, v_t.T, cost.reshape(nprob)

    return jax.shard_map(local_fn, mesh=mesh, in_specs=(P("row", "col"), P("row", "col"), P("row", "prob"), P("col", "prob")), out_specs=(P("row", "prob"), P("col", "prob"), P("prob")), check_vma=False)
```

```python
import jax
import jax.numpy as jnp
from jax import lax
from jax.experimental import pallas as pl
from jax.experimental.pallas import tpu as pltpu
from jax.sharding import PartitionSpec as P

SWEEPS = 6
AHEAD = (8, 7)
WAIT_NS = ((0, 0), (300, 250))
F32 = jnp.float32
BF16 = jnp.bfloat16
MESH = pl.DeviceIdType.MESH


def sinkhorn_kernel(n_chunk, k_hbm, c_hbm, a_hbm, b_hbm, u_out, v_out, cost_all,
                    k_buf, kt_buf, c_buf, kct_buf, a_buf, b_buf, ub_buf, acc,
                    s_out, s_in, t_out, t_in, t0_buf, s0_buf, v_all, cost_part,
                    load_sem, send_sem, kp_recv, s_recv, t_recv, one_recv):
    rows, half = k_hbm.shape
    cols = 2 * half
    rw = rows // n_chunk
    cw = cols // n_chunk
    per_half = n_chunk // 2
    nq = b_buf.shape[1]
    row = lax.axis_index("row")
    col = lax.axis_index("col")
    prob = lax.axis_index("prob")
    x = col // 2
    core = col % 2
    grp = (core + x + row) % 2
    me = row * 4 + col
    mine = pl.ds(pl.multiple_of(grp * nq, nq), nq)
    other = pl.ds(pl.multiple_of((1 - grp) * nq, nq), nq)

    def dev(r, c):
        return (prob, r, c)

    partner = dev(row, 2 * x + 1 - core)
    x_peer = dev(row, 2 * (1 - x) + 1 - core)
    y_peer = dev(1 - row, 2 * x + 1 - core)

    def remote(src, dst, send, recv, to):
        return pltpu.make_async_remote_copy(src_ref=src, dst_ref=dst, send_sem=send, recv_sem=recv,
                                            device_id=to, device_id_type=MESH)

    KP, BP, S0, SS, TT, T0, TP, KC, US, VS, CS = range(11)

    def all_sent(ref, kind):
        remote(ref, ref, send_sem.at[kind], one_recv.at[0], partner).wait_send()

    def all_here(ref, recv):
        remote(ref, ref, send_sem.at[0], recv, partner).wait_recv()

    def krows(i):
        return pl.ds(i * rw, rw)

    k_load = [pltpu.make_async_copy(k_hbm.at[krows(i)], k_buf.at[core, krows(i)], load_sem.at[i]) for i in range(n_chunk)]
    c_load = [pltpu.make_async_copy(c_hbm.at[krows(i)], c_buf.at[krows(i)], load_sem.at[i]) for i in range(n_chunk)]
    a_load = pltpu.make_async_copy(a_hbm, a_buf, load_sem.at[n_chunk])
    b_load = pltpu.make_async_copy(b_hbm.at[mine], b_buf.at[core], load_sem.at[n_chunk + 1])
    for d in k_load:
        d.start()
    a_load.start()
    b_load.start()

    barrier = pltpu.get_barrier_semaphore()
    for dr in range(2):
        for dc in range(4):
            if dr or dc:
                pl.semaphore_signal(barrier, inc=1, device_id=dev((row + dr) % 2, (col + dc) % 4), device_id_type=MESH)

    blk = 256

    def transpose_rows(h, i):
        def body(n, carry):
            jo = pl.multiple_of(n * blk, blk)
            for ii in range(rw // blk):
                kt_buf[pl.ds(pl.multiple_of(h * half + jo, blk), blk), pl.ds(i * rw + ii * blk, blk)] = (
                    k_buf[h, pl.ds(i * rw + ii * blk, blk), pl.ds(jo, blk)].T)
            return carry
        lax.fori_loop(0, half // blk, body, 0)

    kct_pieces = 2 * n_chunk
    kw = rows // kct_pieces

    def build_kct(lo, hi):
        def piece(i, carry):
            rs = pl.ds(pl.multiple_of(i * kw, kw), kw)
            for n in range(half // blk):
                kct_buf[pl.ds(pl.multiple_of(core * half + n * blk, blk), blk), rs] = (
                    k_buf[core, rs, n * blk:(n + 1) * blk] * c_buf[rs, n * blk:(n + 1) * blk]).T
            part = kct_buf.at[pl.ds(pl.multiple_of(core * half, half), half), rs]
            remote(part, part, send_sem.at[KC], one_recv.at[5], partner).start()
            return carry
        lax.fori_loop(lo, hi, piece, 0)

    ahead = grp * (AHEAD[0] + core * (AHEAD[1] - AHEAD[0]))
    middle = grp * kct_pieces + (1 - grp) * (kct_pieces // 2)

    k_push = [remote(k_buf.at[core, krows(i)], k_buf.at[core, krows(i)], send_sem.at[KP], kp_recv.at[i], partner) for i in range(n_chunk)]
    b_push = remote(b_hbm.at[other], b_buf.at[core], send_sem.at[BP], one_recv.at[0], partner)
    pl.semaphore_wait(barrier, 7)
    b_push.start()
    ones = jnp.ones((nq, half), BF16)
    for i in range(n_chunk):
        k_load[i].wait()
        if i == 0:
            k_push[0].start()
        if i % 2:
            part = lax.dot_general(ones, k_buf[core, pl.ds((i - 1) * rw, 2 * rw)], (((1,), (1,)), ((), ())), preferred_element_type=F32)
            for n in range(2 * rw // 128):
                r = (i - 1) * (rw // 128) + n
                s0_buf[col, r:r + 1, :] = part[0:1, n * 128:(n + 1) * 128]
    for n in range(1, 4):
        remote(s0_buf.at[col], s0_buf.at[col], send_sem.at[S0], one_recv.at[1], dev(row, (col + n) % 4)).start()
    for i in range(1, n_chunk):
        k_push[i].start()
    for d in c_load:
        d.start()
    for i in range(n_chunk):
        transpose_rows(core, i)
    a_load.wait()
    b_load.wait()
    all_here(s0_buf.at[0:3], one_recv.at[1])
    s0 = (s0_buf[0] + s0_buf[1]) + (s0_buf[2] + s0_buf[3])
    for r in range(rows // 128):
        cs = slice(r * 128, (r + 1) * 128)
        ub_buf[:, cs] = (a_buf[:, cs] / s0[r:r + 1, :]).astype(BF16)

    def t_copy(par, o):
        return remote(t_out.at[o], t_in.at[par, o], send_sem.at[TT], t_recv.at[par, o], y_peer)

    def s_copy(par, o):
        return remote(s_out.at[o], s_in.at[par, o], send_sem.at[SS], s_recv.at[par, o], x_peer)

    def t0_send(g, n):
        remote(t0_buf.at[g, n], t_in.at[0, core * per_half + n], send_sem.at[T0], t_recv.at[0, core * per_half + n],
               dev(1 - row, 2 * x + (g + x + 1 - row) % 2)).start()

    for n in range(per_half):
        part = jnp.dot(ub_buf[...], k_buf[core, :, n * cw:(n + 1) * cw], preferred_element_type=F32)
        for g in range(2):
            t0_buf[g, n] = part[g * nq:(g + 1) * nq]
        t0_send(0, n)
    for n in range(per_half):
        o = core * per_half + n
        remote(t0_buf.at[1 - grp, n], t_out.at[o], send_sem.at[TP], one_recv.at[2], partner).start()
        t_out[o] = t0_buf[grp, n]

    def v_of(par, o):
        return b_buf[o // per_half, :, (o % per_half) * cw:(o % per_half + 1) * cw] / (t_out[o] + t_in[par, o])

    all_here(b_buf.at[0], one_recv.at[0])
    for i in range(n_chunk):
        all_here(k_buf.at[1 - core, krows(i)], kp_recv.at[i])
        transpose_rows(1 - core, i)
        if i == 1:
            for n in range(per_half):
                t0_send(1, n)

    for d in c_load:
        d.wait()
    build_kct(0, ahead)

    for g in range(2):
        for c in range(2):
            if WAIT_NS[g][c]:
                @pl.when((grp == g) & (core == c))
                def _(g=g, c=c):
                    pl.delay(WAIT_NS[g][c])

    all_here(t0_buf.at[0], one_recv.at[2])
    order = list(range(per_half, n_chunk)) + list(range(per_half))
    for c in order:
        all_here(t_in.at[0, c], t_recv.at[0, c])
        vb = v_of(0, c).astype(BF16)
        js = slice(c * cw, (c + 1) * cw)
        if c != order[-1]:
            prod = jnp.dot(vb, kt_buf[js, :], preferred_element_type=F32)
            acc[...] = prod if c == order[0] else acc[...] + prod
        else:
            for o in range(n_chunk):
                s_out[o] = acc[:, o * rw:(o + 1) * rw] + jnp.dot(vb, kt_buf[js, o * rw:(o + 1) * rw], preferred_element_type=F32)
                s_copy(1, o).start()
    all_sent(t0_buf, T0)
    all_sent(t0_buf.at[0], TP)
    all_sent(s0_buf.at[0:3], S0)
    all_sent(k_buf.at[0], KP)
    all_sent(b_buf.at[0], BP)

    build_kct(ahead, middle)

    def u_and_t(par):
        for c in range(n_chunk):
            all_here(s_in.at[par, c], s_recv.at[par, c])
            w = slice(c * rw, (c + 1) * rw)
            u = a_buf[mine, w] / (s_out[c] + s_in[par, c])
            u_out[mine, w] = u
            ub = u.astype(BF16)
            if c < n_chunk - 1:
                for h in range(2):
                    hc = slice(h * half, (h + 1) * half)
                    prod = jnp.dot(ub, k_buf[h, w, :], preferred_element_type=F32)
                    acc[:, hc] = prod if c == 0 else acc[:, hc] + prod
            else:
                for o in range(n_chunk):
                    oc = slice(o * cw, (o + 1) * cw)
                    hc = slice((o % per_half) * cw, (o % per_half + 1) * cw)
                    t_out[o] = acc[:, oc] + jnp.dot(ub, k_buf[o // per_half, w, hc], preferred_element_type=F32)
                    t_copy(par, o).start()
                all_sent(s_out, SS)

    def v_and_s(par_in, par):
        for c in range(n_chunk):
            all_here(t_in.at[par_in, c], t_recv.at[par_in, c])
            vb = v_of(par_in, c).astype(BF16)
            w = slice(c * cw, (c + 1) * cw)
            if c < n_chunk - 1:
                prod = jnp.dot(vb, kt_buf[w, :], preferred_element_type=F32)
                acc[...] = prod if c == 0 else acc[...] + prod
            else:
                for o in range(n_chunk):
                    oc = slice(o * rw, (o + 1) * rw)
                    s_out[o] = acc[:, oc] + jnp.dot(vb, kt_buf[w, oc], preferred_element_type=F32)
                    s_copy(par, o).start()
                all_sent(t_out, TT)

    def sweep(t, carry):
        u_and_t(t % 2)

        @pl.when(t == 1)
        def _():
            build_kct(middle, kct_pieces)

        v_and_s(t % 2, (t + 1) % 2)
        return carry

    lax.fori_loop(1, SWEEPS - 1, sweep, 0)
    last = (SWEEPS - 1) % 2
    u_and_t(last)

    u_push = remote(u_out.at[mine], u_out.at[mine], send_sem.at[US], one_recv.at[3], partner)
    u_push.start()
    cost_part[...] = jnp.zeros_like(cost_part)
    all_here(kct_buf.at[0:half], one_recv.at[5])
    all_sent(kct_buf.at[0:half], KC)
    for c in range(n_chunk):
        all_here(t_in.at[last, c], t_recv.at[last, c])
        v = v_of(last, c)
        v_all[c // per_half, :, (c % per_half) * cw:(c % per_half + 1) * cw] = v
        prod = jnp.dot(v.astype(BF16), kct_buf[c * cw:(c + 1) * cw, :], preferred_element_type=F32)
        if c < n_chunk - 1:
            acc[...] = prod if c == 0 else acc[...] + prod
        else:
            w = (acc[...] + prod) * u_out[mine]
    v_push = remote(v_all.at[1 - core], v_out.at[mine], send_sem.at[VS], one_recv.at[4], partner)
    v_push.start()
    tot = w[:, 0:128]
    for n in range(1, rows // 128):
        tot = tot + w[:, n * 128:(n + 1) * 128]
    cost_part[mine] = tot
    cost_all[me] = jnp.sum(cost_part[...].T, axis=0, keepdims=True)
    for dr in range(2):
        for dc in range(4):
            if dr or dc:
                remote(cost_all.at[me], cost_all.at[me], send_sem.at[CS], one_recv.at[6], dev((row + dr) % 2, (col + dc) % 4)).start()
    v_out[mine] = v_all[core]
    all_sent(t_out, TT)
    all_here(u_out.at[other], one_recv.at[3])
    u_push.wait_send()
    all_here(v_out.at[other], one_recv.at[4])
    v_push.wait_send()
    all_here(cost_all.at[0:7], one_recv.at[6])
    all_sent(cost_all.at[0:7], CS)


def output_kernel(norm, u_ref, v_ref, c_ref, u_hbm, v_hbm, cost_ref, sem):
    stores = [pltpu.make_async_copy(u_ref, u_hbm, sem.at[0]), pltpu.make_async_copy(v_ref, v_hbm, sem.at[1])]
    for d in stores:
        d.start()
    total = c_ref[0]
    for n in range(1, 8):
        total = total + c_ref[n]
    cost_ref[...] = total[:, :cost_ref.shape[1]] * norm
    for d in stores:
        d.wait()


def solution(mesh):
    n_chunk = 4

    def local_fn(kernel, cost_mat, src_mass, tgt_mass):
        rows, half = kernel.shape
        nprob = src_mass.shape[1]
        nq = nprob // 2
        cols = 2 * half
        rw, cw = rows // n_chunk, cols // n_chunk
        norm = 1.0 / float(rows * mesh.shape["row"] * half * mesh.shape["col"])
        vmem_spec = pl.BlockSpec(memory_space=pltpu.VMEM)
        any_spec = pl.BlockSpec(memory_space=pl.ANY)
        dma = pltpu.SemaphoreType.DMA
        u_vm, v_vm, c_vm = pl.pallas_call(
            lambda *refs: sinkhorn_kernel(n_chunk, *refs),
            out_shape=(pltpu.VMEM((nprob, rows), F32), pltpu.VMEM((nprob, half), F32), pltpu.VMEM((8, 1, 128), F32)),
            in_specs=[any_spec] * 4,
            out_specs=(vmem_spec, vmem_spec, vmem_spec),
            scratch_shapes=[
                pltpu.VMEM((2, rows, half), BF16),
                pltpu.VMEM((cols, rows), BF16),
                pltpu.VMEM((rows, half), BF16),
                pltpu.VMEM((cols, rows), BF16),
                pltpu.VMEM((nprob, rows), F32),
                pltpu.VMEM((2, nq, half), F32),
                pltpu.VMEM((nprob, rows), BF16),
                pltpu.VMEM((nq, max(rows, cols)), F32),
                pltpu.VMEM((n_chunk, nq, rw), F32),
                pltpu.VMEM((2, n_chunk, nq, rw), F32),
                pltpu.VMEM((n_chunk, nq, cw), F32),
                pltpu.VMEM((2, n_chunk, nq, cw), F32),
                pltpu.VMEM((2, n_chunk // 2, nq, cw), F32),
                pltpu.VMEM((4, rows // 128, 128), F32),
                pltpu.VMEM((2, nq, half), F32),
                pltpu.VMEM((128, 128), F32),
                dma((n_chunk + 2,)), dma((11,)), dma((n_chunk,)), dma((2, n_chunk)), dma((2, n_chunk)), dma((7,)),
            ],
            compiler_params=pltpu.CompilerParams(collective_id=0, has_side_effects=True, vmem_limit_bytes=60 * 1024 * 1024),
            name="sinkhorn",
        )(kernel, cost_mat, src_mass.T, tgt_mass.T)
        u_t, v_t, cost = pl.pallas_call(
            lambda *refs: output_kernel(norm, *refs),
            out_shape=(jax.ShapeDtypeStruct((nprob, rows), F32), jax.ShapeDtypeStruct((nprob, half), F32),
                       jax.ShapeDtypeStruct((1, nprob), F32)),
            in_specs=[vmem_spec] * 3,
            out_specs=(any_spec, any_spec, vmem_spec),
            scratch_shapes=[dma((2,))],
            name="outputs",
        )(*(pltpu.with_memory_space_constraint(r, pltpu.VMEM) for r in (u_vm, v_vm, c_vm)))
        return u_t.T, v_t.T, cost.reshape(nprob)

    return jax.shard_map(local_fn, mesh=mesh, in_specs=(P("row", "col"), P("row", "col"), P("row", "prob"), P("col", "prob")), out_specs=(P("row", "prob"), P("col", "prob"), P("prob")), check_vma=False)
```

```python
import jax
import jax.numpy as jnp
from jax import lax
from jax.experimental import pallas as pl
from jax.experimental.pallas import tpu as pltpu
from jax.sharding import PartitionSpec as P

SWEEPS = 6
AHEAD = (8, 6)
WAIT_NS = ((0, 0), (200, 200))
F32 = jnp.float32
BF16 = jnp.bfloat16
MESH = pl.DeviceIdType.MESH


def sinkhorn_kernel(n_chunk, k_hbm, c_hbm, a_hbm, b_hbm, u_out, v_out, cost_all,
                    k_buf, kt_buf, c_buf, kct_buf, a_buf, b_buf, ub_buf, acc,
                    s_out, s_in, t_out, t_in, t0_buf, s0_buf, v_all, cost_part,
                    load_sem, send_sem, kp_recv, s_recv, t_recv, one_recv):
    rows, half = k_hbm.shape
    cols = 2 * half
    rw = rows // n_chunk
    cw = cols // n_chunk
    per_half = n_chunk // 2
    nq = b_buf.shape[1]
    row = lax.axis_index("row")
    col = lax.axis_index("col")
    prob = lax.axis_index("prob")
    x = col // 2
    core = col % 2
    grp = (core + x + row) % 2
    me = row * 4 + col
    mine = pl.ds(pl.multiple_of(grp * nq, nq), nq)
    other = pl.ds(pl.multiple_of((1 - grp) * nq, nq), nq)

    def dev(r, c):
        return (prob, r, c)

    partner = dev(row, 2 * x + 1 - core)
    x_peer = dev(row, 2 * (1 - x) + 1 - core)
    y_peer = dev(1 - row, 2 * x + 1 - core)

    def remote(src, dst, send, recv, to):
        return pltpu.make_async_remote_copy(src_ref=src, dst_ref=dst, send_sem=send, recv_sem=recv,
                                            device_id=to, device_id_type=MESH)

    KP, BP, S0, SS, TT, T0, TP, KC, US, VS, CS = range(11)

    def all_sent(ref, kind):
        remote(ref, ref, send_sem.at[kind], one_recv.at[0], partner).wait_send()

    def all_here(ref, recv):
        remote(ref, ref, send_sem.at[0], recv, partner).wait_recv()

    def krows(i):
        return pl.ds(i * rw, rw)

    k_load = [pltpu.make_async_copy(k_hbm.at[krows(i)], k_buf.at[core, krows(i)], load_sem.at[i]) for i in range(n_chunk)]
    c_load = [pltpu.make_async_copy(c_hbm.at[krows(i)], c_buf.at[krows(i)], load_sem.at[i]) for i in range(n_chunk)]
    a_load = pltpu.make_async_copy(a_hbm, a_buf, load_sem.at[n_chunk])
    b_load = pltpu.make_async_copy(b_hbm.at[mine], b_buf.at[core], load_sem.at[n_chunk + 1])
    for d in k_load:
        d.start()
    a_load.start()
    b_load.start()

    barrier = pltpu.get_barrier_semaphore()
    for dr in range(2):
        for dc in range(4):
            if dr or dc:
                pl.semaphore_signal(barrier, inc=1, device_id=dev((row + dr) % 2, (col + dc) % 4), device_id_type=MESH)

    blk = 256

    def transpose_rows(h, i):
        def body(n, carry):
            jo = pl.multiple_of(n * blk, blk)
            for ii in range(rw // blk):
                kt_buf[pl.ds(pl.multiple_of(h * half + jo, blk), blk), pl.ds(i * rw + ii * blk, blk)] = (
                    k_buf[h, pl.ds(i * rw + ii * blk, blk), pl.ds(jo, blk)].T)
            return carry
        lax.fori_loop(0, half // blk, body, 0)

    kct_pieces = 2 * n_chunk
    kw = rows // kct_pieces

    def build_kct(lo, hi):
        def piece(i, carry):
            rs = pl.ds(pl.multiple_of(i * kw, kw), kw)
            for n in range(half // blk):
                kct_buf[pl.ds(pl.multiple_of(core * half + n * blk, blk), blk), rs] = (
                    k_buf[core, rs, n * blk:(n + 1) * blk] * c_buf[rs, n * blk:(n + 1) * blk]).T
            part = kct_buf.at[pl.ds(pl.multiple_of(core * half, half), half), rs]
            remote(part, part, send_sem.at[KC], one_recv.at[5], partner).start()
            return carry
        lax.fori_loop(lo, hi, piece, 0)

    ahead = grp * (AHEAD[0] + core * (AHEAD[1] - AHEAD[0]))
    middle = grp * kct_pieces + (1 - grp) * (kct_pieces // 2)

    k_push = [remote(k_buf.at[core, krows(i)], k_buf.at[core, krows(i)], send_sem.at[KP], kp_recv.at[i], partner) for i in range(n_chunk)]
    b_push = remote(b_hbm.at[other], b_buf.at[core], send_sem.at[BP], one_recv.at[0], partner)
    pl.semaphore_wait(barrier, 7)
    b_push.start()
    ones = jnp.ones((nq, half), BF16)
    for i in range(n_chunk):
        k_load[i].wait()
        if i == 0:
            k_push[0].start()
        if i % 2:
            part = lax.dot_general(ones, k_buf[core, pl.ds((i - 1) * rw, 2 * rw)], (((1,), (1,)), ((), ())), preferred_element_type=F32)
            for n in range(2 * rw // 128):
                r = (i - 1) * (rw // 128) + n
                s0_buf[col, r:r + 1, :] = part[0:1, n * 128:(n + 1) * 128]
    for n in range(1, 4):
        remote(s0_buf.at[col], s0_buf.at[col], send_sem.at[S0], one_recv.at[1], dev(row, (col + n) % 4)).start()
    for i in range(1, n_chunk):
        k_push[i].start()
    for d in c_load:
        d.start()
    for i in range(n_chunk):
        transpose_rows(core, i)
    a_load.wait()
    b_load.wait()
    all_here(s0_buf.at[0:3], one_recv.at[1])
    s0 = (s0_buf[0] + s0_buf[1]) + (s0_buf[2] + s0_buf[3])
    for r in range(rows // 128):
        cs = slice(r * 128, (r + 1) * 128)
        ub_buf[:, cs] = (a_buf[:, cs] / s0[r:r + 1, :]).astype(BF16)

    def t_copy(par, o):
        return remote(t_out.at[o], t_in.at[par, o], send_sem.at[TT], t_recv.at[par, o], y_peer)

    def s_copy(par, o):
        return remote(s_out.at[o], s_in.at[par, o], send_sem.at[SS], s_recv.at[par, o], x_peer)

    def t0_send(g, n):
        remote(t0_buf.at[g, n], t_in.at[0, core * per_half + n], send_sem.at[T0], t_recv.at[0, core * per_half + n],
               dev(1 - row, 2 * x + (g + x + 1 - row) % 2)).start()

    for n in range(per_half):
        part = jnp.dot(ub_buf[...], k_buf[core, :, n * cw:(n + 1) * cw], preferred_element_type=F32)
        for g in range(2):
            t0_buf[g, n] = part[g * nq:(g + 1) * nq]
        t0_send(0, n)
    for n in range(per_half):
        o = core * per_half + n
        remote(t0_buf.at[1 - grp, n], t_out.at[o], send_sem.at[TP], one_recv.at[2], partner).start()
        t_out[o] = t0_buf[grp, n]

    def v_of(par, o):
        return b_buf[o // per_half, :, (o % per_half) * cw:(o % per_half + 1) * cw] / (t_out[o] + t_in[par, o])

    all_here(b_buf.at[0], one_recv.at[0])
    for i in range(n_chunk):
        all_here(k_buf.at[1 - core, krows(i)], kp_recv.at[i])
        transpose_rows(1 - core, i)
        if i == 1:
            for n in range(per_half):
                t0_send(1, n)

    for d in c_load:
        d.wait()
    build_kct(0, ahead)

    for g in range(2):
        for c in range(2):
            if WAIT_NS[g][c]:
                @pl.when((grp == g) & (core == c))
                def _(g=g, c=c):
                    pl.delay(WAIT_NS[g][c])

    all_here(t0_buf.at[0], one_recv.at[2])
    order = list(range(per_half, n_chunk)) + list(range(per_half))
    for c in order:
        all_here(t_in.at[0, c], t_recv.at[0, c])
        vb = v_of(0, c).astype(BF16)
        js = slice(c * cw, (c + 1) * cw)
        if c != order[-1]:
            prod = jnp.dot(vb, kt_buf[js, :], preferred_element_type=F32)
            acc[...] = prod if c == order[0] else acc[...] + prod
        else:
            for o in range(n_chunk):
                s_out[o] = acc[:, o * rw:(o + 1) * rw] + jnp.dot(vb, kt_buf[js, o * rw:(o + 1) * rw], preferred_element_type=F32)
                s_copy(1, o).start()
    all_sent(t0_buf, T0)
    all_sent(t0_buf.at[0], TP)
    all_sent(s0_buf.at[0:3], S0)
    all_sent(k_buf.at[0], KP)
    all_sent(b_buf.at[0], BP)

    build_kct(ahead, middle)

    def u_and_t(par):
        for c in range(n_chunk):
            all_here(s_in.at[par, c], s_recv.at[par, c])
            w = slice(c * rw, (c + 1) * rw)
            u = a_buf[mine, w] / (s_out[c] + s_in[par, c])
            u_out[mine, w] = u
            ub = u.astype(BF16)
            if c < n_chunk - 1:
                for h in range(2):
                    hc = slice(h * half, (h + 1) * half)
                    prod = jnp.dot(ub, k_buf[h, w, :], preferred_element_type=F32)
                    acc[:, hc] = prod if c == 0 else acc[:, hc] + prod
            else:
                for o in range(n_chunk):
                    oc = slice(o * cw, (o + 1) * cw)
                    hc = slice((o % per_half) * cw, (o % per_half + 1) * cw)
                    t_out[o] = acc[:, oc] + jnp.dot(ub, k_buf[o // per_half, w, hc], preferred_element_type=F32)
                    t_copy(par, o).start()
                all_sent(s_out, SS)

    def v_and_s(par_in, par):
        for c in range(n_chunk):
            all_here(t_in.at[par_in, c], t_recv.at[par_in, c])
            vb = v_of(par_in, c).astype(BF16)
            w = slice(c * cw, (c + 1) * cw)
            if c < n_chunk - 1:
                prod = jnp.dot(vb, kt_buf[w, :], preferred_element_type=F32)
                acc[...] = prod if c == 0 else acc[...] + prod
            else:
                for o in range(n_chunk):
                    oc = slice(o * rw, (o + 1) * rw)
                    s_out[o] = acc[:, oc] + jnp.dot(vb, kt_buf[w, oc], preferred_element_type=F32)
                    s_copy(par, o).start()
                all_sent(t_out, TT)

    def sweep(t, carry):
        u_and_t(t % 2)

        @pl.when(t == 1)
        def _():
            build_kct(middle, kct_pieces)

        v_and_s(t % 2, (t + 1) % 2)
        return carry

    lax.fori_loop(1, SWEEPS - 1, sweep, 0)
    last = (SWEEPS - 1) % 2
    u_and_t(last)

    u_push = remote(u_out.at[mine], u_out.at[mine], send_sem.at[US], one_recv.at[3], partner)
    u_push.start()
    cost_part[...] = jnp.zeros_like(cost_part)
    all_here(kct_buf.at[0:half], one_recv.at[5])
    all_sent(kct_buf.at[0:half], KC)
    for c in range(n_chunk):
        all_here(t_in.at[last, c], t_recv.at[last, c])
        v = v_of(last, c)
        v_all[c // per_half, :, (c % per_half) * cw:(c % per_half + 1) * cw] = v
        prod = jnp.dot(v.astype(BF16), kct_buf[c * cw:(c + 1) * cw, :], preferred_element_type=F32)
        if c < n_chunk - 1:
            acc[...] = prod if c == 0 else acc[...] + prod
        else:
            w = (acc[...] + prod) * u_out[mine]
    v_push = remote(v_all.at[1 - core], v_out.at[mine], send_sem.at[VS], one_recv.at[4], partner)
    v_push.start()
    tot = w[:, 0:128]
    for n in range(1, rows // 128):
        tot = tot + w[:, n * 128:(n + 1) * 128]
    cost_part[mine] = tot
    cost_all[me] = jnp.sum(cost_part[...].T, axis=0, keepdims=True)
    for dr in range(2):
        for dc in range(4):
            if dr or dc:
                remote(cost_all.at[me], cost_all.at[me], send_sem.at[CS], one_recv.at[6], dev((row + dr) % 2, (col + dc) % 4)).start()
    v_out[mine] = v_all[core]
    all_sent(t_out, TT)
    all_here(u_out.at[other], one_recv.at[3])
    u_push.wait_send()
    all_here(v_out.at[other], one_recv.at[4])
    v_push.wait_send()
    all_here(cost_all.at[0:7], one_recv.at[6])
    all_sent(cost_all.at[0:7], CS)


def output_kernel(norm, u_ref, v_ref, c_ref, u_hbm, v_hbm, cost_ref, sem):
    stores = [pltpu.make_async_copy(u_ref, u_hbm, sem.at[0]), pltpu.make_async_copy(v_ref, v_hbm, sem.at[1])]
    for d in stores:
        d.start()
    total = c_ref[0]
    for n in range(1, 8):
        total = total + c_ref[n]
    cost_ref[...] = total[:, :cost_ref.shape[1]] * norm
    for d in stores:
        d.wait()


def solution(mesh):
    n_chunk = 4

    def local_fn(kernel, cost_mat, src_mass, tgt_mass):
        rows, half = kernel.shape
        nprob = src_mass.shape[1]
        nq = nprob // 2
        cols = 2 * half
        rw, cw = rows // n_chunk, cols // n_chunk
        norm = 1.0 / float(rows * mesh.shape["row"] * half * mesh.shape["col"])
        vmem_spec = pl.BlockSpec(memory_space=pltpu.VMEM)
        any_spec = pl.BlockSpec(memory_space=pl.ANY)
        dma = pltpu.SemaphoreType.DMA
        u_vm, v_vm, c_vm = pl.pallas_call(
            lambda *refs: sinkhorn_kernel(n_chunk, *refs),
            out_shape=(pltpu.VMEM((nprob, rows), F32), pltpu.VMEM((nprob, half), F32), pltpu.VMEM((8, 1, 128), F32)),
            in_specs=[any_spec] * 4,
            out_specs=(vmem_spec, vmem_spec, vmem_spec),
            scratch_shapes=[
                pltpu.VMEM((2, rows, half), BF16),
                pltpu.VMEM((cols, rows), BF16),
                pltpu.VMEM((rows, half), BF16),
                pltpu.VMEM((cols, rows), BF16),
                pltpu.VMEM((nprob, rows), F32),
                pltpu.VMEM((2, nq, half), F32),
                pltpu.VMEM((nprob, rows), BF16),
                pltpu.VMEM((nq, max(rows, cols)), F32),
                pltpu.VMEM((n_chunk, nq, rw), F32),
                pltpu.VMEM((2, n_chunk, nq, rw), F32),
                pltpu.VMEM((n_chunk, nq, cw), F32),
                pltpu.VMEM((2, n_chunk, nq, cw), F32),
                pltpu.VMEM((2, n_chunk // 2, nq, cw), F32),
                pltpu.VMEM((4, rows // 128, 128), F32),
                pltpu.VMEM((2, nq, half), F32),
                pltpu.VMEM((128, 128), F32),
                dma((n_chunk + 2,)), dma((11,)), dma((n_chunk,)), dma((2, n_chunk)), dma((2, n_chunk)), dma((7,)),
            ],
            compiler_params=pltpu.CompilerParams(collective_id=0, has_side_effects=True, vmem_limit_bytes=60 * 1024 * 1024),
            name="sinkhorn",
        )(kernel, cost_mat, src_mass.T, tgt_mass.T)
        u_t, v_t, cost = pl.pallas_call(
            lambda *refs: output_kernel(norm, *refs),
            out_shape=(jax.ShapeDtypeStruct((nprob, rows), F32), jax.ShapeDtypeStruct((nprob, half), F32),
                       jax.ShapeDtypeStruct((1, nprob), F32)),
            in_specs=[vmem_spec] * 3,
            out_specs=(any_spec, any_spec, vmem_spec),
            scratch_shapes=[dma((2,))],
            name="outputs",
        )(*(pltpu.with_memory_space_constraint(r, pltpu.VMEM) for r in (u_vm, v_vm, c_vm)))
        return u_t.T, v_t.T, cost.reshape(nprob)

    return jax.shard_map(local_fn, mesh=mesh, in_specs=(P("row", "col"), P("row", "col"), P("row", "prob"), P("col", "prob")), out_specs=(P("row", "prob"), P("col", "prob"), P("prob")), check_vma=False)
```

```python
import jax
import jax.numpy as jnp
from jax import lax
from jax.experimental import pallas as pl
from jax.experimental.pallas import tpu as pltpu
from jax.sharding import PartitionSpec as P

SWEEPS = 6
AHEAD = (8, 7)
WAIT_NS = ((0, 0), (450, 400))
F32 = jnp.float32
BF16 = jnp.bfloat16
MESH = pl.DeviceIdType.MESH


def sinkhorn_kernel(n_chunk, k_hbm, c_hbm, a_hbm, b_hbm, u_out, v_out, cost_all,
                    k_buf, kt_buf, c_buf, kct_buf, a_buf, b_buf, ub_buf, acc,
                    s_out, s_in, t_out, t_in, t0_buf, s0_buf, v_all, cost_part,
                    load_sem, send_sem, kp_recv, s_recv, t_recv, one_recv):
    rows, half = k_hbm.shape
    cols = 2 * half
    rw = rows // n_chunk
    cw = cols // n_chunk
    per_half = n_chunk // 2
    nq = b_buf.shape[1]
    row = lax.axis_index("row")
    col = lax.axis_index("col")
    prob = lax.axis_index("prob")
    x = col // 2
    core = col % 2
    grp = (core + x + row) % 2
    me = row * 4 + col
    mine = pl.ds(pl.multiple_of(grp * nq, nq), nq)
    other = pl.ds(pl.multiple_of((1 - grp) * nq, nq), nq)

    def dev(r, c):
        return (prob, r, c)

    partner = dev(row, 2 * x + 1 - core)
    x_peer = dev(row, 2 * (1 - x) + 1 - core)
    y_peer = dev(1 - row, 2 * x + 1 - core)

    def remote(src, dst, send, recv, to):
        return pltpu.make_async_remote_copy(src_ref=src, dst_ref=dst, send_sem=send, recv_sem=recv,
                                            device_id=to, device_id_type=MESH)

    KP, BP, S0, SS, TT, T0, TP, KC, US, VS, CS = range(11)

    def all_sent(ref, kind):
        remote(ref, ref, send_sem.at[kind], one_recv.at[0], partner).wait_send()

    def all_here(ref, recv):
        remote(ref, ref, send_sem.at[0], recv, partner).wait_recv()

    def krows(i):
        return pl.ds(i * rw, rw)

    k_load = [pltpu.make_async_copy(k_hbm.at[krows(i)], k_buf.at[core, krows(i)], load_sem.at[i]) for i in range(n_chunk)]
    c_load = [pltpu.make_async_copy(c_hbm.at[krows(i)], c_buf.at[krows(i)], load_sem.at[i]) for i in range(n_chunk)]
    a_load = pltpu.make_async_copy(a_hbm, a_buf, load_sem.at[n_chunk])
    b_load = pltpu.make_async_copy(b_hbm.at[mine], b_buf.at[core], load_sem.at[n_chunk + 1])
    for d in k_load:
        d.start()
    a_load.start()
    b_load.start()

    barrier = pltpu.get_barrier_semaphore()
    for dr in range(2):
        for dc in range(4):
            if dr or dc:
                pl.semaphore_signal(barrier, inc=1, device_id=dev((row + dr) % 2, (col + dc) % 4), device_id_type=MESH)

    blk = 256

    def transpose_rows(h, i):
        def body(n, carry):
            jo = pl.multiple_of(n * blk, blk)
            for ii in range(rw // blk):
                kt_buf[pl.ds(pl.multiple_of(h * half + jo, blk), blk), pl.ds(i * rw + ii * blk, blk)] = (
                    k_buf[h, pl.ds(i * rw + ii * blk, blk), pl.ds(jo, blk)].T)
            return carry
        lax.fori_loop(0, half // blk, body, 0)

    kct_pieces = 2 * n_chunk
    kw = rows // kct_pieces

    def build_kct(lo, hi):
        def piece(i, carry):
            rs = pl.ds(pl.multiple_of(i * kw, kw), kw)
            for n in range(half // blk):
                kct_buf[pl.ds(pl.multiple_of(core * half + n * blk, blk), blk), rs] = (
                    k_buf[core, rs, n * blk:(n + 1) * blk] * c_buf[rs, n * blk:(n + 1) * blk]).T
            part = kct_buf.at[pl.ds(pl.multiple_of(core * half, half), half), rs]
            remote(part, part, send_sem.at[KC], one_recv.at[5], partner).start()
            return carry
        lax.fori_loop(lo, hi, piece, 0)

    ahead = grp * (AHEAD[0] + core * (AHEAD[1] - AHEAD[0]))
    middle = grp * kct_pieces + (1 - grp) * (kct_pieces // 2)

    k_push = [remote(k_buf.at[core, krows(i)], k_buf.at[core, krows(i)], send_sem.at[KP], kp_recv.at[i], partner) for i in range(n_chunk)]
    b_push = remote(b_hbm.at[other], b_buf.at[core], send_sem.at[BP], one_recv.at[0], partner)
    pl.semaphore_wait(barrier, 7)
    b_push.start()
    ones = jnp.ones((nq, half), BF16)
    for i in range(n_chunk):
        k_load[i].wait()
        if i == 0:
            k_push[0].start()
        if i % 2:
            part = lax.dot_general(ones, k_buf[core, pl.ds((i - 1) * rw, 2 * rw)], (((1,), (1,)), ((), ())), preferred_element_type=F32)
            for n in range(2 * rw // 128):
                r = (i - 1) * (rw // 128) + n
                s0_buf[col, r:r + 1, :] = part[0:1, n * 128:(n + 1) * 128]
    for n in range(1, 4):
        remote(s0_buf.at[col], s0_buf.at[col], send_sem.at[S0], one_recv.at[1], dev(row, (col + n) % 4)).start()
    for i in range(1, n_chunk):
        k_push[i].start()
    for d in c_load:
        d.start()
    for i in range(n_chunk):
        transpose_rows(core, i)
    a_load.wait()
    b_load.wait()
    all_here(s0_buf.at[0:3], one_recv.at[1])
    s0 = (s0_buf[0] + s0_buf[1]) + (s0_buf[2] + s0_buf[3])
    for r in range(rows // 128):
        cs = slice(r * 128, (r + 1) * 128)
        ub_buf[:, cs] = (a_buf[:, cs] / s0[r:r + 1, :]).astype(BF16)

    def t_copy(par, o):
        return remote(t_out.at[o], t_in.at[par, o], send_sem.at[TT], t_recv.at[par, o], y_peer)

    def s_copy(par, o):
        return remote(s_out.at[o], s_in.at[par, o], send_sem.at[SS], s_recv.at[par, o], x_peer)

    def t0_send(g, n):
        remote(t0_buf.at[g, n], t_in.at[0, core * per_half + n], send_sem.at[T0], t_recv.at[0, core * per_half + n],
               dev(1 - row, 2 * x + (g + x + 1 - row) % 2)).start()

    for n in range(per_half):
        part = jnp.dot(ub_buf[...], k_buf[core, :, n * cw:(n + 1) * cw], preferred_element_type=F32)
        for g in range(2):
            t0_buf[g, n] = part[g * nq:(g + 1) * nq]
        t0_send(0, n)
    for n in range(per_half):
        o = core * per_half + n
        remote(t0_buf.at[1 - grp, n], t_out.at[o], send_sem.at[TP], one_recv.at[2], partner).start()
        t_out[o] = t0_buf[grp, n]

    def v_of(par, o):
        return b_buf[o // per_half, :, (o % per_half) * cw:(o % per_half + 1) * cw] / (t_out[o] + t_in[par, o])

    all_here(b_buf.at[0], one_recv.at[0])
    for i in range(n_chunk):
        all_here(k_buf.at[1 - core, krows(i)], kp_recv.at[i])
        transpose_rows(1 - core, i)
        if i == 1:
            for n in range(per_half):
                t0_send(1, n)

    for d in c_load:
        d.wait()
    build_kct(0, ahead)

    for g in range(2):
        for c in range(2):
            if WAIT_NS[g][c]:
                @pl.when((grp == g) & (core == c))
                def _(g=g, c=c):
                    pl.delay(WAIT_NS[g][c])

    all_here(t0_buf.at[0], one_recv.at[2])
    order = list(range(per_half, n_chunk)) + list(range(per_half))
    for c in order:
        all_here(t_in.at[0, c], t_recv.at[0, c])
        vb = v_of(0, c).astype(BF16)
        js = slice(c * cw, (c + 1) * cw)
        if c != order[-1]:
            prod = jnp.dot(vb, kt_buf[js, :], preferred_element_type=F32)
            acc[...] = prod if c == order[0] else acc[...] + prod
        else:
            for o in range(n_chunk):
                s_out[o] = acc[:, o * rw:(o + 1) * rw] + jnp.dot(vb, kt_buf[js, o * rw:(o + 1) * rw], preferred_element_type=F32)
                s_copy(1, o).start()
    all_sent(t0_buf, T0)
    all_sent(t0_buf.at[0], TP)
    all_sent(s0_buf.at[0:3], S0)
    all_sent(k_buf.at[0], KP)
    all_sent(b_buf.at[0], BP)

    build_kct(ahead, middle)

    def u_and_t(par):
        for c in range(n_chunk):
            all_here(s_in.at[par, c], s_recv.at[par, c])
            w = slice(c * rw, (c + 1) * rw)
            u = a_buf[mine, w] / (s_out[c] + s_in[par, c])
            u_out[mine, w] = u
            ub = u.astype(BF16)
            if c < n_chunk - 1:
                for h in range(2):
                    hc = slice(h * half, (h + 1) * half)
                    prod = jnp.dot(ub, k_buf[h, w, :], preferred_element_type=F32)
                    acc[:, hc] = prod if c == 0 else acc[:, hc] + prod
            else:
                for o in range(n_chunk):
                    oc = slice(o * cw, (o + 1) * cw)
                    hc = slice((o % per_half) * cw, (o % per_half + 1) * cw)
                    t_out[o] = acc[:, oc] + jnp.dot(ub, k_buf[o // per_half, w, hc], preferred_element_type=F32)
                    t_copy(par, o).start()
                all_sent(s_out, SS)

    def v_and_s(par_in, par):
        for c in range(n_chunk):
            all_here(t_in.at[par_in, c], t_recv.at[par_in, c])
            vb = v_of(par_in, c).astype(BF16)
            w = slice(c * cw, (c + 1) * cw)
            if c < n_chunk - 1:
                prod = jnp.dot(vb, kt_buf[w, :], preferred_element_type=F32)
                acc[...] = prod if c == 0 else acc[...] + prod
            else:
                for o in range(n_chunk):
                    oc = slice(o * rw, (o + 1) * rw)
                    s_out[o] = acc[:, oc] + jnp.dot(vb, kt_buf[w, oc], preferred_element_type=F32)
                    s_copy(par, o).start()
                all_sent(t_out, TT)

    def sweep(t, carry):
        u_and_t(t % 2)

        @pl.when(t == 1)
        def _():
            build_kct(middle, kct_pieces)

        v_and_s(t % 2, (t + 1) % 2)
        return carry

    lax.fori_loop(1, SWEEPS - 1, sweep, 0)
    last = (SWEEPS - 1) % 2
    u_and_t(last)

    u_push = remote(u_out.at[mine], u_out.at[mine], send_sem.at[US], one_recv.at[3], partner)
    u_push.start()
    cost_part[...] = jnp.zeros_like(cost_part)
    all_here(kct_buf.at[0:half], one_recv.at[5])
    all_sent(kct_buf.at[0:half], KC)
    for c in range(n_chunk):
        all_here(t_in.at[last, c], t_recv.at[last, c])
        v = v_of(last, c)
        v_all[c // per_half, :, (c % per_half) * cw:(c % per_half + 1) * cw] = v
        prod = jnp.dot(v.astype(BF16), kct_buf[c * cw:(c + 1) * cw, :], preferred_element_type=F32)
        if c < n_chunk - 1:
            acc[...] = prod if c == 0 else acc[...] + prod
        else:
            w = (acc[...] + prod) * u_out[mine]
    v_push = remote(v_all.at[1 - core], v_out.at[mine], send_sem.at[VS], one_recv.at[4], partner)
    v_push.start()
    tot = w[:, 0:128]
    for n in range(1, rows // 128):
        tot = tot + w[:, n * 128:(n + 1) * 128]
    cost_part[mine] = tot
    cost_all[me] = jnp.sum(cost_part[...].T, axis=0, keepdims=True)
    for dr in range(2):
        for dc in range(4):
            if dr or dc:
                remote(cost_all.at[me], cost_all.at[me], send_sem.at[CS], one_recv.at[6], dev((row + dr) % 2, (col + dc) % 4)).start()
    v_out[mine] = v_all[core]
    all_sent(t_out, TT)
    all_here(u_out.at[other], one_recv.at[3])
    u_push.wait_send()
    all_here(v_out.at[other], one_recv.at[4])
    v_push.wait_send()
    all_here(cost_all.at[0:7], one_recv.at[6])
    all_sent(cost_all.at[0:7], CS)


def output_kernel(norm, u_ref, v_ref, c_ref, u_hbm, v_hbm, cost_ref, sem):
    stores = [pltpu.make_async_copy(u_ref, u_hbm, sem.at[0]), pltpu.make_async_copy(v_ref, v_hbm, sem.at[1])]
    for d in stores:
        d.start()
    total = c_ref[0]
    for n in range(1, 8):
        total = total + c_ref[n]
    cost_ref[...] = total[:, :cost_ref.shape[1]] * norm
    for d in stores:
        d.wait()


def solution(mesh):
    n_chunk = 4

    def local_fn(kernel, cost_mat, src_mass, tgt_mass):
        rows, half = kernel.shape
        nprob = src_mass.shape[1]
        nq = nprob // 2
        cols = 2 * half
        rw, cw = rows // n_chunk, cols // n_chunk
        norm = 1.0 / float(rows * mesh.shape["row"] * half * mesh.shape["col"])
        vmem_spec = pl.BlockSpec(memory_space=pltpu.VMEM)
        any_spec = pl.BlockSpec(memory_space=pl.ANY)
        dma = pltpu.SemaphoreType.DMA
        u_vm, v_vm, c_vm = pl.pallas_call(
            lambda *refs: sinkhorn_kernel(n_chunk, *refs),
            out_shape=(pltpu.VMEM((nprob, rows), F32), pltpu.VMEM((nprob, half), F32), pltpu.VMEM((8, 1, 128), F32)),
            in_specs=[any_spec] * 4,
            out_specs=(vmem_spec, vmem_spec, vmem_spec),
            scratch_shapes=[
                pltpu.VMEM((2, rows, half), BF16),
                pltpu.VMEM((cols, rows), BF16),
                pltpu.VMEM((rows, half), BF16),
                pltpu.VMEM((cols, rows), BF16),
                pltpu.VMEM((nprob, rows), F32),
                pltpu.VMEM((2, nq, half), F32),
                pltpu.VMEM((nprob, rows), BF16),
                pltpu.VMEM((nq, max(rows, cols)), F32),
                pltpu.VMEM((n_chunk, nq, rw), F32),
                pltpu.VMEM((2, n_chunk, nq, rw), F32),
                pltpu.VMEM((n_chunk, nq, cw), F32),
                pltpu.VMEM((2, n_chunk, nq, cw), F32),
                pltpu.VMEM((2, n_chunk // 2, nq, cw), F32),
                pltpu.VMEM((4, rows // 128, 128), F32),
                pltpu.VMEM((2, nq, half), F32),
                pltpu.VMEM((128, 128), F32),
                dma((n_chunk + 2,)), dma((11,)), dma((n_chunk,)), dma((2, n_chunk)), dma((2, n_chunk)), dma((7,)),
            ],
            compiler_params=pltpu.CompilerParams(collective_id=0, has_side_effects=True, vmem_limit_bytes=60 * 1024 * 1024),
            name="sinkhorn",
        )(kernel, cost_mat, src_mass.T, tgt_mass.T)
        u_t, v_t, cost = pl.pallas_call(
            lambda *refs: output_kernel(norm, *refs),
            out_shape=(jax.ShapeDtypeStruct((nprob, rows), F32), jax.ShapeDtypeStruct((nprob, half), F32),
                       jax.ShapeDtypeStruct((1, nprob), F32)),
            in_specs=[vmem_spec] * 3,
            out_specs=(any_spec, any_spec, vmem_spec),
            scratch_shapes=[dma((2,))],
            name="outputs",
        )(*(pltpu.with_memory_space_constraint(r, pltpu.VMEM) for r in (u_vm, v_vm, c_vm)))
        return u_t.T, v_t.T, cost.reshape(nprob)

    return jax.shard_map(local_fn, mesh=mesh, in_specs=(P("row", "col"), P("row", "col"), P("row", "prob"), P("col", "prob")), out_specs=(P("row", "prob"), P("col", "prob"), P("prob")), check_vma=False)
```

```python
import jax
import jax.numpy as jnp
from jax import lax
from jax.experimental import pallas as pl
from jax.experimental.pallas import tpu as pltpu
from jax.sharding import PartitionSpec as P

SWEEPS = 6
AHEAD = (8, 7)
WAIT_NS = ((0, 0), (450, 250))
F32 = jnp.float32
BF16 = jnp.bfloat16
MESH = pl.DeviceIdType.MESH


def sinkhorn_kernel(n_chunk, k_hbm, c_hbm, a_hbm, b_hbm, u_out, v_out, cost_all,
                    k_buf, kt_buf, c_buf, kct_buf, a_buf, b_buf, ub_buf, acc,
                    s_out, s_in, t_out, t_in, t0_buf, s0_buf, v_all, cost_part,
                    load_sem, send_sem, kp_recv, s_recv, t_recv, one_recv):
    rows, half = k_hbm.shape
    cols = 2 * half
    rw = rows // n_chunk
    cw = cols // n_chunk
    per_half = n_chunk // 2
    nq = b_buf.shape[1]
    row = lax.axis_index("row")
    col = lax.axis_index("col")
    prob = lax.axis_index("prob")
    x = col // 2
    core = col % 2
    grp = (core + x + row) % 2
    me = row * 4 + col
    mine = pl.ds(pl.multiple_of(grp * nq, nq), nq)
    other = pl.ds(pl.multiple_of((1 - grp) * nq, nq), nq)

    def dev(r, c):
        return (prob, r, c)

    partner = dev(row, 2 * x + 1 - core)
    x_peer = dev(row, 2 * (1 - x) + 1 - core)
    y_peer = dev(1 - row, 2 * x + 1 - core)

    def remote(src, dst, send, recv, to):
        return pltpu.make_async_remote_copy(src_ref=src, dst_ref=dst, send_sem=send, recv_sem=recv,
                                            device_id=to, device_id_type=MESH)

    KP, BP, S0, SS, TT, T0, TP, KC, US, VS, CS = range(11)

    def all_sent(ref, kind):
        remote(ref, ref, send_sem.at[kind], one_recv.at[0], partner).wait_send()

    def all_here(ref, recv):
        remote(ref, ref, send_sem.at[0], recv, partner).wait_recv()

    def krows(i):
        return pl.ds(i * rw, rw)

    k_load = [pltpu.make_async_copy(k_hbm.at[krows(i)], k_buf.at[core, krows(i)], load_sem.at[i]) for i in range(n_chunk)]
    c_load = [pltpu.make_async_copy(c_hbm.at[krows(i)], c_buf.at[krows(i)], load_sem.at[i]) for i in range(n_chunk)]
    a_load = pltpu.make_async_copy(a_hbm, a_buf, load_sem.at[n_chunk])
    b_load = pltpu.make_async_copy(b_hbm.at[mine], b_buf.at[core], load_sem.at[n_chunk + 1])
    for d in k_load:
        d.start()
    a_load.start()
    b_load.start()

    barrier = pltpu.get_barrier_semaphore()
    for dr in range(2):
        for dc in range(4):
            if dr or dc:
                pl.semaphore_signal(barrier, inc=1, device_id=dev((row + dr) % 2, (col + dc) % 4), device_id_type=MESH)

    blk = 256

    def transpose_rows(h, i):
        def body(n, carry):
            jo = pl.multiple_of(n * blk, blk)
            for ii in range(rw // blk):
                kt_buf[pl.ds(pl.multiple_of(h * half + jo, blk), blk), pl.ds(i * rw + ii * blk, blk)] = (
                    k_buf[h, pl.ds(i * rw + ii * blk, blk), pl.ds(jo, blk)].T)
            return carry
        lax.fori_loop(0, half // blk, body, 0)

    kct_pieces = 2 * n_chunk
    kw = rows // kct_pieces

    def build_kct(lo, hi):
        def piece(i, carry):
            rs = pl.ds(pl.multiple_of(i * kw, kw), kw)
            for n in range(half // blk):
                kct_buf[pl.ds(pl.multiple_of(core * half + n * blk, blk), blk), rs] = (
                    k_buf[core, rs, n * blk:(n + 1) * blk] * c_buf[rs, n * blk:(n + 1) * blk]).T
            part = kct_buf.at[pl.ds(pl.multiple_of(core * half, half), half), rs]
            remote(part, part, send_sem.at[KC], one_recv.at[5], partner).start()
            return carry
        lax.fori_loop(lo, hi, piece, 0)

    ahead = grp * (AHEAD[0] + core * (AHEAD[1] - AHEAD[0]))
    middle = grp * kct_pieces + (1 - grp) * (kct_pieces // 2)

    k_push = [remote(k_buf.at[core, krows(i)], k_buf.at[core, krows(i)], send_sem.at[KP], kp_recv.at[i], partner) for i in range(n_chunk)]
    b_push = remote(b_hbm.at[other], b_buf.at[core], send_sem.at[BP], one_recv.at[0], partner)
    pl.semaphore_wait(barrier, 7)
    b_push.start()
    ones = jnp.ones((nq, half), BF16)
    for i in range(n_chunk):
        k_load[i].wait()
        if i == 0:
            k_push[0].start()
        if i % 2:
            part = lax.dot_general(ones, k_buf[core, pl.ds((i - 1) * rw, 2 * rw)], (((1,), (1,)), ((), ())), preferred_element_type=F32)
            for n in range(2 * rw // 128):
                r = (i - 1) * (rw // 128) + n
                s0_buf[col, r:r + 1, :] = part[0:1, n * 128:(n + 1) * 128]
    for n in range(1, 4):
        remote(s0_buf.at[col], s0_buf.at[col], send_sem.at[S0], one_recv.at[1], dev(row, (col + n) % 4)).start()
    for i in range(1, n_chunk):
        k_push[i].start()
    for d in c_load:
        d.start()
    for i in range(n_chunk):
        transpose_rows(core, i)
    a_load.wait()
    b_load.wait()
    all_here(s0_buf.at[0:3], one_recv.at[1])
    s0 = (s0_buf[0] + s0_buf[1]) + (s0_buf[2] + s0_buf[3])
    for r in range(rows // 128):
        cs = slice(r * 128, (r + 1) * 128)
        ub_buf[:, cs] = (a_buf[:, cs] / s0[r:r + 1, :]).astype(BF16)

    def t_copy(par, o):
        return remote(t_out.at[o], t_in.at[par, o], send_sem.at[TT], t_recv.at[par, o], y_peer)

    def s_copy(par, o):
        return remote(s_out.at[o], s_in.at[par, o], send_sem.at[SS], s_recv.at[par, o], x_peer)

    def t0_send(g, n):
        remote(t0_buf.at[g, n], t_in.at[0, core * per_half + n], send_sem.at[T0], t_recv.at[0, core * per_half + n],
               dev(1 - row, 2 * x + (g + x + 1 - row) % 2)).start()

    for n in range(per_half):
        part = jnp.dot(ub_buf[...], k_buf[core, :, n * cw:(n + 1) * cw], preferred_element_type=F32)
        for g in range(2):
            t0_buf[g, n] = part[g * nq:(g + 1) * nq]
        t0_send(0, n)
    for n in range(per_half):
        o = core * per_half + n
        remote(t0_buf.at[1 - grp, n], t_out.at[o], send_sem.at[TP], one_recv.at[2], partner).start()
        t_out[o] = t0_buf[grp, n]

    def v_of(par, o):
        return b_buf[o // per_half, :, (o % per_half) * cw:(o % per_half + 1) * cw] / (t_out[o] + t_in[par, o])

    all_here(b_buf.at[0], one_recv.at[0])
    for i in range(n_chunk):
        all_here(k_buf.at[1 - core, krows(i)], kp_recv.at[i])
        transpose_rows(1 - core, i)
        if i == 1:
            for n in range(per_half):
                t0_send(1, n)

    for d in c_load:
        d.wait()
    build_kct(0, ahead)

    for g in range(2):
        for c in range(2):
            if WAIT_NS[g][c]:
                @pl.when((grp == g) & (core == c))
                def _(g=g, c=c):
                    pl.delay(WAIT_NS[g][c])

    all_here(t0_buf.at[0], one_recv.at[2])
    order = list(range(per_half, n_chunk)) + list(range(per_half))
    for c in order:
        all_here(t_in.at[0, c], t_recv.at[0, c])
        vb = v_of(0, c).astype(BF16)
        js = slice(c * cw, (c + 1) * cw)
        if c != order[-1]:
            prod = jnp.dot(vb, kt_buf[js, :], preferred_element_type=F32)
            acc[...] = prod if c == order[0] else acc[...] + prod
        else:
            for o in range(n_chunk):
                s_out[o] = acc[:, o * rw:(o + 1) * rw] + jnp.dot(vb, kt_buf[js, o * rw:(o + 1) * rw], preferred_element_type=F32)
                s_copy(1, o).start()
    all_sent(t0_buf, T0)
    all_sent(t0_buf.at[0], TP)
    all_sent(s0_buf.at[0:3], S0)
    all_sent(k_buf.at[0], KP)
    all_sent(b_buf.at[0], BP)

    build_kct(ahead, middle)

    def u_and_t(par):
        for c in range(n_chunk):
            all_here(s_in.at[par, c], s_recv.at[par, c])
            w = slice(c * rw, (c + 1) * rw)
            u = a_buf[mine, w] / (s_out[c] + s_in[par, c])
            u_out[mine, w] = u
            ub = u.astype(BF16)
            if c < n_chunk - 1:
                for h in range(2):
                    hc = slice(h * half, (h + 1) * half)
                    prod = jnp.dot(ub, k_buf[h, w, :], preferred_element_type=F32)
                    acc[:, hc] = prod if c == 0 else acc[:, hc] + prod
            else:
                for o in range(n_chunk):
                    oc = slice(o * cw, (o + 1) * cw)
                    hc = slice((o % per_half) * cw, (o % per_half + 1) * cw)
                    t_out[o] = acc[:, oc] + jnp.dot(ub, k_buf[o // per_half, w, hc], preferred_element_type=F32)
                    t_copy(par, o).start()
                all_sent(s_out, SS)

    def v_and_s(par_in, par):
        for c in range(n_chunk):
            all_here(t_in.at[par_in, c], t_recv.at[par_in, c])
            vb = v_of(par_in, c).astype(BF16)
            w = slice(c * cw, (c + 1) * cw)
            if c < n_chunk - 1:
                prod = jnp.dot(vb, kt_buf[w, :], preferred_element_type=F32)
                acc[...] = prod if c == 0 else acc[...] + prod
            else:
                for o in range(n_chunk):
                    oc = slice(o * rw, (o + 1) * rw)
                    s_out[o] = acc[:, oc] + jnp.dot(vb, kt_buf[w, oc], preferred_element_type=F32)
                    s_copy(par, o).start()
                all_sent(t_out, TT)

    def sweep(t, carry):
        u_and_t(t % 2)

        @pl.when(t == 1)
        def _():
            build_kct(middle, kct_pieces)

        v_and_s(t % 2, (t + 1) % 2)
        return carry

    lax.fori_loop(1, SWEEPS - 1, sweep, 0)
    last = (SWEEPS - 1) % 2
    u_and_t(last)

    u_push = remote(u_out.at[mine], u_out.at[mine], send_sem.at[US], one_recv.at[3], partner)
    u_push.start()
    cost_part[...] = jnp.zeros_like(cost_part)
    all_here(kct_buf.at[0:half], one_recv.at[5])
    all_sent(kct_buf.at[0:half], KC)
    for c in range(n_chunk):
        all_here(t_in.at[last, c], t_recv.at[last, c])
        v = v_of(last, c)
        v_all[c // per_half, :, (c % per_half) * cw:(c % per_half + 1) * cw] = v
        prod = jnp.dot(v.astype(BF16), kct_buf[c * cw:(c + 1) * cw, :], preferred_element_type=F32)
        if c < n_chunk - 1:
            acc[...] = prod if c == 0 else acc[...] + prod
        else:
            w = (acc[...] + prod) * u_out[mine]
    v_push = remote(v_all.at[1 - core], v_out.at[mine], send_sem.at[VS], one_recv.at[4], partner)
    v_push.start()
    tot = w[:, 0:128]
    for n in range(1, rows // 128):
        tot = tot + w[:, n * 128:(n + 1) * 128]
    cost_part[mine] = tot
    cost_all[me] = jnp.sum(cost_part[...].T, axis=0, keepdims=True)
    for dr in range(2):
        for dc in range(4):
            if dr or dc:
                remote(cost_all.at[me], cost_all.at[me], send_sem.at[CS], one_recv.at[6], dev((row + dr) % 2, (col + dc) % 4)).start()
    v_out[mine] = v_all[core]
    all_sent(t_out, TT)
    all_here(u_out.at[other], one_recv.at[3])
    u_push.wait_send()
    all_here(v_out.at[other], one_recv.at[4])
    v_push.wait_send()
    all_here(cost_all.at[0:7], one_recv.at[6])
    all_sent(cost_all.at[0:7], CS)


def output_kernel(norm, u_ref, v_ref, c_ref, u_hbm, v_hbm, cost_ref, sem):
    stores = [pltpu.make_async_copy(u_ref, u_hbm, sem.at[0]), pltpu.make_async_copy(v_ref, v_hbm, sem.at[1])]
    for d in stores:
        d.start()
    total = c_ref[0]
    for n in range(1, 8):
        total = total + c_ref[n]
    cost_ref[...] = total[:, :cost_ref.shape[1]] * norm
    for d in stores:
        d.wait()


def solution(mesh):
    n_chunk = 4

    def local_fn(kernel, cost_mat, src_mass, tgt_mass):
        rows, half = kernel.shape
        nprob = src_mass.shape[1]
        nq = nprob // 2
        cols = 2 * half
        rw, cw = rows // n_chunk, cols // n_chunk
        norm = 1.0 / float(rows * mesh.shape["row"] * half * mesh.shape["col"])
        vmem_spec = pl.BlockSpec(memory_space=pltpu.VMEM)
        any_spec = pl.BlockSpec(memory_space=pl.ANY)
        dma = pltpu.SemaphoreType.DMA
        u_vm, v_vm, c_vm = pl.pallas_call(
            lambda *refs: sinkhorn_kernel(n_chunk, *refs),
            out_shape=(pltpu.VMEM((nprob, rows), F32), pltpu.VMEM((nprob, half), F32), pltpu.VMEM((8, 1, 128), F32)),
            in_specs=[any_spec] * 4,
            out_specs=(vmem_spec, vmem_spec, vmem_spec),
            scratch_shapes=[
                pltpu.VMEM((2, rows, half), BF16),
                pltpu.VMEM((cols, rows), BF16),
                pltpu.VMEM((rows, half), BF16),
                pltpu.VMEM((cols, rows), BF16),
                pltpu.VMEM((nprob, rows), F32),
                pltpu.VMEM((2, nq, half), F32),
                pltpu.VMEM((nprob, rows), BF16),
                pltpu.VMEM((nq, max(rows, cols)), F32),
                pltpu.VMEM((n_chunk, nq, rw), F32),
                pltpu.VMEM((2, n_chunk, nq, rw), F32),
                pltpu.VMEM((n_chunk, nq, cw), F32),
                pltpu.VMEM((2, n_chunk, nq, cw), F32),
                pltpu.VMEM((2, n_chunk // 2, nq, cw), F32),
                pltpu.VMEM((4, rows // 128, 128), F32),
                pltpu.VMEM((2, nq, half), F32),
                pltpu.VMEM((128, 128), F32),
                dma((n_chunk + 2,)), dma((11,)), dma((n_chunk,)), dma((2, n_chunk)), dma((2, n_chunk)), dma((7,)),
            ],
            compiler_params=pltpu.CompilerParams(collective_id=0, has_side_effects=True, vmem_limit_bytes=60 * 1024 * 1024),
            name="sinkhorn",
        )(kernel, cost_mat, src_mass.T, tgt_mass.T)
        u_t, v_t, cost = pl.pallas_call(
            lambda *refs: output_kernel(norm, *refs),
            out_shape=(jax.ShapeDtypeStruct((nprob, rows), F32), jax.ShapeDtypeStruct((nprob, half), F32),
                       jax.ShapeDtypeStruct((1, nprob), F32)),
            in_specs=[vmem_spec] * 3,
            out_specs=(any_spec, any_spec, vmem_spec),
            scratch_shapes=[dma((2,))],
            name="outputs",
        )(*(pltpu.with_memory_space_constraint(r, pltpu.VMEM) for r in (u_vm, v_vm, c_vm)))
        return u_t.T, v_t.T, cost.reshape(nprob)

    return jax.shard_map(local_fn, mesh=mesh, in_specs=(P("row", "col"), P("row", "col"), P("row", "prob"), P("col", "prob")), out_specs=(P("row", "prob"), P("col", "prob"), P("prob")), check_vma=False)
```

```python
import jax
import jax.numpy as jnp
from jax import lax
from jax.experimental import pallas as pl
from jax.experimental.pallas import tpu as pltpu
from jax.sharding import PartitionSpec as P

SWEEPS = 6
AHEAD = (8, 7)
WAIT_NS = ((0, 0), (600, 250))
F32 = jnp.float32
BF16 = jnp.bfloat16
MESH = pl.DeviceIdType.MESH


def sinkhorn_kernel(n_chunk, k_hbm, c_hbm, a_hbm, b_hbm, u_out, v_out, cost_all,
                    k_buf, kt_buf, c_buf, kct_buf, a_buf, b_buf, ub_buf, acc,
                    s_out, s_in, t_out, t_in, t0_buf, s0_buf, v_all, cost_part,
                    load_sem, send_sem, kp_recv, s_recv, t_recv, one_recv):
    rows, half = k_hbm.shape
    cols = 2 * half
    rw = rows // n_chunk
    cw = cols // n_chunk
    per_half = n_chunk // 2
    nq = b_buf.shape[1]
    row = lax.axis_index("row")
    col = lax.axis_index("col")
    prob = lax.axis_index("prob")
    x = col // 2
    core = col % 2
    grp = (core + x + row) % 2
    me = row * 4 + col
    mine = pl.ds(pl.multiple_of(grp * nq, nq), nq)
    other = pl.ds(pl.multiple_of((1 - grp) * nq, nq), nq)

    def dev(r, c):
        return (prob, r, c)

    partner = dev(row, 2 * x + 1 - core)
    x_peer = dev(row, 2 * (1 - x) + 1 - core)
    y_peer = dev(1 - row, 2 * x + 1 - core)

    def remote(src, dst, send, recv, to):
        return pltpu.make_async_remote_copy(src_ref=src, dst_ref=dst, send_sem=send, recv_sem=recv,
                                            device_id=to, device_id_type=MESH)

    KP, BP, S0, SS, TT, T0, TP, KC, US, VS, CS = range(11)

    def all_sent(ref, kind):
        remote(ref, ref, send_sem.at[kind], one_recv.at[0], partner).wait_send()

    def all_here(ref, recv):
        remote(ref, ref, send_sem.at[0], recv, partner).wait_recv()

    def krows(i):
        return pl.ds(i * rw, rw)

    k_load = [pltpu.make_async_copy(k_hbm.at[krows(i)], k_buf.at[core, krows(i)], load_sem.at[i]) for i in range(n_chunk)]
    c_load = [pltpu.make_async_copy(c_hbm.at[krows(i)], c_buf.at[krows(i)], load_sem.at[i]) for i in range(n_chunk)]
    a_load = pltpu.make_async_copy(a_hbm, a_buf, load_sem.at[n_chunk])
    b_load = pltpu.make_async_copy(b_hbm.at[mine], b_buf.at[core], load_sem.at[n_chunk + 1])
    for d in k_load:
        d.start()
    a_load.start()
    b_load.start()

    barrier = pltpu.get_barrier_semaphore()
    for dr in range(2):
        for dc in range(4):
            if dr or dc:
                pl.semaphore_signal(barrier, inc=1, device_id=dev((row + dr) % 2, (col + dc) % 4), device_id_type=MESH)

    blk = 256

    def transpose_rows(h, i):
        def body(n, carry):
            jo = pl.multiple_of(n * blk, blk)
            for ii in range(rw // blk):
                kt_buf[pl.ds(pl.multiple_of(h * half + jo, blk), blk), pl.ds(i * rw + ii * blk, blk)] = (
                    k_buf[h, pl.ds(i * rw + ii * blk, blk), pl.ds(jo, blk)].T)
            return carry
        lax.fori_loop(0, half // blk, body, 0)

    kct_pieces = 2 * n_chunk
    kw = rows // kct_pieces

    def build_kct(lo, hi):
        def piece(i, carry):
            rs = pl.ds(pl.multiple_of(i * kw, kw), kw)
            for n in range(half // blk):
                kct_buf[pl.ds(pl.multiple_of(core * half + n * blk, blk), blk), rs] = (
                    k_buf[core, rs, n * blk:(n + 1) * blk] * c_buf[rs, n * blk:(n + 1) * blk]).T
            part = kct_buf.at[pl.ds(pl.multiple_of(core * half, half), half), rs]
            remote(part, part, send_sem.at[KC], one_recv.at[5], partner).start()
            return carry
        lax.fori_loop(lo, hi, piece, 0)

    ahead = grp * (AHEAD[0] + core * (AHEAD[1] - AHEAD[0]))
    middle = grp * kct_pieces + (1 - grp) * (kct_pieces // 2)

    k_push = [remote(k_buf.at[core, krows(i)], k_buf.at[core, krows(i)], send_sem.at[KP], kp_recv.at[i], partner) for i in range(n_chunk)]
    b_push = remote(b_hbm.at[other], b_buf.at[core], send_sem.at[BP], one_recv.at[0], partner)
    pl.semaphore_wait(barrier, 7)
    b_push.start()
    ones = jnp.ones((nq, half), BF16)
    for i in range(n_chunk):
        k_load[i].wait()
        if i == 0:
            k_push[0].start()
        if i % 2:
            part = lax.dot_general(ones, k_buf[core, pl.ds((i - 1) * rw, 2 * rw)], (((1,), (1,)), ((), ())), preferred_element_type=F32)
            for n in range(2 * rw // 128):
                r = (i - 1) * (rw // 128) + n
                s0_buf[col, r:r + 1, :] = part[0:1, n * 128:(n + 1) * 128]
    for n in range(1, 4):
        remote(s0_buf.at[col], s0_buf.at[col], send_sem.at[S0], one_recv.at[1], dev(row, (col + n) % 4)).start()
    for i in range(1, n_chunk):
        k_push[i].start()
    for d in c_load:
        d.start()
    for i in range(n_chunk):
        transpose_rows(core, i)
    a_load.wait()
    b_load.wait()
    all_here(s0_buf.at[0:3], one_recv.at[1])
    s0 = (s0_buf[0] + s0_buf[1]) + (s0_buf[2] + s0_buf[3])
    for r in range(rows // 128):
        cs = slice(r * 128, (r + 1) * 128)
        ub_buf[:, cs] = (a_buf[:, cs] / s0[r:r + 1, :]).astype(BF16)

    def t_copy(par, o):
        return remote(t_out.at[o], t_in.at[par, o], send_sem.at[TT], t_recv.at[par, o], y_peer)

    def s_copy(par, o):
        return remote(s_out.at[o], s_in.at[par, o], send_sem.at[SS], s_recv.at[par, o], x_peer)

    def t0_send(g, n):
        remote(t0_buf.at[g, n], t_in.at[0, core * per_half + n], send_sem.at[T0], t_recv.at[0, core * per_half + n],
               dev(1 - row, 2 * x + (g + x + 1 - row) % 2)).start()

    for n in range(per_half):
        part = jnp.dot(ub_buf[...], k_buf[core, :, n * cw:(n + 1) * cw], preferred_element_type=F32)
        for g in range(2):
            t0_buf[g, n] = part[g * nq:(g + 1) * nq]
        t0_send(0, n)
    for n in range(per_half):
        o = core * per_half + n
        remote(t0_buf.at[1 - grp, n], t_out.at[o], send_sem.at[TP], one_recv.at[2], partner).start()
        t_out[o] = t0_buf[grp, n]

    def v_of(par, o):
        return b_buf[o // per_half, :, (o % per_half) * cw:(o % per_half + 1) * cw] / (t_out[o] + t_in[par, o])

    all_here(b_buf.at[0], one_recv.at[0])
    for i in range(n_chunk):
        all_here(k_buf.at[1 - core, krows(i)], kp_recv.at[i])
        transpose_rows(1 - core, i)
        if i == 1:
            for n in range(per_half):
                t0_send(1, n)

    for d in c_load:
        d.wait()
    build_kct(0, ahead)

    for g in range(2):
        for c in range(2):
            if WAIT_NS[g][c]:
                @pl.when((grp == g) & (core == c))
                def _(g=g, c=c):
                    pl.delay(WAIT_NS[g][c])

    all_here(t0_buf.at[0], one_recv.at[2])
    order = list(range(per_half, n_chunk)) + list(range(per_half))
    for c in order:
        all_here(t_in.at[0, c], t_recv.at[0, c])
        vb = v_of(0, c).astype(BF16)
        js = slice(c * cw, (c + 1) * cw)
        if c != order[-1]:
            prod = jnp.dot(vb, kt_buf[js, :], preferred_element_type=F32)
            acc[...] = prod if c == order[0] else acc[...] + prod
        else:
            for o in range(n_chunk):
                s_out[o] = acc[:, o * rw:(o + 1) * rw] + jnp.dot(vb, kt_buf[js, o * rw:(o + 1) * rw], preferred_element_type=F32)
                s_copy(1, o).start()
    all_sent(t0_buf, T0)
    all_sent(t0_buf.at[0], TP)
    all_sent(s0_buf.at[0:3], S0)
    all_sent(k_buf.at[0], KP)
    all_sent(b_buf.at[0], BP)

    build_kct(ahead, middle)

    def u_and_t(par):
        for c in range(n_chunk):
            all_here(s_in.at[par, c], s_recv.at[par, c])
            w = slice(c * rw, (c + 1) * rw)
            u = a_buf[mine, w] / (s_out[c] + s_in[par, c])
            u_out[mine, w] = u
            ub = u.astype(BF16)
            if c < n_chunk - 1:
                for h in range(2):
                    hc = slice(h * half, (h + 1) * half)
                    prod = jnp.dot(ub, k_buf[h, w, :], preferred_element_type=F32)
                    acc[:, hc] = prod if c == 0 else acc[:, hc] + prod
            else:
                for o in range(n_chunk):
                    oc = slice(o * cw, (o + 1) * cw)
                    hc = slice((o % per_half) * cw, (o % per_half + 1) * cw)
                    t_out[o] = acc[:, oc] + jnp.dot(ub, k_buf[o // per_half, w, hc], preferred_element_type=F32)
                    t_copy(par, o).start()
                all_sent(s_out, SS)

    def v_and_s(par_in, par):
        for c in range(n_chunk):
            all_here(t_in.at[par_in, c], t_recv.at[par_in, c])
            vb = v_of(par_in, c).astype(BF16)
            w = slice(c * cw, (c + 1) * cw)
            if c < n_chunk - 1:
                prod = jnp.dot(vb, kt_buf[w, :], preferred_element_type=F32)
                acc[...] = prod if c == 0 else acc[...] + prod
            else:
                for o in range(n_chunk):
                    oc = slice(o * rw, (o + 1) * rw)
                    s_out[o] = acc[:, oc] + jnp.dot(vb, kt_buf[w, oc], preferred_element_type=F32)
                    s_copy(par, o).start()
                all_sent(t_out, TT)

    def sweep(t, carry):
        u_and_t(t % 2)

        @pl.when(t == 1)
        def _():
            build_kct(middle, kct_pieces)

        v_and_s(t % 2, (t + 1) % 2)
        return carry

    lax.fori_loop(1, SWEEPS - 1, sweep, 0)
    last = (SWEEPS - 1) % 2
    u_and_t(last)

    u_push = remote(u_out.at[mine], u_out.at[mine], send_sem.at[US], one_recv.at[3], partner)
    u_push.start()
    cost_part[...] = jnp.zeros_like(cost_part)
    all_here(kct_buf.at[0:half], one_recv.at[5])
    all_sent(kct_buf.at[0:half], KC)
    for c in range(n_chunk):
        all_here(t_in.at[last, c], t_recv.at[last, c])
        v = v_of(last, c)
        v_all[c // per_half, :, (c % per_half) * cw:(c % per_half + 1) * cw] = v
        prod = jnp.dot(v.astype(BF16), kct_buf[c * cw:(c + 1) * cw, :], preferred_element_type=F32)
        if c < n_chunk - 1:
            acc[...] = prod if c == 0 else acc[...] + prod
        else:
            w = (acc[...] + prod) * u_out[mine]
    v_push = remote(v_all.at[1 - core], v_out.at[mine], send_sem.at[VS], one_recv.at[4], partner)
    v_push.start()
    tot = w[:, 0:128]
    for n in range(1, rows // 128):
        tot = tot + w[:, n * 128:(n + 1) * 128]
    cost_part[mine] = tot
    cost_all[me] = jnp.sum(cost_part[...].T, axis=0, keepdims=True)
    for dr in range(2):
        for dc in range(4):
            if dr or dc:
                remote(cost_all.at[me], cost_all.at[me], send_sem.at[CS], one_recv.at[6], dev((row + dr) % 2, (col + dc) % 4)).start()
    v_out[mine] = v_all[core]
    all_sent(t_out, TT)
    all_here(u_out.at[other], one_recv.at[3])
    u_push.wait_send()
    all_here(v_out.at[other], one_recv.at[4])
    v_push.wait_send()
    all_here(cost_all.at[0:7], one_recv.at[6])
    all_sent(cost_all.at[0:7], CS)


def output_kernel(norm, u_ref, v_ref, c_ref, u_hbm, v_hbm, cost_ref, sem):
    stores = [pltpu.make_async_copy(u_ref, u_hbm, sem.at[0]), pltpu.make_async_copy(v_ref, v_hbm, sem.at[1])]
    for d in stores:
        d.start()
    total = c_ref[0]
    for n in range(1, 8):
        total = total + c_ref[n]
    cost_ref[...] = total[:, :cost_ref.shape[1]] * norm
    for d in stores:
        d.wait()


def solution(mesh):
    n_chunk = 4

    def local_fn(kernel, cost_mat, src_mass, tgt_mass):
        rows, half = kernel.shape
        nprob = src_mass.shape[1]
        nq = nprob // 2
        cols = 2 * half
        rw, cw = rows // n_chunk, cols // n_chunk
        norm = 1.0 / float(rows * mesh.shape["row"] * half * mesh.shape["col"])
        vmem_spec = pl.BlockSpec(memory_space=pltpu.VMEM)
        any_spec = pl.BlockSpec(memory_space=pl.ANY)
        dma = pltpu.SemaphoreType.DMA
        u_vm, v_vm, c_vm = pl.pallas_call(
            lambda *refs: sinkhorn_kernel(n_chunk, *refs),
            out_shape=(pltpu.VMEM((nprob, rows), F32), pltpu.VMEM((nprob, half), F32), pltpu.VMEM((8, 1, 128), F32)),
            in_specs=[any_spec] * 4,
            out_specs=(vmem_spec, vmem_spec, vmem_spec),
            scratch_shapes=[
                pltpu.VMEM((2, rows, half), BF16),
                pltpu.VMEM((cols, rows), BF16),
                pltpu.VMEM((rows, half), BF16),
                pltpu.VMEM((cols, rows), BF16),
                pltpu.VMEM((nprob, rows), F32),
                pltpu.VMEM((2, nq, half), F32),
                pltpu.VMEM((nprob, rows), BF16),
                pltpu.VMEM((nq, max(rows, cols)), F32),
                pltpu.VMEM((n_chunk, nq, rw), F32),
                pltpu.VMEM((2, n_chunk, nq, rw), F32),
                pltpu.VMEM((n_chunk, nq, cw), F32),
                pltpu.VMEM((2, n_chunk, nq, cw), F32),
                pltpu.VMEM((2, n_chunk // 2, nq, cw), F32),
                pltpu.VMEM((4, rows // 128, 128), F32),
                pltpu.VMEM((2, nq, half), F32),
                pltpu.VMEM((128, 128), F32),
                dma((n_chunk + 2,)), dma((11,)), dma((n_chunk,)), dma((2, n_chunk)), dma((2, n_chunk)), dma((7,)),
            ],
            compiler_params=pltpu.CompilerParams(collective_id=0, has_side_effects=True, vmem_limit_bytes=60 * 1024 * 1024),
            name="sinkhorn",
        )(kernel, cost_mat, src_mass.T, tgt_mass.T)
        u_t, v_t, cost = pl.pallas_call(
            lambda *refs: output_kernel(norm, *refs),
            out_shape=(jax.ShapeDtypeStruct((nprob, rows), F32), jax.ShapeDtypeStruct((nprob, half), F32),
                       jax.ShapeDtypeStruct((1, nprob), F32)),
            in_specs=[vmem_spec] * 3,
            out_specs=(any_spec, any_spec, vmem_spec),
            scratch_shapes=[dma((2,))],
            name="outputs",
        )(*(pltpu.with_memory_space_constraint(r, pltpu.VMEM) for r in (u_vm, v_vm, c_vm)))
        return u_t.T, v_t.T, cost.reshape(nprob)

    return jax.shard_map(local_fn, mesh=mesh, in_specs=(P("row", "col"), P("row", "col"), P("row", "prob"), P("col", "prob")), out_specs=(P("row", "prob"), P("col", "prob"), P("prob")), check_vma=False)
```

```python
import jax
import jax.numpy as jnp
from jax import lax
from jax.experimental import pallas as pl
from jax.experimental.pallas import tpu as pltpu
from jax.sharding import PartitionSpec as P

SWEEPS = 6
AHEAD = (8, 7)
WAIT_NS = ((0, 150), (450, 250))
F32 = jnp.float32
BF16 = jnp.bfloat16
MESH = pl.DeviceIdType.MESH


def sinkhorn_kernel(n_chunk, k_hbm, c_hbm, a_hbm, b_hbm, u_out, v_out, cost_all,
                    k_buf, kt_buf, c_buf, kct_buf, a_buf, b_buf, ub_buf, acc,
                    s_out, s_in, t_out, t_in, t0_buf, s0_buf, v_all, cost_part,
                    load_sem, send_sem, kp_recv, s_recv, t_recv, one_recv):
    rows, half = k_hbm.shape
    cols = 2 * half
    rw = rows // n_chunk
    cw = cols // n_chunk
    per_half = n_chunk // 2
    nq = b_buf.shape[1]
    row = lax.axis_index("row")
    col = lax.axis_index("col")
    prob = lax.axis_index("prob")
    x = col // 2
    core = col % 2
    grp = (core + x + row) % 2
    me = row * 4 + col
    mine = pl.ds(pl.multiple_of(grp * nq, nq), nq)
    other = pl.ds(pl.multiple_of((1 - grp) * nq, nq), nq)

    def dev(r, c):
        return (prob, r, c)

    partner = dev(row, 2 * x + 1 - core)
    x_peer = dev(row, 2 * (1 - x) + 1 - core)
    y_peer = dev(1 - row, 2 * x + 1 - core)

    def remote(src, dst, send, recv, to):
        return pltpu.make_async_remote_copy(src_ref=src, dst_ref=dst, send_sem=send, recv_sem=recv,
                                            device_id=to, device_id_type=MESH)

    KP, BP, S0, SS, TT, T0, TP, KC, US, VS, CS = range(11)

    def all_sent(ref, kind):
        remote(ref, ref, send_sem.at[kind], one_recv.at[0], partner).wait_send()

    def all_here(ref, recv):
        remote(ref, ref, send_sem.at[0], recv, partner).wait_recv()

    def krows(i):
        return pl.ds(i * rw, rw)

    k_load = [pltpu.make_async_copy(k_hbm.at[krows(i)], k_buf.at[core, krows(i)], load_sem.at[i]) for i in range(n_chunk)]
    c_load = [pltpu.make_async_copy(c_hbm.at[krows(i)], c_buf.at[krows(i)], load_sem.at[i]) for i in range(n_chunk)]
    a_load = pltpu.make_async_copy(a_hbm, a_buf, load_sem.at[n_chunk])
    b_load = pltpu.make_async_copy(b_hbm.at[mine], b_buf.at[core], load_sem.at[n_chunk + 1])
    for d in k_load:
        d.start()
    a_load.start()
    b_load.start()

    barrier = pltpu.get_barrier_semaphore()
    for dr in range(2):
        for dc in range(4):
            if dr or dc:
                pl.semaphore_signal(barrier, inc=1, device_id=dev((row + dr) % 2, (col + dc) % 4), device_id_type=MESH)

    blk = 256

    def transpose_rows(h, i):
        def body(n, carry):
            jo = pl.multiple_of(n * blk, blk)
            for ii in range(rw // blk):
                kt_buf[pl.ds(pl.multiple_of(h * half + jo, blk), blk), pl.ds(i * rw + ii * blk, blk)] = (
                    k_buf[h, pl.ds(i * rw + ii * blk, blk), pl.ds(jo, blk)].T)
            return carry
        lax.fori_loop(0, half // blk, body, 0)

    kct_pieces = 2 * n_chunk
    kw = rows // kct_pieces

    def build_kct(lo, hi):
        def piece(i, carry):
            rs = pl.ds(pl.multiple_of(i * kw, kw), kw)
            for n in range(half // blk):
                kct_buf[pl.ds(pl.multiple_of(core * half + n * blk, blk), blk), rs] = (
                    k_buf[core, rs, n * blk:(n + 1) * blk] * c_buf[rs, n * blk:(n + 1) * blk]).T
            part = kct_buf.at[pl.ds(pl.multiple_of(core * half, half), half), rs]
            remote(part, part, send_sem.at[KC], one_recv.at[5], partner).start()
            return carry
        lax.fori_loop(lo, hi, piece, 0)

    ahead = grp * (AHEAD[0] + core * (AHEAD[1] - AHEAD[0]))
    middle = grp * kct_pieces + (1 - grp) * (kct_pieces // 2)

    k_push = [remote(k_buf.at[core, krows(i)], k_buf.at[core, krows(i)], send_sem.at[KP], kp_recv.at[i], partner) for i in range(n_chunk)]
    b_push = remote(b_hbm.at[other], b_buf.at[core], send_sem.at[BP], one_recv.at[0], partner)
    pl.semaphore_wait(barrier, 7)
    b_push.start()
    ones = jnp.ones((nq, half), BF16)
    for i in range(n_chunk):
        k_load[i].wait()
        if i == 0:
            k_push[0].start()
        if i % 2:
            part = lax.dot_general(ones, k_buf[core, pl.ds((i - 1) * rw, 2 * rw)], (((1,), (1,)), ((), ())), preferred_element_type=F32)
            for n in range(2 * rw // 128):
                r = (i - 1) * (rw // 128) + n
                s0_buf[col, r:r + 1, :] = part[0:1, n * 128:(n + 1) * 128]
    for n in range(1, 4):
        remote(s0_buf.at[col], s0_buf.at[col], send_sem.at[S0], one_recv.at[1], dev(row, (col + n) % 4)).start()
    for i in range(1, n_chunk):
        k_push[i].start()
    for d in c_load:
        d.start()
    for i in range(n_chunk):
        transpose_rows(core, i)
    a_load.wait()
    b_load.wait()
    all_here(s0_buf.at[0:3], one_recv.at[1])
    s0 = (s0_buf[0] + s0_buf[1]) + (s0_buf[2] + s0_buf[3])
    for r in range(rows // 128):
        cs = slice(r * 128, (r + 1) * 128)
        ub_buf[:, cs] = (a_buf[:, cs] / s0[r:r + 1, :]).astype(BF16)

    def t_copy(par, o):
        return remote(t_out.at[o], t_in.at[par, o], send_sem.at[TT], t_recv.at[par, o], y_peer)

    def s_copy(par, o):
        return remote(s_out.at[o], s_in.at[par, o], send_sem.at[SS], s_recv.at[par, o], x_peer)

    def t0_send(g, n):
        remote(t0_buf.at[g, n], t_in.at[0, core * per_half + n], send_sem.at[T0], t_recv.at[0, core * per_half + n],
               dev(1 - row, 2 * x + (g + x + 1 - row) % 2)).start()

    for n in range(per_half):
        part = jnp.dot(ub_buf[...], k_buf[core, :, n * cw:(n + 1) * cw], preferred_element_type=F32)
        for g in range(2):
            t0_buf[g, n] = part[g * nq:(g + 1) * nq]
        t0_send(0, n)
    for n in range(per_half):
        o = core * per_half + n
        remote(t0_buf.at[1 - grp, n], t_out.at[o], send_sem.at[TP], one_recv.at[2], partner).start()
        t_out[o] = t0_buf[grp, n]

    def v_of(par, o):
        return b_buf[o // per_half, :, (o % per_half) * cw:(o % per_half + 1) * cw] / (t_out[o] + t_in[par, o])

    all_here(b_buf.at[0], one_recv.at[0])
    for i in range(n_chunk):
        all_here(k_buf.at[1 - core, krows(i)], kp_recv.at[i])
        transpose_rows(1 - core, i)
        if i == 1:
            for n in range(per_half):
                t0_send(1, n)

    for d in c_load:
        d.wait()
    build_kct(0, ahead)

    for g in range(2):
        for c in range(2):
            if WAIT_NS[g][c]:
                @pl.when((grp == g) & (core == c))
                def _(g=g, c=c):
                    pl.delay(WAIT_NS[g][c])

    all_here(t0_buf.at[0], one_recv.at[2])
    order = list(range(per_half, n_chunk)) + list(range(per_half))
    for c in order:
        all_here(t_in.at[0, c], t_recv.at[0, c])
        vb = v_of(0, c).astype(BF16)
        js = slice(c * cw, (c + 1) * cw)
        if c != order[-1]:
            prod = jnp.dot(vb, kt_buf[js, :], preferred_element_type=F32)
            acc[...] = prod if c == order[0] else acc[...] + prod
        else:
            for o in range(n_chunk):
                s_out[o] = acc[:, o * rw:(o + 1) * rw] + jnp.dot(vb, kt_buf[js, o * rw:(o + 1) * rw], preferred_element_type=F32)
                s_copy(1, o).start()
    all_sent(t0_buf, T0)
    all_sent(t0_buf.at[0], TP)
    all_sent(s0_buf.at[0:3], S0)
    all_sent(k_buf.at[0], KP)
    all_sent(b_buf.at[0], BP)

    build_kct(ahead, middle)

    def u_and_t(par):
        for c in range(n_chunk):
            all_here(s_in.at[par, c], s_recv.at[par, c])
            w = slice(c * rw, (c + 1) * rw)
            u = a_buf[mine, w] / (s_out[c] + s_in[par, c])
            u_out[mine, w] = u
            ub = u.astype(BF16)
            if c < n_chunk - 1:
                for h in range(2):
                    hc = slice(h * half, (h + 1) * half)
                    prod = jnp.dot(ub, k_buf[h, w, :], preferred_element_type=F32)
                    acc[:, hc] = prod if c == 0 else acc[:, hc] + prod
            else:
                for o in range(n_chunk):
                    oc = slice(o * cw, (o + 1) * cw)
                    hc = slice((o % per_half) * cw, (o % per_half + 1) * cw)
                    t_out[o] = acc[:, oc] + jnp.dot(ub, k_buf[o // per_half, w, hc], preferred_element_type=F32)
                    t_copy(par, o).start()
                all_sent(s_out, SS)

    def v_and_s(par_in, par):
        for c in range(n_chunk):
            all_here(t_in.at[par_in, c], t_recv.at[par_in, c])
            vb = v_of(par_in, c).astype(BF16)
            w = slice(c * cw, (c + 1) * cw)
            if c < n_chunk - 1:
                prod = jnp.dot(vb, kt_buf[w, :], preferred_element_type=F32)
                acc[...] = prod if c == 0 else acc[...] + prod
            else:
                for o in range(n_chunk):
                    oc = slice(o * rw, (o + 1) * rw)
                    s_out[o] = acc[:, oc] + jnp.dot(vb, kt_buf[w, oc], preferred_element_type=F32)
                    s_copy(par, o).start()
                all_sent(t_out, TT)

    def sweep(t, carry):
        u_and_t(t % 2)

        @pl.when(t == 1)
        def _():
            build_kct(middle, kct_pieces)

        v_and_s(t % 2, (t + 1) % 2)
        return carry

    lax.fori_loop(1, SWEEPS - 1, sweep, 0)
    last = (SWEEPS - 1) % 2
    u_and_t(last)

    u_push = remote(u_out.at[mine], u_out.at[mine], send_sem.at[US], one_recv.at[3], partner)
    u_push.start()
    cost_part[...] = jnp.zeros_like(cost_part)
    all_here(kct_buf.at[0:half], one_recv.at[5])
    all_sent(kct_buf.at[0:half], KC)
    for c in range(n_chunk):
        all_here(t_in.at[last, c], t_recv.at[last, c])
        v = v_of(last, c)
        v_all[c // per_half, :, (c % per_half) * cw:(c % per_half + 1) * cw] = v
        prod = jnp.dot(v.astype(BF16), kct_buf[c * cw:(c + 1) * cw, :], preferred_element_type=F32)
        if c < n_chunk - 1:
            acc[...] = prod if c == 0 else acc[...] + prod
        else:
            w = (acc[...] + prod) * u_out[mine]
    v_push = remote(v_all.at[1 - core], v_out.at[mine], send_sem.at[VS], one_recv.at[4], partner)
    v_push.start()
    tot = w[:, 0:128]
    for n in range(1, rows // 128):
        tot = tot + w[:, n * 128:(n + 1) * 128]
    cost_part[mine] = tot
    cost_all[me] = jnp.sum(cost_part[...].T, axis=0, keepdims=True)
    for dr in range(2):
        for dc in range(4):
            if dr or dc:
                remote(cost_all.at[me], cost_all.at[me], send_sem.at[CS], one_recv.at[6], dev((row + dr) % 2, (col + dc) % 4)).start()
    v_out[mine] = v_all[core]
    all_sent(t_out, TT)
    all_here(u_out.at[other], one_recv.at[3])
    u_push.wait_send()
    all_here(v_out.at[other], one_recv.at[4])
    v_push.wait_send()
    all_here(cost_all.at[0:7], one_recv.at[6])
    all_sent(cost_all.at[0:7], CS)


def output_kernel(norm, u_ref, v_ref, c_ref, u_hbm, v_hbm, cost_ref, sem):
    stores = [pltpu.make_async_copy(u_ref, u_hbm, sem.at[0]), pltpu.make_async_copy(v_ref, v_hbm, sem.at[1])]
    for d in stores:
        d.start()
    total = c_ref[0]
    for n in range(1, 8):
        total = total + c_ref[n]
    cost_ref[...] = total[:, :cost_ref.shape[1]] * norm
    for d in stores:
        d.wait()


def solution(mesh):
    n_chunk = 4

    def local_fn(kernel, cost_mat, src_mass, tgt_mass):
        rows, half = kernel.shape
        nprob = src_mass.shape[1]
        nq = nprob // 2
        cols = 2 * half
        rw, cw = rows // n_chunk, cols // n_chunk
        norm = 1.0 / float(rows * mesh.shape["row"] * half * mesh.shape["col"])
        vmem_spec = pl.BlockSpec(memory_space=pltpu.VMEM)
        any_spec = pl.BlockSpec(memory_space=pl.ANY)
        dma = pltpu.SemaphoreType.DMA
        u_vm, v_vm, c_vm = pl.pallas_call(
            lambda *refs: sinkhorn_kernel(n_chunk, *refs),
            out_shape=(pltpu.VMEM((nprob, rows), F32), pltpu.VMEM((nprob, half), F32), pltpu.VMEM((8, 1, 128), F32)),
            in_specs=[any_spec] * 4,
            out_specs=(vmem_spec, vmem_spec, vmem_spec),
            scratch_shapes=[
                pltpu.VMEM((2, rows, half), BF16),
                pltpu.VMEM((cols, rows), BF16),
                pltpu.VMEM((rows, half), BF16),
                pltpu.VMEM((cols, rows), BF16),
                pltpu.VMEM((nprob, rows), F32),
                pltpu.VMEM((2, nq, half), F32),
                pltpu.VMEM((nprob, rows), BF16),
                pltpu.VMEM((nq, max(rows, cols)), F32),
                pltpu.VMEM((n_chunk, nq, rw), F32),
                pltpu.VMEM((2, n_chunk, nq, rw), F32),
                pltpu.VMEM((n_chunk, nq, cw), F32),
                pltpu.VMEM((2, n_chunk, nq, cw), F32),
                pltpu.VMEM((2, n_chunk // 2, nq, cw), F32),
                pltpu.VMEM((4, rows // 128, 128), F32),
                pltpu.VMEM((2, nq, half), F32),
                pltpu.VMEM((128, 128), F32),
                dma((n_chunk + 2,)), dma((11,)), dma((n_chunk,)), dma((2, n_chunk)), dma((2, n_chunk)), dma((7,)),
            ],
            compiler_params=pltpu.CompilerParams(collective_id=0, has_side_effects=True, vmem_limit_bytes=60 * 1024 * 1024),
            name="sinkhorn",
        )(kernel, cost_mat, src_mass.T, tgt_mass.T)
        u_t, v_t, cost = pl.pallas_call(
            lambda *refs: output_kernel(norm, *refs),
            out_shape=(jax.ShapeDtypeStruct((nprob, rows), F32), jax.ShapeDtypeStruct((nprob, half), F32),
                       jax.ShapeDtypeStruct((1, nprob), F32)),
            in_specs=[vmem_spec] * 3,
            out_specs=(any_spec, any_spec, vmem_spec),
            scratch_shapes=[dma((2,))],
            name="outputs",
        )(*(pltpu.with_memory_space_constraint(r, pltpu.VMEM) for r in (u_vm, v_vm, c_vm)))
        return u_t.T, v_t.T, cost.reshape(nprob)

    return jax.shard_map(local_fn, mesh=mesh, in_specs=(P("row", "col"), P("row", "col"), P("row", "prob"), P("col", "prob")), out_specs=(P("row", "prob"), P("col", "prob"), P("prob")), check_vma=False)
```

```python
import jax
import jax.numpy as jnp
from jax import lax
from jax.experimental import pallas as pl
from jax.experimental.pallas import tpu as pltpu
from jax.sharding import PartitionSpec as P

SWEEPS = 6
AHEAD = (8, 7)
WAIT_NS = ((0, 0), (500, 180))
F32 = jnp.float32
BF16 = jnp.bfloat16
MESH = pl.DeviceIdType.MESH


def sinkhorn_kernel(n_chunk, k_hbm, c_hbm, a_hbm, b_hbm, u_out, v_out, cost_all,
                    k_buf, kt_buf, c_buf, kct_buf, a_buf, b_buf, ub_buf, acc,
                    s_out, s_in, t_out, t_in, t0_buf, s0_buf, v_all, cost_part,
                    load_sem, send_sem, kp_recv, s_recv, t_recv, one_recv):
    rows, half = k_hbm.shape
    cols = 2 * half
    rw = rows // n_chunk
    cw = cols // n_chunk
    per_half = n_chunk // 2
    nq = b_buf.shape[1]
    row = lax.axis_index("row")
    col = lax.axis_index("col")
    prob = lax.axis_index("prob")
    x = col // 2
    core = col % 2
    grp = (core + x + row) % 2
    me = row * 4 + col
    mine = pl.ds(pl.multiple_of(grp * nq, nq), nq)
    other = pl.ds(pl.multiple_of((1 - grp) * nq, nq), nq)

    def dev(r, c):
        return (prob, r, c)

    partner = dev(row, 2 * x + 1 - core)
    x_peer = dev(row, 2 * (1 - x) + 1 - core)
    y_peer = dev(1 - row, 2 * x + 1 - core)

    def remote(src, dst, send, recv, to):
        return pltpu.make_async_remote_copy(src_ref=src, dst_ref=dst, send_sem=send, recv_sem=recv,
                                            device_id=to, device_id_type=MESH)

    KP, BP, S0, SS, TT, T0, TP, KC, US, VS, CS = range(11)

    def all_sent(ref, kind):
        remote(ref, ref, send_sem.at[kind], one_recv.at[0], partner).wait_send()

    def all_here(ref, recv):
        remote(ref, ref, send_sem.at[0], recv, partner).wait_recv()

    def krows(i):
        return pl.ds(i * rw, rw)

    k_load = [pltpu.make_async_copy(k_hbm.at[krows(i)], k_buf.at[core, krows(i)], load_sem.at[i]) for i in range(n_chunk)]
    c_load = [pltpu.make_async_copy(c_hbm.at[krows(i)], c_buf.at[krows(i)], load_sem.at[i]) for i in range(n_chunk)]
    a_load = pltpu.make_async_copy(a_hbm, a_buf, load_sem.at[n_chunk])
    b_load = pltpu.make_async_copy(b_hbm.at[mine], b_buf.at[core], load_sem.at[n_chunk + 1])
    for d in k_load:
        d.start()
    a_load.start()
    b_load.start()

    barrier = pltpu.get_barrier_semaphore()
    for dr in range(2):
        for dc in range(4):
            if dr or dc:
                pl.semaphore_signal(barrier, inc=1, device_id=dev((row + dr) % 2, (col + dc) % 4), device_id_type=MESH)

    blk = 256

    def transpose_rows(h, i):
        def body(n, carry):
            jo = pl.multiple_of(n * blk, blk)
            for ii in range(rw // blk):
                kt_buf[pl.ds(pl.multiple_of(h * half + jo, blk), blk), pl.ds(i * rw + ii * blk, blk)] = (
                    k_buf[h, pl.ds(i * rw + ii * blk, blk), pl.ds(jo, blk)].T)
            return carry
        lax.fori_loop(0, half // blk, body, 0)

    kct_pieces = 2 * n_chunk
    kw = rows // kct_pieces

    def build_kct(lo, hi):
        def piece(i, carry):
            rs = pl.ds(pl.multiple_of(i * kw, kw), kw)
            for n in range(half // blk):
                kct_buf[pl.ds(pl.multiple_of(core * half + n * blk, blk), blk), rs] = (
                    k_buf[core, rs, n * blk:(n + 1) * blk] * c_buf[rs, n * blk:(n + 1) * blk]).T
            part = kct_buf.at[pl.ds(pl.multiple_of(core * half, half), half), rs]
            remote(part, part, send_sem.at[KC], one_recv.at[5], partner).start()
            return carry
        lax.fori_loop(lo, hi, piece, 0)

    ahead = grp * (AHEAD[0] + core * (AHEAD[1] - AHEAD[0]))
    middle = grp * kct_pieces + (1 - grp) * (kct_pieces // 2)

    k_push = [remote(k_buf.at[core, krows(i)], k_buf.at[core, krows(i)], send_sem.at[KP], kp_recv.at[i], partner) for i in range(n_chunk)]
    b_push = remote(b_hbm.at[other], b_buf.at[core], send_sem.at[BP], one_recv.at[0], partner)
    pl.semaphore_wait(barrier, 7)
    b_push.start()
    ones = jnp.ones((nq, half), BF16)
    for i in range(n_chunk):
        k_load[i].wait()
        if i == 0:
            k_push[0].start()
        if i % 2:
            part = lax.dot_general(ones, k_buf[core, pl.ds((i - 1) * rw, 2 * rw)], (((1,), (1,)), ((), ())), preferred_element_type=F32)
            for n in range(2 * rw // 128):
                r = (i - 1) * (rw // 128) + n
                s0_buf[col, r:r + 1, :] = part[0:1, n * 128:(n + 1) * 128]
    for n in range(1, 4):
        remote(s0_buf.at[col], s0_buf.at[col], send_sem.at[S0], one_recv.at[1], dev(row, (col + n) % 4)).start()
    for i in range(1, n_chunk):
        k_push[i].start()
    for d in c_load:
        d.start()
    for i in range(n_chunk):
        transpose_rows(core, i)
    a_load.wait()
    b_load.wait()
    all_here(s0_buf.at[0:3], one_recv.at[1])
    s0 = (s0_buf[0] + s0_buf[1]) + (s0_buf[2] + s0_buf[3])
    for r in range(rows // 128):
        cs = slice(r * 128, (r + 1) * 128)
        ub_buf[:, cs] = (a_buf[:, cs] / s0[r:r + 1, :]).astype(BF16)

    def t_copy(par, o):
        return remote(t_out.at[o], t_in.at[par, o], send_sem.at[TT], t_recv.at[par, o], y_peer)

    def s_copy(par, o):
        return remote(s_out.at[o], s_in.at[par, o], send_sem.at[SS], s_recv.at[par, o], x_peer)

    def t0_send(g, n):
        remote(t0_buf.at[g, n], t_in.at[0, core * per_half + n], send_sem.at[T0], t_recv.at[0, core * per_half + n],
               dev(1 - row, 2 * x + (g + x + 1 - row) % 2)).start()

    for n in range(per_half):
        part = jnp.dot(ub_buf[...], k_buf[core, :, n * cw:(n + 1) * cw], preferred_element_type=F32)
        for g in range(2):
            t0_buf[g, n] = part[g * nq:(g + 1) * nq]
        t0_send(0, n)
    for n in range(per_half):
        o = core * per_half + n
        remote(t0_buf.at[1 - grp, n], t_out.at[o], send_sem.at[TP], one_recv.at[2], partner).start()
        t_out[o] = t0_buf[grp, n]

    def v_of(par, o):
        return b_buf[o // per_half, :, (o % per_half) * cw:(o % per_half + 1) * cw] / (t_out[o] + t_in[par, o])

    all_here(b_buf.at[0], one_recv.at[0])
    for i in range(n_chunk):
        all_here(k_buf.at[1 - core, krows(i)], kp_recv.at[i])
        transpose_rows(1 - core, i)
        if i == 1:
            for n in range(per_half):
                t0_send(1, n)

    for d in c_load:
        d.wait()
    build_kct(0, ahead)

    for g in range(2):
        for c in range(2):
            if WAIT_NS[g][c]:
                @pl.when((grp == g) & (core == c))
                def _(g=g, c=c):
                    pl.delay(WAIT_NS[g][c])

    all_here(t0_buf.at[0], one_recv.at[2])
    order = list(range(per_half, n_chunk)) + list(range(per_half))
    for c in order:
        all_here(t_in.at[0, c], t_recv.at[0, c])
        vb = v_of(0, c).astype(BF16)
        js = slice(c * cw, (c + 1) * cw)
        if c != order[-1]:
            prod = jnp.dot(vb, kt_buf[js, :], preferred_element_type=F32)
            acc[...] = prod if c == order[0] else acc[...] + prod
        else:
            for o in range(n_chunk):
                s_out[o] = acc[:, o * rw:(o + 1) * rw] + jnp.dot(vb, kt_buf[js, o * rw:(o + 1) * rw], preferred_element_type=F32)
                s_copy(1, o).start()
    all_sent(t0_buf, T0)
    all_sent(t0_buf.at[0], TP)
    all_sent(s0_buf.at[0:3], S0)
    all_sent(k_buf.at[0], KP)
    all_sent(b_buf.at[0], BP)

    build_kct(ahead, middle)

    def u_and_t(par):
        for c in range(n_chunk):
            all_here(s_in.at[par, c], s_recv.at[par, c])
            w = slice(c * rw, (c + 1) * rw)
            u = a_buf[mine, w] / (s_out[c] + s_in[par, c])
            u_out[mine, w] = u
            ub = u.astype(BF16)
            if c < n_chunk - 1:
                for h in range(2):
                    hc = slice(h * half, (h + 1) * half)
                    prod = jnp.dot(ub, k_buf[h, w, :], preferred_element_type=F32)
                    acc[:, hc] = prod if c == 0 else acc[:, hc] + prod
            else:
                for o in range(n_chunk):
                    oc = slice(o * cw, (o + 1) * cw)
                    hc = slice((o % per_half) * cw, (o % per_half + 1) * cw)
                    t_out[o] = acc[:, oc] + jnp.dot(ub, k_buf[o // per_half, w, hc], preferred_element_type=F32)
                    t_copy(par, o).start()
                all_sent(s_out, SS)

    def v_and_s(par_in, par):
        for c in range(n_chunk):
            all_here(t_in.at[par_in, c], t_recv.at[par_in, c])
            vb = v_of(par_in, c).astype(BF16)
            w = slice(c * cw, (c + 1) * cw)
            if c < n_chunk - 1:
                prod = jnp.dot(vb, kt_buf[w, :], preferred_element_type=F32)
                acc[...] = prod if c == 0 else acc[...] + prod
            else:
                for o in range(n_chunk):
                    oc = slice(o * rw, (o + 1) * rw)
                    s_out[o] = acc[:, oc] + jnp.dot(vb, kt_buf[w, oc], preferred_element_type=F32)
                    s_copy(par, o).start()
                all_sent(t_out, TT)

    def sweep(t, carry):
        u_and_t(t % 2)

        @pl.when(t == 1)
        def _():
            build_kct(middle, kct_pieces)

        v_and_s(t % 2, (t + 1) % 2)
        return carry

    lax.fori_loop(1, SWEEPS - 1, sweep, 0)
    last = (SWEEPS - 1) % 2
    u_and_t(last)

    u_push = remote(u_out.at[mine], u_out.at[mine], send_sem.at[US], one_recv.at[3], partner)
    u_push.start()
    cost_part[...] = jnp.zeros_like(cost_part)
    all_here(kct_buf.at[0:half], one_recv.at[5])
    all_sent(kct_buf.at[0:half], KC)
    for c in range(n_chunk):
        all_here(t_in.at[last, c], t_recv.at[last, c])
        v = v_of(last, c)
        v_all[c // per_half, :, (c % per_half) * cw:(c % per_half + 1) * cw] = v
        prod = jnp.dot(v.astype(BF16), kct_buf[c * cw:(c + 1) * cw, :], preferred_element_type=F32)
        if c < n_chunk - 1:
            acc[...] = prod if c == 0 else acc[...] + prod
        else:
            w = (acc[...] + prod) * u_out[mine]
    v_push = remote(v_all.at[1 - core], v_out.at[mine], send_sem.at[VS], one_recv.at[4], partner)
    v_push.start()
    tot = w[:, 0:128]
    for n in range(1, rows // 128):
        tot = tot + w[:, n * 128:(n + 1) * 128]
    cost_part[mine] = tot
    cost_all[me] = jnp.sum(cost_part[...].T, axis=0, keepdims=True)
    for dr in range(2):
        for dc in range(4):
            if dr or dc:
                remote(cost_all.at[me], cost_all.at[me], send_sem.at[CS], one_recv.at[6], dev((row + dr) % 2, (col + dc) % 4)).start()
    v_out[mine] = v_all[core]
    all_sent(t_out, TT)
    all_here(u_out.at[other], one_recv.at[3])
    u_push.wait_send()
    all_here(v_out.at[other], one_recv.at[4])
    v_push.wait_send()
    all_here(cost_all.at[0:7], one_recv.at[6])
    all_sent(cost_all.at[0:7], CS)


def output_kernel(norm, u_ref, v_ref, c_ref, u_hbm, v_hbm, cost_ref, sem):
    stores = [pltpu.make_async_copy(u_ref, u_hbm, sem.at[0]), pltpu.make_async_copy(v_ref, v_hbm, sem.at[1])]
    for d in stores:
        d.start()
    total = c_ref[0]
    for n in range(1, 8):
        total = total + c_ref[n]
    cost_ref[...] = total[:, :cost_ref.shape[1]] * norm
    for d in stores:
        d.wait()


def solution(mesh):
    n_chunk = 4

    def local_fn(kernel, cost_mat, src_mass, tgt_mass):
        rows, half = kernel.shape
        nprob = src_mass.shape[1]
        nq = nprob // 2
        cols = 2 * half
        rw, cw = rows // n_chunk, cols // n_chunk
        norm = 1.0 / float(rows * mesh.shape["row"] * half * mesh.shape["col"])
        vmem_spec = pl.BlockSpec(memory_space=pltpu.VMEM)
        any_spec = pl.BlockSpec(memory_space=pl.ANY)
        dma = pltpu.SemaphoreType.DMA
        u_vm, v_vm, c_vm = pl.pallas_call(
            lambda *refs: sinkhorn_kernel(n_chunk, *refs),
            out_shape=(pltpu.VMEM((nprob, rows), F32), pltpu.VMEM((nprob, half), F32), pltpu.VMEM((8, 1, 128), F32)),
            in_specs=[any_spec] * 4,
            out_specs=(vmem_spec, vmem_spec, vmem_spec),
            scratch_shapes=[
                pltpu.VMEM((2, rows, half), BF16),
                pltpu.VMEM((cols, rows), BF16),
                pltpu.VMEM((rows, half), BF16),
                pltpu.VMEM((cols, rows), BF16),
                pltpu.VMEM((nprob, rows), F32),
                pltpu.VMEM((2, nq, half), F32),
                pltpu.VMEM((nprob, rows), BF16),
                pltpu.VMEM((nq, max(rows, cols)), F32),
                pltpu.VMEM((n_chunk, nq, rw), F32),
                pltpu.VMEM((2, n_chunk, nq, rw), F32),
                pltpu.VMEM((n_chunk, nq, cw), F32),
                pltpu.VMEM((2, n_chunk, nq, cw), F32),
                pltpu.VMEM((2, n_chunk // 2, nq, cw), F32),
                pltpu.VMEM((4, rows // 128, 128), F32),
                pltpu.VMEM((2, nq, half), F32),
                pltpu.VMEM((128, 128), F32),
                dma((n_chunk + 2,)), dma((11,)), dma((n_chunk,)), dma((2, n_chunk)), dma((2, n_chunk)), dma((7,)),
            ],
            compiler_params=pltpu.CompilerParams(collective_id=0, has_side_effects=True, vmem_limit_bytes=60 * 1024 * 1024),
            name="sinkhorn",
        )(kernel, cost_mat, src_mass.T, tgt_mass.T)
        u_t, v_t, cost = pl.pallas_call(
            lambda *refs: output_kernel(norm, *refs),
            out_shape=(jax.ShapeDtypeStruct((nprob, rows), F32), jax.ShapeDtypeStruct((nprob, half), F32),
                       jax.ShapeDtypeStruct((1, nprob), F32)),
            in_specs=[vmem_spec] * 3,
            out_specs=(any_spec, any_spec, vmem_spec),
            scratch_shapes=[dma((2,))],
            name="outputs",
        )(*(pltpu.with_memory_space_constraint(r, pltpu.VMEM) for r in (u_vm, v_vm, c_vm)))
        return u_t.T, v_t.T, cost.reshape(nprob)

    return jax.shard_map(local_fn, mesh=mesh, in_specs=(P("row", "col"), P("row", "col"), P("row", "prob"), P("col", "prob")), out_specs=(P("row", "prob"), P("col", "prob"), P("prob")), check_vma=False)
```

```python
import jax
import jax.numpy as jnp
from jax import lax
from jax.experimental import pallas as pl
from jax.experimental.pallas import tpu as pltpu
from jax.sharding import PartitionSpec as P

SWEEPS = 6
AHEAD = (8, 6)
WAIT_NS = 550
F32 = jnp.float32
BF16 = jnp.bfloat16
MESH = pl.DeviceIdType.MESH


def sinkhorn_kernel(n_chunk, k_hbm, c_hbm, a_hbm, b_hbm, u_out, v_out, cost_all,
                    k_buf, kt_buf, c_buf, kct_buf, a_buf, b_buf, ub_buf, acc,
                    s_out, s_in, t_out, t_in, t0_buf, s0_buf, v_all, cost_part,
                    load_sem, send_sem, kp_recv, s_recv, t_recv, one_recv):
    rows, half = k_hbm.shape
    cols = 2 * half
    rw = rows // n_chunk
    cw = cols // n_chunk
    per_half = n_chunk // 2
    nq = b_buf.shape[1]
    row = lax.axis_index("row")
    col = lax.axis_index("col")
    prob = lax.axis_index("prob")
    x = col // 2
    core = col % 2
    grp = (core + x + row) % 2
    me = row * 4 + col
    mine = pl.ds(pl.multiple_of(grp * nq, nq), nq)
    other = pl.ds(pl.multiple_of((1 - grp) * nq, nq), nq)

    def dev(r, c):
        return (prob, r, c)

    partner = dev(row, 2 * x + 1 - core)
    x_peer = dev(row, 2 * (1 - x) + 1 - core)
    y_peer = dev(1 - row, 2 * x + 1 - core)

    def remote(src, dst, send, recv, to):
        return pltpu.make_async_remote_copy(src_ref=src, dst_ref=dst, send_sem=send, recv_sem=recv,
                                            device_id=to, device_id_type=MESH)

    KP, BP, S0, SS, TT, T0, TP, KC, US, VS, CS = range(11)

    def all_sent(ref, kind):
        remote(ref, ref, send_sem.at[kind], one_recv.at[0], partner).wait_send()

    def all_here(ref, recv):
        remote(ref, ref, send_sem.at[0], recv, partner).wait_recv()

    def krows(i):
        return pl.ds(i * rw, rw)

    k_load = [pltpu.make_async_copy(k_hbm.at[krows(i)], k_buf.at[core, krows(i)], load_sem.at[i]) for i in range(n_chunk)]
    c_load = [pltpu.make_async_copy(c_hbm.at[krows(i)], c_buf.at[krows(i)], load_sem.at[i]) for i in range(n_chunk)]
    a_load = pltpu.make_async_copy(a_hbm, a_buf, load_sem.at[n_chunk])
    b_load = pltpu.make_async_copy(b_hbm.at[mine], b_buf.at[core], load_sem.at[n_chunk + 1])
    for d in k_load:
        d.start()
    a_load.start()
    b_load.start()

    barrier = pltpu.get_barrier_semaphore()
    for dr in range(2):
        for dc in range(4):
            if dr or dc:
                pl.semaphore_signal(barrier, inc=1, device_id=dev((row + dr) % 2, (col + dc) % 4), device_id_type=MESH)

    blk = 256

    def transpose_rows(h, i):
        def body(n, carry):
            jo = pl.multiple_of(n * blk, blk)
            for ii in range(rw // blk):
                kt_buf[pl.ds(pl.multiple_of(h * half + jo, blk), blk), pl.ds(i * rw + ii * blk, blk)] = (
                    k_buf[h, pl.ds(i * rw + ii * blk, blk), pl.ds(jo, blk)].T)
            return carry
        lax.fori_loop(0, half // blk, body, 0)

    kct_pieces = 2 * n_chunk
    kw = rows // kct_pieces

    def build_kct(lo, hi):
        def piece(i, carry):
            rs = pl.ds(pl.multiple_of(i * kw, kw), kw)
            for n in range(half // blk):
                kct_buf[pl.ds(pl.multiple_of(core * half + n * blk, blk), blk), rs] = (
                    k_buf[core, rs, n * blk:(n + 1) * blk] * c_buf[rs, n * blk:(n + 1) * blk]).T
            part = kct_buf.at[pl.ds(pl.multiple_of(core * half, half), half), rs]
            remote(part, part, send_sem.at[KC], one_recv.at[5], partner).start()
            return carry
        lax.fori_loop(lo, hi, piece, 0)

    ahead = grp * (AHEAD[0] + core * (AHEAD[1] - AHEAD[0]))
    middle = grp * kct_pieces + (1 - grp) * (kct_pieces // 2)

    k_push = [remote(k_buf.at[core, krows(i)], k_buf.at[core, krows(i)], send_sem.at[KP], kp_recv.at[i], partner) for i in range(n_chunk)]
    b_push = remote(b_hbm.at[other], b_buf.at[core], send_sem.at[BP], one_recv.at[0], partner)
    pl.semaphore_wait(barrier, 7)
    b_push.start()
    ones = jnp.ones((nq, half), BF16)
    for i in range(n_chunk):
        k_load[i].wait()
        if i == 0:
            k_push[0].start()
        if i % 2:
            part = lax.dot_general(ones, k_buf[core, pl.ds((i - 1) * rw, 2 * rw)], (((1,), (1,)), ((), ())), preferred_element_type=F32)
            for n in range(2 * rw // 128):
                r = (i - 1) * (rw // 128) + n
                s0_buf[col, r:r + 1, :] = part[0:1, n * 128:(n + 1) * 128]
    for n in range(1, 4):
        remote(s0_buf.at[col], s0_buf.at[col], send_sem.at[S0], one_recv.at[1], dev(row, (col + n) % 4)).start()
    for i in range(1, n_chunk):
        k_push[i].start()
    for d in c_load:
        d.start()
    for i in range(n_chunk):
        transpose_rows(core, i)
    a_load.wait()
    b_load.wait()
    all_here(s0_buf.at[0:3], one_recv.at[1])
    s0 = (s0_buf[0] + s0_buf[1]) + (s0_buf[2] + s0_buf[3])
    for r in range(rows // 128):
        cs = slice(r * 128, (r + 1) * 128)
        ub_buf[:, cs] = (a_buf[:, cs] / s0[r:r + 1, :]).astype(BF16)

    def t_copy(par, o):
        return remote(t_out.at[o], t_in.at[par, o], send_sem.at[TT], t_recv.at[par, o], y_peer)

    def s_copy(par, o):
        return remote(s_out.at[o], s_in.at[par, o], send_sem.at[SS], s_recv.at[par, o], x_peer)

    def t0_send(g, n):
        remote(t0_buf.at[g, n], t_in.at[0, core * per_half + n], send_sem.at[T0], t_recv.at[0, core * per_half + n],
               dev(1 - row, 2 * x + (g + x + 1 - row) % 2)).start()

    for n in range(per_half):
        part = jnp.dot(ub_buf[...], k_buf[core, :, n * cw:(n + 1) * cw], preferred_element_type=F32)
        for g in range(2):
            t0_buf[g, n] = part[g * nq:(g + 1) * nq]
        t0_send(0, n)
    for n in range(per_half):
        o = core * per_half + n
        remote(t0_buf.at[1 - grp, n], t_out.at[o], send_sem.at[TP], one_recv.at[2], partner).start()
        t_out[o] = t0_buf[grp, n]

    def v_of(par, o):
        return b_buf[o // per_half, :, (o % per_half) * cw:(o % per_half + 1) * cw] / (t_out[o] + t_in[par, o])

    all_here(b_buf.at[0], one_recv.at[0])
    for i in range(n_chunk):
        all_here(k_buf.at[1 - core, krows(i)], kp_recv.at[i])
        transpose_rows(1 - core, i)
        if i == 0:
            for n in range(per_half):
                t0_send(1, n)

    for d in c_load:
        d.wait()
    build_kct(0, ahead)

    @pl.when(grp == 1)
    def _():
        pl.delay(WAIT_NS + (1 - core) * 100)

    all_here(t0_buf.at[0], one_recv.at[2])
    order = list(range(per_half, n_chunk)) + list(range(per_half))
    for c in order:
        all_here(t_in.at[0, c], t_recv.at[0, c])
        vb = v_of(0, c).astype(BF16)
        js = slice(c * cw, (c + 1) * cw)
        if c != order[-1]:
            prod = jnp.dot(vb, kt_buf[js, :], preferred_element_type=F32)
            acc[...] = prod if c == order[0] else acc[...] + prod
        else:
            for o in range(n_chunk):
                s_out[o] = acc[:, o * rw:(o + 1) * rw] + jnp.dot(vb, kt_buf[js, o * rw:(o + 1) * rw], preferred_element_type=F32)
                s_copy(1, o).start()
    all_sent(t0_buf, T0)
    all_sent(t0_buf.at[0], TP)
    all_sent(s0_buf.at[0:3], S0)
    all_sent(k_buf.at[0], KP)
    all_sent(b_buf.at[0], BP)

    build_kct(ahead, middle)

    def u_and_t(par):
        for c in range(n_chunk):
            all_here(s_in.at[par, c], s_recv.at[par, c])
            w = slice(c * rw, (c + 1) * rw)
            u = a_buf[mine, w] / (s_out[c] + s_in[par, c])
            u_out[mine, w] = u
            ub = u.astype(BF16)
            if c < n_chunk - 1:
                for h in range(2):
                    hc = slice(h * half, (h + 1) * half)
                    prod = jnp.dot(ub, k_buf[h, w, :], preferred_element_type=F32)
                    acc[:, hc] = prod if c == 0 else acc[:, hc] + prod
            else:
                for o in range(n_chunk):
                    oc = slice(o * cw, (o + 1) * cw)
                    hc = slice((o % per_half) * cw, (o % per_half + 1) * cw)
                    t_out[o] = acc[:, oc] + jnp.dot(ub, k_buf[o // per_half, w, hc], preferred_element_type=F32)
                    t_copy(par, o).start()
                all_sent(s_out, SS)

    def v_and_s(par_in, par):
        for c in range(n_chunk):
            all_here(t_in.at[par_in, c], t_recv.at[par_in, c])
            vb = v_of(par_in, c).astype(BF16)
            w = slice(c * cw, (c + 1) * cw)
            if c < n_chunk - 1:
                prod = jnp.dot(vb, kt_buf[w, :], preferred_element_type=F32)
                acc[...] = prod if c == 0 else acc[...] + prod
            else:
                for o in range(n_chunk):
                    oc = slice(o * rw, (o + 1) * rw)
                    s_out[o] = acc[:, oc] + jnp.dot(vb, kt_buf[w, oc], preferred_element_type=F32)
                    s_copy(par, o).start()
                all_sent(t_out, TT)

    def sweep(t, carry):
        u_and_t(t % 2)

        @pl.when(t == 1)
        def _():
            build_kct(middle, kct_pieces)

        v_and_s(t % 2, (t + 1) % 2)
        return carry

    lax.fori_loop(1, SWEEPS - 1, sweep, 0)
    last = (SWEEPS - 1) % 2
    u_and_t(last)

    u_push = remote(u_out.at[mine], u_out.at[mine], send_sem.at[US], one_recv.at[3], partner)
    u_push.start()
    cost_part[...] = jnp.zeros_like(cost_part)
    all_here(kct_buf.at[0:half], one_recv.at[5])
    all_sent(kct_buf.at[0:half], KC)
    for c in range(n_chunk):
        all_here(t_in.at[last, c], t_recv.at[last, c])
        v = v_of(last, c)
        v_all[c // per_half, :, (c % per_half) * cw:(c % per_half + 1) * cw] = v
        prod = jnp.dot(v.astype(BF16), kct_buf[c * cw:(c + 1) * cw, :], preferred_element_type=F32)
        if c < n_chunk - 1:
            acc[...] = prod if c == 0 else acc[...] + prod
        else:
            w = (acc[...] + prod) * u_out[mine]
    v_push = remote(v_all.at[1 - core], v_out.at[mine], send_sem.at[VS], one_recv.at[4], partner)
    v_push.start()
    tot = w[:, 0:128]
    for n in range(1, rows // 128):
        tot = tot + w[:, n * 128:(n + 1) * 128]
    cost_part[mine] = tot
    cost_all[me] = jnp.sum(cost_part[...].T, axis=0, keepdims=True)
    for dr in range(2):
        for dc in range(4):
            if dr or dc:
                remote(cost_all.at[me], cost_all.at[me], send_sem.at[CS], one_recv.at[6], dev((row + dr) % 2, (col + dc) % 4)).start()
    v_out[mine] = v_all[core]
    all_sent(t_out, TT)
    all_here(u_out.at[other], one_recv.at[3])
    u_push.wait_send()
    all_here(v_out.at[other], one_recv.at[4])
    v_push.wait_send()
    all_here(cost_all.at[0:7], one_recv.at[6])
    all_sent(cost_all.at[0:7], CS)


def output_kernel(norm, u_ref, v_ref, c_ref, u_hbm, v_hbm, cost_ref, sem):
    stores = [pltpu.make_async_copy(u_ref, u_hbm, sem.at[0]), pltpu.make_async_copy(v_ref, v_hbm, sem.at[1])]
    for d in stores:
        d.start()
    total = c_ref[0]
    for n in range(1, 8):
        total = total + c_ref[n]
    cost_ref[...] = total[:, :cost_ref.shape[1]] * norm
    for d in stores:
        d.wait()


def solution(mesh):
    n_chunk = 4

    def local_fn(kernel, cost_mat, src_mass, tgt_mass):
        rows, half = kernel.shape
        nprob = src_mass.shape[1]
        nq = nprob // 2
        cols = 2 * half
        rw, cw = rows // n_chunk, cols // n_chunk
        norm = 1.0 / float(rows * mesh.shape["row"] * half * mesh.shape["col"])
        vmem_spec = pl.BlockSpec(memory_space=pltpu.VMEM)
        any_spec = pl.BlockSpec(memory_space=pl.ANY)
        dma = pltpu.SemaphoreType.DMA
        u_vm, v_vm, c_vm = pl.pallas_call(
            lambda *refs: sinkhorn_kernel(n_chunk, *refs),
            out_shape=(pltpu.VMEM((nprob, rows), F32), pltpu.VMEM((nprob, half), F32), pltpu.VMEM((8, 1, 128), F32)),
            in_specs=[any_spec] * 4,
            out_specs=(vmem_spec, vmem_spec, vmem_spec),
            scratch_shapes=[
                pltpu.VMEM((2, rows, half), BF16),
                pltpu.VMEM((cols, rows), BF16),
                pltpu.VMEM((rows, half), BF16),
                pltpu.VMEM((cols, rows), BF16),
                pltpu.VMEM((nprob, rows), F32),
                pltpu.VMEM((2, nq, half), F32),
                pltpu.VMEM((nprob, rows), BF16),
                pltpu.VMEM((nq, max(rows, cols)), F32),
                pltpu.VMEM((n_chunk, nq, rw), F32),
                pltpu.VMEM((2, n_chunk, nq, rw), F32),
                pltpu.VMEM((n_chunk, nq, cw), F32),
                pltpu.VMEM((2, n_chunk, nq, cw), F32),
                pltpu.VMEM((2, n_chunk // 2, nq, cw), F32),
                pltpu.VMEM((4, rows // 128, 128), F32),
                pltpu.VMEM((2, nq, half), F32),
                pltpu.VMEM((128, 128), F32),
                dma((n_chunk + 2,)), dma((11,)), dma((n_chunk,)), dma((2, n_chunk)), dma((2, n_chunk)), dma((7,)),
            ],
            compiler_params=pltpu.CompilerParams(collective_id=0, has_side_effects=True, vmem_limit_bytes=60 * 1024 * 1024),
            name="sinkhorn",
        )(kernel, cost_mat, src_mass.T, tgt_mass.T)
        u_t, v_t, cost = pl.pallas_call(
            lambda *refs: output_kernel(norm, *refs),
            out_shape=(jax.ShapeDtypeStruct((nprob, rows), F32), jax.ShapeDtypeStruct((nprob, half), F32),
                       jax.ShapeDtypeStruct((1, nprob), F32)),
            in_specs=[vmem_spec] * 3,
            out_specs=(any_spec, any_spec, vmem_spec),
            scratch_shapes=[dma((2,))],
            name="outputs",
        )(*(pltpu.with_memory_space_constraint(r, pltpu.VMEM) for r in (u_vm, v_vm, c_vm)))
        return u_t.T, v_t.T, cost.reshape(nprob)

    return jax.shard_map(local_fn, mesh=mesh, in_specs=(P("row", "col"), P("row", "col"), P("row", "prob"), P("col", "prob")), out_specs=(P("row", "prob"), P("col", "prob"), P("prob")), check_vma=False)
```
